32 devices in a mesh: dp: 8 (over z, y), neg: 4 (over x, core).
Axes of the slice: x: 2, y: 2, z: 4, core: 2. Of those that a mesh axis runs over, the one named last changes fastest.
Arguments:
- query_features: bfloat16 [8192, 512], P(('dp', 'neg')), may hold values from -8 to 8
- positive_features: bfloat16 [8192, 512], P(('dp', 'neg')), may hold values from -6 to 6
- negative_features: bfloat16 [16384, 512], P(('neg', 'dp')), may hold values from -6 to 6
- positive_ids: int32 [8192], P('dp'), may hold values from 0 to 8191, as said below
- positive_counts: int32 [8192], P(('dp', 'neg')), may hold values from 1 to 16
- negative_ids: int32 [16384], P('neg'), may hold values from 0 to 4095, as said below
- negative_counts: int32 [16384], P('neg'), may hold values from 64 to 4096
- query_first: bfloat16 [512, 1024], replicated, may hold values from -0.25 to 0.25
- query_second: bfloat16 [1024, 512], replicated, may hold values from -0.1875 to 0.1875
- query_third: bfloat16 [512, 256], replicated, may hold values from -0.25 to 0.25
- item_first: bfloat16 [512, 1024], replicated, may hold values from -0.25 to 0.25
- item_second: bfloat16 [1024, 512], replicated, may hold values from -0.1875 to 0.1875
- item_third: bfloat16 [512, 256], replicated, may hold values from -0.25 to 0.25
Outputs:
- mean_loss: float32 [], replicated
- clipped_query_first: float32 [512, 1024], P('dp')
- clipped_query_second: float32 [1024, 512], P('dp')
- clipped_query_third: float32 [512, 256], P('dp')
- clipped_item_first: float32 [512, 1024], P('dp')
- clipped_item_second: float32 [1024, 512], P('dp')
- clipped_item_third: float32 [512, 256], P('dp')
The draws below stay inside these ranges and needn't reach their ends.
Inputs may be any that keep to these rules, and one draw needn't show every extreme that they name: `negative_ids`: ids of the sampled negatives; one id may stand for several negatives. `positive_ids`: A query's positive id may equal the ids of some negatives; those negatives are left out of that query's denominator.
All inputs are finite; a program needn't handle non-finite values.
Results may differ from the reference program's by a relative error of at most 0.0075.
Values may be sent and summed in bfloat16 or wider, within the bound.
A program may use at most 128 MiB of HBM per device.

```python
import math
import jax
import jax.numpy as jnp
from jax import lax

FIN = 512
H1 = 1024
H2 = 512
E = 256
NEG = 16384
QUERIES = 8192


def draw_query_features(key, part):
    noise_key, mean_key, scale_key = jax.random.split(key, 3)
    values = jax.random.normal(noise_key, (QUERIES, FIN), jnp.float32)
    return jnp.clip(values, -8.0, 8.0).astype(jnp.bfloat16)


def draw_item_ids(key):
    base = jax.random.fold_in(key, 91)
    pool_key, pick_key, fresh_key, hit_key = jax.random.split(base, 4)
    negatives = jax.random.randint(pool_key, (NEG,), 0, NEG // 4, jnp.int32)
    negatives = negatives.at[0].set(NEG // 4 - 1).at[1].set(0)
    picked = jax.random.randint(pick_key, (QUERIES,), 0, NEG, jnp.int32)
    fresh = jax.random.randint(fresh_key, (QUERIES,), NEG // 4, NEG // 2, jnp.int32)
    choose_hit = jax.random.randint(hit_key, (QUERIES,), 0, 2, jnp.int32)
    positives = jnp.where(choose_hit == 0, negatives[picked], fresh)
    positives = positives.at[0].set(NEG // 2 - 1).at[1].set(0)
    return (negatives, positives)


def draw_negative_ids(key, part):
    return draw_item_ids(key)[0]


def draw_positive_ids(key, part):
    return draw_item_ids(key)[1]


def blocked_counts(key, total, block_rows, low_power, high_power):
    level_key, fine_key = jax.random.split(key)
    levels = jax.random.randint(level_key, (total // block_rows + 1,), low_power, high_power + 1, jnp.int32)
    powers = jnp.left_shift(jnp.ones_like(levels), levels)
    which = jnp.arange(total, dtype=jnp.int32) // block_rows
    base = powers[which]
    fine = jax.random.randint(fine_key, (total,), 0, 65536, jnp.int32) % base
    return base + fine


def draw_negative_counts(key, part):
    counts = blocked_counts(jax.random.fold_in(key, 17), NEG, 256, 6, 11)
    return counts.at[0].set(4096).at[1].set(64)


def draw_positive_counts(key, part):
    counts = blocked_counts(jax.random.fold_in(key, 23), QUERIES, 64, 0, 3)
    return counts.at[0].set(16).at[1].set(1)


def block_scale(key, shape, pieces, least, top_value):
    loudness = 1.0
    for dim, parts in pieces:
        heights = jax.random.uniform(jax.random.fold_in(jax.random.fold_in(key, 6), dim), (parts,), jnp.float32, least / len(pieces), top_value / len(pieces))
        loudness = loudness * jnp.repeat(jnp.exp(heights), shape[dim] // parts).reshape((-1,) + (1,) * (len(shape) - 1 - dim))
    return loudness


def bell_draw(key, shape, scale, limit, shards=(), kind=jnp.bfloat16):
    gain = block_scale(key, shape, shards, -0.22, 0.18) if shards else 1.0
    drawn = jax.random.normal(key, shape, jnp.float32) * scale * gain
    return jnp.minimum(jnp.maximum(drawn, -limit), limit).astype(kind)


def setup_inputs(seed: int = 0) -> dict:
    streams_of = jax.random.split(jax.random.key(seed), 14)
    query_features = draw_query_features(jax.random.fold_in(streams_of[13], 71), 0)
    positive_features = bell_draw(streams_of[1], (QUERIES, FIN), 1.0, 6.0, ((0, 32),))
    negative_features = bell_draw(streams_of[2], (NEG, FIN), 1.0, 6.0, ((0, 32),))
    positive_ids = draw_positive_ids(jax.random.fold_in(streams_of[13], 71), 0)
    positive_counts = draw_positive_counts(jax.random.fold_in(streams_of[13], 71), 0)
    negative_ids = draw_negative_ids(jax.random.fold_in(streams_of[13], 71), 0)
    negative_counts = draw_negative_counts(jax.random.fold_in(streams_of[13], 71), 0)
    query_first = bell_draw(streams_of[7], (FIN, H1), FIN ** -0.5, 0.25)
    query_second = bell_draw(streams_of[8], (H1, H2), H1 ** -0.5, 0.1875)
    query_third = bell_draw(streams_of[9], (H2, E), H2 ** -0.5, 0.25)
    item_first = bell_draw(streams_of[10], (FIN, H1), FIN ** -0.5, 0.25)
    item_second = bell_draw(streams_of[11], (H1, H2), H1 ** -0.5, 0.1875)
    item_third = bell_draw(streams_of[12], (H2, E), H2 ** -0.5, 0.25)
    return dict(query_features=query_features, positive_features=positive_features, negative_features=negative_features, positive_ids=positive_ids, positive_counts=positive_counts, negative_ids=negative_ids, negative_counts=negative_counts, query_first=query_first, query_second=query_second, query_third=query_third, item_first=item_first, item_second=item_second, item_third=item_third)


inv_temp = 20.0
clip_norm = 256.0

def silu_slope(pre):
    sigma = jax.nn.sigmoid(pre)
    return sigma * (1.0 + pre * (1.0 - sigma))

def contract_rows(left, right):
    return lax.dot_general(left, right, (((0,), (0,)), ((), ())), preferred_element_type=jnp.float32)

def contract_cols(left, right):
    return lax.dot_general(left, right, (((1,), (1,)), ((), ())), preferred_element_type=jnp.float32)

def tower_forward(features, first, second, third):
    first_pre = jnp.dot(features, first, preferred_element_type=jnp.float32)
    first_act = jax.nn.silu(first_pre).astype(jnp.bfloat16)
    second_pre = jnp.dot(first_act, second, preferred_element_type=jnp.float32)
    second_act = jax.nn.silu(second_pre).astype(jnp.bfloat16)
    embedding = jnp.dot(second_act, third, preferred_element_type=jnp.float32)
    inv_norm = lax.rsqrt(lax.optimization_barrier(jnp.sum(embedding * embedding, axis=1, keepdims=True)) + 1.0)
    unit = (embedding * inv_norm).astype(jnp.bfloat16)
    return ((first_pre, first_act, second_pre, second_act, embedding, inv_norm), unit)

def tower_backward(features, second, third, saved, unit_grad):
    first_pre, first_act, second_pre, second_act, embedding, inv_norm = saved
    along = lax.optimization_barrier(jnp.sum(embedding * unit_grad, axis=1, keepdims=True))
    embed_grad = (inv_norm * unit_grad - inv_norm * inv_norm * inv_norm * embedding * along).astype(jnp.bfloat16)
    third_grad = contract_rows(second_act, embed_grad)
    second_slope = (contract_cols(embed_grad, third) * silu_slope(second_pre)).astype(jnp.bfloat16)
    second_grad = contract_rows(first_act, second_slope)
    first_slope = (contract_cols(second_slope, second) * silu_slope(first_pre)).astype(jnp.bfloat16)
    first_grad = contract_rows(features, first_slope)
    return (first_grad, second_grad, third_grad)

def reference(query_features, positive_features, negative_features, positive_ids, positive_counts, negative_ids, negative_counts, query_first, query_second, query_third, item_first, item_second, item_third):
    query_saved, query_unit = tower_forward(query_features, query_first, query_second, query_third)
    item_features = jnp.concatenate([positive_features, negative_features], axis=0)
    item_saved, item_unit = tower_forward(item_features, item_first, item_second, item_third)
    positive_unit = item_unit[:QUERIES]
    negative_unit = item_unit[QUERIES:]
    negative_log = jnp.log(negative_counts.astype(jnp.float32))
    positive_logit = lax.optimization_barrier(jnp.sum(query_unit.astype(jnp.float32) * positive_unit.astype(jnp.float32), axis=1)) * inv_temp - jnp.log(positive_counts.astype(jnp.float32))
    block_rows = math.gcd(QUERIES, 2048)
    blocks = QUERIES // block_rows

    def block_step(carry, inputs):
        negative_sum, loss_sum = carry
        query_block, positive_block, logit_block, ids_block = inputs
        scores = contract_cols(query_block, negative_unit) * inv_temp - negative_log[None, :]
        weights = jnp.where(ids_block[:, None] != negative_ids[None, :], jnp.exp(scores), 0.0)
        positive_exp = jnp.exp(logit_block)
        denom = positive_exp + lax.optimization_barrier(jnp.sum(weights, axis=1))
        loss_sum = loss_sum + jnp.sum(jnp.log(denom) - logit_block)
        softmax_weights = (weights / denom[:, None]).astype(jnp.bfloat16)
        positive_slope = positive_exp / denom - 1.0
        query_grad = (jnp.dot(softmax_weights, negative_unit, preferred_element_type=jnp.float32) + positive_slope[:, None] * positive_block.astype(jnp.float32)) * inv_temp
        positive_grad = positive_slope[:, None] * query_block.astype(jnp.float32) * inv_temp
        negative_sum = negative_sum + contract_rows(softmax_weights, query_block)
        return ((negative_sum, loss_sum), (query_grad, positive_grad))
    inputs = (query_unit.reshape(blocks, block_rows, E), positive_unit.reshape(blocks, block_rows, E), positive_logit.reshape(blocks, block_rows), positive_ids.reshape(blocks, block_rows))
    initial = (jnp.zeros((NEG, E), jnp.float32), jnp.zeros((), jnp.float32))
    (negative_sum, loss_sum), (query_grad, positive_grad) = lax.scan(block_step, initial, inputs)
    query_grad = query_grad.reshape(QUERIES, E)
    item_grad = jnp.concatenate([positive_grad.reshape(QUERIES, E), negative_sum * inv_temp], axis=0)
    query_grads = tower_backward(query_features, query_second, query_third, query_saved, query_grad)
    item_grads = tower_backward(item_features, item_second, item_third, item_saved, item_grad)
    gradients = query_grads + item_grads
    squares = jnp.zeros((), jnp.float32)
    for gradient in gradients:
        squares = squares + jnp.sum(gradient * gradient)
    grad_norm = jnp.sqrt(squares)
    clip_factor = clip_norm / jnp.maximum(grad_norm, clip_norm)
    mean_loss = loss_sum / QUERIES
    return (mean_loss, gradients[0] * clip_factor, gradients[1] * clip_factor, gradients[2] * clip_factor, gradients[3] * clip_factor, gradients[4] * clip_factor, gradients[5] * clip_factor)
```

```python
import functools

import jax
import jax.numpy as jnp
from jax import lax
from jax.experimental import pallas as pl
from jax.experimental.pallas import tpu as pltpu
from jax.sharding import PartitionSpec as P

inv_temp = 20.0
clip_norm = 256.0


def silu_slope(pre):
    sigma = jax.nn.sigmoid(pre)
    return sigma * (1.0 + pre * (1.0 - sigma))


def contract_rows(left, right):
    return lax.dot_general(
        left, right, (((0,), (0,)), ((), ())), preferred_element_type=jnp.float32
    )


def contract_cols(left, right):
    return lax.dot_general(
        left, right, (((1,), (1,)), ((), ())), preferred_element_type=jnp.float32
    )


def tower_forward(features, first, second, third):
    first_pre = jnp.dot(features, first, preferred_element_type=jnp.float32)
    first_act = jax.nn.silu(first_pre).astype(jnp.bfloat16)
    second_pre = jnp.dot(first_act, second, preferred_element_type=jnp.float32)
    second_act = jax.nn.silu(second_pre).astype(jnp.bfloat16)
    embedding = jnp.dot(second_act, third, preferred_element_type=jnp.float32)
    inv_norm = lax.rsqrt(jnp.sum(embedding * embedding, axis=1, keepdims=True) + 1.0)
    unit = (embedding * inv_norm).astype(jnp.bfloat16)
    return ((first_pre, first_act, second_pre, second_act, embedding, inv_norm), unit)


def tower_backward(features, second, third, saved, unit_grad):
    first_pre, first_act, second_pre, second_act, embedding, inv_norm = saved
    along = jnp.sum(embedding * unit_grad, axis=1, keepdims=True)
    embed_grad = (inv_norm * unit_grad - inv_norm * inv_norm * inv_norm * embedding * along).astype(
        jnp.bfloat16
    )
    third_grad = contract_rows(second_act, embed_grad)
    second_slope = (contract_cols(embed_grad, third) * silu_slope(second_pre)).astype(jnp.bfloat16)
    second_grad = contract_rows(first_act, second_slope)
    first_slope = (contract_cols(second_slope, second) * silu_slope(first_pre)).astype(jnp.bfloat16)
    first_grad = contract_rows(features, first_slope)
    return (first_grad, second_grad, third_grad)


pack_columns = 256
vmem = pl.BlockSpec(memory_space=pltpu.VMEM)


def greet(ndp, nneg, me_dp, me_neg):
    barrier = pltpu.get_barrier_semaphore()
    for k in range(1, nneg):
        pl.semaphore_signal(
            barrier, inc=1, device_id={"neg": lax.rem(me_neg + k, nneg)}, device_id_type=pl.DeviceIdType.MESH
        )
    for k in range(1, ndp):
        pl.semaphore_signal(
            barrier, inc=1, device_id={"dp": lax.rem(me_dp + k, ndp)}, device_id_type=pl.DeviceIdType.MESH
        )
    pl.semaphore_wait(barrier, (nneg - 1) + (ndp - 1))


def send(src, dst, send_sem, recv_sem, axis, target):
    copy = pltpu.make_async_remote_copy(
        src_ref=src,
        dst_ref=dst,
        send_sem=send_sem,
        recv_sem=recv_sem,
        device_id={axis: target},
        device_id_type=pl.DeviceIdType.MESH,
    )
    copy.start()
    return copy


def share(axis, n, me, src_of, dst, send_sem, recv_sem):
    return [
        send(src_of(lax.rem(me + k, n)), dst.at[me], send_sem.at[k], recv_sem.at[k], axis, lax.rem(me + k, n))
        for k in range(1, n)
    ]


def finish(copies):
    for copy in copies:
        copy.wait()


def link(src, dst, sems, index, axis, target, send_index=None):
    send_sems, recv_sems = sems
    return pltpu.make_async_remote_copy(
        src_ref=src,
        dst_ref=dst,
        send_sem=send_sems.at[index if send_index is None else send_index],
        recv_sem=recv_sems.at[index],
        device_id={axis: target},
        device_id_type=pl.DeviceIdType.MESH,
    )


def score_kernel(
    ndp, nneg, query_ref, negative_ref, pid_ref, nid_ref, count_ref, pexp_ref, sum_ref, denom_ref, nsum_ref,
    q_land, n_land, meta_out, meta, rows, pid_out, pid_land, pid_col, w, den, dpart, dland, scaled,
    q_out, q_part, q_in, c_out, c_in, own, out, lx, ly, l2y, l2x,
    sx, sy, rn, sm, rm, sr, sl, rq, s_meta, r_meta, s_pid, r_pid, sd, rd, sq, rqs,
    sc, rc, s1x, r1x, s1y, r1y, s2y, r2y, s2x, r2x,
):
    me_dp, me_neg = lax.axis_index("dp"), lax.axis_index("neg")
    line, nx = ndp // 2, nneg // 2
    place, side = me_dp // 2, lax.rem(me_dp, 2)
    me_x, me_core = me_neg // 2, lax.rem(me_neg, 2)
    far, other = 1 - side, 1 - me_core
    partner, mate = 2 * place + far, 2 * me_x + other
    rows_q, width = query_ref.shape
    block = 2 * negative_ref.shape[1]
    lanes = den.shape[2]
    cuts = q_land.shape[1]
    half_w = width // 2
    blocks = nneg * 2
    here = (me_x * 2 + side) * 2 + me_core

    def along(k):
        return lax.rem(me_x + k, nx)

    def at_place(z):
        return 2 * z + side

    barrier = pltpu.get_barrier_semaphore()
    for k in range(1, line):
        pl.semaphore_signal(
            barrier, inc=1, device_id={"dp": at_place(lax.rem(place + k, line))}, device_id_type=pl.DeviceIdType.MESH
        )

    def quad(k):
        b = lax.rem(here + k, blocks)
        return {"dp": 2 * place + lax.rem(b // 2, 2), "neg": 2 * (b // 4) + lax.rem(b, 2)}

    for k in range(1, blocks):
        pl.semaphore_signal(barrier, inc=1, device_id=quad(k), device_id_type=pl.DeviceIdType.MESH)
    meta_out[0:1, :] = nid_ref[pl.ds(me_dp, 1), :]
    meta_out[1:2, :] = count_ref[pl.ds(me_dp, 1), :]
    pid_out[...] = pid_ref[pl.ds(me_neg, 1), :]
    pl.semaphore_wait(barrier, (line - 1) + (blocks - 1))

    def slot(x, y, half):
        return (x * 2 + y) * 2 + half

    def piece(x, y, half):
        return n_land.at[(x * 2 + y) * 2 + me_core, half]

    def push(src, x, y, half, send_sems, index, axis, target):
        return link(src, piece(x, y, half), (send_sems, rn), slot(x, y, half), axis, target, index)

    def relay(src, x, y, half):
        i = slot(x, y, half)
        return link(src, piece(x, y, half), (sm, rm), i, "neg", mate)

    def landed(x, y, half):
        ref = piece(x, y, half)
        link(ref, ref, (sy, rn), slot(x, y, half), "neg", mate, 0).wait_recv()

    sends = []

    def go(copy):
        copy.start()
        sends.append(copy)

    def to_x(src, x, y, half, kind):
        for k in range(1, nx):
            go(push(src, x, y, half, sx, kind * nx + k, "neg", 2 * along(k) + me_core))

    def to_y(src, x, y, half, index):
        go(push(src, x, y, half, sy, index, "dp", partner))

    first, second = negative_ref.at[0], negative_ref.at[1]
    to_x(first, me_x, side, 0, 0)
    to_y(second, me_x, side, 1, 0)
    to_x(second, me_x, side, 1, 1)
    to_y(first, me_x, side, 0, 1)
    go(relay(first, me_x, side, 0))
    go(relay(second, me_x, side, 1))

    def chain(slot_z, j, distance, sems, target):
        src = query_ref.at[pl.ds(j * (rows_q // cuts), rows_q // cuts)] if distance == 0 else q_land.at[slot_z, j]
        return link(src, q_land.at[slot_z, j], (sems, rq), slot_z * cuts + j, "dp", target, distance * cuts + j)

    def right(distance, j):
        return chain(place - distance, j, distance, sr, at_place(lax.rem(place + 1, line)))

    def left(distance, j):
        return chain(place + distance, j, distance, sl, at_place(lax.rem(place + line - 1, line)))

    goes_right, goes_left = place < line - 1, place > 0
    for j in range(cuts):
        pl.when(goes_right)(lambda j=j: right(0, j).start())
        pl.when(goes_left)(lambda j=j: left(0, j).start())
    for k in range(1, blocks):
        b = lax.rem(here + k, blocks)
        copy = pltpu.make_async_remote_copy(
            src_ref=meta_out, dst_ref=meta.at[here], send_sem=s_meta.at[k], recv_sem=r_meta.at[here],
            device_id=quad(k), device_id_type=pl.DeviceIdType.MESH,
        )
        go(copy)
    for k in range(1, line):
        z = lax.rem(place + k, line)
        go(link(pid_out, pid_land.at[place], (s_pid, r_pid), place, "dp", at_place(z), k))
    n_land[here] = negative_ref[...]
    for j in range(cuts):
        q_land[place, j] = query_ref[pl.ds(j * (rows_q // cuts), rows_q // cuts), :]
    meta[here] = meta_out[...]
    pid_land[place] = pid_out[...]

    for k in range(1, nx):
        x = along(k)
        landed(x, side, 0)
        to_y(piece(x, side, 0), x, side, 0, 1 + k)
        go(relay(piece(x, side, 0), x, side, 0))
    landed(me_x, far, 1)
    to_x(piece(me_x, far, 1), me_x, far, 1, 2)
    go(relay(piece(me_x, far, 1), me_x, far, 1))

    def q_step(distance):
        for j in range(cuts):

            @pl.when(place >= distance)
            def _():
                ref = q_land.at[place - distance, j]
                link(ref, ref, (sr, rq), (place - distance) * cuts + j, "dp", partner, 0).wait_recv()
                pl.when(goes_right)(lambda: right(distance, j).start())

            @pl.when(place + distance < line)
            def _():
                ref = q_land.at[place + distance, j]
                link(ref, ref, (sl, rq), (place + distance) * cuts + j, "dp", partner, 0).wait_recv()
                pl.when(goes_left)(lambda: left(distance, j).start())

    q_step(1)
    for k in range(1, nx):
        x = along(k)
        landed(x, side, 1)
        go(relay(piece(x, side, 1), x, side, 1))
    landed(me_x, far, 0)
    go(relay(piece(me_x, far, 0), me_x, far, 0))
    for distance in range(2, line):
        q_step(distance)
    for half in range(2):
        for k in range(1, nx):
            x = along(k)
            landed(x, far, half)
            go(relay(piece(x, far, half), x, far, half))
    for x in range(nx):
        for y in range(2):
            for half in range(2):
                i = slot(x, y, half)
                ref = n_land.at[(x * 2 + y) * 2 + other, half]
                link(ref, ref, (sm, rm), i, "neg", mate).wait_recv()
    for k in range(1, blocks):
        b = lax.rem(here + k, blocks)
        link(meta.at[b], meta.at[b], (s_meta, r_meta), b, "neg", mate).wait_recv()
    for k in range(1, line):
        z = lax.rem(place + k, line)
        link(pid_land.at[z], pid_land.at[z], (s_pid, r_pid), z, "dp", partner).wait_recv()

    for b in range(blocks):
        rows[b, 0:1, :] = meta[b, 0:1, :].astype(jnp.float32)
        rows[b, 1:2, :] = jnp.log(meta[b, 1:2, :].astype(jnp.float32))
    for z in range(line):
        pid_col[z] = jnp.broadcast_to(pid_land[z].astype(jnp.float32), (lanes, rows_q)).T
        den[z] = jnp.zeros((rows_q, lanes), jnp.float32)

    def unit(i, carry):
        b, z = i // line, lax.rem(i, line)
        dots = contract_cols(q_land[z].reshape(rows_q, width), n_land[b].reshape(block, width))
        value = jnp.exp(dots * inv_temp - rows[b, 1:2, :])
        ids = jnp.concatenate([pid_col[z]] * (block // lanes), axis=1)
        value = jnp.where(ids != rows[b, 0:1, :], value, 0.0)
        w[b, z] = value.astype(jnp.bfloat16)
        total = den[z]
        for c in range(0, block, lanes):
            total = total + value[:, c : c + lanes]
        den[z] = total
        return carry

    lax.fori_loop(0, blocks * line, unit, 0)
    for z in range(line):
        dpart[z] = jnp.sum(den[z].T, axis=0, keepdims=True)
    dpart[place] = dpart[place] + pexp_ref[...]
    for k in range(1, line):
        z = lax.rem(place + k, line)
        go(link(dpart, dland.at[place], (sd, rd), place, "dp", at_place(z), k))

    def q_block(z):
        if block % 128 == 0:
            left_side = jnp.concatenate([w[b, z] for b in range(blocks)], axis=1)
            return jnp.dot(
                left_side, n_land[...].reshape(blocks * block, width), preferred_element_type=jnp.float32
            )
        total = jnp.zeros((rows_q, width), jnp.float32)
        for b in range(blocks):
            total = total + jnp.dot(w[b, z], n_land[b].reshape(block, width), preferred_element_type=jnp.float32)
        return total

    def q_send(k, z):
        return link(q_out.at[z], q_in.at[place], (sq, rqs), place, "dp", at_place(z), k)

    def q_push(k, carry):
        z = lax.rem(place + k, line)
        q_out[z] = q_block(z).astype(jnp.bfloat16)
        q_send(k, z).start()
        return carry

    lax.fori_loop(1, line, q_push, 0)
    q_part[...] = q_block(place)
    total = dpart[...]
    for k in range(1, line):
        z = lax.rem(place + k, line)
        link(dland.at[z], dland.at[z], (sd, rd), z, "dp", partner).wait_recv()
        total = total + dland[z]
    dpart2 = 1.0 / total
    for z in range(line):
        q_t = q_land[z].reshape(rows_q, width).astype(jnp.float32).T
        scaled[:, z * rows_q : (z + 1) * rows_q] = (q_t * dpart2[z]).astype(jnp.bfloat16)
    denom_ref[...] = dpart[place]
    for k in range(1, line):
        denom_ref[...] = denom_ref[...] + dland[lax.rem(place + k, line), place]

    def dest(i):
        x = lax.rem(me_x + 1 + i // 2, nx)
        y = lax.rem(side + 1 + lax.rem(i, 2), 2)
        return x, y

    def part(x, y, core):
        return jnp.dot(
            scaled[...], w[(x * 2 + y) * 2 + core].reshape(line * rows_q, block), preferred_element_type=jnp.float32
        )

    def c_send(i):
        x, y = dest(i)
        return link(c_out.at[x, y], c_in.at[x, y], (sc, rc), x * 2 + y, "neg", mate)

    def far_step(i, carry):
        x, y = dest(i)
        c_out[x, y] = part(x, y, other).astype(jnp.bfloat16).reshape(2, half_w, block)
        c_send(i).start()
        return carry

    def send_1x(i):
        x, y = dest(i)
        return link(out.at[x, y, 0], lx.at[me_x, y], (s1x, r1x), me_x * 2 + y, "neg", 2 * x + me_core, x * 2 + y)

    def send_1y(i):
        x, y = dest(i)
        return link(out.at[x, y, 1], ly.at[x], (s1y, r1y), x, "dp", partner)

    def own_step(i, carry):
        x, y = dest(i)
        value = part(x, y, me_core).reshape(2, half_w, block)
        link(c_in.at[x, y], c_in.at[x, y], (sc, rc), x * 2 + y, "neg", mate).wait_recv()
        value = value + c_in[x, y].astype(jnp.float32)
        own[x, y] = value

        @pl.when(i < 2 * (nx - 1))
        def _():
            out[x, y, 0] = value[0].astype(jnp.bfloat16)
            send_1x(i).start()

        @pl.when(lax.rem(i, 2) == 0)
        def _():
            out[x, y, 1] = value[1].astype(jnp.bfloat16)
            send_1y(i).start()

        return carry

    lax.fori_loop(0, 2 * nx, far_step, 0)
    lax.fori_loop(0, 2 * nx, own_step, 0)
    value = own[me_x, far, 0]
    for k in range(1, nx):
        x = along(k)
        ref = lx.at[x, far]
        link(ref, ref, (s1x, r1x), x * 2 + far, "neg", mate).wait_recv()
        value = value + lx[x, far].astype(jnp.float32)
    out[me_x, far, 0] = value.astype(jnp.bfloat16)
    go(link(out.at[me_x, far, 0], l2y, (s2y, r2y), 0, "dp", partner))
    for k in range(1, nx):
        x = along(k)
        link(ly.at[x], ly.at[x], (s1y, r1y), x, "dp", partner).wait_recv()
        out[x, side, 1] = (own[x, side, 1] + ly[x].astype(jnp.float32)).astype(jnp.bfloat16)
        go(link(out.at[x, side, 1], l2x.at[me_x], (s2x, r2x), me_x, "neg", 2 * x + me_core, x))
    result = q_part[...]
    for k in range(1, line):
        z = lax.rem(place + k, line)
        link(q_in.at[z], q_in.at[z], (sq, rqs), z, "dp", partner).wait_recv()
        result = result + q_in[z].astype(jnp.float32)
    sum_ref[...] = result
    low = own[me_x, side, 0]
    for k in range(1, nx):
        x = along(k)
        ref = lx.at[x, side]
        link(ref, ref, (s1x, r1x), x * 2 + side, "neg", mate).wait_recv()
        low = low + lx[x, side].astype(jnp.float32)
    link(ly.at[me_x], ly.at[me_x], (s1y, r1y), me_x, "dp", partner).wait_recv()
    high = own[me_x, side, 1] + ly[me_x].astype(jnp.float32)
    link(l2y, l2y, (s2y, r2y), 0, "dp", partner).wait_recv()
    nsum_ref[0] = low + l2y[...].astype(jnp.float32)
    for k in range(1, nx):
        x = along(k)
        link(l2x.at[x], l2x.at[x], (s2x, r2x), x, "neg", mate).wait_recv()
        high = high + l2x[x].astype(jnp.float32)
    nsum_ref[1] = high

    for copy in sends:
        copy.wait_send()
    for distance in range(line):
        for j in range(cuts):
            if distance < line - 1:
                pl.when((place >= distance) & goes_right)(lambda: right(distance, j).wait_send())
                pl.when((place + distance < line) & goes_left)(lambda: left(distance, j).wait_send())
    for k in range(1, line):
        q_send(k, lax.rem(place + k, line)).wait_send()
    for i in range(2 * nx):
        c_send(i).wait_send()
        if i < 2 * (nx - 1):
            send_1x(i).wait_send()
        if i % 2 == 0:
            send_1y(i).wait_send()


def weight_kernel(
    ndp, nneg, packed_ref, loss_ref, gathered_ref, stats_ref,
    core_land, sum_a, sum_b, land_a, land_b, half_a, half_b, last_a, last_b, line_sum, line_land,
    stat_dp, stat_dp_land, stat_neg, stat_neg_land,
    cs, cr, xs, xr, ys, yr, ps, pr, ss, sr, ts, tr, gs, gr, hs, hr,
):
    me_dp, me_neg = lax.axis_index("dp"), lax.axis_index("neg")
    nx, line = nneg // 2, ndp // 2
    me_x, me_core = me_neg // 2, lax.rem(me_neg, 2)
    place, side = me_dp // 2, lax.rem(me_dp, 2)
    other, far = 1 - me_core, 1 - side
    mate, partner = 2 * me_x + other, 2 * place + far
    greet(ndp, nneg, me_dp, me_neg)
    turn = list(range(1, nx)) + [0]

    def x_of(k):
        return lax.rem(me_x + k, nx)

    core = {}
    for k in turn:
        x = x_of(k)
        core[k] = send(packed_ref.at[2 * x + other], core_land.at[x], cs.at[k], cr.at[k], "neg", mate)

    def add_core(x, y, half, target):
        def body(z, carry):
            target[z] = (
                packed_ref[2 * x + me_core, 2 * z + y, half].astype(jnp.float32)
                + core_land[x, 2 * z + y, half].astype(jnp.float32)
            ).astype(jnp.bfloat16)
            return carry

        lax.fori_loop(0, line, body, 0)

    def add(target, *terms):
        def body(z, carry):
            value = terms[0][z].astype(jnp.float32)
            for term in terms[1:]:
                value = value + term[z].astype(jnp.float32)
            target[z] = value.astype(jnp.bfloat16)
            return carry

        lax.fori_loop(0, line, body, 0)

    first_a = []
    for k in turn:
        x = x_of(k)
        core[k].wait_recv()
        if k:
            for y in range(2):
                add_core(x, y, 0, sum_a.at[x, y])
            first_a.append(send(sum_a.at[x], land_a.at[k], xs.at[k], xr.at[k], "neg", 2 * x + me_core))
        add_core(x, far, 1, sum_b.at[far, x])
    first_b = send(sum_b.at[far], land_b, ys.at[0], yr.at[0], "dp", partner)
    for y in range(2):
        add_core(me_x, y, 0, sum_a.at[me_x, y])
    for k in range(nx):
        add_core(x_of(k), side, 1, sum_b.at[side, x_of(k)])
    for copy in first_a:
        copy.wait_recv()
    add(half_a.at[far], sum_a.at[me_x, far], *[land_a.at[k, far] for k in range(1, nx)])
    second_a = send(half_a.at[far], last_a, ys.at[1], yr.at[1], "dp", partner)
    first_b.wait_recv()
    second_b = []
    for k in turn:
        x = x_of(k)
        add(half_b.at[x], sum_b.at[side, x], land_b.at[x])
        if k:
            second_b.append(
                send(half_b.at[x], last_b.at[k], xs.at[nx + k], xr.at[nx + k], "neg", 2 * x + me_core)
            )
    add(half_a.at[side], sum_a.at[me_x, side], *[land_a.at[k, side] for k in range(1, nx)])
    second_a.wait_recv()
    add(line_sum.at[0], half_a.at[side], last_a)
    third = []
    for half in range(2):
        if half:
            for copy in second_b:
                copy.wait_recv()
            add(line_sum.at[1], half_b.at[me_x], *[last_b.at[k] for k in range(1, nx)])
        for k in range(1, line):
            z = lax.rem(place + k, line)
            third.append(
                send(line_sum.at[half, z], line_land.at[half, k], ps.at[half * line + k], pr.at[half * line + k], "dp", 2 * z + side)
            )
    for copy in third:
        copy.wait_recv()
    squares = jnp.zeros((), jnp.float32)
    for half in range(2):
        piece = line_sum[half, place].astype(jnp.float32)
        for k in range(1, line):
            piece = piece + line_land[half, k].astype(jnp.float32)
        gathered_ref[me_neg, half] = piece.astype(jnp.bfloat16)
        squares = squares + jnp.sum(piece * piece)
    lane = lax.broadcasted_iota(jnp.int32, (8, 128), 1)
    stat_dp[...] = jnp.where(lane == 0, squares, loss_ref[0])
    stat_copies = share("dp", ndp, me_dp, lambda t: stat_dp, stat_dp_land, ss, sr)
    mine = gathered_ref.at[me_neg]
    spread = [send(mine, mine, gs.at[k], gr.at[k], "neg", 2 * x_of(k) + me_core) for k in range(1, nx)]
    spread.append(send(mine, mine, gs.at[0], gr.at[0], "neg", mate))
    finish(stat_copies)
    total = stat_dp[...]
    for k in range(1, ndp):
        total = total + stat_dp_land[lax.rem(me_dp + k, ndp)]
    stat_neg[...] = total
    stat_copies = share("neg", nneg, me_neg, lambda t: stat_neg, stat_neg_land, ts, tr)
    relay = []
    for k in range(1, nx):
        spread[k - 1].wait_recv()
        x = lax.rem(me_x + nx - k, nx)
        came = gathered_ref.at[2 * x + me_core]
        relay.append(send(came, came, hs.at[k], hr.at[k], "neg", mate))
    finish(stat_copies)
    total = stat_neg[...]
    for k in range(1, nneg):
        total = total + stat_neg_land[lax.rem(me_neg + k, nneg)]
    stats_ref[...] = total
    spread[-1].wait_recv()
    finish(relay)
    for copy in [*core.values(), *first_a, first_b, second_a, *second_b, *third, *spread]:
        copy.wait_send()


def call(kernel, collective, ndp, nneg, out_shape, scratch, in_specs):
    return pl.pallas_call(
        functools.partial(kernel, ndp, nneg),
        out_shape=out_shape,
        in_specs=in_specs,
        out_specs=tuple(vmem for _ in out_shape),
        scratch_shapes=scratch,
        compiler_params=pltpu.CompilerParams(
            collective_id=collective, has_side_effects=True, vmem_limit_bytes=48 * 1024 * 1024
        ),
    )


def sems(*counts):
    return [pltpu.SemaphoreType.DMA((count,)) for count in counts]


def to_packed(gradient, ndp):
    rows, columns = gradient.shape
    blocks = gradient.astype(jnp.bfloat16).reshape(ndp, rows // ndp, columns)
    return [blocks[:, :, c : c + pack_columns] for c in range(0, columns, pack_columns)]


def per_device(
    query_features,
    positive_features,
    negative_features,
    positive_ids,
    positive_counts,
    negative_ids,
    negative_counts,
    query_first,
    query_second,
    query_third,
    item_first,
    item_second,
    item_third,
):
    own_rows = query_features.shape[0]
    query_saved, query_unit = tower_forward(query_features, query_first, query_second, query_third)
    item_features = jnp.concatenate([positive_features, negative_features], axis=0)
    item_saved, item_unit = tower_forward(item_features, item_first, item_second, item_third)
    positive_unit = item_unit[:own_rows]
    negative_unit = item_unit[own_rows:]
    ndp, nneg = lax.axis_size("dp"), lax.axis_size("neg")
    width = query_unit.shape[1]
    line, nx = ndp // 2, nneg // 2
    block = negative_unit.shape[0]
    blocks, cuts, lanes = 2 * nneg, 2, min(block, 128)
    bf16, f32, i32 = jnp.bfloat16, jnp.float32, jnp.int32
    positive_logit = jnp.sum(
        query_unit.astype(f32) * positive_unit.astype(f32), axis=1
    ) * inv_temp - jnp.log(positive_counts.astype(f32))
    positive_exp = jnp.exp(positive_logit)
    rows_half = (width // 2, block)
    query_total, denom, negative_sum = call(
        score_kernel,
        0,
        ndp,
        nneg,
        (
            jax.ShapeDtypeStruct((own_rows, width), f32),
            jax.ShapeDtypeStruct((1, own_rows), f32),
            jax.ShapeDtypeStruct((2,) + rows_half, f32),
        ),
        [
            pltpu.VMEM((line, cuts, own_rows // cuts, width), bf16),
            pltpu.VMEM((blocks, 2, block // 2, width), bf16),
            pltpu.VMEM((2, block), i32),
            pltpu.VMEM((blocks, 2, block), i32),
            pltpu.VMEM((blocks, 2, block), f32),
            pltpu.VMEM((1, own_rows), i32),
            pltpu.VMEM((line, 1, own_rows), i32),
            pltpu.VMEM((line, own_rows, lanes), f32),
            pltpu.VMEM((blocks, line, own_rows, block), bf16),
            pltpu.VMEM((line, own_rows, lanes), f32),
            pltpu.VMEM((line, 1, own_rows), f32),
            pltpu.VMEM((line, line, 1, own_rows), f32),
            pltpu.VMEM((width, line * own_rows), bf16),
            pltpu.VMEM((line, own_rows, width), bf16),
            pltpu.VMEM((own_rows, width), f32),
            pltpu.VMEM((line, own_rows, width), bf16),
            pltpu.VMEM((nx, 2, 2) + rows_half, bf16),
            pltpu.VMEM((nx, 2, 2) + rows_half, bf16),
            pltpu.VMEM((nx, 2, 2) + rows_half, f32),
            pltpu.VMEM((nx, 2, 2) + rows_half, bf16),
            pltpu.VMEM((nx, 2) + rows_half, bf16),
            pltpu.VMEM((nx,) + rows_half, bf16),
            pltpu.VMEM(rows_half, bf16),
            pltpu.VMEM((nx,) + rows_half, bf16),
        ]
        + sems(
            3 * nx, 1 + nx, 4 * nx, 4 * nx, 4 * nx, line * cuts, line * cuts, line * cuts,
            blocks, blocks, line, line, line, line, line, line,
            2 * nx, 2 * nx, 2 * nx, 2 * nx, nx, nx, 1, 1, nx, nx,
        ),
        [vmem] * 6,
    )(
        query_unit,
        negative_unit.reshape(2, block // 2, width),
        positive_ids.reshape(nneg, own_rows),
        negative_ids.reshape(ndp, block),
        negative_counts.reshape(ndp, block),
        positive_exp.reshape(1, own_rows),
    )
    own_denom = denom.reshape(-1)
    loss_part = jnp.sum(jnp.log(own_denom) - positive_logit)
    positive_slope = positive_exp / own_denom - 1.0
    query_sum = query_total / own_denom[:, None]
    negative_sum = negative_sum.reshape(width, block).T
    query_grad = (
        query_sum + positive_slope[:, None] * positive_unit.astype(jnp.float32)
    ) * inv_temp
    positive_grad = positive_slope[:, None] * query_unit.astype(jnp.float32) * inv_temp
    item_grad = jnp.concatenate([positive_grad, negative_sum * inv_temp], axis=0)
    query_grads = tower_backward(query_features, query_second, query_third, query_saved, query_grad)
    item_grads = tower_backward(item_features, item_second, item_third, item_saved, item_grad)
    gradients = query_grads + item_grads
    parts = [part for gradient in gradients for part in to_packed(gradient, ndp)]
    packed = jnp.concatenate(parts, axis=1)
    rows = packed.shape[1] // nneg
    packed = packed.reshape(ndp, nneg, 2, rows // 2, pack_columns).transpose(1, 0, 2, 3, 4)
    piece = (rows // 2, pack_columns)
    gathered, stats = call(
        weight_kernel,
        3,
        ndp,
        nneg,
        (jax.ShapeDtypeStruct((nneg, 2) + piece, bf16), jax.ShapeDtypeStruct((8, 128), f32)),
        [
            pltpu.VMEM((nx, ndp, 2) + piece, bf16),
            pltpu.VMEM((nx, 2, line) + piece, bf16),
            pltpu.VMEM((2, nx, line) + piece, bf16),
            pltpu.VMEM((nx, 2, line) + piece, bf16),
            pltpu.VMEM((nx, line) + piece, bf16),
            pltpu.VMEM((2, line) + piece, bf16),
            pltpu.VMEM((nx, line) + piece, bf16),
            pltpu.VMEM((line,) + piece, bf16),
            pltpu.VMEM((nx, line) + piece, bf16),
            pltpu.VMEM((2, line) + piece, bf16),
            pltpu.VMEM((2, line) + piece, bf16),
            pltpu.VMEM((8, 128), f32),
            pltpu.VMEM((ndp, 8, 128), f32),
            pltpu.VMEM((8, 128), f32),
            pltpu.VMEM((nneg, 8, 128), f32),
        ]
        + sems(nx, nx, 2 * nx, 2 * nx, 2, 2, ndp, ndp, ndp, ndp, nneg, nneg, nx, nx, nx, nx),
        [vmem, pl.BlockSpec(memory_space=pltpu.SMEM)],
    )(packed, loss_part.reshape(1))
    grad_norm = jnp.sqrt(stats[0, 0])
    mean_loss = stats[0, 1] / (own_rows * ndp * nneg)
    clip_factor = clip_norm / jnp.maximum(grad_norm, clip_norm)
    flat = gathered.reshape(nneg * rows, pack_columns)
    clipped = []
    start = 0
    for gradient in gradients:
        height, columns = gradient.shape[0] // ndp, gradient.shape[1]
        groups = columns // pack_columns
        blocks = [flat[start + g * height : start + (g + 1) * height] for g in range(groups)]
        start += groups * height
        clipped.append(jnp.concatenate(blocks, axis=1).astype(jnp.float32) * clip_factor)
    return (mean_loss, *clipped)


def solution(mesh):
    placed = (
        P(("dp", "neg"), None),
        P(("dp", "neg"), None),
        P(("neg", "dp"), None),
        P("dp"),
        P(("dp", "neg")),
        P("neg"),
        P("neg"),
        P(),
        P(),
        P(),
        P(),
        P(),
        P(),
    )
    return jax.shard_map(
        per_device,
        mesh=mesh,
        in_specs=placed,
        out_specs=(
            P(),
            P("dp", None),
            P("dp", None),
            P("dp", None),
            P("dp", None),
            P("dp", None),
            P("dp", None),
        ),
        check_vma=False,
    )
```

```python
import functools

import jax
import jax.numpy as jnp
from jax import lax
from jax.experimental import pallas as pl
from jax.experimental.pallas import tpu as pltpu
from jax.sharding import PartitionSpec as P

inv_temp = 20.0
clip_norm = 256.0


def silu_slope(pre):
    sigma = jax.nn.sigmoid(pre)
    return sigma * (1.0 + pre * (1.0 - sigma))


def contract_rows(left, right):
    return lax.dot_general(
        left, right, (((0,), (0,)), ((), ())), preferred_element_type=jnp.float32
    )


def contract_cols(left, right):
    return lax.dot_general(
        left, right, (((1,), (1,)), ((), ())), preferred_element_type=jnp.float32
    )


def tower_forward(features, first, second, third):
    first_pre = jnp.dot(features, first, preferred_element_type=jnp.float32)
    first_act = jax.nn.silu(first_pre).astype(jnp.bfloat16)
    second_pre = jnp.dot(first_act, second, preferred_element_type=jnp.float32)
    second_act = jax.nn.silu(second_pre).astype(jnp.bfloat16)
    embedding = jnp.dot(second_act, third, preferred_element_type=jnp.float32)
    inv_norm = lax.rsqrt(jnp.sum(embedding * embedding, axis=1, keepdims=True) + 1.0)
    unit = (embedding * inv_norm).astype(jnp.bfloat16)
    saved = (silu_slope(first_pre), first_act, silu_slope(second_pre), second_act, embedding, inv_norm)
    return saved, unit


def tower_backward(features, second, third, saved, unit_grad):
    first_slope, first_act, second_slope, second_act, embedding, inv_norm = saved
    along = jnp.sum(embedding * unit_grad, axis=1, keepdims=True)
    embed_grad = (inv_norm * unit_grad - inv_norm * inv_norm * inv_norm * embedding * along).astype(
        jnp.bfloat16
    )
    third_grad = contract_rows(second_act, embed_grad)
    second_step = (contract_cols(embed_grad, third) * second_slope).astype(jnp.bfloat16)
    second_grad = contract_rows(first_act, second_step)
    first_step = (contract_cols(second_step, second) * first_slope).astype(jnp.bfloat16)
    first_grad = contract_rows(features, first_step)
    return (first_grad, second_grad, third_grad)


pack_columns = 256
vmem = pl.BlockSpec(memory_space=pltpu.VMEM)


def greet(ndp, nneg, me_dp, me_neg):
    barrier = pltpu.get_barrier_semaphore()
    for k in range(1, nneg):
        pl.semaphore_signal(
            barrier, inc=1, device_id={"neg": lax.rem(me_neg + k, nneg)}, device_id_type=pl.DeviceIdType.MESH
        )
    for k in range(1, ndp):
        pl.semaphore_signal(
            barrier, inc=1, device_id={"dp": lax.rem(me_dp + k, ndp)}, device_id_type=pl.DeviceIdType.MESH
        )
    pl.semaphore_wait(barrier, (nneg - 1) + (ndp - 1))


def send(src, dst, send_sem, recv_sem, axis, target):
    copy = pltpu.make_async_remote_copy(
        src_ref=src,
        dst_ref=dst,
        send_sem=send_sem,
        recv_sem=recv_sem,
        device_id={axis: target},
        device_id_type=pl.DeviceIdType.MESH,
    )
    copy.start()
    return copy


def share(axis, n, me, src_of, dst, send_sem, recv_sem):
    return [
        send(src_of(lax.rem(me + k, n)), dst.at[me], send_sem.at[k], recv_sem.at[k], axis, lax.rem(me + k, n))
        for k in range(1, n)
    ]


def finish(copies):
    for copy in copies:
        copy.wait()


def link(src, dst, sems, index, axis, target, send_index=None):
    send_sems, recv_sems = sems
    return pltpu.make_async_remote_copy(
        src_ref=src,
        dst_ref=dst,
        send_sem=send_sems.at[index if send_index is None else send_index],
        recv_sem=recv_sems.at[index],
        device_id={axis: target},
        device_id_type=pl.DeviceIdType.MESH,
    )


def score_kernel(
    ndp, nneg, query_ref, negative_ref, pid_ref, nid_ref, count_ref, pexp_ref, sum_ref, denom_ref, nsum_ref,
    q_land, n_land, meta_out, meta, rows, pid_out, pid_land, pid_col, w, den, dpart, dland, scaled,
    q_out, q_part, q_in, c_out, c_in, own, out, lx, ly, l2y, l2x,
    sx, sy, rn, sm, rm, sr, sl, rq, s_meta, r_meta, s_pid, r_pid, sd, rd, sq, rqs,
    sc, rc, s1x, r1x, s1y, r1y, s2y, r2y, s2x, r2x,
):
    me_dp, me_neg = lax.axis_index("dp"), lax.axis_index("neg")
    line, nx = ndp // 2, nneg // 2
    place, side = me_dp // 2, lax.rem(me_dp, 2)
    me_x, me_core = me_neg // 2, lax.rem(me_neg, 2)
    far, other = 1 - side, 1 - me_core
    partner, mate = 2 * place + far, 2 * me_x + other
    rows_q, width = query_ref.shape
    block = 2 * negative_ref.shape[1]
    lanes = den.shape[2]
    cuts = q_land.shape[1]
    half_w = width // 2
    blocks = nneg * 2
    here = (me_x * 2 + side) * 2 + me_core

    def along(k):
        return lax.rem(me_x + k, nx)

    def at_place(z):
        return 2 * z + side

    barrier = pltpu.get_barrier_semaphore()
    for k in range(1, line):
        pl.semaphore_signal(
            barrier, inc=1, device_id={"dp": at_place(lax.rem(place + k, line))}, device_id_type=pl.DeviceIdType.MESH
        )

    def quad(k):
        b = lax.rem(here + k, blocks)
        return {"dp": 2 * place + lax.rem(b // 2, 2), "neg": 2 * (b // 4) + lax.rem(b, 2)}

    for k in range(1, blocks):
        pl.semaphore_signal(barrier, inc=1, device_id=quad(k), device_id_type=pl.DeviceIdType.MESH)
    meta_out[0:1, :] = nid_ref[pl.ds(me_dp, 1), :]
    meta_out[1:2, :] = count_ref[pl.ds(me_dp, 1), :]
    pid_out[...] = pid_ref[pl.ds(me_neg, 1), :]
    pl.semaphore_wait(barrier, (line - 1) + (blocks - 1))

    def slot(x, y, half):
        return (x * 2 + y) * 2 + half

    def piece(x, y, half):
        return n_land.at[(x * 2 + y) * 2 + me_core, half]

    def push(src, x, y, half, send_sems, index, axis, target):
        return link(src, piece(x, y, half), (send_sems, rn), slot(x, y, half), axis, target, index)

    def relay(src, x, y, half):
        i = slot(x, y, half)
        return link(src, piece(x, y, half), (sm, rm), i, "neg", mate)

    def landed(x, y, half):
        ref = piece(x, y, half)
        link(ref, ref, (sy, rn), slot(x, y, half), "neg", mate, 0).wait_recv()

    sends = []

    def go(copy):
        copy.start()
        sends.append(copy)

    def to_x(src, x, y, half, kind):
        for k in range(1, nx):
            go(push(src, x, y, half, sx, kind * nx + k, "neg", 2 * along(k) + me_core))

    def to_y(src, x, y, half, index):
        go(push(src, x, y, half, sy, index, "dp", partner))

    first, second = negative_ref.at[0], negative_ref.at[1]
    to_x(first, me_x, side, 0, 0)
    to_y(second, me_x, side, 1, 0)
    to_x(second, me_x, side, 1, 1)
    to_y(first, me_x, side, 0, 1)
    go(relay(first, me_x, side, 0))
    go(relay(second, me_x, side, 1))

    def chain(slot_z, j, distance, sems, target):
        src = query_ref.at[pl.ds(j * (rows_q // cuts), rows_q // cuts)] if distance == 0 else q_land.at[slot_z, j]
        return link(src, q_land.at[slot_z, j], (sems, rq), slot_z * cuts + j, "dp", target, distance * cuts + j)

    def right(distance, j):
        return chain(place - distance, j, distance, sr, at_place(lax.rem(place + 1, line)))

    def left(distance, j):
        return chain(place + distance, j, distance, sl, at_place(lax.rem(place + line - 1, line)))

    goes_right, goes_left = place < line - 1, place > 0
    for j in range(cuts):
        pl.when(goes_right)(lambda j=j: right(0, j).start())
        pl.when(goes_left)(lambda j=j: left(0, j).start())
    for k in range(1, blocks):
        b = lax.rem(here + k, blocks)
        copy = pltpu.make_async_remote_copy(
            src_ref=meta_out, dst_ref=meta.at[here], send_sem=s_meta.at[k], recv_sem=r_meta.at[here],
            device_id=quad(k), device_id_type=pl.DeviceIdType.MESH,
        )
        go(copy)
    for k in range(1, line):
        z = lax.rem(place + k, line)
        go(link(pid_out, pid_land.at[place], (s_pid, r_pid), place, "dp", at_place(z), k))
    n_land[here] = negative_ref[...]
    for j in range(cuts):
        q_land[place, j] = query_ref[pl.ds(j * (rows_q // cuts), rows_q // cuts), :]
    meta[here] = meta_out[...]
    pid_land[place] = pid_out[...]

    for k in range(1, nx):
        x = along(k)
        landed(x, side, 0)
        to_y(piece(x, side, 0), x, side, 0, 1 + k)
        go(relay(piece(x, side, 0), x, side, 0))
    landed(me_x, far, 1)
    to_x(piece(me_x, far, 1), me_x, far, 1, 2)
    go(relay(piece(me_x, far, 1), me_x, far, 1))

    def q_step(distance):
        for j in range(cuts):

            @pl.when(place >= distance)
            def _():
                ref = q_land.at[place - distance, j]
                link(ref, ref, (sr, rq), (place - distance) * cuts + j, "dp", partner, 0).wait_recv()
                pl.when(goes_right)(lambda: right(distance, j).start())

            @pl.when(place + distance < line)
            def _():
                ref = q_land.at[place + distance, j]
                link(ref, ref, (sl, rq), (place + distance) * cuts + j, "dp", partner, 0).wait_recv()
                pl.when(goes_left)(lambda: left(distance, j).start())

    q_step(1)
    for k in range(1, nx):
        x = along(k)
        landed(x, side, 1)
        go(relay(piece(x, side, 1), x, side, 1))
    landed(me_x, far, 0)
    go(relay(piece(me_x, far, 0), me_x, far, 0))
    for distance in range(2, line):
        q_step(distance)
    for half in range(2):
        for k in range(1, nx):
            x = along(k)
            landed(x, far, half)
            go(relay(piece(x, far, half), x, far, half))
    for x in range(nx):
        for y in range(2):
            for half in range(2):
                i = slot(x, y, half)
                ref = n_land.at[(x * 2 + y) * 2 + other, half]
                link(ref, ref, (sm, rm), i, "neg", mate).wait_recv()
    for k in range(1, blocks):
        b = lax.rem(here + k, blocks)
        link(meta.at[b], meta.at[b], (s_meta, r_meta), b, "neg", mate).wait_recv()
    for k in range(1, line):
        z = lax.rem(place + k, line)
        link(pid_land.at[z], pid_land.at[z], (s_pid, r_pid), z, "dp", partner).wait_recv()

    for b in range(blocks):
        rows[b, 0:1, :] = meta[b, 0:1, :].astype(jnp.float32)
        rows[b, 1:2, :] = jnp.log(meta[b, 1:2, :].astype(jnp.float32))
    for z in range(line):
        pid_col[z] = jnp.broadcast_to(pid_land[z].astype(jnp.float32), (lanes, rows_q)).T
        den[z] = jnp.zeros((rows_q, lanes), jnp.float32)

    def unit(i, carry):
        b, z = i // line, lax.rem(i, line)
        dots = contract_cols(q_land[z].reshape(rows_q, width), n_land[b].reshape(block, width))
        value = jnp.exp(dots * inv_temp - rows[b, 1:2, :])
        ids = jnp.concatenate([pid_col[z]] * (block // lanes), axis=1)
        value = jnp.where(ids != rows[b, 0:1, :], value, 0.0)
        w[b, z] = value.astype(jnp.bfloat16)
        total = den[z]
        for c in range(0, block, lanes):
            total = total + value[:, c : c + lanes]
        den[z] = total
        return carry

    lax.fori_loop(0, blocks * line, unit, 0)
    for z in range(line):
        dpart[z] = jnp.sum(den[z].T, axis=0, keepdims=True)
    dpart[place] = dpart[place] + pexp_ref[...]
    for k in range(1, line):
        z = lax.rem(place + k, line)
        go(link(dpart, dland.at[place], (sd, rd), place, "dp", at_place(z), k))

    def q_block(z):
        if block % 128 == 0:
            left_side = jnp.concatenate([w[b, z] for b in range(blocks)], axis=1)
            return jnp.dot(
                left_side, n_land[...].reshape(blocks * block, width), preferred_element_type=jnp.float32
            )
        total = jnp.zeros((rows_q, width), jnp.float32)
        for b in range(blocks):
            total = total + jnp.dot(w[b, z], n_land[b].reshape(block, width), preferred_element_type=jnp.float32)
        return total

    def q_send(k, z):
        return link(q_out.at[z], q_in.at[place], (sq, rqs), place, "dp", at_place(z), k)

    def q_push(k, carry):
        z = lax.rem(place + k, line)
        q_out[z] = q_block(z).astype(jnp.bfloat16)
        q_send(k, z).start()
        return carry

    lax.fori_loop(1, line, q_push, 0)
    q_part[...] = q_block(place)
    total = dpart[...]
    for k in range(1, line):
        z = lax.rem(place + k, line)
        link(dland.at[z], dland.at[z], (sd, rd), z, "dp", partner).wait_recv()
        total = total + dland[z]
    dpart2 = 1.0 / total
    for z in range(line):
        q_t = q_land[z].reshape(rows_q, width).astype(jnp.float32).T
        scaled[:, z * rows_q : (z + 1) * rows_q] = (q_t * dpart2[z]).astype(jnp.bfloat16)
    denom_ref[...] = dpart[place]
    for k in range(1, line):
        denom_ref[...] = denom_ref[...] + dland[lax.rem(place + k, line), place]

    def dest(i):
        x = lax.rem(me_x + 1 + i // 2, nx)
        y = lax.rem(side + 1 + lax.rem(i, 2), 2)
        return x, y

    def part(x, y, core):
        return jnp.dot(
            scaled[...], w[(x * 2 + y) * 2 + core].reshape(line * rows_q, block), preferred_element_type=jnp.float32
        )

    def c_send(i):
        x, y = dest(i)
        return link(c_out.at[x, y], c_in.at[x, y], (sc, rc), x * 2 + y, "neg", mate)

    def far_step(i, carry):
        x, y = dest(i)
        c_out[x, y] = part(x, y, other).astype(jnp.bfloat16).reshape(2, half_w, block)
        c_send(i).start()
        return carry

    def send_1x(i):
        x, y = dest(i)
        return link(out.at[x, y, 0], lx.at[me_x, y], (s1x, r1x), me_x * 2 + y, "neg", 2 * x + me_core, x * 2 + y)

    def send_1y(i):
        x, y = dest(i)
        return link(out.at[x, y, 1], ly.at[x], (s1y, r1y), x, "dp", partner)

    def own_step(i, carry):
        x, y = dest(i)
        value = part(x, y, me_core).reshape(2, half_w, block)
        link(c_in.at[x, y], c_in.at[x, y], (sc, rc), x * 2 + y, "neg", mate).wait_recv()
        value = value + c_in[x, y].astype(jnp.float32)
        own[x, y] = value

        @pl.when(i < 2 * (nx - 1))
        def _():
            out[x, y, 0] = value[0].astype(jnp.bfloat16)
            send_1x(i).start()

        @pl.when(lax.rem(i, 2) == 0)
        def _():
            out[x, y, 1] = value[1].astype(jnp.bfloat16)
            send_1y(i).start()

        return carry

    lax.fori_loop(0, 2 * nx, far_step, 0)
    lax.fori_loop(0, 2 * nx, own_step, 0)
    value = own[me_x, far, 0]
    for k in range(1, nx):
        x = along(k)
        ref = lx.at[x, far]
        link(ref, ref, (s1x, r1x), x * 2 + far, "neg", mate).wait_recv()
        value = value + lx[x, far].astype(jnp.float32)
    out[me_x, far, 0] = value.astype(jnp.bfloat16)
    go(link(out.at[me_x, far, 0], l2y, (s2y, r2y), 0, "dp", partner))
    for k in range(1, nx):
        x = along(k)
        link(ly.at[x], ly.at[x], (s1y, r1y), x, "dp", partner).wait_recv()
        out[x, side, 1] = (own[x, side, 1] + ly[x].astype(jnp.float32)).astype(jnp.bfloat16)
        go(link(out.at[x, side, 1], l2x.at[me_x], (s2x, r2x), me_x, "neg", 2 * x + me_core, x))
    result = q_part[...]
    for k in range(1, line):
        z = lax.rem(place + k, line)
        link(q_in.at[z], q_in.at[z], (sq, rqs), z, "dp", partner).wait_recv()
        result = result + q_in[z].astype(jnp.float32)
    sum_ref[...] = result
    low = own[me_x, side, 0]
    for k in range(1, nx):
        x = along(k)
        ref = lx.at[x, side]
        link(ref, ref, (s1x, r1x), x * 2 + side, "neg", mate).wait_recv()
        low = low + lx[x, side].astype(jnp.float32)
    link(ly.at[me_x], ly.at[me_x], (s1y, r1y), me_x, "dp", partner).wait_recv()
    high = own[me_x, side, 1] + ly[me_x].astype(jnp.float32)
    link(l2y, l2y, (s2y, r2y), 0, "dp", partner).wait_recv()
    nsum_ref[0] = low + l2y[...].astype(jnp.float32)
    for k in range(1, nx):
        x = along(k)
        link(l2x.at[x], l2x.at[x], (s2x, r2x), x, "neg", mate).wait_recv()
        high = high + l2x[x].astype(jnp.float32)
    nsum_ref[1] = high

    for copy in sends:
        copy.wait_send()
    for distance in range(line):
        for j in range(cuts):
            if distance < line - 1:
                pl.when((place >= distance) & goes_right)(lambda: right(distance, j).wait_send())
                pl.when((place + distance < line) & goes_left)(lambda: left(distance, j).wait_send())
    for k in range(1, line):
        q_send(k, lax.rem(place + k, line)).wait_send()
    for i in range(2 * nx):
        c_send(i).wait_send()
        if i < 2 * (nx - 1):
            send_1x(i).wait_send()
        if i % 2 == 0:
            send_1y(i).wait_send()


def weight_kernel(
    ndp, nneg, packed_ref, loss_ref, gathered_ref, stats_ref,
    core_land, sum_a, sum_b, land_a, land_b, half_a, half_b, last_a, last_b, line_sum, line_land,
    stat_dp, stat_dp_land, stat_neg, stat_neg_land,
    cs, cr, xs, xr, ys, yr, ps, pr, ss, sr, ts, tr, gs, gr, hs, hr,
):
    me_dp, me_neg = lax.axis_index("dp"), lax.axis_index("neg")
    nx, line = nneg // 2, ndp // 2
    me_x, me_core = me_neg // 2, lax.rem(me_neg, 2)
    place, side = me_dp // 2, lax.rem(me_dp, 2)
    other, far = 1 - me_core, 1 - side
    mate, partner = 2 * me_x + other, 2 * place + far
    greet(ndp, nneg, me_dp, me_neg)
    turn = list(range(1, nx)) + [0]

    def x_of(k):
        return lax.rem(me_x + k, nx)

    core = {}
    for k in turn:
        x = x_of(k)
        core[k] = send(packed_ref.at[2 * x + other], core_land.at[x], cs.at[k], cr.at[k], "neg", mate)

    def add_core(x, y, half, target):
        def body(z, carry):
            target[z] = (
                packed_ref[2 * x + me_core, 2 * z + y, half].astype(jnp.float32)
                + core_land[x, 2 * z + y, half].astype(jnp.float32)
            ).astype(jnp.bfloat16)
            return carry

        lax.fori_loop(0, line, body, 0)

    def add(target, *terms):
        def body(z, carry):
            value = terms[0][z].astype(jnp.float32)
            for term in terms[1:]:
                value = value + term[z].astype(jnp.float32)
            target[z] = value.astype(jnp.bfloat16)
            return carry

        lax.fori_loop(0, line, body, 0)

    first_a = []
    for k in turn:
        x = x_of(k)
        core[k].wait_recv()
        if k:
            for y in range(2):
                add_core(x, y, 0, sum_a.at[x, y])
            first_a.append(send(sum_a.at[x], land_a.at[k], xs.at[k], xr.at[k], "neg", 2 * x + me_core))
        add_core(x, far, 1, sum_b.at[far, x])
    first_b = send(sum_b.at[far], land_b, ys.at[0], yr.at[0], "dp", partner)
    for y in range(2):
        add_core(me_x, y, 0, sum_a.at[me_x, y])
    for k in range(nx):
        add_core(x_of(k), side, 1, sum_b.at[side, x_of(k)])
    for copy in first_a:
        copy.wait_recv()
    add(half_a.at[far], sum_a.at[me_x, far], *[land_a.at[k, far] for k in range(1, nx)])
    second_a = send(half_a.at[far], last_a, ys.at[1], yr.at[1], "dp", partner)
    first_b.wait_recv()
    second_b = []
    for k in turn:
        x = x_of(k)
        add(half_b.at[x], sum_b.at[side, x], land_b.at[x])
        if k:
            second_b.append(
                send(half_b.at[x], last_b.at[k], xs.at[nx + k], xr.at[nx + k], "neg", 2 * x + me_core)
            )
    add(half_a.at[side], sum_a.at[me_x, side], *[land_a.at[k, side] for k in range(1, nx)])
    second_a.wait_recv()
    add(line_sum.at[0], half_a.at[side], last_a)
    third = []
    for half in range(2):
        if half:
            for copy in second_b:
                copy.wait_recv()
            add(line_sum.at[1], half_b.at[me_x], *[last_b.at[k] for k in range(1, nx)])
        for k in range(1, line):
            z = lax.rem(place + k, line)
            third.append(
                send(line_sum.at[half, z], line_land.at[half, k], ps.at[half * line + k], pr.at[half * line + k], "dp", 2 * z + side)
            )
    for copy in third:
        copy.wait_recv()
    squares = jnp.zeros((), jnp.float32)
    for half in range(2):
        piece = line_sum[half, place].astype(jnp.float32)
        for k in range(1, line):
            piece = piece + line_land[half, k].astype(jnp.float32)
        gathered_ref[me_neg, half] = piece.astype(jnp.bfloat16)
        squares = squares + jnp.sum(piece * piece)
    lane = lax.broadcasted_iota(jnp.int32, (8, 128), 1)
    stat_dp[...] = jnp.where(lane == 0, squares, loss_ref[0])
    stat_copies = share("dp", ndp, me_dp, lambda t: stat_dp, stat_dp_land, ss, sr)
    mine = gathered_ref.at[me_neg]
    spread = [send(mine, mine, gs.at[k], gr.at[k], "neg", 2 * x_of(k) + me_core) for k in range(1, nx)]
    spread.append(send(mine, mine, gs.at[0], gr.at[0], "neg", mate))
    finish(stat_copies)
    total = stat_dp[...]
    for k in range(1, ndp):
        total = total + stat_dp_land[lax.rem(me_dp + k, ndp)]
    stat_neg[...] = total
    stat_copies = share("neg", nneg, me_neg, lambda t: stat_neg, stat_neg_land, ts, tr)
    relay = []
    for k in range(1, nx):
        spread[k - 1].wait_recv()
        x = lax.rem(me_x + nx - k, nx)
        came = gathered_ref.at[2 * x + me_core]
        relay.append(send(came, came, hs.at[k], hr.at[k], "neg", mate))
    finish(stat_copies)
    total = stat_neg[...]
    for k in range(1, nneg):
        total = total + stat_neg_land[lax.rem(me_neg + k, nneg)]
    stats_ref[...] = total
    spread[-1].wait_recv()
    finish(relay)
    for copy in [*core.values(), *first_a, first_b, second_a, *second_b, *third, *spread]:
        copy.wait_send()


def call(kernel, collective, ndp, nneg, out_shape, scratch, in_specs):
    return pl.pallas_call(
        functools.partial(kernel, ndp, nneg),
        out_shape=out_shape,
        in_specs=in_specs,
        out_specs=tuple(vmem for _ in out_shape),
        scratch_shapes=scratch,
        compiler_params=pltpu.CompilerParams(
            collective_id=collective, has_side_effects=True, vmem_limit_bytes=48 * 1024 * 1024
        ),
    )


def sems(*counts):
    return [pltpu.SemaphoreType.DMA((count,)) for count in counts]


def to_packed(gradient, ndp):
    rows, columns = gradient.shape
    blocks = gradient.astype(jnp.bfloat16).reshape(ndp, rows // ndp, columns)
    return [blocks[:, :, c : c + pack_columns] for c in range(0, columns, pack_columns)]


def backward_kernel(ndp, nneg, groups, *refs):
    refs = list(refs)
    take = iter(refs)
    towers = [[next(take) for _ in range(9)] for _ in range(2)]
    loss_ref = next(take)
    stats_ref = next(take)
    outs = [next(take) for _ in range(6)]
    scratch = [[next(take) for _ in range(3)] for _ in range(2)]
    names = ["packed", "c_in", "o1x", "l1x", "o1y", "l1y", "o2y", "l2y", "o2x", "l2x", "zs", "l3", "ag"]
    bufs = [{name: next(take) for name in names} for _ in groups]
    stat_dp, stat_dp_land, stat_neg, stat_neg_land = [next(take) for _ in range(4)]
    sem_names = ["cs", "cr", "s1x", "r1x", "s1y", "r1y", "s2y", "r2y", "s2x", "r2x", "s3", "r3", "sg", "rg", "sh", "rh"]
    for buf in bufs:
        for name in sem_names:
            buf[name] = next(take)
    ss, sr, ts, tr = [next(take) for _ in range(4)]

    me_dp, me_neg = lax.axis_index("dp"), lax.axis_index("neg")
    line, nx = ndp // 2, nneg // 2
    place, side = me_dp // 2, lax.rem(me_dp, 2)
    me_x, me_core = me_neg // 2, lax.rem(me_neg, 2)
    far, other = 1 - side, 1 - me_core
    partner, mate = 2 * place + far, 2 * me_x + other
    f32, bf16 = jnp.float32, jnp.bfloat16
    greet(ndp, nneg, me_dp, me_neg)
    pending = []

    def go(copy):
        copy.start()
        pending.append(copy)

    def x_of(k):
        return lax.rem(me_x + k, nx)

    def same_core(x):
        return 2 * x + me_core

    def z_of(k):
        return lax.rem(place + k, line)

    def arrived(ref, sem_array, index):
        link(ref, ref, (sem_array, sem_array), index, "neg", mate).wait_recv()

    def store(group, offset, value, dp, hg):
        packed = bufs[group]["packed"]
        pieces = hg // nneg
        for p in range(value.shape[1] // pack_columns):
            part = value[:, p * pack_columns : (p + 1) * pack_columns].astype(bf16)
            part = part.reshape(value.shape[0] // hg, nx, 2, pieces, pack_columns)
            lo = offset + p * pieces
            for core in range(2):
                packed[core, pl.ds(dp, value.shape[0] // hg), :, lo : lo + pieces, :] = part[:, :, core]

    def weight_grad(group, offset, left_ref, right_ref):
        rows, columns = left_ref.shape[1], right_ref.shape[1]
        hg = rows // ndp
        step = 2 * hg

        def body(m, carry):
            left = left_ref[:, pl.ds(pl.multiple_of(m * step, step), step)]
            store(group, offset, contract_rows(left, right_ref[...]), 2 * m, hg)
            return carry

        lax.fori_loop(0, rows // step, body, 0)
        return offset + hg // nneg * (columns // pack_columns)

    def row_loop(count, body):
        step = 256 if count % 256 == 0 else count

        def wrapped(i, carry):
            body(pl.ds(pl.multiple_of(i * step, step), step))
            return carry

        lax.fori_loop(0, count // step, wrapped, 0)

    def embed_stage(t):
        feat, act1, slope1, act2, slope2, emb_ref, grad_ref, second, third = towers[t]
        eg, s2, s1 = scratch[t]

        def body(rows):
            emb, grad = emb_ref[rows, :], grad_ref[rows, :]
            inv_norm = lax.rsqrt(jnp.sum(emb * emb, axis=1, keepdims=True) + 1.0)
            along = jnp.sum(emb * grad, axis=1, keepdims=True)
            value = (inv_norm * grad - inv_norm * inv_norm * inv_norm * emb * along).astype(bf16)
            eg[rows, :] = value
            s2[rows, :] = (contract_cols(value, third[...]) * slope2[rows, :]).astype(bf16)

        row_loop(feat.shape[0], body)

    def second_stage(t, group):
        feat, act1, slope1, act2, slope2, emb_ref, grad_ref, second, third = towers[t]
        eg, s2, s1 = scratch[t]
        offset = weight_grad(group, 0, act2, eg)
        weight_grad(group, offset, act1, s2)

    def slope_stage(t):
        feat, act1, slope1, act2, slope2, emb_ref, grad_ref, second, third = towers[t]
        eg, s2, s1 = scratch[t]
        columns = second.shape[0]

        def body(rows):
            for c in range(0, columns, 512):
                value = contract_cols(s2[rows, :], second[c : c + 512, :]) * slope1[rows, c : c + 512]
                s1[rows, c : c + 512] = value.astype(bf16)

        row_loop(feat.shape[0], body)

    def first_stage(t, group):
        weight_grad(group, 0, towers[t][0], scratch[t][2])

    def stage0(g):
        b = bufs[g]
        go(link(b["packed"].at[other], b["c_in"], (b["cs"], b["cr"]), 0, "neg", mate))

    def base(b, dp, x, lo, hi):
        return b["packed"][me_core, dp, x, lo:hi, :].astype(f32) + b["c_in"][dp, x, lo:hi, :].astype(f32)

    def loop(count, body):
        def wrapped(i, carry):
            body(i)
            return carry

        lax.fori_loop(0, count, wrapped, 0)

    def stage1(g):
        b, (r1, r) = bufs[g], groups[g]
        arrived(b["c_in"], b["cr"], 0)
        for k in range(1, nx):
            x = x_of(k)

            def body(dp):
                b["o1x"][x, dp] = base(b, dp, x, 0, r1).astype(bf16)

            loop(ndp, body)
            go(link(b["o1x"].at[x], b["l1x"].at[me_x], (b["s1x"], b["r1x"]), me_x, "neg", same_core(x), x))

        def body_y(z):
            for x in range(nx):
                b["o1y"][z, x] = base(b, 2 * z + far, x, r1, r).astype(bf16)

        loop(line, body_y)
        go(link(b["o1y"], b["l1y"], (b["s1y"], b["r1y"]), 0, "dp", partner))

    def low(b, dp, r1):
        value = base(b, dp, me_x, 0, r1)
        for k in range(1, nx):
            value = value + b["l1x"][x_of(k), dp].astype(f32)
        return value

    def stage2(g):
        b, (r1, r) = bufs[g], groups[g]
        for k in range(1, nx):
            x = x_of(k)
            arrived(b["l1x"].at[x], b["r1x"], x)

        def body(z):
            b["o2y"][z] = low(b, 2 * z + far, r1).astype(bf16)

        loop(line, body)
        go(link(b["o2y"], b["l2y"], (b["s2y"], b["r2y"]), 0, "dp", partner))
        arrived(b["l1y"], b["r1y"], 0)
        for k in range(1, nx):
            x = x_of(k)

            def body_x(z):
                value = base(b, 2 * z + side, x, r1, r) + b["l1y"][z, x].astype(f32)
                b["o2x"][x, z] = value.astype(bf16)

            loop(line, body_x)
            go(link(b["o2x"].at[x], b["l2x"].at[me_x], (b["s2x"], b["r2x"]), me_x, "neg", same_core(x), x))

    def stage3(g):
        b, (r1, r) = bufs[g], groups[g]
        arrived(b["l2y"], b["r2y"], 0)
        for k in range(1, nx):
            x = x_of(k)
            arrived(b["l2x"].at[x], b["r2x"], x)

        def body(z):
            dp = 2 * z + side
            b["zs"][z, 0:r1, :] = (low(b, dp, r1) + b["l2y"][z].astype(f32)).astype(bf16)
            value = base(b, dp, me_x, r1, r) + b["l1y"][z, me_x].astype(f32)
            for k in range(1, nx):
                value = value + b["l2x"][x_of(k), z].astype(f32)
            b["zs"][z, r1:r, :] = value.astype(bf16)

        loop(line, body)
        for k in range(1, line):
            z = z_of(k)
            go(link(b["zs"].at[z], b["l3"].at[place], (b["s3"], b["r3"]), place, "dp", 2 * z + side, z))

    squares = []

    def stage4(g):
        b = bufs[g]
        for k in range(1, line):
            z = z_of(k)
            arrived(b["l3"].at[z], b["r3"], z)
        value = b["zs"][place].astype(f32)
        for k in range(1, line):
            value = value + b["l3"][z_of(k)].astype(f32)
        squares.append(jnp.sum(value * value))
        b["ag"][me_neg] = value.astype(bf16)
        mine = b["ag"].at[me_neg]
        for k in range(1, nx):
            x = x_of(k)
            go(link(mine, mine, (b["sg"], b["rg"]), me_x, "neg", same_core(x), x))
        go(link(mine, mine, (b["sh"], b["rh"]), me_x, "neg", mate))

    def stage5(g):
        b = bufs[g]
        for k in range(1, nx):
            x = x_of(k)
            ref = b["ag"].at[same_core(x)]
            arrived(ref, b["rg"], x)
            go(link(ref, ref, (b["sh"], b["rh"]), x, "neg", mate))

    def stage6(g):
        b = bufs[g]
        for x in range(nx):
            arrived(b["ag"].at[2 * x + other], b["rh"], x)

    embed_stage(0)
    second_stage(0, 0)
    stage0(0)
    slope_stage(0)
    first_stage(0, 1)
    stage0(1)
    stage1(0)
    embed_stage(1)
    stage1(1)
    second_stage(1, 2)
    stage0(2)
    stage2(0)
    slope_stage(1)
    stage1(2)
    stage2(1)
    first_stage(1, 3)
    stage0(3)
    stage3(0)
    stage1(3)
    stage3(1)
    stage2(2)
    stage4(0)
    stage2(3)
    stage4(1)
    stage3(2)
    stage3(3)
    stage4(2)
    stage4(3)
    total_squares = squares[0] + squares[1] + squares[2] + squares[3]
    lane = lax.broadcasted_iota(jnp.int32, (8, 128), 1)
    stat_dp[...] = jnp.where(lane == 0, total_squares, loss_ref[0])
    stat_copies = share("dp", ndp, me_dp, lambda t: stat_dp, stat_dp_land, ss, sr)
    for g in range(4):
        stage5(g)
    finish(stat_copies)
    total = stat_dp[...]
    for k in range(1, ndp):
        total = total + stat_dp_land[lax.rem(me_dp + k, ndp)]
    stat_neg[...] = total
    stat_copies = share("neg", nneg, me_neg, lambda t: stat_neg, stat_neg_land, ts, tr)
    for g in range(4):
        stage6(g)
    finish(stat_copies)
    total = stat_neg[...]
    for k in range(1, nneg):
        total = total + stat_neg_land[lax.rem(me_neg + k, nneg)]
    stats_ref[...] = total
    clip = clip_norm / jnp.maximum(jnp.sqrt(total[0:1, 0:1]), clip_norm)
    for t in range(2):
        third_out, second_out, first_out = outs[3 * t + 2], outs[3 * t + 1], outs[3 * t]
        for group, out_ref, offset in (
            (2 * t, third_out, 0),
            (2 * t, second_out, third_out.shape[0] // nneg),
            (2 * t + 1, first_out, 0),
        ):
            pieces = out_ref.shape[0] // nneg
            for p in range(out_ref.shape[1] // pack_columns):
                lo = offset + p * pieces
                for n in range(nneg):
                    value = bufs[group]["ag"][n, lo : lo + pieces, :].astype(f32) * clip
                    out_ref[n * pieces : (n + 1) * pieces, p * pack_columns : (p + 1) * pack_columns] = value
    for copy in pending:
        copy.wait_send()


def fused_backward(ndp, nneg, towers, loss_part):
    line, nx = ndp // 2, nneg // 2
    bf16, f32 = jnp.bfloat16, jnp.float32
    groups, outs, scratch, buffers, semaphores = [], [], [], [], []
    for feat, act1, slope1, act2, slope2, emb, grad, second, third in towers:
        rows, fin = feat.shape
        h1, h2, width = act1.shape[1], act2.shape[1], emb.shape[1]
        for height, columns in ((fin, h1), (h1, h2), (h2, width)):
            outs.append(jax.ShapeDtypeStruct((height // ndp, columns), f32))
        both = h2 // (ndp * nneg) * (width // pack_columns) + h1 // (ndp * nneg) * (h2 // pack_columns)
        alone = fin // (ndp * nneg) * (h1 // pack_columns)
        for r in (both, alone):
            groups.append((r * 4 // 9 // 16 * 16, r))
        scratch += [pltpu.VMEM((rows, width), bf16), pltpu.VMEM((rows, h2), bf16), pltpu.VMEM((rows, h1), bf16)]
    for r1, r in groups:
        r2, c = r - r1, pack_columns
        for shape in (
            (2, ndp, nx, r, c), (ndp, nx, r, c), (nx, ndp, r1, c), (nx, ndp, r1, c), (line, nx, r2, c),
            (line, nx, r2, c), (line, r1, c), (line, r1, c), (nx, line, r2, c), (nx, line, r2, c),
            (line, r, c), (line, r, c), (nneg, r, c),
        ):
            buffers.append(pltpu.VMEM(shape, bf16))
        semaphores += sems(1, 1, nx, nx, 1, 1, 1, 1, nx, nx, line, line, nx, nx, nx, nx)
    stat = [pltpu.VMEM((8, 128), f32), pltpu.VMEM((ndp, 8, 128), f32), pltpu.VMEM((8, 128), f32), pltpu.VMEM((nneg, 8, 128), f32)]
    operands = [operand for tower in towers for operand in tower]
    return pl.pallas_call(
        lambda *refs: backward_kernel(ndp, nneg, tuple(groups), *refs),
        out_shape=(jax.ShapeDtypeStruct((8, 128), f32), *outs),
        in_specs=[vmem] * len(operands) + [pl.BlockSpec(memory_space=pltpu.SMEM)],
        out_specs=(vmem,) * 7,
        scratch_shapes=scratch + buffers + stat + semaphores + sems(ndp, ndp, nneg, nneg),
        compiler_params=pltpu.CompilerParams(
            collective_id=1, has_side_effects=True, vmem_limit_bytes=56 * 1024 * 1024
        ),
    )(*operands, loss_part.reshape(1))


def per_device(
    query_features,
    positive_features,
    negative_features,
    positive_ids,
    positive_counts,
    negative_ids,
    negative_counts,
    query_first,
    query_second,
    query_third,
    item_first,
    item_second,
    item_third,
):
    own_rows = query_features.shape[0]
    query_saved, query_unit = tower_forward(query_features, query_first, query_second, query_third)
    item_features = jnp.concatenate([positive_features, negative_features], axis=0)
    item_saved, item_unit = tower_forward(item_features, item_first, item_second, item_third)
    positive_unit = item_unit[:own_rows]
    negative_unit = item_unit[own_rows:]
    ndp, nneg = lax.axis_size("dp"), lax.axis_size("neg")
    width = query_unit.shape[1]
    line, nx = ndp // 2, nneg // 2
    block = negative_unit.shape[0]
    blocks, cuts, lanes = 2 * nneg, 2, min(block, 128)
    bf16, f32, i32 = jnp.bfloat16, jnp.float32, jnp.int32
    positive_logit = jnp.sum(
        query_unit.astype(f32) * positive_unit.astype(f32), axis=1
    ) * inv_temp - jnp.log(positive_counts.astype(f32))
    positive_exp = jnp.exp(positive_logit)
    rows_half = (width // 2, block)
    query_total, denom, negative_sum = call(
        score_kernel,
        0,
        ndp,
        nneg,
        (
            jax.ShapeDtypeStruct((own_rows, width), f32),
            jax.ShapeDtypeStruct((1, own_rows), f32),
            jax.ShapeDtypeStruct((2,) + rows_half, f32),
        ),
        [
            pltpu.VMEM((line, cuts, own_rows // cuts, width), bf16),
            pltpu.VMEM((blocks, 2, block // 2, width), bf16),
            pltpu.VMEM((2, block), i32),
            pltpu.VMEM((blocks, 2, block), i32),
            pltpu.VMEM((blocks, 2, block), f32),
            pltpu.VMEM((1, own_rows), i32),
            pltpu.VMEM((line, 1, own_rows), i32),
            pltpu.VMEM((line, own_rows, lanes), f32),
            pltpu.VMEM((blocks, line, own_rows, block), bf16),
            pltpu.VMEM((line, own_rows, lanes), f32),
            pltpu.VMEM((line, 1, own_rows), f32),
            pltpu.VMEM((line, line, 1, own_rows), f32),
            pltpu.VMEM((width, line * own_rows), bf16),
            pltpu.VMEM((line, own_rows, width), bf16),
            pltpu.VMEM((own_rows, width), f32),
            pltpu.VMEM((line, own_rows, width), bf16),
            pltpu.VMEM((nx, 2, 2) + rows_half, bf16),
            pltpu.VMEM((nx, 2, 2) + rows_half, bf16),
            pltpu.VMEM((nx, 2, 2) + rows_half, f32),
            pltpu.VMEM((nx, 2, 2) + rows_half, bf16),
            pltpu.VMEM((nx, 2) + rows_half, bf16),
            pltpu.VMEM((nx,) + rows_half, bf16),
            pltpu.VMEM(rows_half, bf16),
            pltpu.VMEM((nx,) + rows_half, bf16),
        ]
        + sems(
            3 * nx, 1 + nx, 4 * nx, 4 * nx, 4 * nx, line * cuts, line * cuts, line * cuts,
            blocks, blocks, line, line, line, line, line, line,
            2 * nx, 2 * nx, 2 * nx, 2 * nx, nx, nx, 1, 1, nx, nx,
        ),
        [vmem] * 6,
    )(
        query_unit,
        negative_unit.reshape(2, block // 2, width),
        positive_ids.reshape(nneg, own_rows),
        negative_ids.reshape(ndp, block),
        negative_counts.reshape(ndp, block),
        positive_exp.reshape(1, own_rows),
    )
    own_denom = denom.reshape(-1)
    loss_part = jnp.sum(jnp.log(own_denom) - positive_logit)
    positive_slope = positive_exp / own_denom - 1.0
    query_sum = query_total / own_denom[:, None]
    negative_sum = negative_sum.reshape(width, block).T
    query_grad = (
        query_sum + positive_slope[:, None] * positive_unit.astype(jnp.float32)
    ) * inv_temp
    positive_grad = positive_slope[:, None] * query_unit.astype(jnp.float32) * inv_temp
    item_grad = jnp.concatenate([positive_grad, negative_sum * inv_temp], axis=0)
    heights = (query_first.shape[0], query_second.shape[0], query_third.shape[0])
    if all(height % (16 * ndp * nneg) == 0 for height in heights):
        towers = [
            (features, saved[1], saved[0], saved[3], saved[2], saved[4], grad, second, third)
            for features, saved, grad, second, third in (
                (query_features, query_saved, query_grad, query_second, query_third),
                (item_features, item_saved, item_grad, item_second, item_third),
            )
        ]
        stats, *clipped = fused_backward(ndp, nneg, towers, loss_part)
        return (stats[0, 1] / (own_rows * ndp * nneg), *clipped)
    query_grads = tower_backward(query_features, query_second, query_third, query_saved, query_grad)
    item_grads = tower_backward(item_features, item_second, item_third, item_saved, item_grad)
    gradients = query_grads + item_grads
    parts = [part for gradient in gradients for part in to_packed(gradient, ndp)]
    packed = jnp.concatenate(parts, axis=1)
    rows = packed.shape[1] // nneg
    packed = packed.reshape(ndp, nneg, 2, rows // 2, pack_columns).transpose(1, 0, 2, 3, 4)
    piece = (rows // 2, pack_columns)
    gathered, stats = call(
        weight_kernel,
        3,
        ndp,
        nneg,
        (jax.ShapeDtypeStruct((nneg, 2) + piece, bf16), jax.ShapeDtypeStruct((8, 128), f32)),
        [
            pltpu.VMEM((nx, ndp, 2) + piece, bf16),
            pltpu.VMEM((nx, 2, line) + piece, bf16),
            pltpu.VMEM((2, nx, line) + piece, bf16),
            pltpu.VMEM((nx, 2, line) + piece, bf16),
            pltpu.VMEM((nx, line) + piece, bf16),
            pltpu.VMEM((2, line) + piece, bf16),
            pltpu.VMEM((nx, line) + piece, bf16),
            pltpu.VMEM((line,) + piece, bf16),
            pltpu.VMEM((nx, line) + piece, bf16),
            pltpu.VMEM((2, line) + piece, bf16),
            pltpu.VMEM((2, line) + piece, bf16),
            pltpu.VMEM((8, 128), f32),
            pltpu.VMEM((ndp, 8, 128), f32),
            pltpu.VMEM((8, 128), f32),
            pltpu.VMEM((nneg, 8, 128), f32),
        ]
        + sems(nx, nx, 2 * nx, 2 * nx, 2, 2, ndp, ndp, ndp, ndp, nneg, nneg, nx, nx, nx, nx),
        [vmem, pl.BlockSpec(memory_space=pltpu.SMEM)],
    )(packed, loss_part.reshape(1))
    grad_norm = jnp.sqrt(stats[0, 0])
    mean_loss = stats[0, 1] / (own_rows * ndp * nneg)
    clip_factor = clip_norm / jnp.maximum(grad_norm, clip_norm)
    flat = gathered.reshape(nneg * rows, pack_columns)
    clipped = []
    start = 0
    for gradient in gradients:
        height, columns = gradient.shape[0] // ndp, gradient.shape[1]
        groups = columns // pack_columns
        blocks = [flat[start + g * height : start + (g + 1) * height] for g in range(groups)]
        start += groups * height
        clipped.append(jnp.concatenate(blocks, axis=1).astype(jnp.float32) * clip_factor)
    return (mean_loss, *clipped)


def solution(mesh):
    placed = (
        P(("dp", "neg"), None),
        P(("dp", "neg"), None),
        P(("neg", "dp"), None),
        P("dp"),
        P(("dp", "neg")),
        P("neg"),
        P("neg"),
        P(),
        P(),
        P(),
        P(),
        P(),
        P(),
    )
    return jax.shard_map(
        per_device,
        mesh=mesh,
        in_specs=placed,
        out_specs=(
            P(),
            P("dp", None),
            P("dp", None),
            P("dp", None),
            P("dp", None),
            P("dp", None),
            P("dp", None),
        ),
        check_vma=False,
    )
```

```python
import functools

import jax
import jax.numpy as jnp
from jax import lax
from jax.experimental import pallas as pl
from jax.experimental.pallas import tpu as pltpu
from jax.sharding import PartitionSpec as P

inv_temp = 20.0
log2_e = 1.4426950408889634
clip_norm = 256.0


def silu_slope(pre):
    sigma = jax.nn.sigmoid(pre)
    return sigma * (1.0 + pre * (1.0 - sigma))


def contract_rows(left, right):
    return lax.dot_general(
        left, right, (((0,), (0,)), ((), ())), preferred_element_type=jnp.float32
    )


def contract_cols(left, right):
    return lax.dot_general(
        left, right, (((1,), (1,)), ((), ())), preferred_element_type=jnp.float32
    )


def tower_forward(features, first, second, third):
    first_pre = jnp.dot(features, first, preferred_element_type=jnp.float32)
    first_act = jax.nn.silu(first_pre).astype(jnp.bfloat16)
    second_pre = jnp.dot(first_act, second, preferred_element_type=jnp.float32)
    second_act = jax.nn.silu(second_pre).astype(jnp.bfloat16)
    embedding = jnp.dot(second_act, third, preferred_element_type=jnp.float32)
    inv_norm = lax.rsqrt(jnp.sum(embedding * embedding, axis=1, keepdims=True) + 1.0)
    unit = (embedding * inv_norm).astype(jnp.bfloat16)
    saved = (silu_slope(first_pre), first_act, silu_slope(second_pre), second_act, embedding, inv_norm)
    return saved, unit


def tower_backward(features, second, third, saved, unit_grad):
    first_slope, first_act, second_slope, second_act, embedding, inv_norm = saved
    along = jnp.sum(embedding * unit_grad, axis=1, keepdims=True)
    embed_grad = (inv_norm * unit_grad - inv_norm * inv_norm * inv_norm * embedding * along).astype(
        jnp.bfloat16
    )
    third_grad = contract_rows(second_act, embed_grad)
    second_step = (contract_cols(embed_grad, third) * second_slope).astype(jnp.bfloat16)
    second_grad = contract_rows(first_act, second_step)
    first_step = (contract_cols(second_step, second) * first_slope).astype(jnp.bfloat16)
    first_grad = contract_rows(features, first_step)
    return (first_grad, second_grad, third_grad)


pack_columns = 256
vmem = pl.BlockSpec(memory_space=pltpu.VMEM)


def greet(ndp, nneg, me_dp, me_neg):
    barrier = pltpu.get_barrier_semaphore()
    for k in range(1, nneg):
        pl.semaphore_signal(
            barrier, inc=1, device_id={"neg": lax.rem(me_neg + k, nneg)}, device_id_type=pl.DeviceIdType.MESH
        )
    for k in range(1, ndp):
        pl.semaphore_signal(
            barrier, inc=1, device_id={"dp": lax.rem(me_dp + k, ndp)}, device_id_type=pl.DeviceIdType.MESH
        )
    pl.semaphore_wait(barrier, (nneg - 1) + (ndp - 1))


def send(src, dst, send_sem, recv_sem, axis, target):
    copy = pltpu.make_async_remote_copy(
        src_ref=src,
        dst_ref=dst,
        send_sem=send_sem,
        recv_sem=recv_sem,
        device_id={axis: target},
        device_id_type=pl.DeviceIdType.MESH,
    )
    copy.start()
    return copy


def share(axis, n, me, src_of, dst, send_sem, recv_sem):
    return [
        send(src_of(lax.rem(me + k, n)), dst.at[me], send_sem.at[k], recv_sem.at[k], axis, lax.rem(me + k, n))
        for k in range(1, n)
    ]


def finish(copies):
    for copy in copies:
        copy.wait()


def link(src, dst, sems, index, axis, target, send_index=None):
    send_sems, recv_sems = sems
    return pltpu.make_async_remote_copy(
        src_ref=src,
        dst_ref=dst,
        send_sem=send_sems.at[index if send_index is None else send_index],
        recv_sem=recv_sems.at[index],
        device_id={axis: target},
        device_id_type=pl.DeviceIdType.MESH,
    )


def score_kernel(
    ndp, nneg, query_ref, negative_ref, pid_ref, nid_ref, count_ref, pexp_ref, sum_ref, denom_ref, nsum_ref,
    q_land, n_land, meta_out, meta, rows, pid_out, pid_land, pid_col, w, den, dpart, dland, scaled,
    q_out, q_part, q_in, c_out, c_in, own, out, lx, ly, l2y, l2x,
    sx, sy, rn, sm, rm, sr, sl, rq, s_meta, r_meta, s_pid, r_pid, sd, rd, sq, rqs,
    sc, rc, s1x, r1x, s1y, r1y, s2y, r2y, s2x, r2x,
):
    me_dp, me_neg = lax.axis_index("dp"), lax.axis_index("neg")
    line, nx = ndp // 2, nneg // 2
    place, side = me_dp // 2, lax.rem(me_dp, 2)
    me_x, me_core = me_neg // 2, lax.rem(me_neg, 2)
    far, other = 1 - side, 1 - me_core
    partner, mate = 2 * place + far, 2 * me_x + other
    rows_q, width = query_ref.shape
    block = 2 * negative_ref.shape[1]
    lanes = den.shape[2]
    cuts = q_land.shape[1]
    half_w = width // 2
    blocks = nneg * 2
    here = (me_x * 2 + side) * 2 + me_core

    def along(k):
        return lax.rem(me_x + k, nx)

    def at_place(z):
        return 2 * z + side

    barrier = pltpu.get_barrier_semaphore()
    for k in range(1, line):
        pl.semaphore_signal(
            barrier, inc=1, device_id={"dp": at_place(lax.rem(place + k, line))}, device_id_type=pl.DeviceIdType.MESH
        )

    def quad(k):
        b = lax.rem(here + k, blocks)
        return {"dp": 2 * place + lax.rem(b // 2, 2), "neg": 2 * (b // 4) + lax.rem(b, 2)}

    for k in range(1, blocks):
        pl.semaphore_signal(barrier, inc=1, device_id=quad(k), device_id_type=pl.DeviceIdType.MESH)
    def own_ids(ref, index, count):
        if count % 128 == 0:
            return ref[:, pl.ds(pl.multiple_of(index * count, count), count)]
        return ref[pl.ds(index, 1), :]

    meta_out[0:1, :] = own_ids(nid_ref, me_dp, block)
    meta_out[1:2, :] = own_ids(count_ref, me_dp, block)
    pid_out[...] = own_ids(pid_ref, me_neg, rows_q)
    pl.semaphore_wait(barrier, (line - 1) + (blocks - 1))

    def slot(x, y, half):
        return (x * 2 + y) * 2 + half

    def piece(x, y, half):
        return n_land.at[(x * 2 + y) * 2 + me_core, half]

    def push(src, x, y, half, send_sems, index, axis, target):
        return link(src, piece(x, y, half), (send_sems, rn), slot(x, y, half), axis, target, index)

    def relay(src, x, y, half):
        i = slot(x, y, half)
        return link(src, piece(x, y, half), (sm, rm), i, "neg", mate)

    def landed(x, y, half):
        ref = piece(x, y, half)
        link(ref, ref, (sy, rn), slot(x, y, half), "neg", mate, 0).wait_recv()

    sends = []

    def go(copy):
        copy.start()
        sends.append(copy)

    def to_x(src, x, y, half, kind):
        for k in range(1, nx):
            go(push(src, x, y, half, sx, kind * nx + k, "neg", 2 * along(k) + me_core))

    def to_y(src, x, y, half, index):
        go(push(src, x, y, half, sy, index, "dp", partner))

    first, second = negative_ref.at[0], negative_ref.at[1]
    to_x(first, me_x, side, 0, 0)
    to_y(second, me_x, side, 1, 0)
    to_x(second, me_x, side, 1, 1)
    to_y(first, me_x, side, 0, 1)
    go(relay(first, me_x, side, 0))
    go(relay(second, me_x, side, 1))

    def chain(slot_z, j, distance, sems, target):
        src = query_ref.at[pl.ds(j * (rows_q // cuts), rows_q // cuts)] if distance == 0 else q_land.at[slot_z, j]
        return link(src, q_land.at[slot_z, j], (sems, rq), slot_z * cuts + j, "dp", target, distance * cuts + j)

    def right(distance, j):
        return chain(place - distance, j, distance, sr, at_place(lax.rem(place + 1, line)))

    def left(distance, j):
        return chain(place + distance, j, distance, sl, at_place(lax.rem(place + line - 1, line)))

    goes_right, goes_left = place < line - 1, place > 0
    for j in range(cuts):
        pl.when(goes_right)(lambda j=j: right(0, j).start())
        pl.when(goes_left)(lambda j=j: left(0, j).start())
    for k in range(1, blocks):
        b = lax.rem(here + k, blocks)
        copy = pltpu.make_async_remote_copy(
            src_ref=meta_out, dst_ref=meta.at[here], send_sem=s_meta.at[k], recv_sem=r_meta.at[here],
            device_id=quad(k), device_id_type=pl.DeviceIdType.MESH,
        )
        go(copy)
    for k in range(1, line):
        z = lax.rem(place + k, line)
        go(link(pid_out, pid_land.at[place], (s_pid, r_pid), place, "dp", at_place(z), k))
    n_land[here] = negative_ref[...]
    for j in range(cuts):
        q_land[place, j] = query_ref[pl.ds(j * (rows_q // cuts), rows_q // cuts), :]
    meta[here] = meta_out[...]
    pid_land[place] = pid_out[...]

    for k in range(1, nx):
        x = along(k)
        landed(x, side, 0)
        to_y(piece(x, side, 0), x, side, 0, 1 + k)
        go(relay(piece(x, side, 0), x, side, 0))
    landed(me_x, far, 1)
    to_x(piece(me_x, far, 1), me_x, far, 1, 2)
    go(relay(piece(me_x, far, 1), me_x, far, 1))

    def q_step(distance):
        for j in range(cuts):

            @pl.when(place >= distance)
            def _():
                ref = q_land.at[place - distance, j]
                link(ref, ref, (sr, rq), (place - distance) * cuts + j, "dp", partner, 0).wait_recv()
                pl.when(goes_right)(lambda: right(distance, j).start())

            @pl.when(place + distance < line)
            def _():
                ref = q_land.at[place + distance, j]
                link(ref, ref, (sl, rq), (place + distance) * cuts + j, "dp", partner, 0).wait_recv()
                pl.when(goes_left)(lambda: left(distance, j).start())

    q_step(1)
    for k in range(1, nx):
        x = along(k)
        landed(x, side, 1)
        go(relay(piece(x, side, 1), x, side, 1))
    landed(me_x, far, 0)
    go(relay(piece(me_x, far, 0), me_x, far, 0))
    for distance in range(2, line):
        q_step(distance)
    for half in range(2):
        for k in range(1, nx):
            x = along(k)
            landed(x, far, half)
            go(relay(piece(x, far, half), x, far, half))
    for x in range(nx):
        for y in range(2):
            for half in range(2):
                i = slot(x, y, half)
                ref = n_land.at[(x * 2 + y) * 2 + other, half]
                link(ref, ref, (sm, rm), i, "neg", mate).wait_recv()
    for k in range(1, blocks):
        b = lax.rem(here + k, blocks)
        link(meta.at[b], meta.at[b], (s_meta, r_meta), b, "neg", mate).wait_recv()
    for k in range(1, line):
        z = lax.rem(place + k, line)
        link(pid_land.at[z], pid_land.at[z], (s_pid, r_pid), z, "dp", partner).wait_recv()

    for b in range(blocks):
        rows[b, 0:1, :] = meta[b, 0:1, :].astype(jnp.float32)
        rows[b, 1:2, :] = jnp.log2(meta[b, 1:2, :].astype(jnp.float32))
    for z in range(line):
        pid_col[z] = jnp.broadcast_to(pid_land[z].astype(jnp.float32), (lanes, rows_q)).T
        den[z] = jnp.zeros((rows_q, lanes), jnp.float32)

    def unit(b, z):
        dots = contract_cols(q_land[z].reshape(rows_q, width), n_land[b].reshape(block, width))
        value = jnp.exp2(dots * (inv_temp * log2_e) - rows[b, 1:2, :])
        ids = jnp.concatenate([pid_col[z]] * (block // lanes), axis=1)
        value = jnp.where(ids != rows[b, 0:1, :], value, 0.0)
        w[b, z] = value.astype(jnp.bfloat16)
        total = den[z]
        for c in range(0, block, lanes):
            total = total + value[:, c : c + lanes]
        den[z] = total

    def units(b, carry):
        for z in range(line):
            unit(b, z)
        return carry

    lax.fori_loop(0, blocks, units, 0)
    for z in range(line):
        dpart[z] = jnp.sum(den[z].T, axis=0, keepdims=True)
    dpart[place] = dpart[place] + pexp_ref[...]
    for k in range(1, line):
        z = lax.rem(place + k, line)
        go(link(dpart, dland.at[place], (sd, rd), place, "dp", at_place(z), k))

    def q_block(z):
        if block % 128 == 0:
            left_side = jnp.concatenate([w[b, z] for b in range(blocks)], axis=1)
            return jnp.dot(
                left_side, n_land[...].reshape(blocks * block, width), preferred_element_type=jnp.float32
            )
        total = jnp.zeros((rows_q, width), jnp.float32)
        for b in range(blocks):
            total = total + jnp.dot(w[b, z], n_land[b].reshape(block, width), preferred_element_type=jnp.float32)
        return total

    def q_send(k, z):
        return link(q_out.at[z], q_in.at[place], (sq, rqs), place, "dp", at_place(z), k)

    def q_push(k, carry):
        z = lax.rem(place + k, line)
        q_out[z] = q_block(z).astype(jnp.bfloat16)
        q_send(k, z).start()
        return carry

    lax.fori_loop(1, line, q_push, 0)
    q_part[...] = q_block(place)
    total = dpart[...]
    for k in range(1, line):
        z = lax.rem(place + k, line)
        link(dland.at[z], dland.at[z], (sd, rd), z, "dp", partner).wait_recv()
        total = total + dland[z]
    dpart2 = 1.0 / total
    for z in range(line):
        q_t = q_land[z].reshape(rows_q, width).astype(jnp.float32).T
        scaled[:, z * rows_q : (z + 1) * rows_q] = (q_t * dpart2[z]).astype(jnp.bfloat16)
    denom_ref[...] = dpart[place]
    for k in range(1, line):
        denom_ref[...] = denom_ref[...] + dland[lax.rem(place + k, line), place]

    def dest(i):
        x = lax.rem(me_x + 1 + i // 2, nx)
        y = lax.rem(side + 1 + lax.rem(i, 2), 2)
        return x, y

    def part(x, y, core):
        return jnp.dot(
            scaled[...], w[(x * 2 + y) * 2 + core].reshape(line * rows_q, block), preferred_element_type=jnp.float32
        )

    def c_send(i):
        x, y = dest(i)
        return link(c_out.at[x, y], c_in.at[x, y], (sc, rc), x * 2 + y, "neg", mate)

    def far_step(i, carry):
        x, y = dest(i)
        c_out[x, y] = part(x, y, other).astype(jnp.bfloat16).reshape(2, half_w, block)
        c_send(i).start()
        return carry

    def send_1x(i):
        x, y = dest(i)
        return link(out.at[x, y, 0], lx.at[me_x, y], (s1x, r1x), me_x * 2 + y, "neg", 2 * x + me_core, x * 2 + y)

    def send_1y(i):
        x, y = dest(i)
        return link(out.at[x, y, 1], ly.at[x], (s1y, r1y), x, "dp", partner)

    def own_step(i, carry):
        x, y = dest(i)
        value = part(x, y, me_core).reshape(2, half_w, block)
        link(c_in.at[x, y], c_in.at[x, y], (sc, rc), x * 2 + y, "neg", mate).wait_recv()
        value = value + c_in[x, y].astype(jnp.float32)
        own[x, y] = value

        @pl.when(i < 2 * (nx - 1))
        def _():
            out[x, y, 0] = value[0].astype(jnp.bfloat16)
            send_1x(i).start()

        @pl.when(lax.rem(i, 2) == 0)
        def _():
            out[x, y, 1] = value[1].astype(jnp.bfloat16)
            send_1y(i).start()

        return carry

    lax.fori_loop(0, 2 * nx, far_step, 0)
    lax.fori_loop(0, 2 * nx, own_step, 0)
    value = own[me_x, far, 0]
    for k in range(1, nx):
        x = along(k)
        ref = lx.at[x, far]
        link(ref, ref, (s1x, r1x), x * 2 + far, "neg", mate).wait_recv()
        value = value + lx[x, far].astype(jnp.float32)
    out[me_x, far, 0] = value.astype(jnp.bfloat16)
    go(link(out.at[me_x, far, 0], l2y, (s2y, r2y), 0, "dp", partner))
    for k in range(1, nx):
        x = along(k)
        link(ly.at[x], ly.at[x], (s1y, r1y), x, "dp", partner).wait_recv()
        out[x, side, 1] = (own[x, side, 1] + ly[x].astype(jnp.float32)).astype(jnp.bfloat16)
        go(link(out.at[x, side, 1], l2x.at[me_x], (s2x, r2x), me_x, "neg", 2 * x + me_core, x))
    result = q_part[...]
    for k in range(1, line):
        z = lax.rem(place + k, line)
        link(q_in.at[z], q_in.at[z], (sq, rqs), z, "dp", partner).wait_recv()
        result = result + q_in[z].astype(jnp.float32)
    sum_ref[...] = result
    low = own[me_x, side, 0]
    for k in range(1, nx):
        x = along(k)
        ref = lx.at[x, side]
        link(ref, ref, (s1x, r1x), x * 2 + side, "neg", mate).wait_recv()
        low = low + lx[x, side].astype(jnp.float32)
    link(ly.at[me_x], ly.at[me_x], (s1y, r1y), me_x, "dp", partner).wait_recv()
    high = own[me_x, side, 1] + ly[me_x].astype(jnp.float32)
    link(l2y, l2y, (s2y, r2y), 0, "dp", partner).wait_recv()
    nsum_ref[0] = low + l2y[...].astype(jnp.float32)
    for k in range(1, nx):
        x = along(k)
        link(l2x.at[x], l2x.at[x], (s2x, r2x), x, "neg", mate).wait_recv()
        high = high + l2x[x].astype(jnp.float32)
    nsum_ref[1] = high

    for copy in sends:
        copy.wait_send()
    for distance in range(line):
        for j in range(cuts):
            if distance < line - 1:
                pl.when((place >= distance) & goes_right)(lambda: right(distance, j).wait_send())
                pl.when((place + distance < line) & goes_left)(lambda: left(distance, j).wait_send())
    for k in range(1, line):
        q_send(k, lax.rem(place + k, line)).wait_send()
    for i in range(2 * nx):
        c_send(i).wait_send()
        if i < 2 * (nx - 1):
            send_1x(i).wait_send()
        if i % 2 == 0:
            send_1y(i).wait_send()


def weight_kernel(
    ndp, nneg, packed_ref, loss_ref, gathered_ref, stats_ref,
    core_land, sum_a, sum_b, land_a, land_b, half_a, half_b, last_a, last_b, line_sum, line_land,
    stat_dp, stat_dp_land, stat_neg, stat_neg_land,
    cs, cr, xs, xr, ys, yr, ps, pr, ss, sr, ts, tr, gs, gr, hs, hr,
):
    me_dp, me_neg = lax.axis_index("dp"), lax.axis_index("neg")
    nx, line = nneg // 2, ndp // 2
    me_x, me_core = me_neg // 2, lax.rem(me_neg, 2)
    place, side = me_dp // 2, lax.rem(me_dp, 2)
    other, far = 1 - me_core, 1 - side
    mate, partner = 2 * me_x + other, 2 * place + far
    greet(ndp, nneg, me_dp, me_neg)
    turn = list(range(1, nx)) + [0]

    def x_of(k):
        return lax.rem(me_x + k, nx)

    core = {}
    for k in turn:
        x = x_of(k)
        core[k] = send(packed_ref.at[2 * x + other], core_land.at[x], cs.at[k], cr.at[k], "neg", mate)

    def add_core(x, y, half, target):
        def body(z, carry):
            target[z] = (
                packed_ref[2 * x + me_core, 2 * z + y, half].astype(jnp.float32)
                + core_land[x, 2 * z + y, half].astype(jnp.float32)
            ).astype(jnp.bfloat16)
            return carry

        lax.fori_loop(0, line, body, 0)

    def add(target, *terms):
        def body(z, carry):
            value = terms[0][z].astype(jnp.float32)
            for term in terms[1:]:
                value = value + term[z].astype(jnp.float32)
            target[z] = value.astype(jnp.bfloat16)
            return carry

        lax.fori_loop(0, line, body, 0)

    first_a = []
    for k in turn:
        x = x_of(k)
        core[k].wait_recv()
        if k:
            for y in range(2):
                add_core(x, y, 0, sum_a.at[x, y])
            first_a.append(send(sum_a.at[x], land_a.at[k], xs.at[k], xr.at[k], "neg", 2 * x + me_core))
        add_core(x, far, 1, sum_b.at[far, x])
    first_b = send(sum_b.at[far], land_b, ys.at[0], yr.at[0], "dp", partner)
    for y in range(2):
        add_core(me_x, y, 0, sum_a.at[me_x, y])
    for k in range(nx):
        add_core(x_of(k), side, 1, sum_b.at[side, x_of(k)])
    for copy in first_a:
        copy.wait_recv()
    add(half_a.at[far], sum_a.at[me_x, far], *[land_a.at[k, far] for k in range(1, nx)])
    second_a = send(half_a.at[far], last_a, ys.at[1], yr.at[1], "dp", partner)
    first_b.wait_recv()
    second_b = []
    for k in turn:
        x = x_of(k)
        add(half_b.at[x], sum_b.at[side, x], land_b.at[x])
        if k:
            second_b.append(
                send(half_b.at[x], last_b.at[k], xs.at[nx + k], xr.at[nx + k], "neg", 2 * x + me_core)
            )
    add(half_a.at[side], sum_a.at[me_x, side], *[land_a.at[k, side] for k in range(1, nx)])
    second_a.wait_recv()
    add(line_sum.at[0], half_a.at[side], last_a)
    third = []
    for half in range(2):
        if half:
            for copy in second_b:
                copy.wait_recv()
            add(line_sum.at[1], half_b.at[me_x], *[last_b.at[k] for k in range(1, nx)])
        for k in range(1, line):
            z = lax.rem(place + k, line)
            third.append(
                send(line_sum.at[half, z], line_land.at[half, k], ps.at[half * line + k], pr.at[half * line + k], "dp", 2 * z + side)
            )
    for copy in third:
        copy.wait_recv()
    squares = jnp.zeros((), jnp.float32)
    for half in range(2):
        piece = line_sum[half, place].astype(jnp.float32)
        for k in range(1, line):
            piece = piece + line_land[half, k].astype(jnp.float32)
        gathered_ref[me_neg, half] = piece.astype(jnp.bfloat16)
        squares = squares + jnp.sum(piece * piece)
    lane = lax.broadcasted_iota(jnp.int32, (8, 128), 1)
    stat_dp[...] = jnp.where(lane == 0, squares, loss_ref[0])
    stat_copies = share("dp", ndp, me_dp, lambda t: stat_dp, stat_dp_land, ss, sr)
    mine = gathered_ref.at[me_neg]
    spread = [send(mine, mine, gs.at[k], gr.at[k], "neg", 2 * x_of(k) + me_core) for k in range(1, nx)]
    spread.append(send(mine, mine, gs.at[0], gr.at[0], "neg", mate))
    finish(stat_copies)
    total = stat_dp[...]
    for k in range(1, ndp):
        total = total + stat_dp_land[lax.rem(me_dp + k, ndp)]
    stat_neg[...] = total
    stat_copies = share("neg", nneg, me_neg, lambda t: stat_neg, stat_neg_land, ts, tr)
    relay = []
    for k in range(1, nx):
        spread[k - 1].wait_recv()
        x = lax.rem(me_x + nx - k, nx)
        came = gathered_ref.at[2 * x + me_core]
        relay.append(send(came, came, hs.at[k], hr.at[k], "neg", mate))
    finish(stat_copies)
    total = stat_neg[...]
    for k in range(1, nneg):
        total = total + stat_neg_land[lax.rem(me_neg + k, nneg)]
    stats_ref[...] = total
    spread[-1].wait_recv()
    finish(relay)
    for copy in [*core.values(), *first_a, first_b, second_a, *second_b, *third, *spread]:
        copy.wait_send()


def call(kernel, collective, ndp, nneg, out_shape, scratch, in_specs, megabytes=48):
    return pl.pallas_call(
        functools.partial(kernel, ndp, nneg),
        out_shape=out_shape,
        in_specs=in_specs,
        out_specs=tuple(vmem for _ in out_shape),
        scratch_shapes=scratch,
        compiler_params=pltpu.CompilerParams(
            collective_id=collective, has_side_effects=True, vmem_limit_bytes=megabytes * 1024 * 1024
        ),
    )


def sems(*counts):
    return [pltpu.SemaphoreType.DMA((count,)) for count in counts]


def to_packed(gradient, ndp):
    rows, columns = gradient.shape
    blocks = gradient.astype(jnp.bfloat16).reshape(ndp, rows // ndp, columns)
    return [blocks[:, :, c : c + pack_columns] for c in range(0, columns, pack_columns)]


def backward_kernel(ndp, nneg, groups, *refs):
    refs = list(refs)
    take = iter(refs)
    towers = [[next(take) for _ in range(9)] for _ in range(2)]
    loss_ref = next(take)
    stats_ref = next(take)
    gathered = [next(take) for _ in groups]
    scratch = [[next(take) for _ in range(3)] for _ in range(2)]
    names = ["packed", "c_in", "o1x", "l1x", "o1y", "l1y", "o2y", "l2y", "o2x", "l2x", "zs", "l3"]
    bufs = [{name: next(take) for name in names} for _ in groups]
    for buf, ref in zip(bufs, gathered):
        buf["ag"] = ref
    stat_dp, stat_dp_land, stat_neg, stat_neg_land = [next(take) for _ in range(4)]
    sem_names = ["cs", "cr", "s1x", "r1x", "s1y", "r1y", "s2y", "r2y", "s2x", "r2x", "s3", "r3", "sg", "rg", "sh", "rh"]
    for buf in bufs:
        for name in sem_names:
            buf[name] = next(take)
    ss, sr, ts, tr = [next(take) for _ in range(4)]

    me_dp, me_neg = lax.axis_index("dp"), lax.axis_index("neg")
    line, nx = ndp // 2, nneg // 2
    place, side = me_dp // 2, lax.rem(me_dp, 2)
    me_x, me_core = me_neg // 2, lax.rem(me_neg, 2)
    far, other = 1 - side, 1 - me_core
    partner, mate = 2 * place + far, 2 * me_x + other
    f32, bf16 = jnp.float32, jnp.bfloat16
    greet(ndp, nneg, me_dp, me_neg)
    pending = []

    def go(copy):
        copy.start()
        pending.append(copy)

    def x_of(k):
        return lax.rem(me_x + k, nx)

    def same_core(x):
        return 2 * x + me_core

    def z_of(k):
        return lax.rem(place + k, line)

    def arrived(ref, sem_array, index):
        link(ref, ref, (sem_array, sem_array), index, "neg", mate).wait_recv()

    def store(group, offset, value, dp, hg):
        packed = bufs[group]["packed"]
        pieces = hg // nneg
        for p in range(value.shape[1] // pack_columns):
            part = value[:, p * pack_columns : (p + 1) * pack_columns].astype(bf16)
            part = part.reshape(value.shape[0] // hg, nx, 2, pieces, pack_columns)
            lo = offset + p * pieces
            for core in range(2):
                packed[core, pl.ds(dp, value.shape[0] // hg), :, lo : lo + pieces, :] = part[:, :, core]

    def weight_grad(group, offset, left_ref, right_ref):
        rows, columns = left_ref.shape[1], right_ref.shape[1]
        hg = rows // ndp
        step = 2 * hg

        def body(m, carry):
            left = left_ref[:, pl.ds(pl.multiple_of(m * step, step), step)]
            store(group, offset, contract_rows(left, right_ref[...]), 2 * m, hg)
            return carry

        lax.fori_loop(0, rows // step, body, 0)
        return offset + hg // nneg * (columns // pack_columns)

    def row_loop(count, body):
        step = 256 if count % 256 == 0 else count

        def wrapped(i, carry):
            body(pl.ds(pl.multiple_of(i * step, step), step))
            return carry

        lax.fori_loop(0, count // step, wrapped, 0)

    def embed_stage(t):
        feat, act1, slope1, act2, slope2, emb_ref, grad_ref, second, third = towers[t]
        eg, s2, s1 = scratch[t]

        def body(rows):
            emb, grad = emb_ref[rows, :], grad_ref[rows, :]
            inv_norm = lax.rsqrt(jnp.sum(emb * emb, axis=1, keepdims=True) + 1.0)
            along = jnp.sum(emb * grad, axis=1, keepdims=True)
            value = (inv_norm * grad - inv_norm * inv_norm * inv_norm * emb * along).astype(bf16)
            eg[rows, :] = value
            s2[rows, :] = (contract_cols(value, third[...]) * slope2[rows, :]).astype(bf16)

        row_loop(feat.shape[0], body)

    def second_stage(t, group):
        feat, act1, slope1, act2, slope2, emb_ref, grad_ref, second, third = towers[t]
        eg, s2, s1 = scratch[t]
        offset = weight_grad(group, 0, act2, eg)
        weight_grad(group, offset, act1, s2)

    def slope_stage(t):
        feat, act1, slope1, act2, slope2, emb_ref, grad_ref, second, third = towers[t]
        eg, s2, s1 = scratch[t]
        columns = second.shape[0]

        def body(rows):
            for c in range(0, columns, 512):
                value = contract_cols(s2[rows, :], second[c : c + 512, :]) * slope1[rows, c : c + 512]
                s1[rows, c : c + 512] = value.astype(bf16)

        row_loop(feat.shape[0], body)

    def first_stage(t, group):
        weight_grad(group, 0, towers[t][0], scratch[t][2])

    def stage0(g):
        b = bufs[g]
        go(link(b["packed"].at[other], b["c_in"], (b["cs"], b["cr"]), 0, "neg", mate))

    def base(b, dp, x, lo, hi):
        return b["packed"][me_core, dp, x, lo:hi, :].astype(f32) + b["c_in"][dp, x, lo:hi, :].astype(f32)

    def loop(count, body):
        def wrapped(i, carry):
            body(i)
            return carry

        lax.fori_loop(0, count, wrapped, 0)

    def stage1(g):
        b, (r1, r) = bufs[g], groups[g]
        arrived(b["c_in"], b["cr"], 0)
        for k in range(1, nx):
            x = x_of(k)

            def body(dp):
                b["o1x"][x, dp] = base(b, dp, x, 0, r1).astype(bf16)

            loop(ndp, body)
            go(link(b["o1x"].at[x], b["l1x"].at[me_x], (b["s1x"], b["r1x"]), me_x, "neg", same_core(x), x))

        def body_y(z):
            for x in range(nx):
                b["o1y"][z, x] = base(b, 2 * z + far, x, r1, r).astype(bf16)

        loop(line, body_y)
        go(link(b["o1y"], b["l1y"], (b["s1y"], b["r1y"]), 0, "dp", partner))

    def low(b, dp, r1):
        value = base(b, dp, me_x, 0, r1)
        for k in range(1, nx):
            value = value + b["l1x"][x_of(k), dp].astype(f32)
        return value

    def stage2(g):
        b, (r1, r) = bufs[g], groups[g]
        for k in range(1, nx):
            x = x_of(k)
            arrived(b["l1x"].at[x], b["r1x"], x)

        def body(z):
            b["o2y"][z] = low(b, 2 * z + far, r1).astype(bf16)

        loop(line, body)
        go(link(b["o2y"], b["l2y"], (b["s2y"], b["r2y"]), 0, "dp", partner))
        arrived(b["l1y"], b["r1y"], 0)
        for k in range(1, nx):
            x = x_of(k)

            def body_x(z):
                value = base(b, 2 * z + side, x, r1, r) + b["l1y"][z, x].astype(f32)
                b["o2x"][x, z] = value.astype(bf16)

            loop(line, body_x)
            go(link(b["o2x"].at[x], b["l2x"].at[me_x], (b["s2x"], b["r2x"]), me_x, "neg", same_core(x), x))

    def stage3(g):
        b, (r1, r) = bufs[g], groups[g]
        arrived(b["l2y"], b["r2y"], 0)
        for k in range(1, nx):
            x = x_of(k)
            arrived(b["l2x"].at[x], b["r2x"], x)

        def body(z):
            dp = 2 * z + side
            b["zs"][z, 0:r1, :] = (low(b, dp, r1) + b["l2y"][z].astype(f32)).astype(bf16)
            value = base(b, dp, me_x, r1, r) + b["l1y"][z, me_x].astype(f32)
            for k in range(1, nx):
                value = value + b["l2x"][x_of(k), z].astype(f32)
            b["zs"][z, r1:r, :] = value.astype(bf16)

        loop(line, body)
        for k in range(1, line):
            z = z_of(k)
            go(link(b["zs"].at[z], b["l3"].at[place], (b["s3"], b["r3"]), place, "dp", 2 * z + side, z))

    squares = []

    def stage4(g):
        b = bufs[g]
        for k in range(1, line):
            z = z_of(k)
            arrived(b["l3"].at[z], b["r3"], z)
        value = b["zs"][place].astype(f32)
        for k in range(1, line):
            value = value + b["l3"][z_of(k)].astype(f32)
        squares.append(jnp.sum(value * value))
        b["ag"][me_neg] = value.astype(bf16)
        mine = b["ag"].at[me_neg]
        for k in range(1, nx):
            x = x_of(k)
            go(link(mine, mine, (b["sg"], b["rg"]), me_x, "neg", same_core(x), x))
        go(link(mine, mine, (b["sh"], b["rh"]), me_x, "neg", mate))

    def stage5(g):
        b = bufs[g]
        for k in range(1, nx):
            x = x_of(k)
            ref = b["ag"].at[same_core(x)]
            arrived(ref, b["rg"], x)
            go(link(ref, ref, (b["sh"], b["rh"]), x, "neg", mate))

    def stage6(g):
        b = bufs[g]
        for x in range(nx):
            arrived(b["ag"].at[2 * x + other], b["rh"], x)

    embed_stage(0)
    second_stage(0, 0)
    stage0(0)
    slope_stage(0)
    first_stage(0, 1)
    stage0(1)
    stage1(0)
    embed_stage(1)
    stage1(1)
    second_stage(1, 2)
    stage0(2)
    stage2(0)
    slope_stage(1)
    stage1(2)
    stage2(1)
    first_stage(1, 3)
    stage0(3)
    stage3(0)
    stage1(3)
    stage3(1)
    stage2(2)
    stage4(0)
    stage2(3)
    stage4(1)
    stage3(2)
    stage3(3)
    stage4(2)
    stage4(3)
    total_squares = squares[0] + squares[1] + squares[2] + squares[3]
    lane = lax.broadcasted_iota(jnp.int32, (8, 128), 1)
    stat_dp[...] = jnp.where(lane == 0, total_squares, loss_ref[0])
    stat_copies = share("dp", ndp, me_dp, lambda t: stat_dp, stat_dp_land, ss, sr)
    for g in range(4):
        stage5(g)
    finish(stat_copies)
    total = stat_dp[...]
    for k in range(1, ndp):
        total = total + stat_dp_land[lax.rem(me_dp + k, ndp)]
    stat_neg[...] = total
    stat_copies = share("neg", nneg, me_neg, lambda t: stat_neg, stat_neg_land, ts, tr)
    for g in range(4):
        stage6(g)
    finish(stat_copies)
    total = stat_neg[...]
    for k in range(1, nneg):
        total = total + stat_neg_land[lax.rem(me_neg + k, nneg)]
    stats_ref[...] = total
    for copy in pending:
        copy.wait_send()


def fused_backward(ndp, nneg, towers, loss_part, own_queries):
    line, nx = ndp // 2, nneg // 2
    bf16, f32 = jnp.bfloat16, jnp.float32
    groups, outs, scratch, buffers, semaphores = [], [], [], [], []
    for feat, act1, slope1, act2, slope2, emb, grad, second, third in towers:
        rows, fin = feat.shape
        h1, h2, width = act1.shape[1], act2.shape[1], emb.shape[1]
        for height, columns in ((fin, h1), (h1, h2), (h2, width)):
            outs.append(jax.ShapeDtypeStruct((height // ndp, columns), f32))
        both = h2 // (ndp * nneg) * (width // pack_columns) + h1 // (ndp * nneg) * (h2 // pack_columns)
        alone = fin // (ndp * nneg) * (h1 // pack_columns)
        for r in (both, alone):
            groups.append((r * 4 // 9 // 16 * 16, r))
        scratch += [pltpu.VMEM((rows, width), bf16), pltpu.VMEM((rows, h2), bf16), pltpu.VMEM((rows, h1), bf16)]
    for r1, r in groups:
        r2, c = r - r1, pack_columns
        for shape in (
            (2, ndp, nx, r, c), (ndp, nx, r, c), (nx, ndp, r1, c), (nx, ndp, r1, c), (line, nx, r2, c),
            (line, nx, r2, c), (line, r1, c), (line, r1, c), (nx, line, r2, c), (nx, line, r2, c),
            (line, r, c), (line, r, c),
        ):
            buffers.append(pltpu.VMEM(shape, bf16))
        semaphores += sems(1, 1, nx, nx, 1, 1, 1, 1, nx, nx, line, line, nx, nx, nx, nx)
    stat = [pltpu.VMEM((8, 128), f32), pltpu.VMEM((ndp, 8, 128), f32), pltpu.VMEM((8, 128), f32), pltpu.VMEM((nneg, 8, 128), f32)]
    operands = [operand for tower in towers for operand in tower]
    stats, *gathered = pl.pallas_call(
        lambda *refs: backward_kernel(ndp, nneg, tuple(groups), *refs),
        out_shape=(
            jax.ShapeDtypeStruct((8, 128), f32),
            *[jax.ShapeDtypeStruct((nneg, r, pack_columns), bf16) for _, r in groups],
        ),
        in_specs=[vmem] * len(operands) + [pl.BlockSpec(memory_space=pltpu.SMEM)],
        out_specs=(vmem,) * 5,
        scratch_shapes=scratch + buffers + stat + semaphores + sems(ndp, ndp, nneg, nneg),
        compiler_params=pltpu.CompilerParams(
            collective_id=1, has_side_effects=True, vmem_limit_bytes=40 * 1024 * 1024
        ),
    )(*operands, loss_part.reshape(1))
    any_space = pl.BlockSpec(memory_space=pl.ANY)
    mean_loss, *clipped = pl.pallas_call(
        functools.partial(finish_kernel, nneg, own_queries * ndp * nneg),
        out_shape=(jax.ShapeDtypeStruct((1,), f32), *outs),
        in_specs=[vmem] * 5,
        out_specs=(pl.BlockSpec(memory_space=pltpu.SMEM), *([any_space] * 6)),
        scratch_shapes=[pltpu.VMEM(out.shape, f32) for out in outs] + sems(6),
    )(stats, *gathered)
    return (mean_loss.reshape(()), *clipped)


def finish_kernel(nneg, count, stats_ref, *refs):
    gathered, loss_ref, outs, staged, done = refs[:4], refs[4], refs[5:11], refs[11:17], refs[17]
    clip = clip_norm / jnp.maximum(jnp.sqrt(stats_ref[0:1, 0:1]), clip_norm)
    copies = []
    for t in range(2):
        third_ref, second_ref, first_ref = staged[3 * t + 2], staged[3 * t + 1], staged[3 * t]
        for index, group, ref, offset in (
            (3 * t + 1, 2 * t, second_ref, third_ref.shape[0] // nneg),
            (3 * t, 2 * t + 1, first_ref, 0),
            (3 * t + 2, 2 * t, third_ref, 0),
        ):
            pieces = ref.shape[0] // nneg
            for p in range(ref.shape[1] // pack_columns):
                lo = offset + p * pieces
                for n in range(nneg):
                    value = gathered[group][n, lo : lo + pieces, :].astype(jnp.float32) * clip
                    ref[n * pieces : (n + 1) * pieces, p * pack_columns : (p + 1) * pack_columns] = value
            copy = pltpu.make_async_copy(ref, outs[index], done.at[index])
            copy.start()
            copies.append(copy)
    loss_ref[0] = jnp.sum(stats_ref[0:1, 1:2]) / count
    for copy in copies:
        copy.wait()


def per_device(
    query_features,
    positive_features,
    negative_features,
    positive_ids,
    positive_counts,
    negative_ids,
    negative_counts,
    query_first,
    query_second,
    query_third,
    item_first,
    item_second,
    item_third,
):
    own_rows = query_features.shape[0]
    query_saved, query_unit = tower_forward(query_features, query_first, query_second, query_third)
    item_features = jnp.concatenate([positive_features, negative_features], axis=0)
    item_saved, item_unit = tower_forward(item_features, item_first, item_second, item_third)
    positive_unit = item_unit[:own_rows]
    negative_unit = item_unit[own_rows:]
    ndp, nneg = lax.axis_size("dp"), lax.axis_size("neg")
    width = query_unit.shape[1]
    line, nx = ndp // 2, nneg // 2
    block = negative_unit.shape[0]
    blocks, cuts, lanes = 2 * nneg, 2, min(block, 128)
    bf16, f32, i32 = jnp.bfloat16, jnp.float32, jnp.int32
    positive_logit = jnp.sum(
        query_unit.astype(f32) * positive_unit.astype(f32), axis=1
    ) * inv_temp - jnp.log(positive_counts.astype(f32))
    positive_exp = jnp.exp(positive_logit)
    rows_half = (width // 2, block)
    query_total, denom, negative_sum = call(
        score_kernel,
        0,
        ndp,
        nneg,
        (
            jax.ShapeDtypeStruct((own_rows, width), f32),
            jax.ShapeDtypeStruct((1, own_rows), f32),
            jax.ShapeDtypeStruct((2,) + rows_half, f32),
        ),
        [
            pltpu.VMEM((line, cuts, own_rows // cuts, width), bf16),
            pltpu.VMEM((blocks, 2, block // 2, width), bf16),
            pltpu.VMEM((2, block), i32),
            pltpu.VMEM((blocks, 2, block), i32),
            pltpu.VMEM((blocks, 2, block), f32),
            pltpu.VMEM((1, own_rows), i32),
            pltpu.VMEM((line, 1, own_rows), i32),
            pltpu.VMEM((line, own_rows, lanes), f32),
            pltpu.VMEM((blocks, line, own_rows, block), bf16),
            pltpu.VMEM((line, own_rows, lanes), f32),
            pltpu.VMEM((line, 1, own_rows), f32),
            pltpu.VMEM((line, line, 1, own_rows), f32),
            pltpu.VMEM((width, line * own_rows), bf16),
            pltpu.VMEM((line, own_rows, width), bf16),
            pltpu.VMEM((own_rows, width), f32),
            pltpu.VMEM((line, own_rows, width), bf16),
            pltpu.VMEM((nx, 2, 2) + rows_half, bf16),
            pltpu.VMEM((nx, 2, 2) + rows_half, bf16),
            pltpu.VMEM((nx, 2, 2) + rows_half, f32),
            pltpu.VMEM((nx, 2, 2) + rows_half, bf16),
            pltpu.VMEM((nx, 2) + rows_half, bf16),
            pltpu.VMEM((nx,) + rows_half, bf16),
            pltpu.VMEM(rows_half, bf16),
            pltpu.VMEM((nx,) + rows_half, bf16),
        ]
        + sems(
            3 * nx, 1 + nx, 4 * nx, 4 * nx, 4 * nx, line * cuts, line * cuts, line * cuts,
            blocks, blocks, line, line, line, line, line, line,
            2 * nx, 2 * nx, 2 * nx, 2 * nx, nx, nx, 1, 1, nx, nx,
        ),
        [vmem] * 6,
        40,
    )(
        query_unit,
        negative_unit.reshape(2, block // 2, width),
        positive_ids.reshape((1, -1) if own_rows % 128 == 0 else (nneg, own_rows)),
        negative_ids.reshape((1, -1) if block % 128 == 0 else (ndp, block)),
        negative_counts.reshape((1, -1) if block % 128 == 0 else (ndp, block)),
        positive_exp.reshape(1, own_rows),
    )
    own_denom = denom.reshape(-1)
    loss_part = jnp.sum(jnp.log(own_denom) - positive_logit)
    positive_slope = positive_exp / own_denom - 1.0
    query_sum = query_total / own_denom[:, None]
    negative_sum = negative_sum.reshape(width, block).T
    query_grad = (
        query_sum + positive_slope[:, None] * positive_unit.astype(jnp.float32)
    ) * inv_temp
    positive_grad = positive_slope[:, None] * query_unit.astype(jnp.float32) * inv_temp
    item_grad = jnp.concatenate([positive_grad, negative_sum * inv_temp], axis=0)
    heights = (query_first.shape[0], query_second.shape[0], query_third.shape[0])
    if all(height % (16 * ndp * nneg) == 0 for height in heights):
        towers = [
            (features, saved[1], saved[0], saved[3], saved[2], saved[4], grad, second, third)
            for features, saved, grad, second, third in (
                (query_features, query_saved, query_grad, query_second, query_third),
                (item_features, item_saved, item_grad, item_second, item_third),
            )
        ]
        return fused_backward(ndp, nneg, towers, loss_part, own_rows)
    query_grads = tower_backward(query_features, query_second, query_third, query_saved, query_grad)
    item_grads = tower_backward(item_features, item_second, item_third, item_saved, item_grad)
    gradients = query_grads + item_grads
    parts = [part for gradient in gradients for part in to_packed(gradient, ndp)]
    packed = jnp.concatenate(parts, axis=1)
    rows = packed.shape[1] // nneg
    packed = packed.reshape(ndp, nneg, 2, rows // 2, pack_columns).transpose(1, 0, 2, 3, 4)
    piece = (rows // 2, pack_columns)
    gathered, stats = call(
        weight_kernel,
        3,
        ndp,
        nneg,
        (jax.ShapeDtypeStruct((nneg, 2) + piece, bf16), jax.ShapeDtypeStruct((8, 128), f32)),
        [
            pltpu.VMEM((nx, ndp, 2) + piece, bf16),
            pltpu.VMEM((nx, 2, line) + piece, bf16),
            pltpu.VMEM((2, nx, line) + piece, bf16),
            pltpu.VMEM((nx, 2, line) + piece, bf16),
            pltpu.VMEM((nx, line) + piece, bf16),
            pltpu.VMEM((2, line) + piece, bf16),
            pltpu.VMEM((nx, line) + piece, bf16),
            pltpu.VMEM((line,) + piece, bf16),
            pltpu.VMEM((nx, line) + piece, bf16),
            pltpu.VMEM((2, line) + piece, bf16),
            pltpu.VMEM((2, line) + piece, bf16),
            pltpu.VMEM((8, 128), f32),
            pltpu.VMEM((ndp, 8, 128), f32),
            pltpu.VMEM((8, 128), f32),
            pltpu.VMEM((nneg, 8, 128), f32),
        ]
        + sems(nx, nx, 2 * nx, 2 * nx, 2, 2, ndp, ndp, ndp, ndp, nneg, nneg, nx, nx, nx, nx),
        [vmem, pl.BlockSpec(memory_space=pltpu.SMEM)],
    )(packed, loss_part.reshape(1))
    grad_norm = jnp.sqrt(stats[0, 0])
    mean_loss = stats[0, 1] / (own_rows * ndp * nneg)
    clip_factor = clip_norm / jnp.maximum(grad_norm, clip_norm)
    flat = gathered.reshape(nneg * rows, pack_columns)
    clipped = []
    start = 0
    for gradient in gradients:
        height, columns = gradient.shape[0] // ndp, gradient.shape[1]
        groups = columns // pack_columns
        blocks = [flat[start + g * height : start + (g + 1) * height] for g in range(groups)]
        start += groups * height
        clipped.append(jnp.concatenate(blocks, axis=1).astype(jnp.float32) * clip_factor)
    return (mean_loss, *clipped)


def solution(mesh):
    placed = (
        P(("dp", "neg"), None),
        P(("dp", "neg"), None),
        P(("neg", "dp"), None),
        P("dp"),
        P(("dp", "neg")),
        P("neg"),
        P("neg"),
        P(),
        P(),
        P(),
        P(),
        P(),
        P(),
    )
    return jax.shard_map(
        per_device,
        mesh=mesh,
        in_specs=placed,
        out_specs=(
            P(),
            P("dp", None),
            P("dp", None),
            P("dp", None),
            P("dp", None),
            P("dp", None),
            P("dp", None),
        ),
        check_vma=False,
    )
```

```python
import functools

import jax
import jax.numpy as jnp
from jax import lax
from jax.experimental import pallas as pl
from jax.experimental.pallas import tpu as pltpu
from jax.sharding import PartitionSpec as P

inv_temp = 20.0
log2_e = 1.4426950408889634
clip_norm = 256.0


def silu_slope(pre):
    sigma = jax.nn.sigmoid(pre)
    return sigma * (1.0 + pre * (1.0 - sigma))


def contract_rows(left, right):
    return lax.dot_general(
        left, right, (((0,), (0,)), ((), ())), preferred_element_type=jnp.float32
    )


def contract_cols(left, right):
    return lax.dot_general(
        left, right, (((1,), (1,)), ((), ())), preferred_element_type=jnp.float32
    )


def tower_forward(features, first, second, third):
    first_pre = jnp.dot(features, first, preferred_element_type=jnp.float32)
    first_act = jax.nn.silu(first_pre).astype(jnp.bfloat16)
    second_pre = jnp.dot(first_act, second, preferred_element_type=jnp.float32)
    second_act = jax.nn.silu(second_pre).astype(jnp.bfloat16)
    embedding = jnp.dot(second_act, third, preferred_element_type=jnp.float32)
    inv_norm = lax.rsqrt(jnp.sum(embedding * embedding, axis=1, keepdims=True) + 1.0)
    unit = (embedding * inv_norm).astype(jnp.bfloat16)
    saved = (silu_slope(first_pre), first_act, silu_slope(second_pre), second_act, embedding, inv_norm)
    return saved, unit


def tower_backward(features, second, third, saved, unit_grad):
    first_slope, first_act, second_slope, second_act, embedding, inv_norm = saved
    along = jnp.sum(embedding * unit_grad, axis=1, keepdims=True)
    embed_grad = (inv_norm * unit_grad - inv_norm * inv_norm * inv_norm * embedding * along).astype(
        jnp.bfloat16
    )
    third_grad = contract_rows(second_act, embed_grad)
    second_step = (contract_cols(embed_grad, third) * second_slope).astype(jnp.bfloat16)
    second_grad = contract_rows(first_act, second_step)
    first_step = (contract_cols(second_step, second) * first_slope).astype(jnp.bfloat16)
    first_grad = contract_rows(features, first_step)
    return (first_grad, second_grad, third_grad)


pack_columns = 256
vmem = pl.BlockSpec(memory_space=pltpu.VMEM)


def greet(ndp, nneg, me_dp, me_neg):
    barrier = pltpu.get_barrier_semaphore()
    for k in range(1, nneg):
        pl.semaphore_signal(
            barrier, inc=1, device_id={"neg": lax.rem(me_neg + k, nneg)}, device_id_type=pl.DeviceIdType.MESH
        )
    for k in range(1, ndp):
        pl.semaphore_signal(
            barrier, inc=1, device_id={"dp": lax.rem(me_dp + k, ndp)}, device_id_type=pl.DeviceIdType.MESH
        )
    pl.semaphore_wait(barrier, (nneg - 1) + (ndp - 1))


def send(src, dst, send_sem, recv_sem, axis, target):
    copy = pltpu.make_async_remote_copy(
        src_ref=src,
        dst_ref=dst,
        send_sem=send_sem,
        recv_sem=recv_sem,
        device_id={axis: target},
        device_id_type=pl.DeviceIdType.MESH,
    )
    copy.start()
    return copy


def share(axis, n, me, src_of, dst, send_sem, recv_sem):
    return [
        send(src_of(lax.rem(me + k, n)), dst.at[me], send_sem.at[k], recv_sem.at[k], axis, lax.rem(me + k, n))
        for k in range(1, n)
    ]


def finish(copies):
    for copy in copies:
        copy.wait()


def link(src, dst, sems, index, axis, target, send_index=None):
    send_sems, recv_sems = sems
    return pltpu.make_async_remote_copy(
        src_ref=src,
        dst_ref=dst,
        send_sem=send_sems.at[index if send_index is None else send_index],
        recv_sem=recv_sems.at[index],
        device_id={axis: target},
        device_id_type=pl.DeviceIdType.MESH,
    )


def score_kernel(
    ndp, nneg, query_ref, negative_ref, pid_ref, nid_ref, count_ref, pexp_ref, sum_ref, denom_ref, nsum_ref,
    q_land, n_land, meta_out, meta, rows, pid_out, pid_land, pid_col, w, den, dpart, dland, scaled,
    q_out, q_part, q_in, c_out, c_in, own, out, lx, ly, l2y, l2x,
    sx, sy, rn, sm, rm, sr, sl, rq, s_meta, r_meta, s_pid, r_pid, sd, rd, sq, rqs,
    sc, rc, s1x, r1x, s1y, r1y, s2y, r2y, s2x, r2x,
):
    me_dp, me_neg = lax.axis_index("dp"), lax.axis_index("neg")
    line, nx = ndp // 2, nneg // 2
    place, side = me_dp // 2, lax.rem(me_dp, 2)
    me_x, me_core = me_neg // 2, lax.rem(me_neg, 2)
    far, other = 1 - side, 1 - me_core
    partner, mate = 2 * place + far, 2 * me_x + other
    rows_q, width = query_ref.shape
    block = 2 * negative_ref.shape[1]
    lanes = den.shape[2]
    cuts = q_land.shape[1]
    half_w = width // 2
    blocks = nneg * 2
    here = (me_x * 2 + side) * 2 + me_core

    def along(k):
        return lax.rem(me_x + k, nx)

    def at_place(z):
        return 2 * z + side

    barrier = pltpu.get_barrier_semaphore()
    for k in range(1, line):
        pl.semaphore_signal(
            barrier, inc=1, device_id={"dp": at_place(lax.rem(place + k, line))}, device_id_type=pl.DeviceIdType.MESH
        )

    def quad(k):
        b = lax.rem(here + k, blocks)
        return {"dp": 2 * place + lax.rem(b // 2, 2), "neg": 2 * (b // 4) + lax.rem(b, 2)}

    for k in range(1, blocks):
        pl.semaphore_signal(barrier, inc=1, device_id=quad(k), device_id_type=pl.DeviceIdType.MESH)
    def own_ids(ref, index, count):
        if count % 128 == 0:
            return ref[:, pl.ds(pl.multiple_of(index * count, count), count)]
        return ref[pl.ds(index, 1), :]

    meta_out[0:1, :] = own_ids(nid_ref, me_dp, block)
    meta_out[1:2, :] = own_ids(count_ref, me_dp, block)
    pid_out[...] = own_ids(pid_ref, me_neg, rows_q)
    pl.semaphore_wait(barrier, (line - 1) + (blocks - 1))

    def slot(x, y, half):
        return (x * 2 + y) * 2 + half

    def piece(x, y, half):
        return n_land.at[(x * 2 + y) * 2 + me_core, half]

    def push(src, x, y, half, send_sems, index, axis, target):
        return link(src, piece(x, y, half), (send_sems, rn), slot(x, y, half), axis, target, index)

    def relay(src, x, y, half):
        i = slot(x, y, half)
        return link(src, piece(x, y, half), (sm, rm), i, "neg", mate)

    def landed(x, y, half):
        ref = piece(x, y, half)
        link(ref, ref, (sy, rn), slot(x, y, half), "neg", mate, 0).wait_recv()

    sends = []

    def go(copy):
        copy.start()
        sends.append(copy)

    def to_x(src, x, y, half, kind):
        for k in range(1, nx):
            go(push(src, x, y, half, sx, kind * nx + k, "neg", 2 * along(k) + me_core))

    def to_y(src, x, y, half, index):
        go(push(src, x, y, half, sy, index, "dp", partner))

    first, second = negative_ref.at[0], negative_ref.at[1]
    to_x(first, me_x, side, 0, 0)
    to_y(second, me_x, side, 1, 0)
    to_x(second, me_x, side, 1, 1)
    to_y(first, me_x, side, 0, 1)
    go(relay(first, me_x, side, 0))
    go(relay(second, me_x, side, 1))

    def chain(slot_z, j, distance, sems, target):
        src = query_ref.at[pl.ds(j * (rows_q // cuts), rows_q // cuts)] if distance == 0 else q_land.at[slot_z, j]
        return link(src, q_land.at[slot_z, j], (sems, rq), slot_z * cuts + j, "dp", target, distance * cuts + j)

    def right(distance, j):
        return chain(place - distance, j, distance, sr, at_place(lax.rem(place + 1, line)))

    def left(distance, j):
        return chain(place + distance, j, distance, sl, at_place(lax.rem(place + line - 1, line)))

    goes_right, goes_left = place < line - 1, place > 0
    for j in range(cuts):
        pl.when(goes_right)(lambda j=j: right(0, j).start())
        pl.when(goes_left)(lambda j=j: left(0, j).start())
    for k in range(1, blocks):
        b = lax.rem(here + k, blocks)
        copy = pltpu.make_async_remote_copy(
            src_ref=meta_out, dst_ref=meta.at[here], send_sem=s_meta.at[k], recv_sem=r_meta.at[here],
            device_id=quad(k), device_id_type=pl.DeviceIdType.MESH,
        )
        go(copy)
    for k in range(1, line):
        z = lax.rem(place + k, line)
        go(link(pid_out, pid_land.at[place], (s_pid, r_pid), place, "dp", at_place(z), k))
    n_land[here] = negative_ref[...]
    for j in range(cuts):
        q_land[place, j] = query_ref[pl.ds(j * (rows_q // cuts), rows_q // cuts), :]
    meta[here] = meta_out[...]
    pid_land[place] = pid_out[...]

    for k in range(1, nx):
        x = along(k)
        landed(x, side, 0)
        to_y(piece(x, side, 0), x, side, 0, 1 + k)
        go(relay(piece(x, side, 0), x, side, 0))
    landed(me_x, far, 1)
    to_x(piece(me_x, far, 1), me_x, far, 1, 2)
    go(relay(piece(me_x, far, 1), me_x, far, 1))

    def q_step(distance):
        for j in range(cuts):

            @pl.when(place >= distance)
            def _():
                ref = q_land.at[place - distance, j]
                link(ref, ref, (sr, rq), (place - distance) * cuts + j, "dp", partner, 0).wait_recv()
                pl.when(goes_right)(lambda: right(distance, j).start())

            @pl.when(place + distance < line)
            def _():
                ref = q_land.at[place + distance, j]
                link(ref, ref, (sl, rq), (place + distance) * cuts + j, "dp", partner, 0).wait_recv()
                pl.when(goes_left)(lambda: left(distance, j).start())

    q_step(1)
    for k in range(1, nx):
        x = along(k)
        landed(x, side, 1)
        go(relay(piece(x, side, 1), x, side, 1))
    landed(me_x, far, 0)
    go(relay(piece(me_x, far, 0), me_x, far, 0))
    for distance in range(2, line):
        q_step(distance)
    for half in range(2):
        for k in range(1, nx):
            x = along(k)
            landed(x, far, half)
            go(relay(piece(x, far, half), x, far, half))
    for x in range(nx):
        for y in range(2):
            for half in range(2):
                i = slot(x, y, half)
                ref = n_land.at[(x * 2 + y) * 2 + other, half]
                link(ref, ref, (sm, rm), i, "neg", mate).wait_recv()
    for k in range(1, blocks):
        b = lax.rem(here + k, blocks)
        link(meta.at[b], meta.at[b], (s_meta, r_meta), b, "neg", mate).wait_recv()
    for k in range(1, line):
        z = lax.rem(place + k, line)
        link(pid_land.at[z], pid_land.at[z], (s_pid, r_pid), z, "dp", partner).wait_recv()

    for b in range(blocks):
        rows[b, 0:1, :] = meta[b, 0:1, :].astype(jnp.float32)
        rows[b, 1:2, :] = jnp.log2(meta[b, 1:2, :].astype(jnp.float32))
    for z in range(line):
        pid_col[z] = jnp.broadcast_to(pid_land[z].astype(jnp.float32), (lanes, rows_q)).T
        den[z] = jnp.zeros((rows_q, lanes), jnp.float32)

    def unit(b, z):
        dots = contract_cols(q_land[z].reshape(rows_q, width), n_land[b].reshape(block, width))
        value = jnp.exp2(dots * (inv_temp * log2_e) - rows[b, 1:2, :])
        ids = jnp.concatenate([pid_col[z]] * (block // lanes), axis=1)
        value = jnp.where(ids != rows[b, 0:1, :], value, 0.0)
        w[b, z] = value.astype(jnp.bfloat16)
        total = den[z]
        for c in range(0, block, lanes):
            total = total + value[:, c : c + lanes]
        den[z] = total

    def units(b, carry):
        for z in range(line):
            unit(b, z)
        return carry

    lax.fori_loop(0, blocks, units, 0)
    for z in range(line):
        dpart[z] = jnp.sum(den[z].T, axis=0, keepdims=True)
    dpart[place] = dpart[place] + pexp_ref[...]
    for k in range(1, line):
        z = lax.rem(place + k, line)
        go(link(dpart, dland.at[place], (sd, rd), place, "dp", at_place(z), k))

    def q_block(z):
        if block % 128 == 0:
            left_side = jnp.concatenate([w[b, z] for b in range(blocks)], axis=1)
            return jnp.dot(
                left_side, n_land[...].reshape(blocks * block, width), preferred_element_type=jnp.float32
            )
        total = jnp.zeros((rows_q, width), jnp.float32)
        for b in range(blocks):
            total = total + jnp.dot(w[b, z], n_land[b].reshape(block, width), preferred_element_type=jnp.float32)
        return total

    def q_send(k, z):
        return link(q_out.at[z], q_in.at[place], (sq, rqs), place, "dp", at_place(z), k)

    def q_push(k, carry):
        z = lax.rem(place + k, line)
        q_out[z] = q_block(z).astype(jnp.bfloat16)
        q_send(k, z).start()
        return carry

    lax.fori_loop(1, line, q_push, 0)
    q_part[...] = q_block(place)
    total = dpart[...]
    for k in range(1, line):
        z = lax.rem(place + k, line)
        link(dland.at[z], dland.at[z], (sd, rd), z, "dp", partner).wait_recv()
        total = total + dland[z]
    dpart2 = 1.0 / total
    for z in range(line):
        q_t = q_land[z].reshape(rows_q, width).astype(jnp.float32).T
        scaled[:, z * rows_q : (z + 1) * rows_q] = (q_t * dpart2[z]).astype(jnp.bfloat16)
    denom_ref[...] = dpart[place]
    for k in range(1, line):
        denom_ref[...] = denom_ref[...] + dland[lax.rem(place + k, line), place]

    def dest(i):
        x = lax.rem(me_x + 1 + i // 2, nx)
        y = lax.rem(side + 1 + lax.rem(i, 2), 2)
        return x, y

    def part(x, y, core):
        return jnp.dot(
            scaled[...], w[(x * 2 + y) * 2 + core].reshape(line * rows_q, block), preferred_element_type=jnp.float32
        )

    def c_send(i):
        x, y = dest(i)
        return link(c_out.at[x, y], c_in.at[x, y], (sc, rc), x * 2 + y, "neg", mate)

    def far_step(i, carry):
        x, y = dest(i)
        c_out[x, y] = part(x, y, other).astype(jnp.bfloat16).reshape(2, half_w, block)
        c_send(i).start()
        return carry

    def send_1x(i):
        x, y = dest(i)
        return link(out.at[x, y, 0], lx.at[me_x, y], (s1x, r1x), me_x * 2 + y, "neg", 2 * x + me_core, x * 2 + y)

    def send_1y(i):
        x, y = dest(i)
        return link(out.at[x, y, 1], ly.at[x], (s1y, r1y), x, "dp", partner)

    def own_step(i, carry):
        x, y = dest(i)
        value = part(x, y, me_core).reshape(2, half_w, block)
        link(c_in.at[x, y], c_in.at[x, y], (sc, rc), x * 2 + y, "neg", mate).wait_recv()
        value = value + c_in[x, y].astype(jnp.float32)
        own[x, y] = value

        @pl.when(i < 2 * (nx - 1))
        def _():
            out[x, y, 0] = value[0].astype(jnp.bfloat16)
            send_1x(i).start()

        @pl.when(lax.rem(i, 2) == 0)
        def _():
            out[x, y, 1] = value[1].astype(jnp.bfloat16)
            send_1y(i).start()

        return carry

    lax.fori_loop(0, 2 * nx, far_step, 0)
    lax.fori_loop(0, 2 * nx, own_step, 0)
    value = own[me_x, far, 0]
    for k in range(1, nx):
        x = along(k)
        ref = lx.at[x, far]
        link(ref, ref, (s1x, r1x), x * 2 + far, "neg", mate).wait_recv()
        value = value + lx[x, far].astype(jnp.float32)
    out[me_x, far, 0] = value.astype(jnp.bfloat16)
    go(link(out.at[me_x, far, 0], l2y, (s2y, r2y), 0, "dp", partner))
    for k in range(1, nx):
        x = along(k)
        link(ly.at[x], ly.at[x], (s1y, r1y), x, "dp", partner).wait_recv()
        out[x, side, 1] = (own[x, side, 1] + ly[x].astype(jnp.float32)).astype(jnp.bfloat16)
        go(link(out.at[x, side, 1], l2x.at[me_x], (s2x, r2x), me_x, "neg", 2 * x + me_core, x))
    result = q_part[...]
    for k in range(1, line):
        z = lax.rem(place + k, line)
        link(q_in.at[z], q_in.at[z], (sq, rqs), z, "dp", partner).wait_recv()
        result = result + q_in[z].astype(jnp.float32)
    sum_ref[...] = result
    low = own[me_x, side, 0]
    for k in range(1, nx):
        x = along(k)
        ref = lx.at[x, side]
        link(ref, ref, (s1x, r1x), x * 2 + side, "neg", mate).wait_recv()
        low = low + lx[x, side].astype(jnp.float32)
    link(ly.at[me_x], ly.at[me_x], (s1y, r1y), me_x, "dp", partner).wait_recv()
    high = own[me_x, side, 1] + ly[me_x].astype(jnp.float32)
    link(l2y, l2y, (s2y, r2y), 0, "dp", partner).wait_recv()
    nsum_ref[0] = low + l2y[...].astype(jnp.float32)
    for k in range(1, nx):
        x = along(k)
        link(l2x.at[x], l2x.at[x], (s2x, r2x), x, "neg", mate).wait_recv()
        high = high + l2x[x].astype(jnp.float32)
    nsum_ref[1] = high

    for copy in sends:
        copy.wait_send()
    for distance in range(line):
        for j in range(cuts):
            if distance < line - 1:
                pl.when((place >= distance) & goes_right)(lambda: right(distance, j).wait_send())
                pl.when((place + distance < line) & goes_left)(lambda: left(distance, j).wait_send())
    for k in range(1, line):
        q_send(k, lax.rem(place + k, line)).wait_send()
    for i in range(2 * nx):
        c_send(i).wait_send()
        if i < 2 * (nx - 1):
            send_1x(i).wait_send()
        if i % 2 == 0:
            send_1y(i).wait_send()


def weight_kernel(
    ndp, nneg, packed_ref, loss_ref, gathered_ref, stats_ref,
    core_land, sum_a, sum_b, land_a, land_b, half_a, half_b, last_a, last_b, line_sum, line_land,
    stat_dp, stat_dp_land, stat_neg, stat_neg_land,
    cs, cr, xs, xr, ys, yr, ps, pr, ss, sr, ts, tr, gs, gr, hs, hr,
):
    me_dp, me_neg = lax.axis_index("dp"), lax.axis_index("neg")
    nx, line = nneg // 2, ndp // 2
    me_x, me_core = me_neg // 2, lax.rem(me_neg, 2)
    place, side = me_dp // 2, lax.rem(me_dp, 2)
    other, far = 1 - me_core, 1 - side
    mate, partner = 2 * me_x + other, 2 * place + far
    greet(ndp, nneg, me_dp, me_neg)
    turn = list(range(1, nx)) + [0]

    def x_of(k):
        return lax.rem(me_x + k, nx)

    core = {}
    for k in turn:
        x = x_of(k)
        core[k] = send(packed_ref.at[2 * x + other], core_land.at[x], cs.at[k], cr.at[k], "neg", mate)

    def add_core(x, y, half, target):
        def body(z, carry):
            target[z] = (
                packed_ref[2 * x + me_core, 2 * z + y, half].astype(jnp.float32)
                + core_land[x, 2 * z + y, half].astype(jnp.float32)
            ).astype(jnp.bfloat16)
            return carry

        lax.fori_loop(0, line, body, 0)

    def add(target, *terms):
        def body(z, carry):
            value = terms[0][z].astype(jnp.float32)
            for term in terms[1:]:
                value = value + term[z].astype(jnp.float32)
            target[z] = value.astype(jnp.bfloat16)
            return carry

        lax.fori_loop(0, line, body, 0)

    first_a = []
    for k in turn:
        x = x_of(k)
        core[k].wait_recv()
        if k:
            for y in range(2):
                add_core(x, y, 0, sum_a.at[x, y])
            first_a.append(send(sum_a.at[x], land_a.at[k], xs.at[k], xr.at[k], "neg", 2 * x + me_core))
        add_core(x, far, 1, sum_b.at[far, x])
    first_b = send(sum_b.at[far], land_b, ys.at[0], yr.at[0], "dp", partner)
    for y in range(2):
        add_core(me_x, y, 0, sum_a.at[me_x, y])
    for k in range(nx):
        add_core(x_of(k), side, 1, sum_b.at[side, x_of(k)])
    for copy in first_a:
        copy.wait_recv()
    add(half_a.at[far], sum_a.at[me_x, far], *[land_a.at[k, far] for k in range(1, nx)])
    second_a = send(half_a.at[far], last_a, ys.at[1], yr.at[1], "dp", partner)
    first_b.wait_recv()
    second_b = []
    for k in turn:
        x = x_of(k)
        add(half_b.at[x], sum_b.at[side, x], land_b.at[x])
        if k:
            second_b.append(
                send(half_b.at[x], last_b.at[k], xs.at[nx + k], xr.at[nx + k], "neg", 2 * x + me_core)
            )
    add(half_a.at[side], sum_a.at[me_x, side], *[land_a.at[k, side] for k in range(1, nx)])
    second_a.wait_recv()
    add(line_sum.at[0], half_a.at[side], last_a)
    third = []
    for half in range(2):
        if half:
            for copy in second_b:
                copy.wait_recv()
            add(line_sum.at[1], half_b.at[me_x], *[last_b.at[k] for k in range(1, nx)])
        for k in range(1, line):
            z = lax.rem(place + k, line)
            third.append(
                send(line_sum.at[half, z], line_land.at[half, k], ps.at[half * line + k], pr.at[half * line + k], "dp", 2 * z + side)
            )
    for copy in third:
        copy.wait_recv()
    squares = jnp.zeros((), jnp.float32)
    for half in range(2):
        piece = line_sum[half, place].astype(jnp.float32)
        for k in range(1, line):
            piece = piece + line_land[half, k].astype(jnp.float32)
        gathered_ref[me_neg, half] = piece.astype(jnp.bfloat16)
        squares = squares + jnp.sum(piece * piece)
    lane = lax.broadcasted_iota(jnp.int32, (8, 128), 1)
    stat_dp[...] = jnp.where(lane == 0, squares, loss_ref[0])
    stat_copies = share("dp", ndp, me_dp, lambda t: stat_dp, stat_dp_land, ss, sr)
    mine = gathered_ref.at[me_neg]
    spread = [send(mine, mine, gs.at[k], gr.at[k], "neg", 2 * x_of(k) + me_core) for k in range(1, nx)]
    spread.append(send(mine, mine, gs.at[0], gr.at[0], "neg", mate))
    finish(stat_copies)
    total = stat_dp[...]
    for k in range(1, ndp):
        total = total + stat_dp_land[lax.rem(me_dp + k, ndp)]
    stat_neg[...] = total
    stat_copies = share("neg", nneg, me_neg, lambda t: stat_neg, stat_neg_land, ts, tr)
    relay = []
    for k in range(1, nx):
        spread[k - 1].wait_recv()
        x = lax.rem(me_x + nx - k, nx)
        came = gathered_ref.at[2 * x + me_core]
        relay.append(send(came, came, hs.at[k], hr.at[k], "neg", mate))
    finish(stat_copies)
    total = stat_neg[...]
    for k in range(1, nneg):
        total = total + stat_neg_land[lax.rem(me_neg + k, nneg)]
    stats_ref[...] = total
    spread[-1].wait_recv()
    finish(relay)
    for copy in [*core.values(), *first_a, first_b, second_a, *second_b, *third, *spread]:
        copy.wait_send()


def call(kernel, collective, ndp, nneg, out_shape, scratch, in_specs, megabytes=48):
    return pl.pallas_call(
        functools.partial(kernel, ndp, nneg),
        out_shape=out_shape,
        in_specs=in_specs,
        out_specs=tuple(vmem for _ in out_shape),
        scratch_shapes=scratch,
        compiler_params=pltpu.CompilerParams(
            collective_id=collective, has_side_effects=True, vmem_limit_bytes=megabytes * 1024 * 1024
        ),
    )


def sems(*counts):
    return [pltpu.SemaphoreType.DMA((count,)) for count in counts]


def to_packed(gradient, ndp):
    rows, columns = gradient.shape
    blocks = gradient.astype(jnp.bfloat16).reshape(ndp, rows // ndp, columns)
    return [blocks[:, :, c : c + pack_columns] for c in range(0, columns, pack_columns)]


step_inputs = (
    "query_features", "positive_features", "negative_features", "positive_ids", "positive_counts", "negative_ids",
    "negative_counts", "query_first", "query_second", "query_third", "item_first", "item_second", "item_third",
)


def step_kernel(ndp, nneg, names, groups, *refs):
    refs = list(refs)
    inputs = dict(zip(step_inputs, refs))
    stats_ref, gathered = refs[13], refs[14:18]
    (
        sources, q_unit, n_unit, p_unit, towers, grads, pexp, logit,
        q_land, n_land, meta_out, meta, rows, pid_out, pid_land, pid_col, w, den, dpart, dland, scaled,
        q_out, q_part, q_in, c_out, c_in, own, out, lx, ly, l2y, l2x,
        sx, sy, rn, sm, rm, sr, sl, rq, s_meta, r_meta, s_pid, r_pid, sd, rd, sq, rqs,
        sc, rc, s1x, r1x, s1y, r1y, s2y, r2y, s2x, r2x, loaded,
        scratch, bufs, stat_dp, stat_dp_land, stat_neg, stat_neg_land, ss, sr2, ts, tr,
    ) = jax.tree.unflatten(names, refs[18:])
    for buf, ref in zip(bufs, gathered):
        buf["ag"] = ref
    me_dp, me_neg = lax.axis_index("dp"), lax.axis_index("neg")
    line, nx = ndp // 2, nneg // 2
    place, side = me_dp // 2, lax.rem(me_dp, 2)
    me_x, me_core = me_neg // 2, lax.rem(me_neg, 2)
    far, other = 1 - side, 1 - me_core
    partner, mate = 2 * place + far, 2 * me_x + other
    f32, bf16 = jnp.float32, jnp.bfloat16
    rows_q, width = q_unit.shape
    block = 2 * n_unit.shape[1]
    half_n = block // 2
    lanes = den.shape[2]
    cuts = q_land.shape[1]
    half_w = width // 2
    blocks = nneg * 2
    here = (me_x * 2 + side) * 2 + me_core

    order = (
        "item_first", "negative_features", "item_second", "item_third", "query_features", "query_first", "query_second",
        "query_third", "positive_features", "negative_ids", "negative_counts", "positive_ids", "positive_counts",
    )
    item_features = sources["item_features"]
    places = dict(sources)
    places["negative_features"] = item_features.at[0:block]
    places["positive_features"] = item_features.at[block : block + rows_q]
    loads = {}
    for i, name in enumerate(order):
        loads[name] = pltpu.make_async_copy(inputs[name], places[name], loaded.at[i])
        loads[name].start()

    def along(k):
        return lax.rem(me_x + k, nx)

    def at_place(z):
        return 2 * z + side

    barrier = pltpu.get_barrier_semaphore()

    def quad(k):
        b = lax.rem(here + k, blocks)
        return {"dp": 2 * place + lax.rem(b // 2, 2), "neg": 2 * (b // 4) + lax.rem(b, 2)}

    for k in range(1, line):
        for y in range(2):
            target = 2 * lax.rem(place + k, line) + y
            pl.semaphore_signal(barrier, inc=1, device_id={"dp": target}, device_id_type=pl.DeviceIdType.MESH)
    for k in range(1, blocks):
        pl.semaphore_signal(barrier, inc=1, device_id=quad(k), device_id_type=pl.DeviceIdType.MESH)

    def slot(x, y, half):
        return (x * 2 + y) * 2 + half

    def piece(x, y, half):
        return n_land.at[(x * 2 + y) * 2 + me_core, half]

    def push(src, x, y, half, send_sems, index, axis, target):
        return link(src, piece(x, y, half), (send_sems, rn), slot(x, y, half), axis, target, index)

    def relay(src, x, y, half):
        i = slot(x, y, half)
        return link(src, piece(x, y, half), (sm, rm), i, "neg", mate)

    def landed(x, y, half):
        ref = piece(x, y, half)
        link(ref, ref, (sy, rn), slot(x, y, half), "neg", mate, 0).wait_recv()

    sends = []

    def go(copy):
        copy.start()
        sends.append(copy)

    def to_x(src, x, y, half, kind):
        for k in range(1, nx):
            go(push(src, x, y, half, sx, kind * nx + k, "neg", 2 * along(k) + me_core))

    def to_y(src, x, y, half, index):
        go(push(src, x, y, half, sy, index, "dp", partner))

    def chain(slot_z, j, distance, sems, target):
        src = q_unit.at[pl.ds(j * (rows_q // cuts), rows_q // cuts)] if distance == 0 else q_land.at[slot_z, j]
        return link(src, q_land.at[slot_z, j], (sems, rq), slot_z * cuts + j, "dp", target, distance * cuts + j)

    def right(distance, j):
        return chain(place - distance, j, distance, sr, at_place(lax.rem(place + 1, line)))

    def left(distance, j):
        return chain(place + distance, j, distance, sl, at_place(lax.rem(place + line - 1, line)))

    goes_right, goes_left = place < line - 1, place > 0

    def q_step(distance):
        for j in range(cuts):

            @pl.when(place >= distance)
            def _():
                ref = q_land.at[place - distance, j]
                link(ref, ref, (sr, rq), (place - distance) * cuts + j, "dp", partner, 0).wait_recv()
                pl.when(goes_right)(lambda: right(distance, j).start())

            @pl.when(place + distance < line)
            def _():
                ref = q_land.at[place + distance, j]
                link(ref, ref, (sl, rq), (place + distance) * cuts + j, "dp", partner, 0).wait_recv()
                pl.when(goes_left)(lambda: left(distance, j).start())

    def forward(lo, count, features, first, second, third, saved, unit_ref):
        act1, slope1, act2, slope2, emb = saved
        span = slice(lo, lo + count)

        def layer(source, weight, act, slope):
            columns = weight.shape[1]
            step = 512 if columns % 512 == 0 else columns
            for c in range(0, columns, step):
                pre = jnp.dot(source[span, :], weight[:, c : c + step], preferred_element_type=f32)
                sigma = jax.nn.sigmoid(pre)
                act[span, c : c + step] = (pre * sigma).astype(bf16)
                slope[span, c : c + step] = sigma * (1.0 + pre * (1.0 - sigma))

        layer(features, first, act1, slope1)
        layer(act1, second, act2, slope2)
        value = jnp.dot(act2[span, :], third[...], preferred_element_type=f32)
        emb[span, :] = value
        inv_norm = lax.rsqrt(jnp.sum(value * value, axis=1, keepdims=True) + 1.0)
        unit_ref[...] = (value * inv_norm).astype(bf16)

    item_weights = tuple(sources[name] for name in ("item_first", "item_second", "item_third"))
    query_weights = tuple(sources[name] for name in ("query_first", "query_second", "query_third"))
    for name in ("negative_ids", "negative_counts", "positive_ids", "item_first", "negative_features", "item_second", "item_third"):
        loads[name].wait()

    def own_ids(ref, index, count):
        return ref[:, pl.ds(pl.multiple_of(index * count, count), count)]

    meta_out[0:1, :] = own_ids(sources["negative_ids"], me_dp, block)
    meta_out[1:2, :] = own_ids(sources["negative_counts"], me_dp, block)
    pid_out[...] = own_ids(sources["positive_ids"], me_neg, rows_q)
    meta[here] = meta_out[...]
    pid_land[place] = pid_out[...]
    forward(0, half_n, item_features, *item_weights, towers[1], n_unit.at[0])
    pl.semaphore_wait(barrier, 2 * (line - 1) + (blocks - 1))
    for k in range(1, blocks):
        copy = pltpu.make_async_remote_copy(
            src_ref=meta_out, dst_ref=meta.at[here], send_sem=s_meta.at[k], recv_sem=r_meta.at[here],
            device_id=quad(k), device_id_type=pl.DeviceIdType.MESH,
        )
        go(copy)
    for k in range(1, line):
        z = lax.rem(place + k, line)
        go(link(pid_out, pid_land.at[place], (s_pid, r_pid), place, "dp", at_place(z), k))
    n_first, n_second = n_unit.at[0], n_unit.at[1]
    to_x(n_first, me_x, side, 0, 0)
    to_y(n_first, me_x, side, 0, 1)
    go(relay(n_first, me_x, side, 0))
    n_land[here, 0] = n_unit[0]
    for name in ("query_features", "query_first", "query_second", "query_third"):
        loads[name].wait()
    forward(0, rows_q, sources["query_features"], *query_weights, towers[0], q_unit)
    for j in range(cuts):
        pl.when(goes_right)(lambda j=j: right(0, j).start())
        pl.when(goes_left)(lambda j=j: left(0, j).start())
    for j in range(cuts):
        q_land[place, j] = q_unit[pl.ds(j * (rows_q // cuts), rows_q // cuts), :]
    forward(half_n, half_n, item_features, *item_weights, towers[1], n_unit.at[1])
    to_y(n_second, me_x, side, 1, 0)
    to_x(n_second, me_x, side, 1, 1)
    go(relay(n_second, me_x, side, 1))
    n_land[here, 1] = n_unit[1]
    loads["positive_features"].wait()
    loads["positive_counts"].wait()
    forward(block, rows_q, item_features, *item_weights, towers[1], p_unit)
    product = q_unit[...].astype(f32) * p_unit[...].astype(f32)
    logit[...] = jnp.sum(product.T, axis=0, keepdims=True) * inv_temp - jnp.log(sources["positive_counts"][...].astype(f32))
    pexp[...] = jnp.exp(logit[...])

    for k in range(1, nx):
        x = along(k)
        landed(x, side, 0)
        to_y(piece(x, side, 0), x, side, 0, 1 + k)
        go(relay(piece(x, side, 0), x, side, 0))
    for k in range(1, blocks):
        b = lax.rem(here + k, blocks)
        link(meta.at[b], meta.at[b], (s_meta, r_meta), b, "neg", mate).wait_recv()
    for k in range(1, line):
        z = lax.rem(place + k, line)
        link(pid_land.at[z], pid_land.at[z], (s_pid, r_pid), z, "dp", partner).wait_recv()
    for b in range(blocks):
        rows[b, 0:1, :] = meta[b, 0:1, :].astype(f32)
        rows[b, 1:2, :] = jnp.log2(meta[b, 1:2, :].astype(f32))
    for z in range(line):
        pid_col[z] = jnp.broadcast_to(pid_land[z].astype(f32), (lanes, rows_q)).T
        den[z] = jnp.zeros((rows_q, lanes), f32)

    def unit(b, z):
        dots = contract_cols(q_land[z].reshape(rows_q, width), n_land[b].reshape(block, width))
        value = jnp.exp2(dots * (inv_temp * log2_e) - rows[b, 1:2, :])
        ids = jnp.concatenate([pid_col[z]] * (block // lanes), axis=1)
        value = jnp.where(ids != rows[b, 0:1, :], value, 0.0)
        w[b, z] = value.astype(jnp.bfloat16)
        total = den[z]
        for c in range(0, block, lanes):
            total = total + value[:, c : c + lanes]
        den[z] = total

    def relayed(x, y):
        for half in range(2):
            ref = n_land.at[(x * 2 + y) * 2 + other, half]
            link(ref, ref, (sm, rm), slot(x, y, half), "neg", mate).wait_recv()

    def both_cores(x, y):
        return [(x * 2 + y) * 2 + core for core in range(2)]

    near_blocks = both_cores(me_x, side)
    mid_blocks = both_cores(me_x, far)
    far_blocks = []
    for k in range(1, nx):
        mid_blocks = mid_blocks + both_cores(along(k), side)
        far_blocks = far_blocks + both_cores(along(k), far)

    def units(lo, hi, chosen):
        def body(z, carry):
            for b in chosen:
                unit(b, z)
            return carry

        lax.fori_loop(jnp.maximum(lo, 0), jnp.minimum(hi, line), body, 0)

    relayed(me_x, side)
    units(place, place + 1, near_blocks)
    q_step(1)
    units(place - 1, place, near_blocks)
    units(place + 1, place + 2, near_blocks)
    landed(me_x, far, 1)
    to_x(piece(me_x, far, 1), me_x, far, 1, 2)
    go(relay(piece(me_x, far, 1), me_x, far, 1))
    landed(me_x, far, 0)
    go(relay(piece(me_x, far, 0), me_x, far, 0))
    for k in range(1, nx):
        x = along(k)
        landed(x, side, 1)
        go(relay(piece(x, side, 1), x, side, 1))
    q_step(2)
    relayed(me_x, far)
    for k in range(1, nx):
        relayed(along(k), side)
    units(place - 1, place + 2, mid_blocks)
    units(place - 2, place - 1, near_blocks + mid_blocks)
    units(place + 2, place + 3, near_blocks + mid_blocks)
    for half in range(2):
        for k in range(1, nx):
            x = along(k)
            landed(x, far, half)
            go(relay(piece(x, far, half), x, far, half))
    for distance in range(3, line):
        q_step(distance)
    for k in range(1, nx):
        relayed(along(k), far)
    units(place - 2, place + 3, far_blocks)
    units(0, place - 2, near_blocks + mid_blocks + far_blocks)
    units(place + 3, line, near_blocks + mid_blocks + far_blocks)
    for z in range(line):
        dpart[z] = jnp.sum(den[z].T, axis=0, keepdims=True)
    dpart[place] = dpart[place] + pexp[...]
    for k in range(1, line):
        z = lax.rem(place + k, line)
        go(link(dpart, dland.at[place], (sd, rd), place, "dp", at_place(z), k))

    def q_block(z):
        if block % 128 == 0:
            left_side = jnp.concatenate([w[b, z] for b in range(blocks)], axis=1)
            return jnp.dot(
                left_side, n_land[...].reshape(blocks * block, width), preferred_element_type=jnp.float32
            )
        total = jnp.zeros((rows_q, width), jnp.float32)
        for b in range(blocks):
            total = total + jnp.dot(w[b, z], n_land[b].reshape(block, width), preferred_element_type=jnp.float32)
        return total

    def q_send(k, z):
        return link(q_out.at[z], q_in.at[place], (sq, rqs), place, "dp", at_place(z), k)

    def q_push(k, carry):
        z = lax.rem(place + k, line)
        q_out[z] = q_block(z).astype(jnp.bfloat16)
        q_send(k, z).start()
        return carry

    lax.fori_loop(1, line, q_push, 0)
    q_part[...] = q_block(place)
    total = dpart[...]
    for k in range(1, line):
        z = lax.rem(place + k, line)
        link(dland.at[z], dland.at[z], (sd, rd), z, "dp", partner).wait_recv()
        total = total + dland[z]
    dpart2 = 1.0 / total
    for z in range(line):
        q_t = q_land[z].reshape(rows_q, width).astype(jnp.float32).T
        scaled[:, z * rows_q : (z + 1) * rows_q] = (q_t * dpart2[z]).astype(jnp.bfloat16)
    def dest(i):
        x = lax.rem(me_x + 1 + i // 2, nx)
        y = lax.rem(side + 1 + lax.rem(i, 2), 2)
        return x, y

    def part(x, y, core):
        return jnp.dot(
            scaled[...], w[(x * 2 + y) * 2 + core].reshape(line * rows_q, block), preferred_element_type=jnp.float32
        )

    def c_send(i):
        x, y = dest(i)
        return link(c_out.at[x, y], c_in.at[x, y], (sc, rc), x * 2 + y, "neg", mate)

    def far_step(i, carry):
        x, y = dest(i)
        c_out[x, y] = part(x, y, other).astype(jnp.bfloat16).reshape(2, half_w, block)
        c_send(i).start()
        return carry

    def send_1x(i):
        x, y = dest(i)
        return link(out.at[x, y, 0], lx.at[me_x, y], (s1x, r1x), me_x * 2 + y, "neg", 2 * x + me_core, x * 2 + y)

    def send_1y(i):
        x, y = dest(i)
        return link(out.at[x, y, 1], ly.at[x], (s1y, r1y), x, "dp", partner)

    def own_step(i, carry):
        x, y = dest(i)
        value = part(x, y, me_core).reshape(2, half_w, block)
        link(c_in.at[x, y], c_in.at[x, y], (sc, rc), x * 2 + y, "neg", mate).wait_recv()
        value = value + c_in[x, y].astype(jnp.float32)
        own[x, y] = value

        @pl.when(i < 2 * (nx - 1))
        def _():
            out[x, y, 0] = value[0].astype(jnp.bfloat16)
            send_1x(i).start()

        @pl.when(lax.rem(i, 2) == 0)
        def _():
            out[x, y, 1] = value[1].astype(jnp.bfloat16)
            send_1y(i).start()

        return carry

    lax.fori_loop(0, 2 * nx, far_step, 0)
    lax.fori_loop(0, 2 * nx, own_step, 0)
    value = own[me_x, far, 0]
    for k in range(1, nx):
        x = along(k)
        ref = lx.at[x, far]
        link(ref, ref, (s1x, r1x), x * 2 + far, "neg", mate).wait_recv()
        value = value + lx[x, far].astype(jnp.float32)
    out[me_x, far, 0] = value.astype(jnp.bfloat16)
    go(link(out.at[me_x, far, 0], l2y, (s2y, r2y), 0, "dp", partner))
    for k in range(1, nx):
        x = along(k)
        link(ly.at[x], ly.at[x], (s1y, r1y), x, "dp", partner).wait_recv()
        out[x, side, 1] = (own[x, side, 1] + ly[x].astype(jnp.float32)).astype(jnp.bfloat16)
        go(link(out.at[x, side, 1], l2x.at[me_x], (s2x, r2x), me_x, "neg", 2 * x + me_core, x))
    denom = dpart[place]
    for k in range(1, line):
        denom = denom + dland[lax.rem(place + k, line), place]
    loss_part = jnp.sum(jnp.log(denom) - logit[...])

    def to_columns(row):
        column = jnp.broadcast_to(row, (lanes, rows_q)).T
        return jnp.concatenate([column] * (width // lanes), axis=1)

    slope_columns = to_columns(pexp[...] / denom - 1.0) * inv_temp
    grads[1][block : block + rows_q, :] = slope_columns * q_unit[...].astype(f32)
    result = q_part[...]
    for k in range(1, line):
        z = lax.rem(place + k, line)
        link(q_in.at[z], q_in.at[z], (sq, rqs), z, "dp", partner).wait_recv()
        result = result + q_in[z].astype(jnp.float32)
    grads[0][...] = result * (to_columns(1.0 / denom) * inv_temp) + slope_columns * p_unit[...].astype(f32)

    pending = []

    def queue(copy):
        copy.start()
        pending.append(copy)

    def x_of(k):
        return lax.rem(me_x + k, nx)

    def same_core(x):
        return 2 * x + me_core

    def z_of(k):
        return lax.rem(place + k, line)

    def arrived(ref, sem_array, index):
        link(ref, ref, (sem_array, sem_array), index, "neg", mate).wait_recv()

    steps = [
        (sources["query_features"], *towers[0], grads[0], sources["query_second"], sources["query_third"]),
        (item_features, *towers[1], grads[1], sources["item_second"], sources["item_third"]),
    ]

    def store(group, offset, value, dp, hg):
        packed = bufs[group]["packed"]
        pieces = hg // nneg
        for p in range(value.shape[1] // pack_columns):
            part = value[:, p * pack_columns : (p + 1) * pack_columns].astype(bf16)
            part = part.reshape(value.shape[0] // hg, nx, 2, pieces, pack_columns)
            lo = offset + p * pieces
            for core in range(2):
                packed[core, pl.ds(dp, value.shape[0] // hg), :, lo : lo + pieces, :] = part[:, :, core]

    def weight_grad(group, offset, left_ref, right_ref):
        rows, columns = left_ref.shape[1], right_ref.shape[1]
        hg = rows // ndp
        step = 2 * hg

        def body(m, carry):
            left = left_ref[:, pl.ds(pl.multiple_of(m * step, step), step)]
            store(group, offset, contract_rows(left, right_ref[...]), 2 * m, hg)
            return carry

        lax.fori_loop(0, rows // step, body, 0)
        return offset + hg // nneg * (columns // pack_columns)

    def row_loop(count, body):
        step = 256 if count % 256 == 0 else count

        def wrapped(i, carry):
            body(pl.ds(pl.multiple_of(i * step, step), step))
            return carry

        lax.fori_loop(0, count // step, wrapped, 0)

    def embed_stage(t):
        feat, act1, slope1, act2, slope2, emb_ref, grad_ref, second, third = steps[t]
        eg, s2, s1 = scratch[t]

        def body(rows):
            emb, grad = emb_ref[rows, :], grad_ref[rows, :]
            inv_norm = lax.rsqrt(jnp.sum(emb * emb, axis=1, keepdims=True) + 1.0)
            along = jnp.sum(emb * grad, axis=1, keepdims=True)
            value = (inv_norm * grad - inv_norm * inv_norm * inv_norm * emb * along).astype(bf16)
            eg[rows, :] = value
            s2[rows, :] = (contract_cols(value, third[...]) * slope2[rows, :]).astype(bf16)

        row_loop(feat.shape[0], body)

    def second_stage(t, group):
        feat, act1, slope1, act2, slope2, emb_ref, grad_ref, second, third = steps[t]
        eg, s2, s1 = scratch[t]
        offset = weight_grad(group, 0, act2, eg)
        weight_grad(group, offset, act1, s2)

    def slope_stage(t):
        feat, act1, slope1, act2, slope2, emb_ref, grad_ref, second, third = steps[t]
        eg, s2, s1 = scratch[t]
        columns = second.shape[0]

        def body(rows):
            for c in range(0, columns, 512):
                value = contract_cols(s2[rows, :], second[c : c + 512, :]) * slope1[rows, c : c + 512]
                s1[rows, c : c + 512] = value.astype(bf16)

        row_loop(feat.shape[0], body)

    def first_stage(t, group):
        weight_grad(group, 0, steps[t][0], scratch[t][2])

    def stage0(g):
        b = bufs[g]
        queue(link(b["packed"].at[other], b["c_in"], (b["cs"], b["cr"]), 0, "neg", mate))

    def base(b, dp, x, lo, hi):
        return b["packed"][me_core, dp, x, lo:hi, :].astype(f32) + b["c_in"][dp, x, lo:hi, :].astype(f32)

    def loop(count, body):
        def wrapped(i, carry):
            body(i)
            return carry

        lax.fori_loop(0, count, wrapped, 0)

    def stage1(g):
        b, (r1, r) = bufs[g], groups[g]
        arrived(b["c_in"], b["cr"], 0)
        for k in range(1, nx):
            x = x_of(k)

            def body(dp):
                b["o1x"][x, dp] = base(b, dp, x, 0, r1).astype(bf16)

            loop(ndp, body)
            queue(link(b["o1x"].at[x], b["l1x"].at[me_x], (b["s1x"], b["r1x"]), me_x, "neg", same_core(x), x))

        def body_y(z):
            for x in range(nx):
                b["o1y"][z, x] = base(b, 2 * z + far, x, r1, r).astype(bf16)

        loop(line, body_y)
        queue(link(b["o1y"], b["l1y"], (b["s1y"], b["r1y"]), 0, "dp", partner))

    def low(b, dp, r1):
        value = base(b, dp, me_x, 0, r1)
        for k in range(1, nx):
            value = value + b["l1x"][x_of(k), dp].astype(f32)
        return value

    def stage2(g):
        b, (r1, r) = bufs[g], groups[g]
        for k in range(1, nx):
            x = x_of(k)
            arrived(b["l1x"].at[x], b["r1x"], x)

        def body(z):
            b["o2y"][z] = low(b, 2 * z + far, r1).astype(bf16)

        loop(line, body)
        queue(link(b["o2y"], b["l2y"], (b["s2y"], b["r2y"]), 0, "dp", partner))
        arrived(b["l1y"], b["r1y"], 0)
        for k in range(1, nx):
            x = x_of(k)

            def body_x(z):
                value = base(b, 2 * z + side, x, r1, r) + b["l1y"][z, x].astype(f32)
                b["o2x"][x, z] = value.astype(bf16)

            loop(line, body_x)
            queue(link(b["o2x"].at[x], b["l2x"].at[me_x], (b["s2x"], b["r2x"]), me_x, "neg", same_core(x), x))

    def stage3(g):
        b, (r1, r) = bufs[g], groups[g]
        arrived(b["l2y"], b["r2y"], 0)
        for k in range(1, nx):
            x = x_of(k)
            arrived(b["l2x"].at[x], b["r2x"], x)

        def body(z):
            dp = 2 * z + side
            b["zs"][z, 0:r1, :] = (low(b, dp, r1) + b["l2y"][z].astype(f32)).astype(bf16)
            value = base(b, dp, me_x, r1, r) + b["l1y"][z, me_x].astype(f32)
            for k in range(1, nx):
                value = value + b["l2x"][x_of(k), z].astype(f32)
            b["zs"][z, r1:r, :] = value.astype(bf16)

        loop(line, body)
        for k in range(1, line):
            z = z_of(k)
            queue(link(b["zs"].at[z], b["l3"].at[place], (b["s3"], b["r3"]), place, "dp", 2 * z + side, z))

    squares = []

    def stage4(g):
        b = bufs[g]
        for k in range(1, line):
            z = z_of(k)
            arrived(b["l3"].at[z], b["r3"], z)
        value = b["zs"][place].astype(f32)
        for k in range(1, line):
            value = value + b["l3"][z_of(k)].astype(f32)
        squares.append(jnp.sum(value * value))
        b["ag"][me_neg] = value.astype(bf16)
        mine = b["ag"].at[me_neg]
        for k in range(1, nx):
            x = x_of(k)
            queue(link(mine, mine, (b["sg"], b["rg"]), me_x, "neg", same_core(x), x))
        queue(link(mine, mine, (b["sh"], b["rh"]), me_x, "neg", mate))

    def stage5(g):
        b = bufs[g]
        for k in range(1, nx):
            x = x_of(k)
            ref = b["ag"].at[same_core(x)]
            arrived(ref, b["rg"], x)
            queue(link(ref, ref, (b["sh"], b["rh"]), x, "neg", mate))

    def stage6(g):
        b = bufs[g]
        for x in range(nx):
            arrived(b["ag"].at[2 * x + other], b["rh"], x)

    embed_stage(0)
    second_stage(0, 0)
    stage0(0)
    slope_stage(0)
    first_stage(0, 1)
    stage0(1)
    n_low = own[me_x, side, 0]
    for k in range(1, nx):
        x = along(k)
        ref = lx.at[x, side]
        link(ref, ref, (s1x, r1x), x * 2 + side, "neg", mate).wait_recv()
        n_low = n_low + lx[x, side].astype(jnp.float32)
    link(ly.at[me_x], ly.at[me_x], (s1y, r1y), me_x, "dp", partner).wait_recv()
    n_high = own[me_x, side, 1] + ly[me_x].astype(jnp.float32)
    link(l2y, l2y, (s2y, r2y), 0, "dp", partner).wait_recv()
    n_low = n_low + l2y[...].astype(jnp.float32)
    for k in range(1, nx):
        x = along(k)
        link(l2x.at[x], l2x.at[x], (s2x, r2x), x, "neg", mate).wait_recv()
        n_high = n_high + l2x[x].astype(jnp.float32)

    grads[1][0:block, 0:half_w] = n_low.T * inv_temp
    grads[1][0:block, half_w:width] = n_high.T * inv_temp
    stage1(0)
    embed_stage(1)
    stage1(1)
    second_stage(1, 2)
    stage0(2)
    stage2(0)
    slope_stage(1)
    stage1(2)
    stage2(1)
    first_stage(1, 3)
    stage0(3)
    stage3(0)
    stage1(3)
    stage3(1)
    stage2(2)
    stage4(0)
    stage2(3)
    stage4(1)
    stage3(2)
    stage3(3)
    stage4(2)
    stage4(3)
    total_squares = squares[0] + squares[1] + squares[2] + squares[3]
    lane = lax.broadcasted_iota(jnp.int32, (8, 128), 1)
    stat_dp[...] = jnp.where(lane == 0, total_squares, loss_part)
    stat_copies = share("dp", ndp, me_dp, lambda t: stat_dp, stat_dp_land, ss, sr2)
    for g in range(4):
        stage5(g)
    finish(stat_copies)
    total = stat_dp[...]
    for k in range(1, ndp):
        total = total + stat_dp_land[lax.rem(me_dp + k, ndp)]
    stat_neg[...] = total
    stat_copies = share("neg", nneg, me_neg, lambda t: stat_neg, stat_neg_land, ts, tr)
    for g in range(4):
        stage6(g)
    finish(stat_copies)
    total = stat_neg[...]
    for k in range(1, nneg):
        total = total + stat_neg_land[lax.rem(me_neg + k, nneg)]
    stats_ref[...] = total
    for copy in pending:
        copy.wait_send()


    for copy in sends:
        copy.wait_send()
    for distance in range(line):
        for j in range(cuts):
            if distance < line - 1:
                pl.when((place >= distance) & goes_right)(lambda: right(distance, j).wait_send())
                pl.when((place + distance < line) & goes_left)(lambda: left(distance, j).wait_send())
    for k in range(1, line):
        q_send(k, lax.rem(place + k, line)).wait_send()
    for i in range(2 * nx):
        c_send(i).wait_send()
        if i < 2 * (nx - 1):
            send_1x(i).wait_send()
        if i % 2 == 0:
            send_1y(i).wait_send()


def fused_step(ndp, nneg, arguments):
    line, nx = ndp // 2, nneg // 2
    bf16, f32, i32 = jnp.bfloat16, jnp.float32, jnp.int32
    named = dict(zip(step_inputs, arguments))
    fin, h1 = named["item_first"].shape
    h2, width = named["item_third"].shape
    own_rows, block = named["query_features"].shape[0], named["negative_features"].shape[0]
    blocks, cuts, lanes = 2 * nneg, 2, 128
    rows_half = (width // 2, block)
    sources = {"item_features": pltpu.VMEM((block + own_rows, fin), bf16)}
    for name, value in named.items():
        if name not in ("positive_features", "negative_features"):
            sources[name] = pltpu.VMEM(value.shape, value.dtype)
    counts = (own_rows, block + own_rows)
    towers = [
        [
            pltpu.VMEM((count, h1), bf16), pltpu.VMEM((count, h1), f32), pltpu.VMEM((count, h2), bf16),
            pltpu.VMEM((count, h2), f32), pltpu.VMEM((count, width), f32),
        ]
        for count in counts
    ]
    scratch = [
        [pltpu.VMEM((count, width), bf16), pltpu.VMEM((count, h2), bf16), pltpu.VMEM((count, h1), bf16)]
        for count in counts
    ]
    row = pltpu.VMEM((1, own_rows), f32)
    score = [
        pltpu.VMEM((line, cuts, own_rows // cuts, width), bf16),
        pltpu.VMEM((blocks, 2, block // 2, width), bf16),
        pltpu.VMEM((2, block), i32),
        pltpu.VMEM((blocks, 2, block), i32),
        pltpu.VMEM((blocks, 2, block), f32),
        pltpu.VMEM((1, own_rows), i32),
        pltpu.VMEM((line, 1, own_rows), i32),
        pltpu.VMEM((line, own_rows, lanes), f32),
        pltpu.VMEM((blocks, line, own_rows, block), bf16),
        pltpu.VMEM((line, own_rows, lanes), f32),
        pltpu.VMEM((line, 1, own_rows), f32),
        pltpu.VMEM((line, line, 1, own_rows), f32),
        pltpu.VMEM((width, line * own_rows), bf16),
        pltpu.VMEM((line, own_rows, width), bf16),
        pltpu.VMEM((own_rows, width), f32),
        pltpu.VMEM((line, own_rows, width), bf16),
        pltpu.VMEM((nx, 2, 2) + rows_half, bf16),
        pltpu.VMEM((nx, 2, 2) + rows_half, bf16),
        pltpu.VMEM((nx, 2, 2) + rows_half, f32),
        pltpu.VMEM((nx, 2, 2) + rows_half, bf16),
        pltpu.VMEM((nx, 2) + rows_half, bf16),
        pltpu.VMEM((nx,) + rows_half, bf16),
        pltpu.VMEM(rows_half, bf16),
        pltpu.VMEM((nx,) + rows_half, bf16),
    ] + sems(
        3 * nx, 1 + nx, 4 * nx, 4 * nx, 4 * nx, line * cuts, line * cuts, line * cuts,
        blocks, blocks, line, line, line, line, line, line,
        2 * nx, 2 * nx, 2 * nx, 2 * nx, nx, nx, 1, 1, nx, nx, len(step_inputs),
    )
    groups, outs, bufs = [], [], []
    for _ in counts:
        for height, columns in ((fin, h1), (h1, h2), (h2, width)):
            outs.append(jax.ShapeDtypeStruct((height // ndp, columns), f32))
        both = h2 // (ndp * nneg) * (width // pack_columns) + h1 // (ndp * nneg) * (h2 // pack_columns)
        alone = fin // (ndp * nneg) * (h1 // pack_columns)
        for r in (both, alone):
            groups.append((max((r * 4 + 72) // 144, 1) * 16, r))
    c = pack_columns
    sem_names = ["cs", "cr", "s1x", "r1x", "s1y", "r1y", "s2y", "r2y", "s2x", "r2x", "s3", "r3", "sg", "rg", "sh", "rh"]
    for r1, r in groups:
        r2 = r - r1
        shapes = dict(
            packed=(2, ndp, nx, r, c), c_in=(ndp, nx, r, c), o1x=(nx, ndp, r1, c), l1x=(nx, ndp, r1, c),
            o1y=(line, nx, r2, c), l1y=(line, nx, r2, c), o2y=(line, r1, c), l2y=(line, r1, c),
            o2x=(nx, line, r2, c), l2x=(nx, line, r2, c), zs=(line, r, c), l3=(line, r, c),
        )
        buf = {name: pltpu.VMEM(shape, bf16) for name, shape in shapes.items()}
        buf.update(zip(sem_names, sems(1, 1, nx, nx, 1, 1, 1, 1, nx, nx, line, line, nx, nx, nx, nx)))
        bufs.append(buf)
    tree = (
        sources, pltpu.VMEM((own_rows, width), bf16), pltpu.VMEM((2, block // 2, width), bf16),
        pltpu.VMEM((own_rows, width), bf16), towers, [pltpu.VMEM((count, width), f32) for count in counts], row, row,
        *score, scratch, bufs,
        pltpu.VMEM((8, 128), f32), pltpu.VMEM((ndp, 8, 128), f32), pltpu.VMEM((8, 128), f32), pltpu.VMEM((nneg, 8, 128), f32),
        *sems(ndp, ndp, nneg, nneg),
    )
    leaves, names = jax.tree.flatten(tree)
    any_space = pl.BlockSpec(memory_space=pl.ANY)
    stats, *gathered = pl.pallas_call(
        functools.partial(step_kernel, ndp, nneg, names, tuple(groups)),
        out_shape=(
            jax.ShapeDtypeStruct((8, 128), f32),
            *[jax.ShapeDtypeStruct((nneg, r, pack_columns), bf16) for _, r in groups],
        ),
        in_specs=[any_space] * len(arguments),
        out_specs=(vmem,) * 5,
        scratch_shapes=leaves,
        compiler_params=pltpu.CompilerParams(
            collective_id=1, has_side_effects=True, vmem_limit_bytes=67043328
        ),
    )(*arguments)
    mean_loss, *clipped = pl.pallas_call(
        functools.partial(finish_kernel, nneg, own_rows * ndp * nneg),
        out_shape=(jax.ShapeDtypeStruct((1,), f32), *outs),
        in_specs=[vmem] * 5,
        out_specs=(pl.BlockSpec(memory_space=pltpu.SMEM), *([any_space] * 6)),
        scratch_shapes=[pltpu.VMEM(out.shape, f32) for out in outs] + sems(6),
    )(stats, *gathered)
    return (mean_loss.reshape(()), *clipped)


def finish_kernel(nneg, count, stats_ref, *refs):
    gathered, loss_ref, outs, staged, done = refs[:4], refs[4], refs[5:11], refs[11:17], refs[17]
    clip = clip_norm / jnp.maximum(jnp.sqrt(stats_ref[0:1, 0:1]), clip_norm)
    copies = []
    for t in range(2):
        third_ref, second_ref, first_ref = staged[3 * t + 2], staged[3 * t + 1], staged[3 * t]
        for index, group, ref, offset in (
            (3 * t + 1, 2 * t, second_ref, third_ref.shape[0] // nneg),
            (3 * t, 2 * t + 1, first_ref, 0),
            (3 * t + 2, 2 * t, third_ref, 0),
        ):
            pieces = ref.shape[0] // nneg
            for p in range(ref.shape[1] // pack_columns):
                lo = offset + p * pieces
                for n in range(nneg):
                    value = gathered[group][n, lo : lo + pieces, :].astype(jnp.float32) * clip
                    ref[n * pieces : (n + 1) * pieces, p * pack_columns : (p + 1) * pack_columns] = value
            copy = pltpu.make_async_copy(ref, outs[index], done.at[index])
            copy.start()
            copies.append(copy)
    loss_ref[0] = jnp.sum(stats_ref[0:1, 1:2]) / count
    for copy in copies:
        copy.wait()


def per_device(
    query_features,
    positive_features,
    negative_features,
    positive_ids,
    positive_counts,
    negative_ids,
    negative_counts,
    query_first,
    query_second,
    query_third,
    item_first,
    item_second,
    item_third,
):
    own_rows = query_features.shape[0]
    ndp, nneg = lax.axis_size("dp"), lax.axis_size("neg")
    heights = (query_first.shape[0], query_second.shape[0], query_third.shape[0])
    tiled = all(height % (16 * ndp * nneg) == 0 for height in heights)
    if tiled and own_rows % 256 == 0 and negative_features.shape[0] % 256 == 0:
        return fused_step(
            ndp,
            nneg,
            (
                query_features, positive_features, negative_features, positive_ids.reshape(1, -1),
                positive_counts.reshape(1, -1), negative_ids.reshape(1, -1), negative_counts.reshape(1, -1),
                query_first, query_second, query_third, item_first, item_second, item_third,
            ),
        )
    query_saved, query_unit = tower_forward(query_features, query_first, query_second, query_third)
    item_features = jnp.concatenate([positive_features, negative_features], axis=0)
    item_saved, item_unit = tower_forward(item_features, item_first, item_second, item_third)
    positive_unit = item_unit[:own_rows]
    negative_unit = item_unit[own_rows:]
    ndp, nneg = lax.axis_size("dp"), lax.axis_size("neg")
    width = query_unit.shape[1]
    line, nx = ndp // 2, nneg // 2
    block = negative_unit.shape[0]
    blocks, cuts, lanes = 2 * nneg, 2, min(block, 128)
    bf16, f32, i32 = jnp.bfloat16, jnp.float32, jnp.int32
    positive_logit = jnp.sum(
        query_unit.astype(f32) * positive_unit.astype(f32), axis=1
    ) * inv_temp - jnp.log(positive_counts.astype(f32))
    positive_exp = jnp.exp(positive_logit)
    rows_half = (width // 2, block)
    query_total, denom, negative_sum = call(
        score_kernel,
        0,
        ndp,
        nneg,
        (
            jax.ShapeDtypeStruct((own_rows, width), f32),
            jax.ShapeDtypeStruct((1, own_rows), f32),
            jax.ShapeDtypeStruct((2,) + rows_half, f32),
        ),
        [
            pltpu.VMEM((line, cuts, own_rows // cuts, width), bf16),
            pltpu.VMEM((blocks, 2, block // 2, width), bf16),
            pltpu.VMEM((2, block), i32),
            pltpu.VMEM((blocks, 2, block), i32),
            pltpu.VMEM((blocks, 2, block), f32),
            pltpu.VMEM((1, own_rows), i32),
            pltpu.VMEM((line, 1, own_rows), i32),
            pltpu.VMEM((line, own_rows, lanes), f32),
            pltpu.VMEM((blocks, line, own_rows, block), bf16),
            pltpu.VMEM((line, own_rows, lanes), f32),
            pltpu.VMEM((line, 1, own_rows), f32),
            pltpu.VMEM((line, line, 1, own_rows), f32),
            pltpu.VMEM((width, line * own_rows), bf16),
            pltpu.VMEM((line, own_rows, width), bf16),
            pltpu.VMEM((own_rows, width), f32),
            pltpu.VMEM((line, own_rows, width), bf16),
            pltpu.VMEM((nx, 2, 2) + rows_half, bf16),
            pltpu.VMEM((nx, 2, 2) + rows_half, bf16),
            pltpu.VMEM((nx, 2, 2) + rows_half, f32),
            pltpu.VMEM((nx, 2, 2) + rows_half, bf16),
            pltpu.VMEM((nx, 2) + rows_half, bf16),
            pltpu.VMEM((nx,) + rows_half, bf16),
            pltpu.VMEM(rows_half, bf16),
            pltpu.VMEM((nx,) + rows_half, bf16),
        ]
        + sems(
            3 * nx, 1 + nx, 4 * nx, 4 * nx, 4 * nx, line * cuts, line * cuts, line * cuts,
            blocks, blocks, line, line, line, line, line, line,
            2 * nx, 2 * nx, 2 * nx, 2 * nx, nx, nx, 1, 1, nx, nx,
        ),
        [vmem] * 6,
        40,
    )(
        query_unit,
        negative_unit.reshape(2, block // 2, width),
        positive_ids.reshape((1, -1) if own_rows % 128 == 0 else (nneg, own_rows)),
        negative_ids.reshape((1, -1) if block % 128 == 0 else (ndp, block)),
        negative_counts.reshape((1, -1) if block % 128 == 0 else (ndp, block)),
        positive_exp.reshape(1, own_rows),
    )
    own_denom = denom.reshape(-1)
    loss_part = jnp.sum(jnp.log(own_denom) - positive_logit)
    positive_slope = positive_exp / own_denom - 1.0
    query_sum = query_total / own_denom[:, None]
    negative_sum = negative_sum.reshape(width, block).T
    query_grad = (
        query_sum + positive_slope[:, None] * positive_unit.astype(jnp.float32)
    ) * inv_temp
    positive_grad = positive_slope[:, None] * query_unit.astype(jnp.float32) * inv_temp
    item_grad = jnp.concatenate([positive_grad, negative_sum * inv_temp], axis=0)
    query_grads = tower_backward(query_features, query_second, query_third, query_saved, query_grad)
    item_grads = tower_backward(item_features, item_second, item_third, item_saved, item_grad)
    gradients = query_grads + item_grads
    parts = [part for gradient in gradients for part in to_packed(gradient, ndp)]
    packed = jnp.concatenate(parts, axis=1)
    rows = packed.shape[1] // nneg
    packed = packed.reshape(ndp, nneg, 2, rows // 2, pack_columns).transpose(1, 0, 2, 3, 4)
    piece = (rows // 2, pack_columns)
    gathered, stats = call(
        weight_kernel,
        3,
        ndp,
        nneg,
        (jax.ShapeDtypeStruct((nneg, 2) + piece, bf16), jax.ShapeDtypeStruct((8, 128), f32)),
        [
            pltpu.VMEM((nx, ndp, 2) + piece, bf16),
            pltpu.VMEM((nx, 2, line) + piece, bf16),
            pltpu.VMEM((2, nx, line) + piece, bf16),
            pltpu.VMEM((nx, 2, line) + piece, bf16),
            pltpu.VMEM((nx, line) + piece, bf16),
            pltpu.VMEM((2, line) + piece, bf16),
            pltpu.VMEM((nx, line) + piece, bf16),
            pltpu.VMEM((line,) + piece, bf16),
            pltpu.VMEM((nx, line) + piece, bf16),
            pltpu.VMEM((2, line) + piece, bf16),
            pltpu.VMEM((2, line) + piece, bf16),
            pltpu.VMEM((8, 128), f32),
            pltpu.VMEM((ndp, 8, 128), f32),
            pltpu.VMEM((8, 128), f32),
            pltpu.VMEM((nneg, 8, 128), f32),
        ]
        + sems(nx, nx, 2 * nx, 2 * nx, 2, 2, ndp, ndp, ndp, ndp, nneg, nneg, nx, nx, nx, nx),
        [vmem, pl.BlockSpec(memory_space=pltpu.SMEM)],
    )(packed, loss_part.reshape(1))
    grad_norm = jnp.sqrt(stats[0, 0])
    mean_loss = stats[0, 1] / (own_rows * ndp * nneg)
    clip_factor = clip_norm / jnp.maximum(grad_norm, clip_norm)
    flat = gathered.reshape(nneg * rows, pack_columns)
    clipped = []
    start = 0
    for gradient in gradients:
        height, columns = gradient.shape[0] // ndp, gradient.shape[1]
        groups = columns // pack_columns
        blocks = [flat[start + g * height : start + (g + 1) * height] for g in range(groups)]
        start += groups * height
        clipped.append(jnp.concatenate(blocks, axis=1).astype(jnp.float32) * clip_factor)
    return (mean_loss, *clipped)


def solution(mesh):
    placed = (
        P(("dp", "neg"), None),
        P(("dp", "neg"), None),
        P(("neg", "dp"), None),
        P("dp"),
        P(("dp", "neg")),
        P("neg"),
        P("neg"),
        P(),
        P(),
        P(),
        P(),
        P(),
        P(),
    )
    return jax.shard_map(
        per_device,
        mesh=mesh,
        in_specs=placed,
        out_specs=(
            P(),
            P("dp", None),
            P("dp", None),
            P("dp", None),
            P("dp", None),
            P("dp", None),
            P("dp", None),
        ),
        check_vma=False,
    )
```

```python
import functools

import jax
import jax.numpy as jnp
from jax import lax
from jax.experimental import pallas as pl
from jax.experimental.pallas import tpu as pltpu
from jax.sharding import PartitionSpec as P

inv_temp = 20.0
log2_e = 1.4426950408889634
clip_norm = 256.0


def silu_slope(pre):
    sigma = jax.nn.sigmoid(pre)
    return sigma * (1.0 + pre * (1.0 - sigma))


def contract_rows(left, right):
    return lax.dot_general(
        left, right, (((0,), (0,)), ((), ())), preferred_element_type=jnp.float32
    )


def contract_cols(left, right):
    return lax.dot_general(
        left, right, (((1,), (1,)), ((), ())), preferred_element_type=jnp.float32
    )


def tower_forward(features, first, second, third):
    first_pre = jnp.dot(features, first, preferred_element_type=jnp.float32)
    first_act = jax.nn.silu(first_pre).astype(jnp.bfloat16)
    second_pre = jnp.dot(first_act, second, preferred_element_type=jnp.float32)
    second_act = jax.nn.silu(second_pre).astype(jnp.bfloat16)
    embedding = jnp.dot(second_act, third, preferred_element_type=jnp.float32)
    inv_norm = lax.rsqrt(jnp.sum(embedding * embedding, axis=1, keepdims=True) + 1.0)
    unit = (embedding * inv_norm).astype(jnp.bfloat16)
    saved = (silu_slope(first_pre), first_act, silu_slope(second_pre), second_act, embedding, inv_norm)
    return saved, unit


def tower_backward(features, second, third, saved, unit_grad):
    first_slope, first_act, second_slope, second_act, embedding, inv_norm = saved
    along = jnp.sum(embedding * unit_grad, axis=1, keepdims=True)
    embed_grad = (inv_norm * unit_grad - inv_norm * inv_norm * inv_norm * embedding * along).astype(
        jnp.bfloat16
    )
    third_grad = contract_rows(second_act, embed_grad)
    second_step = (contract_cols(embed_grad, third) * second_slope).astype(jnp.bfloat16)
    second_grad = contract_rows(first_act, second_step)
    first_step = (contract_cols(second_step, second) * first_slope).astype(jnp.bfloat16)
    first_grad = contract_rows(features, first_step)
    return (first_grad, second_grad, third_grad)


pack_columns = 256
vmem = pl.BlockSpec(memory_space=pltpu.VMEM)


def greet(ndp, nneg, me_dp, me_neg):
    barrier = pltpu.get_barrier_semaphore()
    for k in range(1, nneg):
        pl.semaphore_signal(
            barrier, inc=1, device_id={"neg": lax.rem(me_neg + k, nneg)}, device_id_type=pl.DeviceIdType.MESH
        )
    for k in range(1, ndp):
        pl.semaphore_signal(
            barrier, inc=1, device_id={"dp": lax.rem(me_dp + k, ndp)}, device_id_type=pl.DeviceIdType.MESH
        )
    pl.semaphore_wait(barrier, (nneg - 1) + (ndp - 1))


def send(src, dst, send_sem, recv_sem, axis, target):
    copy = pltpu.make_async_remote_copy(
        src_ref=src,
        dst_ref=dst,
        send_sem=send_sem,
        recv_sem=recv_sem,
        device_id={axis: target},
        device_id_type=pl.DeviceIdType.MESH,
    )
    copy.start()
    return copy


def share(axis, n, me, src_of, dst, send_sem, recv_sem):
    return [
        send(src_of(lax.rem(me + k, n)), dst.at[me], send_sem.at[k], recv_sem.at[k], axis, lax.rem(me + k, n))
        for k in range(1, n)
    ]


def finish(copies):
    for copy in copies:
        copy.wait()


def link(src, dst, sems, index, axis, target, send_index=None):
    send_sems, recv_sems = sems
    return pltpu.make_async_remote_copy(
        src_ref=src,
        dst_ref=dst,
        send_sem=send_sems.at[index if send_index is None else send_index],
        recv_sem=recv_sems.at[index],
        device_id={axis: target},
        device_id_type=pl.DeviceIdType.MESH,
    )


def score_kernel(
    ndp, nneg, query_ref, negative_ref, pid_ref, nid_ref, count_ref, pexp_ref, sum_ref, denom_ref, nsum_ref,
    q_land, n_land, meta_out, meta, rows, pid_out, pid_land, pid_col, w, den, dpart, dland, scaled,
    q_out, q_part, q_in, c_out, c_in, own, out, lx, ly, l2y, l2x,
    sx, sy, rn, sm, rm, sr, sl, rq, s_meta, r_meta, s_pid, r_pid, sd, rd, sq, rqs,
    sc, rc, s1x, r1x, s1y, r1y, s2y, r2y, s2x, r2x,
):
    me_dp, me_neg = lax.axis_index("dp"), lax.axis_index("neg")
    line, nx = ndp // 2, nneg // 2
    place, side = me_dp // 2, lax.rem(me_dp, 2)
    me_x, me_core = me_neg // 2, lax.rem(me_neg, 2)
    far, other = 1 - side, 1 - me_core
    partner, mate = 2 * place + far, 2 * me_x + other
    rows_q, width = query_ref.shape
    block = 2 * negative_ref.shape[1]
    lanes = den.shape[2]
    cuts = q_land.shape[1]
    half_w = width // 2
    blocks = nneg * 2
    here = (me_x * 2 + side) * 2 + me_core

    def along(k):
        return lax.rem(me_x + k, nx)

    def at_place(z):
        return 2 * z + side

    barrier = pltpu.get_barrier_semaphore()
    for k in range(1, line):
        pl.semaphore_signal(
            barrier, inc=1, device_id={"dp": at_place(lax.rem(place + k, line))}, device_id_type=pl.DeviceIdType.MESH
        )

    def quad(k):
        b = lax.rem(here + k, blocks)
        return {"dp": 2 * place + lax.rem(b // 2, 2), "neg": 2 * (b // 4) + lax.rem(b, 2)}

    for k in range(1, blocks):
        pl.semaphore_signal(barrier, inc=1, device_id=quad(k), device_id_type=pl.DeviceIdType.MESH)
    def own_ids(ref, index, count):
        if count % 128 == 0:
            return ref[:, pl.ds(pl.multiple_of(index * count, count), count)]
        return ref[pl.ds(index, 1), :]

    meta_out[0:1, :] = own_ids(nid_ref, me_dp, block)
    meta_out[1:2, :] = own_ids(count_ref, me_dp, block)
    pid_out[...] = own_ids(pid_ref, me_neg, rows_q)
    pl.semaphore_wait(barrier, (line - 1) + (blocks - 1))

    def slot(x, y, half):
        return (x * 2 + y) * 2 + half

    def piece(x, y, half):
        return n_land.at[(x * 2 + y) * 2 + me_core, half]

    def push(src, x, y, half, send_sems, index, axis, target):
        return link(src, piece(x, y, half), (send_sems, rn), slot(x, y, half), axis, target, index)

    def relay(src, x, y, half):
        i = slot(x, y, half)
        return link(src, piece(x, y, half), (sm, rm), i, "neg", mate)

    def landed(x, y, half):
        ref = piece(x, y, half)
        link(ref, ref, (sy, rn), slot(x, y, half), "neg", mate, 0).wait_recv()

    sends = []

    def go(copy):
        copy.start()
        sends.append(copy)

    def to_x(src, x, y, half, kind):
        for k in range(1, nx):
            go(push(src, x, y, half, sx, kind * nx + k, "neg", 2 * along(k) + me_core))

    def to_y(src, x, y, half, index):
        go(push(src, x, y, half, sy, index, "dp", partner))

    first, second = negative_ref.at[0], negative_ref.at[1]
    to_x(first, me_x, side, 0, 0)
    to_y(second, me_x, side, 1, 0)
    to_x(second, me_x, side, 1, 1)
    to_y(first, me_x, side, 0, 1)
    go(relay(first, me_x, side, 0))
    go(relay(second, me_x, side, 1))

    def chain(slot_z, j, distance, sems, target):
        src = query_ref.at[pl.ds(j * (rows_q // cuts), rows_q // cuts)] if distance == 0 else q_land.at[slot_z, j]
        return link(src, q_land.at[slot_z, j], (sems, rq), slot_z * cuts + j, "dp", target, distance * cuts + j)

    def right(distance, j):
        return chain(place - distance, j, distance, sr, at_place(lax.rem(place + 1, line)))

    def left(distance, j):
        return chain(place + distance, j, distance, sl, at_place(lax.rem(place + line - 1, line)))

    goes_right, goes_left = place < line - 1, place > 0
    for j in range(cuts):
        pl.when(goes_right)(lambda j=j: right(0, j).start())
        pl.when(goes_left)(lambda j=j: left(0, j).start())
    for k in range(1, blocks):
        b = lax.rem(here + k, blocks)
        copy = pltpu.make_async_remote_copy(
            src_ref=meta_out, dst_ref=meta.at[here], send_sem=s_meta.at[k], recv_sem=r_meta.at[here],
            device_id=quad(k), device_id_type=pl.DeviceIdType.MESH,
        )
        go(copy)
    for k in range(1, line):
        z = lax.rem(place + k, line)
        go(link(pid_out, pid_land.at[place], (s_pid, r_pid), place, "dp", at_place(z), k))
    n_land[here] = negative_ref[...]
    for j in range(cuts):
        q_land[place, j] = query_ref[pl.ds(j * (rows_q // cuts), rows_q // cuts), :]
    meta[here] = meta_out[...]
    pid_land[place] = pid_out[...]

    for k in range(1, nx):
        x = along(k)
        landed(x, side, 0)
        to_y(piece(x, side, 0), x, side, 0, 1 + k)
        go(relay(piece(x, side, 0), x, side, 0))
    landed(me_x, far, 1)
    to_x(piece(me_x, far, 1), me_x, far, 1, 2)
    go(relay(piece(me_x, far, 1), me_x, far, 1))

    def q_step(distance):
        for j in range(cuts):

            @pl.when(place >= distance)
            def _():
                ref = q_land.at[place - distance, j]
                link(ref, ref, (sr, rq), (place - distance) * cuts + j, "dp", partner, 0).wait_recv()
                pl.when(goes_right)(lambda: right(distance, j).start())

            @pl.when(place + distance < line)
            def _():
                ref = q_land.at[place + distance, j]
                link(ref, ref, (sl, rq), (place + distance) * cuts + j, "dp", partner, 0).wait_recv()
                pl.when(goes_left)(lambda: left(distance, j).start())

    q_step(1)
    for k in range(1, nx):
        x = along(k)
        landed(x, side, 1)
        go(relay(piece(x, side, 1), x, side, 1))
    landed(me_x, far, 0)
    go(relay(piece(me_x, far, 0), me_x, far, 0))
    for distance in range(2, line):
        q_step(distance)
    for half in range(2):
        for k in range(1, nx):
            x = along(k)
            landed(x, far, half)
            go(relay(piece(x, far, half), x, far, half))
    for x in range(nx):
        for y in range(2):
            for half in range(2):
                i = slot(x, y, half)
                ref = n_land.at[(x * 2 + y) * 2 + other, half]
                link(ref, ref, (sm, rm), i, "neg", mate).wait_recv()
    for k in range(1, blocks):
        b = lax.rem(here + k, blocks)
        link(meta.at[b], meta.at[b], (s_meta, r_meta), b, "neg", mate).wait_recv()
    for k in range(1, line):
        z = lax.rem(place + k, line)
        link(pid_land.at[z], pid_land.at[z], (s_pid, r_pid), z, "dp", partner).wait_recv()

    for b in range(blocks):
        rows[b, 0:1, :] = meta[b, 0:1, :].astype(jnp.float32)
        rows[b, 1:2, :] = jnp.log2(meta[b, 1:2, :].astype(jnp.float32))
    for z in range(line):
        pid_col[z] = jnp.broadcast_to(pid_land[z].astype(jnp.float32), (lanes, rows_q)).T
        den[z] = jnp.zeros((rows_q, lanes), jnp.float32)

    def unit(b, z):
        dots = contract_cols(q_land[z].reshape(rows_q, width), n_land[b].reshape(block, width))
        value = jnp.exp2(dots * (inv_temp * log2_e) - rows[b, 1:2, :])
        ids = jnp.concatenate([pid_col[z]] * (block // lanes), axis=1)
        value = jnp.where(ids != rows[b, 0:1, :], value, 0.0)
        w[b, z] = value.astype(jnp.bfloat16)
        total = den[z]
        for c in range(0, block, lanes):
            total = total + value[:, c : c + lanes]
        den[z] = total

    def units(b, carry):
        for z in range(line):
            unit(b, z)
        return carry

    lax.fori_loop(0, blocks, units, 0)
    for z in range(line):
        dpart[z] = jnp.sum(den[z].T, axis=0, keepdims=True)
    dpart[place] = dpart[place] + pexp_ref[...]
    for k in range(1, line):
        z = lax.rem(place + k, line)
        go(link(dpart, dland.at[place], (sd, rd), place, "dp", at_place(z), k))

    def q_block(z):
        if block % 128 == 0:
            left_side = jnp.concatenate([w[b, z] for b in range(blocks)], axis=1)
            return jnp.dot(
                left_side, n_land[...].reshape(blocks * block, width), preferred_element_type=jnp.float32
            )
        total = jnp.zeros((rows_q, width), jnp.float32)
        for b in range(blocks):
            total = total + jnp.dot(w[b, z], n_land[b].reshape(block, width), preferred_element_type=jnp.float32)
        return total

    def q_send(k, z):
        return link(q_out.at[z], q_in.at[place], (sq, rqs), place, "dp", at_place(z), k)

    def q_push(k, carry):
        z = lax.rem(place + k, line)
        q_out[z] = q_block(z).astype(jnp.bfloat16)
        q_send(k, z).start()
        return carry

    lax.fori_loop(1, line, q_push, 0)
    q_part[...] = q_block(place)
    total = dpart[...]
    for k in range(1, line):
        z = lax.rem(place + k, line)
        link(dland.at[z], dland.at[z], (sd, rd), z, "dp", partner).wait_recv()
        total = total + dland[z]
    dpart2 = 1.0 / total
    for z in range(line):
        q_t = q_land[z].reshape(rows_q, width).astype(jnp.float32).T
        scaled[:, z * rows_q : (z + 1) * rows_q] = (q_t * dpart2[z]).astype(jnp.bfloat16)
    denom_ref[...] = dpart[place]
    for k in range(1, line):
        denom_ref[...] = denom_ref[...] + dland[lax.rem(place + k, line), place]

    def dest(i):
        x = lax.rem(me_x + 1 + i // 2, nx)
        y = lax.rem(side + 1 + lax.rem(i, 2), 2)
        return x, y

    def part(x, y, core):
        return jnp.dot(
            scaled[...], w[(x * 2 + y) * 2 + core].reshape(line * rows_q, block), preferred_element_type=jnp.float32
        )

    def c_send(i):
        x, y = dest(i)
        return link(c_out.at[x, y], c_in.at[x, y], (sc, rc), x * 2 + y, "neg", mate)

    def far_step(i, carry):
        x, y = dest(i)
        c_out[x, y] = part(x, y, other).astype(jnp.bfloat16).reshape(2, half_w, block)
        c_send(i).start()
        return carry

    def send_1x(i):
        x, y = dest(i)
        return link(out.at[x, y, 0], lx.at[me_x, y], (s1x, r1x), me_x * 2 + y, "neg", 2 * x + me_core, x * 2 + y)

    def send_1y(i):
        x, y = dest(i)
        return link(out.at[x, y, 1], ly.at[x], (s1y, r1y), x, "dp", partner)

    def own_step(i, carry):
        x, y = dest(i)
        value = part(x, y, me_core).reshape(2, half_w, block)
        link(c_in.at[x, y], c_in.at[x, y], (sc, rc), x * 2 + y, "neg", mate).wait_recv()
        value = value + c_in[x, y].astype(jnp.float32)
        own[x, y] = value

        @pl.when(i < 2 * (nx - 1))
        def _():
            out[x, y, 0] = value[0].astype(jnp.bfloat16)
            send_1x(i).start()

        @pl.when(lax.rem(i, 2) == 0)
        def _():
            out[x, y, 1] = value[1].astype(jnp.bfloat16)
            send_1y(i).start()

        return carry

    lax.fori_loop(0, 2 * nx, far_step, 0)
    lax.fori_loop(0, 2 * nx, own_step, 0)
    value = own[me_x, far, 0]
    for k in range(1, nx):
        x = along(k)
        ref = lx.at[x, far]
        link(ref, ref, (s1x, r1x), x * 2 + far, "neg", mate).wait_recv()
        value = value + lx[x, far].astype(jnp.float32)
    out[me_x, far, 0] = value.astype(jnp.bfloat16)
    go(link(out.at[me_x, far, 0], l2y, (s2y, r2y), 0, "dp", partner))
    for k in range(1, nx):
        x = along(k)
        link(ly.at[x], ly.at[x], (s1y, r1y), x, "dp", partner).wait_recv()
        out[x, side, 1] = (own[x, side, 1] + ly[x].astype(jnp.float32)).astype(jnp.bfloat16)
        go(link(out.at[x, side, 1], l2x.at[me_x], (s2x, r2x), me_x, "neg", 2 * x + me_core, x))
    result = q_part[...]
    for k in range(1, line):
        z = lax.rem(place + k, line)
        link(q_in.at[z], q_in.at[z], (sq, rqs), z, "dp", partner).wait_recv()
        result = result + q_in[z].astype(jnp.float32)
    sum_ref[...] = result
    low = own[me_x, side, 0]
    for k in range(1, nx):
        x = along(k)
        ref = lx.at[x, side]
        link(ref, ref, (s1x, r1x), x * 2 + side, "neg", mate).wait_recv()
        low = low + lx[x, side].astype(jnp.float32)
    link(ly.at[me_x], ly.at[me_x], (s1y, r1y), me_x, "dp", partner).wait_recv()
    high = own[me_x, side, 1] + ly[me_x].astype(jnp.float32)
    link(l2y, l2y, (s2y, r2y), 0, "dp", partner).wait_recv()
    nsum_ref[0] = low + l2y[...].astype(jnp.float32)
    for k in range(1, nx):
        x = along(k)
        link(l2x.at[x], l2x.at[x], (s2x, r2x), x, "neg", mate).wait_recv()
        high = high + l2x[x].astype(jnp.float32)
    nsum_ref[1] = high

    for copy in sends:
        copy.wait_send()
    for distance in range(line):
        for j in range(cuts):
            if distance < line - 1:
                pl.when((place >= distance) & goes_right)(lambda: right(distance, j).wait_send())
                pl.when((place + distance < line) & goes_left)(lambda: left(distance, j).wait_send())
    for k in range(1, line):
        q_send(k, lax.rem(place + k, line)).wait_send()
    for i in range(2 * nx):
        c_send(i).wait_send()
        if i < 2 * (nx - 1):
            send_1x(i).wait_send()
        if i % 2 == 0:
            send_1y(i).wait_send()


def weight_kernel(
    ndp, nneg, packed_ref, loss_ref, gathered_ref, stats_ref,
    core_land, sum_a, sum_b, land_a, land_b, half_a, half_b, last_a, last_b, line_sum, line_land,
    stat_dp, stat_dp_land, stat_neg, stat_neg_land,
    cs, cr, xs, xr, ys, yr, ps, pr, ss, sr, ts, tr, gs, gr, hs, hr,
):
    me_dp, me_neg = lax.axis_index("dp"), lax.axis_index("neg")
    nx, line = nneg // 2, ndp // 2
    me_x, me_core = me_neg // 2, lax.rem(me_neg, 2)
    place, side = me_dp // 2, lax.rem(me_dp, 2)
    other, far = 1 - me_core, 1 - side
    mate, partner = 2 * me_x + other, 2 * place + far
    greet(ndp, nneg, me_dp, me_neg)
    turn = list(range(1, nx)) + [0]

    def x_of(k):
        return lax.rem(me_x + k, nx)

    core = {}
    for k in turn:
        x = x_of(k)
        core[k] = send(packed_ref.at[2 * x + other], core_land.at[x], cs.at[k], cr.at[k], "neg", mate)

    def add_core(x, y, half, target):
        def body(z, carry):
            target[z] = (
                packed_ref[2 * x + me_core, 2 * z + y, half].astype(jnp.float32)
                + core_land[x, 2 * z + y, half].astype(jnp.float32)
            ).astype(jnp.bfloat16)
            return carry

        lax.fori_loop(0, line, body, 0)

    def add(target, *terms):
        def body(z, carry):
            value = terms[0][z].astype(jnp.float32)
            for term in terms[1:]:
                value = value + term[z].astype(jnp.float32)
            target[z] = value.astype(jnp.bfloat16)
            return carry

        lax.fori_loop(0, line, body, 0)

    first_a = []
    for k in turn:
        x = x_of(k)
        core[k].wait_recv()
        if k:
            for y in range(2):
                add_core(x, y, 0, sum_a.at[x, y])
            first_a.append(send(sum_a.at[x], land_a.at[k], xs.at[k], xr.at[k], "neg", 2 * x + me_core))
        add_core(x, far, 1, sum_b.at[far, x])
    first_b = send(sum_b.at[far], land_b, ys.at[0], yr.at[0], "dp", partner)
    for y in range(2):
        add_core(me_x, y, 0, sum_a.at[me_x, y])
    for k in range(nx):
        add_core(x_of(k), side, 1, sum_b.at[side, x_of(k)])
    for copy in first_a:
        copy.wait_recv()
    add(half_a.at[far], sum_a.at[me_x, far], *[land_a.at[k, far] for k in range(1, nx)])
    second_a = send(half_a.at[far], last_a, ys.at[1], yr.at[1], "dp", partner)
    first_b.wait_recv()
    second_b = []
    for k in turn:
        x = x_of(k)
        add(half_b.at[x], sum_b.at[side, x], land_b.at[x])
        if k:
            second_b.append(
                send(half_b.at[x], last_b.at[k], xs.at[nx + k], xr.at[nx + k], "neg", 2 * x + me_core)
            )
    add(half_a.at[side], sum_a.at[me_x, side], *[land_a.at[k, side] for k in range(1, nx)])
    second_a.wait_recv()
    add(line_sum.at[0], half_a.at[side], last_a)
    third = []
    for half in range(2):
        if half:
            for copy in second_b:
                copy.wait_recv()
            add(line_sum.at[1], half_b.at[me_x], *[last_b.at[k] for k in range(1, nx)])
        for k in range(1, line):
            z = lax.rem(place + k, line)
            third.append(
                send(line_sum.at[half, z], line_land.at[half, k], ps.at[half * line + k], pr.at[half * line + k], "dp", 2 * z + side)
            )
    for copy in third:
        copy.wait_recv()
    squares = jnp.zeros((), jnp.float32)
    for half in range(2):
        piece = line_sum[half, place].astype(jnp.float32)
        for k in range(1, line):
            piece = piece + line_land[half, k].astype(jnp.float32)
        gathered_ref[me_neg, half] = piece.astype(jnp.bfloat16)
        squares = squares + jnp.sum(piece * piece)
    lane = lax.broadcasted_iota(jnp.int32, (8, 128), 1)
    stat_dp[...] = jnp.where(lane == 0, squares, loss_ref[0])
    stat_copies = share("dp", ndp, me_dp, lambda t: stat_dp, stat_dp_land, ss, sr)
    mine = gathered_ref.at[me_neg]
    spread = [send(mine, mine, gs.at[k], gr.at[k], "neg", 2 * x_of(k) + me_core) for k in range(1, nx)]
    spread.append(send(mine, mine, gs.at[0], gr.at[0], "neg", mate))
    finish(stat_copies)
    total = stat_dp[...]
    for k in range(1, ndp):
        total = total + stat_dp_land[lax.rem(me_dp + k, ndp)]
    stat_neg[...] = total
    stat_copies = share("neg", nneg, me_neg, lambda t: stat_neg, stat_neg_land, ts, tr)
    relay = []
    for k in range(1, nx):
        spread[k - 1].wait_recv()
        x = lax.rem(me_x + nx - k, nx)
        came = gathered_ref.at[2 * x + me_core]
        relay.append(send(came, came, hs.at[k], hr.at[k], "neg", mate))
    finish(stat_copies)
    total = stat_neg[...]
    for k in range(1, nneg):
        total = total + stat_neg_land[lax.rem(me_neg + k, nneg)]
    stats_ref[...] = total
    spread[-1].wait_recv()
    finish(relay)
    for copy in [*core.values(), *first_a, first_b, second_a, *second_b, *third, *spread]:
        copy.wait_send()


def call(kernel, collective, ndp, nneg, out_shape, scratch, in_specs, megabytes=48):
    return pl.pallas_call(
        functools.partial(kernel, ndp, nneg),
        out_shape=out_shape,
        in_specs=in_specs,
        out_specs=tuple(vmem for _ in out_shape),
        scratch_shapes=scratch,
        compiler_params=pltpu.CompilerParams(
            collective_id=collective, has_side_effects=True, vmem_limit_bytes=megabytes * 1024 * 1024
        ),
    )


def sems(*counts):
    return [pltpu.SemaphoreType.DMA((count,)) for count in counts]


def to_packed(gradient, ndp):
    rows, columns = gradient.shape
    blocks = gradient.astype(jnp.bfloat16).reshape(ndp, rows // ndp, columns)
    return [blocks[:, :, c : c + pack_columns] for c in range(0, columns, pack_columns)]


step_inputs = (
    "query_features", "positive_features", "negative_features", "positive_ids", "positive_counts", "negative_ids",
    "negative_counts", "query_first", "query_second", "query_third", "item_first", "item_second", "item_third",
)


def step_kernel(ndp, nneg, names, groups, *refs):
    refs = list(refs)
    inputs = dict(zip(step_inputs, refs))
    stats_ref, gathered = refs[13], refs[14:18]
    (
        sources, q_unit, n_unit, p_unit, towers, grads, pexp, logit,
        q_land, n_land, meta_out, meta, rows, pid_out, pid_land, pid_col, w, den, dpart, dland, scaled,
        q_out, q_part, q_in, c_out, c_in, own, out, lx, ly, l2y, l2x,
        sx, sy, rn, sm, rm, sr, sl, rq, s_meta, r_meta, s_pid, r_pid, sd, rd, sq, rqs,
        sc, rc, s1x, r1x, s1y, r1y, s2y, r2y, s2x, r2x, loaded,
        scratch, bufs, stat, stat_land, ss, sr2, left_sems,
    ) = jax.tree.unflatten(names, refs[18:])
    me_dp, me_neg = lax.axis_index("dp"), lax.axis_index("neg")
    line, nx = ndp // 2, nneg // 2
    place, side = me_dp // 2, lax.rem(me_dp, 2)
    me_x, me_core = me_neg // 2, lax.rem(me_neg, 2)
    far, other = 1 - side, 1 - me_core
    partner, mate = 2 * place + far, 2 * me_x + other
    f32, bf16 = jnp.float32, jnp.bfloat16
    rows_q, width = q_unit.shape
    block = 2 * n_unit.shape[1]
    half_n = block // 2
    lanes = den.shape[2]
    cuts = q_land.shape[1]
    half_w = width // 2
    blocks = nneg * 2
    here = (me_x * 2 + side) * 2 + me_core

    order = (
        "query_features", "query_first", "query_second", "query_third", "negative_features", "item_first", "item_second",
        "item_third", "negative_ids", "negative_counts", "positive_ids", "positive_features", "positive_counts",
    )
    item_features = sources["item_features"]
    places = dict(sources)
    places["negative_features"] = item_features.at[0:block]
    places["positive_features"] = item_features.at[block : block + rows_q]
    loads = {}
    for i, name in enumerate(order):
        loads[name] = pltpu.make_async_copy(inputs[name], places[name], loaded.at[i])
        loads[name].start()

    def along(k):
        return lax.rem(me_x + k, nx)

    def at_place(z):
        return 2 * z + side

    barrier = pltpu.get_barrier_semaphore()

    def quad(k):
        b = lax.rem(here + k, blocks)
        return {"dp": 2 * place + lax.rem(b // 2, 2), "neg": 2 * (b // 4) + lax.rem(b, 2)}

    devices = ndp * nneg
    me = me_dp * nneg + me_neg

    def everyone(n):
        target = lax.rem(me + n, devices)
        return target // nneg, lax.rem(target, nneg)

    for n in range(1, devices):
        dp, neg = everyone(n)
        pl.semaphore_signal(barrier, inc=1, device_id={"dp": dp, "neg": neg}, device_id_type=pl.DeviceIdType.MESH)

    def slot(x, y, half):
        return (x * 2 + y) * 2 + half

    def piece(x, y, half):
        return n_land.at[(x * 2 + y) * 2 + me_core, half]

    def push(src, x, y, half, send_sems, index, axis, target):
        return link(src, piece(x, y, half), (send_sems, rn), slot(x, y, half), axis, target, index)

    def relay(src, x, y, half):
        i = slot(x, y, half)
        return link(src, piece(x, y, half), (sm, rm), i, "neg", mate)

    def landed(x, y, half):
        ref = piece(x, y, half)
        link(ref, ref, (sy, rn), slot(x, y, half), "neg", mate, 0).wait_recv()

    sends = []

    def go(copy):
        copy.start()
        sends.append(copy)

    def to_x(src, x, y, half, kind):
        for k in range(1, nx):
            go(push(src, x, y, half, sx, kind * nx + k, "neg", 2 * along(k) + me_core))

    def to_y(src, x, y, half, index):
        go(push(src, x, y, half, sy, index, "dp", partner))

    def chain(slot_z, j, distance, sems, target):
        src = q_unit.at[pl.ds(j * (rows_q // cuts), rows_q // cuts)] if distance == 0 else q_land.at[slot_z, j]
        return link(src, q_land.at[slot_z, j], (sems, rq), slot_z * cuts + j, "dp", target, distance * cuts + j)

    def right(distance, j):
        return chain(place - distance, j, distance, sr, at_place(lax.rem(place + 1, line)))

    def left(distance, j):
        return chain(place + distance, j, distance, sl, at_place(lax.rem(place + line - 1, line)))

    goes_right, goes_left = place < line - 1, place > 0

    def q_step(distance):
        for j in range(cuts):

            @pl.when(place >= distance)
            def _():
                ref = q_land.at[place - distance, j]
                link(ref, ref, (sr, rq), (place - distance) * cuts + j, "dp", partner, 0).wait_recv()
                pl.when(goes_right)(lambda: right(distance, j).start())

            @pl.when(place + distance < line)
            def _():
                ref = q_land.at[place + distance, j]
                link(ref, ref, (sl, rq), (place + distance) * cuts + j, "dp", partner, 0).wait_recv()
                pl.when(goes_left)(lambda: left(distance, j).start())

    def forward(lo, count, features, first, second, third, saved, unit_ref, waits=((), (), ())):
        act1, slope1, act2, slope2, emb = saved
        span = slice(lo, lo + count)

        def layer(source, weight, act, slope):
            columns = weight.shape[1]
            step = 512 if columns % 512 == 0 else columns
            for c in range(0, columns, step):
                pre = jnp.dot(source[span, :], weight[:, c : c + step], preferred_element_type=f32)
                sigma = jax.nn.sigmoid(pre)
                act[span, c : c + step] = (pre * sigma).astype(bf16)
                slope[span, c : c + step] = sigma * (1.0 + pre * (1.0 - sigma))

        ready(waits[0])
        layer(features, first, act1, slope1)
        ready(waits[1])
        layer(act1, second, act2, slope2)
        ready(waits[2])
        value = jnp.dot(act2[span, :], third[...], preferred_element_type=f32)
        emb[span, :] = value
        inv_norm = lax.rsqrt(jnp.sum(value * value, axis=1, keepdims=True) + 1.0)
        unit_ref[...] = (value * inv_norm).astype(bf16)

    def ready(chosen):
        for name in chosen:
            loads[name].wait()

    item_weights = tuple(sources[name] for name in ("item_first", "item_second", "item_third"))
    query_weights = tuple(sources[name] for name in ("query_first", "query_second", "query_third"))
    def own_ids(ref, index, count):
        return ref[:, pl.ds(pl.multiple_of(index * count, count), count)]

    forward(
        0, rows_q, sources["query_features"], *query_weights, towers[0], q_unit,
        (("query_features", "query_first"), ("query_second",), ("query_third",)),
    )
    pl.semaphore_wait(barrier, devices - 1)
    for j in range(cuts):
        pl.when(goes_right)(lambda j=j: right(0, j).start())
        pl.when(goes_left)(lambda j=j: left(0, j).start())
    for j in range(cuts):
        q_land[place, j] = q_unit[pl.ds(j * (rows_q // cuts), rows_q // cuts), :]
    ready(("negative_ids", "negative_counts", "positive_ids"))
    meta_out[0:1, :] = own_ids(sources["negative_ids"], me_dp, block)
    meta_out[1:2, :] = own_ids(sources["negative_counts"], me_dp, block)
    pid_out[...] = own_ids(sources["positive_ids"], me_neg, rows_q)
    meta[here] = meta_out[...]
    pid_land[place] = pid_out[...]
    for k in range(1, blocks):
        copy = pltpu.make_async_remote_copy(
            src_ref=meta_out, dst_ref=meta.at[here], send_sem=s_meta.at[k], recv_sem=r_meta.at[here],
            device_id=quad(k), device_id_type=pl.DeviceIdType.MESH,
        )
        go(copy)
    for k in range(1, line):
        z = lax.rem(place + k, line)
        go(link(pid_out, pid_land.at[place], (s_pid, r_pid), place, "dp", at_place(z), k))
    n_first, n_second = n_unit.at[0], n_unit.at[1]
    forward(
        0, half_n, item_features, *item_weights, towers[1], n_first,
        (("negative_features", "item_first"), ("item_second",), ("item_third",)),
    )
    to_x(n_first, me_x, side, 0, 0)
    go(relay(n_first, me_x, side, 0))
    n_land[here, 0] = n_unit[0]
    forward(half_n, half_n, item_features, *item_weights, towers[1], n_second)
    to_y(n_second, me_x, side, 1, 0)
    to_x(n_second, me_x, side, 1, 1)
    to_y(n_first, me_x, side, 0, 1)
    go(relay(n_second, me_x, side, 1))
    n_land[here, 1] = n_unit[1]
    ready(("positive_features", "positive_counts"))
    forward(block, rows_q, item_features, *item_weights, towers[1], p_unit)
    q_step(1)
    product = q_unit[...].astype(f32) * p_unit[...].astype(f32)
    logit[...] = jnp.sum(product.T, axis=0, keepdims=True) * inv_temp - jnp.log(sources["positive_counts"][...].astype(f32))
    pexp[...] = jnp.exp(logit[...])

    for k in range(1, nx):
        x = along(k)
        landed(x, side, 0)
        to_y(piece(x, side, 0), x, side, 0, 1 + k)
        go(relay(piece(x, side, 0), x, side, 0))
    for k in range(1, blocks):
        b = lax.rem(here + k, blocks)
        link(meta.at[b], meta.at[b], (s_meta, r_meta), b, "neg", mate).wait_recv()
    for k in range(1, line):
        z = lax.rem(place + k, line)
        link(pid_land.at[z], pid_land.at[z], (s_pid, r_pid), z, "dp", partner).wait_recv()
    for b in range(blocks):
        rows[b, 0:1, :] = meta[b, 0:1, :].astype(f32)
        rows[b, 1:2, :] = jnp.log2(meta[b, 1:2, :].astype(f32))
    for z in range(line):
        pid_col[z] = jnp.broadcast_to(pid_land[z].astype(f32), (lanes, rows_q)).T
        den[z] = jnp.zeros((rows_q, lanes), f32)

    def unit(b, z):
        dots = contract_cols(q_land[z].reshape(rows_q, width), n_land[b].reshape(block, width))
        value = jnp.exp2(dots * (inv_temp * log2_e) - rows[b, 1:2, :])
        ids = jnp.concatenate([pid_col[z]] * (block // lanes), axis=1)
        value = jnp.where(ids != rows[b, 0:1, :], value, 0.0)
        w[b, z] = value.astype(jnp.bfloat16)
        total = den[z]
        for c in range(0, block, lanes):
            total = total + value[:, c : c + lanes]
        den[z] = total

    def relayed(x, y):
        for half in range(2):
            ref = n_land.at[(x * 2 + y) * 2 + other, half]
            link(ref, ref, (sm, rm), slot(x, y, half), "neg", mate).wait_recv()

    def both_cores(x, y):
        return [(x * 2 + y) * 2 + core for core in range(2)]

    near_blocks = both_cores(me_x, side)
    mid_blocks = both_cores(me_x, far)
    far_blocks = []
    for k in range(1, nx):
        mid_blocks = mid_blocks + both_cores(along(k), side)
        far_blocks = far_blocks + both_cores(along(k), far)

    def units(lo, hi, chosen):
        def body(z, carry):
            for b in chosen:
                unit(b, z)
            return carry

        lax.fori_loop(jnp.maximum(lo, 0), jnp.minimum(hi, line), body, 0)

    relayed(me_x, side)
    units(place - 1, place + 2, near_blocks)
    landed(me_x, far, 1)
    to_x(piece(me_x, far, 1), me_x, far, 1, 2)
    go(relay(piece(me_x, far, 1), me_x, far, 1))
    q_step(2)
    units(place - 2, place - 1, near_blocks)
    units(place + 2, place + 3, near_blocks)
    for k in range(1, nx):
        x = along(k)
        landed(x, side, 1)
        go(relay(piece(x, side, 1), x, side, 1))
    for k in range(1, nx):
        relayed(along(k), side)
    landed(me_x, far, 0)
    go(relay(piece(me_x, far, 0), me_x, far, 0))
    relayed(me_x, far)
    units(place - 2, place + 3, mid_blocks)
    for distance in range(3, line):
        q_step(distance)
    for half in range(2):
        for k in range(1, nx):
            x = along(k)
            landed(x, far, half)
            go(relay(piece(x, far, half), x, far, half))
    units(0, place - 2, near_blocks + mid_blocks)
    units(place + 3, line, near_blocks + mid_blocks)
    for k in range(1, nx):
        relayed(along(k), far)
    units(0, line, far_blocks)
    for z in range(line):
        dpart[z] = jnp.sum(den[z].T, axis=0, keepdims=True)
    dpart[place] = dpart[place] + pexp[...]
    for k in range(1, line):
        z = lax.rem(place + k, line)
        go(link(dpart, dland.at[place], (sd, rd), place, "dp", at_place(z), k))

    def q_block(z):
        if block % 128 == 0:
            left_side = jnp.concatenate([w[b, z] for b in range(blocks)], axis=1)
            return jnp.dot(
                left_side, n_land[...].reshape(blocks * block, width), preferred_element_type=jnp.float32
            )
        total = jnp.zeros((rows_q, width), jnp.float32)
        for b in range(blocks):
            total = total + jnp.dot(w[b, z], n_land[b].reshape(block, width), preferred_element_type=jnp.float32)
        return total

    def q_send(k, z):
        return link(q_out.at[z], q_in.at[place], (sq, rqs), place, "dp", at_place(z), k)

    def q_push(k, carry):
        z = lax.rem(place + k, line)
        q_out[z] = q_block(z).astype(jnp.bfloat16)
        q_send(k, z).start()
        return carry

    lax.fori_loop(1, line, q_push, 0)
    q_part[...] = q_block(place)
    total = dpart[...]
    for k in range(1, line):
        z = lax.rem(place + k, line)
        link(dland.at[z], dland.at[z], (sd, rd), z, "dp", partner).wait_recv()
        total = total + dland[z]
    dpart2 = 1.0 / total
    for z in range(line):
        q_t = q_land[z].reshape(rows_q, width).astype(jnp.float32).T
        scaled[:, z * rows_q : (z + 1) * rows_q] = (q_t * dpart2[z]).astype(jnp.bfloat16)
    def dest(i):
        x = lax.rem(me_x + 1 + i // 2, nx)
        y = lax.rem(side + 1 + lax.rem(i, 2), 2)
        return x, y

    def part(x, y, core):
        return jnp.dot(
            scaled[...], w[(x * 2 + y) * 2 + core].reshape(line * rows_q, block), preferred_element_type=jnp.float32
        )

    def c_send(i):
        x, y = dest(i)
        return link(c_out.at[x, y], c_in.at[x, y], (sc, rc), x * 2 + y, "neg", mate)

    def far_step(i, carry):
        x, y = dest(i)
        c_out[x, y] = part(x, y, other).astype(jnp.bfloat16).reshape(2, half_w, block)
        c_send(i).start()
        return carry

    def send_1x(i):
        x, y = dest(i)
        return link(out.at[x, y, 0], lx.at[me_x, y], (s1x, r1x), me_x * 2 + y, "neg", 2 * x + me_core, x * 2 + y)

    def send_1y(i):
        x, y = dest(i)
        return link(out.at[x, y, 1], ly.at[x], (s1y, r1y), x, "dp", partner)

    def own_step(i, carry):
        x, y = dest(i)
        value = part(x, y, me_core).reshape(2, half_w, block)
        link(c_in.at[x, y], c_in.at[x, y], (sc, rc), x * 2 + y, "neg", mate).wait_recv()
        value = value + c_in[x, y].astype(jnp.float32)
        own[x, y] = value

        @pl.when(i < 2 * (nx - 1))
        def _():
            out[x, y, 0] = value[0].astype(jnp.bfloat16)
            send_1x(i).start()

        @pl.when(lax.rem(i, 2) == 0)
        def _():
            out[x, y, 1] = value[1].astype(jnp.bfloat16)
            send_1y(i).start()

        return carry

    ahead = 2

    def both_steps(i, carry):
        far_step(i + ahead, 0)
        own_step(i, 0)
        return carry

    lax.fori_loop(0, ahead, far_step, 0)
    lax.fori_loop(0, 2 * nx - ahead, both_steps, 0)
    lax.fori_loop(2 * nx - ahead, 2 * nx, own_step, 0)
    value = own[me_x, far, 0]
    for k in range(1, nx):
        x = along(k)
        ref = lx.at[x, far]
        link(ref, ref, (s1x, r1x), x * 2 + far, "neg", mate).wait_recv()
        value = value + lx[x, far].astype(jnp.float32)
    out[me_x, far, 0] = value.astype(jnp.bfloat16)
    go(link(out.at[me_x, far, 0], l2y, (s2y, r2y), 0, "dp", partner))
    for k in range(1, nx):
        x = along(k)
        link(ly.at[x], ly.at[x], (s1y, r1y), x, "dp", partner).wait_recv()
        out[x, side, 1] = (own[x, side, 1] + ly[x].astype(jnp.float32)).astype(jnp.bfloat16)
        go(link(out.at[x, side, 1], l2x.at[me_x], (s2x, r2x), me_x, "neg", 2 * x + me_core, x))
    denom = dpart[place]
    for k in range(1, line):
        denom = denom + dland[lax.rem(place + k, line), place]
    loss_part = jnp.sum(jnp.log(denom) - logit[...])

    def to_columns(row):
        column = jnp.broadcast_to(row, (lanes, rows_q)).T
        return jnp.concatenate([column] * (width // lanes), axis=1)

    slope_columns = to_columns(pexp[...] / denom - 1.0) * inv_temp
    grads[1][block : block + rows_q, :] = slope_columns * q_unit[...].astype(f32)
    result = q_part[...]
    for k in range(1, line):
        z = lax.rem(place + k, line)
        link(q_in.at[z], q_in.at[z], (sq, rqs), z, "dp", partner).wait_recv()
        result = result + q_in[z].astype(jnp.float32)
    grads[0][...] = result * (to_columns(1.0 / denom) * inv_temp) + slope_columns * p_unit[...].astype(f32)

    pending = []

    def queue(copy):
        copy.start()
        pending.append(copy)

    def x_of(k):
        return lax.rem(me_x + k, nx)

    def same_core(x):
        return 2 * x + me_core

    def z_of(k):
        return lax.rem(place + k, line)

    def arrived(ref, sem_array, index):
        link(ref, ref, (sem_array, sem_array), index, "neg", mate).wait_recv()

    steps = [
        (sources["query_features"], *towers[0], grads[0], sources["query_second"], sources["query_third"]),
        (item_features, *towers[1], grads[1], sources["item_second"], sources["item_third"]),
    ]

    def store(group, offset, value, dp, hg):
        packed = bufs[group]["packed"]
        pieces = hg // nneg
        for p in range(value.shape[1] // pack_columns):
            part = value[:, p * pack_columns : (p + 1) * pack_columns].astype(bf16)
            part = part.reshape(value.shape[0] // hg, nx, 2, pieces, pack_columns)
            lo = offset + p * pieces
            for core in range(2):
                packed[core, pl.ds(dp, value.shape[0] // hg), :, lo : lo + pieces, :] = part[:, :, core]

    def weight_grad(group, offset, left_ref, right_ref):
        rows, columns = left_ref.shape[1], right_ref.shape[1]
        hg = rows // ndp
        step = 2 * hg

        def body(m, carry):
            left = left_ref[:, pl.ds(pl.multiple_of(m * step, step), step)]
            store(group, offset, contract_rows(left, right_ref[...]), 2 * m, hg)
            return carry

        lax.fori_loop(0, rows // step, body, 0, unroll=True)
        return offset + hg // nneg * (columns // pack_columns)

    def row_loop(count, body):
        step = 256 if count % 256 == 0 else count

        def wrapped(i, carry):
            body(pl.ds(pl.multiple_of(i * step, step), step))
            return carry

        lax.fori_loop(0, count // step, wrapped, 0)

    def embed_stage(t):
        feat, act1, slope1, act2, slope2, emb_ref, grad_ref, second, third = steps[t]
        eg, s2, s1 = scratch[t]

        def body(rows):
            emb, grad = emb_ref[rows, :], grad_ref[rows, :]
            inv_norm = lax.rsqrt(jnp.sum(emb * emb, axis=1, keepdims=True) + 1.0)
            along = jnp.sum(emb * grad, axis=1, keepdims=True)
            value = (inv_norm * grad - inv_norm * inv_norm * inv_norm * emb * along).astype(bf16)
            eg[rows, :] = value
            s2[rows, :] = (contract_cols(value, third[...]) * slope2[rows, :]).astype(bf16)

        row_loop(feat.shape[0], body)

    def second_stage(t, group):
        feat, act1, slope1, act2, slope2, emb_ref, grad_ref, second, third = steps[t]
        eg, s2, s1 = scratch[t]
        offset = weight_grad(group, 0, act2, eg)
        weight_grad(group, offset, act1, s2)

    def slope_stage(t):
        feat, act1, slope1, act2, slope2, emb_ref, grad_ref, second, third = steps[t]
        eg, s2, s1 = scratch[t]
        columns = second.shape[0]

        def body(rows):
            for c in range(0, columns, 512):
                value = contract_cols(s2[rows, :], second[c : c + 512, :]) * slope1[rows, c : c + 512]
                s1[rows, c : c + 512] = value.astype(bf16)

        row_loop(feat.shape[0], body)

    def first_stage(t, group):
        weight_grad(group, 0, steps[t][0], scratch[t][2])

    def stage0(g):
        b = bufs[g]
        queue(link(b["packed"].at[other], b["c_in"], (b["cs"], b["cr"]), 0, "neg", mate))

    def base(b, dp, x, lo, hi):
        return b["packed"][me_core, dp, x, lo:hi, :].astype(f32) + b["c_in"][dp, x, lo:hi, :].astype(f32)

    def loop(count, body):
        def wrapped(i, carry):
            body(i)
            return carry

        lax.fori_loop(0, count, wrapped, 0)

    def stage1(g):
        b, (r1, r) = bufs[g], groups[g]
        arrived(b["c_in"], b["cr"], 0)
        for k in range(1, nx):
            x = x_of(k)

            def body(dp):
                b["o1x"][x, dp] = base(b, dp, x, 0, r1).astype(bf16)

            loop(ndp, body)
            queue(link(b["o1x"].at[x], b["l1x"].at[me_x], (b["s1x"], b["r1x"]), me_x, "neg", same_core(x), x))

        def body_y(z):
            for x in range(nx):
                b["o1y"][z, x] = base(b, 2 * z + far, x, r1, r).astype(bf16)

        loop(line, body_y)
        queue(link(b["o1y"], b["l1y"], (b["s1y"], b["r1y"]), 0, "dp", partner))

    def low(b, dp, r1):
        value = base(b, dp, me_x, 0, r1)
        for k in range(1, nx):
            value = value + b["l1x"][x_of(k), dp].astype(f32)
        return value

    def stage2(g):
        b, (r1, r) = bufs[g], groups[g]
        for k in range(1, nx):
            x = x_of(k)
            arrived(b["l1x"].at[x], b["r1x"], x)

        def body(z):
            b["o2y"][z] = low(b, 2 * z + far, r1).astype(bf16)

        loop(line, body)
        queue(link(b["o2y"], b["l2y"], (b["s2y"], b["r2y"]), 0, "dp", partner))
        arrived(b["l1y"], b["r1y"], 0)
        for k in range(1, nx):
            x = x_of(k)

            def body_x(z):
                value = base(b, 2 * z + side, x, r1, r) + b["l1y"][z, x].astype(f32)
                b["o2x"][x, z] = value.astype(bf16)

            loop(line, body_x)
            queue(link(b["o2x"].at[x], b["l2x"].at[me_x], (b["s2x"], b["r2x"]), me_x, "neg", same_core(x), x))

    def stage3(g):
        b, (r1, r) = bufs[g], groups[g]
        arrived(b["l2y"], b["r2y"], 0)
        for k in range(1, nx):
            x = x_of(k)
            arrived(b["l2x"].at[x], b["r2x"], x)

        def body(z):
            dp = 2 * z + side
            b["zs"][z, 0:r1, :] = (low(b, dp, r1) + b["l2y"][z].astype(f32)).astype(bf16)
            value = base(b, dp, me_x, r1, r) + b["l1y"][z, me_x].astype(f32)
            for k in range(1, nx):
                value = value + b["l2x"][x_of(k), z].astype(f32)
            b["zs"][z, r1:r, :] = value.astype(bf16)

        loop(line, body)
        for k in range(1, line):
            z = z_of(k)
            queue(link(b["zs"].at[z], b["l3"].at[place], (b["s3"], b["r3"]), place, "dp", 2 * z + side, z))

    squares = []

    def stage4(g):
        b = bufs[g]
        for k in range(1, line):
            z = z_of(k)
            arrived(b["l3"].at[z], b["r3"], z)
        value = b["zs"][place].astype(f32)
        for k in range(1, line):
            value = value + b["l3"][z_of(k)].astype(f32)
        squares.append(jnp.sum(value * value))
        b["ag"][me_neg] = value.astype(bf16)
        mine = b["ag"].at[me_neg]
        for k in range(1, nx):
            x = x_of(k)
            queue(link(mine, mine, (b["sg"], b["rg"]), me_x, "neg", same_core(x), x))
        queue(link(mine, mine, (b["sh"], b["rh"]), me_x, "neg", mate))

    def stage5(g):
        b = bufs[g]
        for k in range(1, nx):
            x = x_of(k)
            ref = b["ag"].at[same_core(x)]
            arrived(ref, b["rg"], x)
            queue(link(ref, ref, (b["sh"], b["rh"]), x, "neg", mate))

    leaving = []

    def leave(source, target, index):
        copy = pltpu.make_async_copy(source, target, left_sems.at[index])
        copy.start()
        leaving.append(copy)

    def stage6(g):
        b = bufs[g]
        for x in range(nx):
            arrived(b["ag"].at[2 * x + other], b["rh"], x)
        leave(b["ag"], gathered[g], g)

    embed_stage(0)
    second_stage(0, 0)
    stage0(0)
    slope_stage(0)
    first_stage(0, 1)
    stage0(1)
    stage1(0)
    n_low = own[me_x, side, 0]
    for k in range(1, nx):
        x = along(k)
        ref = lx.at[x, side]
        link(ref, ref, (s1x, r1x), x * 2 + side, "neg", mate).wait_recv()
        n_low = n_low + lx[x, side].astype(jnp.float32)
    link(ly.at[me_x], ly.at[me_x], (s1y, r1y), me_x, "dp", partner).wait_recv()
    n_high = own[me_x, side, 1] + ly[me_x].astype(jnp.float32)
    link(l2y, l2y, (s2y, r2y), 0, "dp", partner).wait_recv()
    n_low = n_low + l2y[...].astype(jnp.float32)
    for k in range(1, nx):
        x = along(k)
        link(l2x.at[x], l2x.at[x], (s2x, r2x), x, "neg", mate).wait_recv()
        n_high = n_high + l2x[x].astype(jnp.float32)

    grads[1][0:block, 0:half_w] = n_low.T * inv_temp
    grads[1][0:block, half_w:width] = n_high.T * inv_temp
    embed_stage(1)
    stage1(1)
    second_stage(1, 2)
    stage0(2)
    stage2(0)
    slope_stage(1)
    stage1(2)
    stage2(1)
    first_stage(1, 3)
    stage0(3)
    stage3(0)
    stage1(3)
    stage2(2)
    stage3(1)
    stage2(3)
    stage3(2)
    stage3(3)
    for g in range(4):
        stage4(g)
    total_squares = squares[0] + squares[1] + squares[2] + squares[3]
    lane = lax.broadcasted_iota(jnp.int32, (1, 128), 1)
    stat[...] = jnp.where(lane == 0, total_squares, loss_part)
    for n in range(1, devices):
        dp, neg = everyone(n)
        copy = pltpu.make_async_remote_copy(
            src_ref=stat, dst_ref=stat_land.at[me], send_sem=ss.at[n], recv_sem=sr2.at[me],
            device_id={"dp": dp, "neg": neg}, device_id_type=pl.DeviceIdType.MESH,
        )
        queue(copy)
    for g in range(4):
        stage5(g)
    for g in range(4):
        stage6(g)
    stat_land[me] = stat[...]
    for n in range(1, devices):
        source = lax.rem(me + n, devices)
        arrived(stat_land.at[source], sr2, source)
    stat_land[me] = jnp.sum(stat_land[...], axis=0)
    leave(stat_land.at[me], stats_ref, 4)
    for copy in pending:
        copy.wait_send()
    for copy in leaving:
        copy.wait()


    for copy in sends:
        copy.wait_send()
    for distance in range(line):
        for j in range(cuts):
            if distance < line - 1:
                pl.when((place >= distance) & goes_right)(lambda: right(distance, j).wait_send())
                pl.when((place + distance < line) & goes_left)(lambda: left(distance, j).wait_send())
    for k in range(1, line):
        q_send(k, lax.rem(place + k, line)).wait_send()
    for i in range(2 * nx):
        c_send(i).wait_send()
        if i < 2 * (nx - 1):
            send_1x(i).wait_send()
        if i % 2 == 0:
            send_1y(i).wait_send()


def fused_step(ndp, nneg, arguments):
    line, nx = ndp // 2, nneg // 2
    bf16, f32, i32 = jnp.bfloat16, jnp.float32, jnp.int32
    named = dict(zip(step_inputs, arguments))
    fin, h1 = named["item_first"].shape
    h2, width = named["item_third"].shape
    own_rows, block = named["query_features"].shape[0], named["negative_features"].shape[0]
    blocks, cuts, lanes = 2 * nneg, 4, 128
    rows_half = (width // 2, block)
    sources = {"item_features": pltpu.VMEM((block + own_rows, fin), bf16)}
    for name, value in named.items():
        if name not in ("positive_features", "negative_features"):
            sources[name] = pltpu.VMEM(value.shape, value.dtype)
    counts = (own_rows, block + own_rows)
    towers = [
        [
            pltpu.VMEM((count, h1), bf16), pltpu.VMEM((count, h1), f32), pltpu.VMEM((count, h2), bf16),
            pltpu.VMEM((count, h2), f32), pltpu.VMEM((count, width), f32),
        ]
        for count in counts
    ]
    scratch = [
        [pltpu.VMEM((count, width), bf16), pltpu.VMEM((count, h2), bf16), pltpu.VMEM((count, h1), bf16)]
        for count in counts
    ]
    row = pltpu.VMEM((1, own_rows), f32)
    score = [
        pltpu.VMEM((line, cuts, own_rows // cuts, width), bf16),
        pltpu.VMEM((blocks, 2, block // 2, width), bf16),
        pltpu.VMEM((2, block), i32),
        pltpu.VMEM((blocks, 2, block), i32),
        pltpu.VMEM((blocks, 2, block), f32),
        pltpu.VMEM((1, own_rows), i32),
        pltpu.VMEM((line, 1, own_rows), i32),
        pltpu.VMEM((line, own_rows, lanes), f32),
        pltpu.VMEM((blocks, line, own_rows, block), bf16),
        pltpu.VMEM((line, own_rows, lanes), f32),
        pltpu.VMEM((line, 1, own_rows), f32),
        pltpu.VMEM((line, line, 1, own_rows), f32),
        pltpu.VMEM((width, line * own_rows), bf16),
        pltpu.VMEM((line, own_rows, width), bf16),
        pltpu.VMEM((own_rows, width), f32),
        pltpu.VMEM((line, own_rows, width), bf16),
        pltpu.VMEM((nx, 2, 2) + rows_half, bf16),
        pltpu.VMEM((nx, 2, 2) + rows_half, bf16),
        pltpu.VMEM((nx, 2, 2) + rows_half, f32),
        pltpu.VMEM((nx, 2, 2) + rows_half, bf16),
        pltpu.VMEM((nx, 2) + rows_half, bf16),
        pltpu.VMEM((nx,) + rows_half, bf16),
        pltpu.VMEM(rows_half, bf16),
        pltpu.VMEM((nx,) + rows_half, bf16),
    ] + sems(
        3 * nx, 1 + nx, 4 * nx, 4 * nx, 4 * nx, line * cuts, line * cuts, line * cuts,
        blocks, blocks, line, line, line, line, line, line,
        2 * nx, 2 * nx, 2 * nx, 2 * nx, nx, nx, 1, 1, nx, nx, len(step_inputs),
    )
    groups, outs, bufs = [], [], []
    for _ in counts:
        for height, columns in ((fin, h1), (h1, h2), (h2, width)):
            outs.append(jax.ShapeDtypeStruct((height // ndp, columns), f32))
        both = h2 // (ndp * nneg) * (width // pack_columns) + h1 // (ndp * nneg) * (h2 // pack_columns)
        alone = fin // (ndp * nneg) * (h1 // pack_columns)
        for r in (both, alone):
            groups.append((max((r * 4 + 72) // 144, 1) * 16, r))
    c = pack_columns
    sem_names = ["cs", "cr", "s1x", "r1x", "s1y", "r1y", "s2y", "r2y", "s2x", "r2x", "s3", "r3", "sg", "rg", "sh", "rh"]
    for r1, r in groups:
        r2 = r - r1
        shapes = dict(
            packed=(2, ndp, nx, r, c), c_in=(ndp, nx, r, c), o1x=(nx, ndp, r1, c), l1x=(nx, ndp, r1, c),
            o1y=(line, nx, r2, c), l1y=(line, nx, r2, c), o2y=(line, r1, c), l2y=(line, r1, c),
            o2x=(nx, line, r2, c), l2x=(nx, line, r2, c), zs=(line, r, c), l3=(line, r, c), ag=(nneg, r, c),
        )
        buf = {name: pltpu.VMEM(shape, bf16) for name, shape in shapes.items()}
        buf.update(zip(sem_names, sems(1, 1, nx, nx, 1, 1, 1, 1, nx, nx, line, line, nx, nx, nx, nx)))
        bufs.append(buf)
    tree = (
        sources, pltpu.VMEM((own_rows, width), bf16), pltpu.VMEM((2, block // 2, width), bf16),
        pltpu.VMEM((own_rows, width), bf16), towers, [pltpu.VMEM((count, width), f32) for count in counts], row, row,
        *score, scratch, bufs,
        pltpu.VMEM((1, 128), f32), pltpu.VMEM((ndp * nneg, 1, 128), f32), *sems(ndp * nneg, ndp * nneg, 5),
    )
    leaves, names = jax.tree.flatten(tree)
    space = sems(1)[0].memory_space
    is_flag = [leaf.memory_space == space for leaf in leaves]
    flags = [leaf for leaf, flag in zip(leaves, is_flag) if flag]
    kept = [leaf for leaf, flag in zip(leaves, is_flag) if not flag]

    def kernel(*refs):
        fixed = refs[: len(refs) - len(kept)]
        held = refs[len(refs) - len(kept) :]

        def scoped(*flag_refs):
            held_refs, flags_left = iter(held), iter(flag_refs)
            merged = [next(flags_left) if flag else next(held_refs) for flag in is_flag]
            step_kernel(ndp, nneg, names, tuple(groups), *fixed, *merged)

        pl.run_scoped(scoped, *flags)

    any_space = pl.BlockSpec(memory_space=pl.ANY)
    stats, *gathered = pl.pallas_call(
        kernel,
        out_shape=(
            jax.ShapeDtypeStruct((1, 128), f32),
            *[jax.ShapeDtypeStruct((nneg, r, pack_columns), bf16) for _, r in groups],
        ),
        in_specs=[any_space] * len(arguments),
        out_specs=(any_space,) * 5,
        scratch_shapes=kept,
        compiler_params=pltpu.CompilerParams(
            collective_id=1, has_side_effects=True, vmem_limit_bytes=67043328
        ),
    )(*arguments)
    mean_loss, *clipped = pl.pallas_call(
        functools.partial(finish_kernel, nneg, own_rows * ndp * nneg),
        out_shape=(jax.ShapeDtypeStruct((1,), f32), *outs),
        in_specs=[any_space] * 5,
        out_specs=(pl.BlockSpec(memory_space=pltpu.SMEM), *([any_space] * 6)),
        scratch_shapes=[pltpu.VMEM((1, 128), f32)]
        + [pltpu.VMEM((nneg, r, pack_columns), bf16) for _, r in groups]
        + [pltpu.VMEM(out.shape, f32) for out in outs]
        + sems(5, 6),
    )(stats, *gathered)
    return (mean_loss.reshape(()), *clipped)


def finish_kernel(nneg, count, *refs):
    given, loss_ref, outs, stats_ref, gathered, staged = refs[:5], refs[5], refs[6:12], refs[12], refs[13:17], refs[17:23]
    loaded, done = refs[23:]
    loads = [
        pltpu.make_async_copy(source, target, loaded.at[i])
        for i, (source, target) in enumerate(zip(given, (stats_ref, *gathered)))
    ]
    for copy in loads:
        copy.start()
    for copy in loads:
        copy.wait()
    clip = clip_norm / jnp.maximum(jnp.sqrt(stats_ref[0:1, 0:1]), clip_norm)
    copies = []
    for t in range(2):
        third_ref, second_ref, first_ref = staged[3 * t + 2], staged[3 * t + 1], staged[3 * t]
        for index, group, ref, offset in (
            (3 * t + 1, 2 * t, second_ref, third_ref.shape[0] // nneg),
            (3 * t, 2 * t + 1, first_ref, 0),
            (3 * t + 2, 2 * t, third_ref, 0),
        ):
            pieces = ref.shape[0] // nneg
            for p in range(ref.shape[1] // pack_columns):
                lo = offset + p * pieces
                for n in range(nneg):
                    value = gathered[group][n, lo : lo + pieces, :].astype(jnp.float32) * clip
                    ref[n * pieces : (n + 1) * pieces, p * pack_columns : (p + 1) * pack_columns] = value
            copy = pltpu.make_async_copy(ref, outs[index], done.at[index])
            copy.start()
            copies.append(copy)
    loss_ref[0] = jnp.sum(stats_ref[0:1, 1:2]) / count
    for copy in copies:
        copy.wait()


def per_device(
    query_features,
    positive_features,
    negative_features,
    positive_ids,
    positive_counts,
    negative_ids,
    negative_counts,
    query_first,
    query_second,
    query_third,
    item_first,
    item_second,
    item_third,
):
    own_rows = query_features.shape[0]
    ndp, nneg = lax.axis_size("dp"), lax.axis_size("neg")
    heights = (query_first.shape[0], query_second.shape[0], query_third.shape[0])
    tiled = all(height % (16 * ndp * nneg) == 0 for height in heights)
    if tiled and own_rows % 256 == 0 and negative_features.shape[0] % 256 == 0:
        return fused_step(
            ndp,
            nneg,
            (
                query_features, positive_features, negative_features, positive_ids.reshape(1, -1),
                positive_counts.reshape(1, -1), negative_ids.reshape(1, -1), negative_counts.reshape(1, -1),
                query_first, query_second, query_third, item_first, item_second, item_third,
            ),
        )
    query_saved, query_unit = tower_forward(query_features, query_first, query_second, query_third)
    item_features = jnp.concatenate([positive_features, negative_features], axis=0)
    item_saved, item_unit = tower_forward(item_features, item_first, item_second, item_third)
    positive_unit = item_unit[:own_rows]
    negative_unit = item_unit[own_rows:]
    ndp, nneg = lax.axis_size("dp"), lax.axis_size("neg")
    width = query_unit.shape[1]
    line, nx = ndp // 2, nneg // 2
    block = negative_unit.shape[0]
    blocks, cuts, lanes = 2 * nneg, 2, min(block, 128)
    bf16, f32, i32 = jnp.bfloat16, jnp.float32, jnp.int32
    positive_logit = jnp.sum(
        query_unit.astype(f32) * positive_unit.astype(f32), axis=1
    ) * inv_temp - jnp.log(positive_counts.astype(f32))
    positive_exp = jnp.exp(positive_logit)
    rows_half = (width // 2, block)
    query_total, denom, negative_sum = call(
        score_kernel,
        0,
        ndp,
        nneg,
        (
            jax.ShapeDtypeStruct((own_rows, width), f32),
            jax.ShapeDtypeStruct((1, own_rows), f32),
            jax.ShapeDtypeStruct((2,) + rows_half, f32),
        ),
        [
            pltpu.VMEM((line, cuts, own_rows // cuts, width), bf16),
            pltpu.VMEM((blocks, 2, block // 2, width), bf16),
            pltpu.VMEM((2, block), i32),
            pltpu.VMEM((blocks, 2, block), i32),
            pltpu.VMEM((blocks, 2, block), f32),
            pltpu.VMEM((1, own_rows), i32),
            pltpu.VMEM((line, 1, own_rows), i32),
            pltpu.VMEM((line, own_rows, lanes), f32),
            pltpu.VMEM((blocks, line, own_rows, block), bf16),
            pltpu.VMEM((line, own_rows, lanes), f32),
            pltpu.VMEM((line, 1, own_rows), f32),
            pltpu.VMEM((line, line, 1, own_rows), f32),
            pltpu.VMEM((width, line * own_rows), bf16),
            pltpu.VMEM((line, own_rows, width), bf16),
            pltpu.VMEM((own_rows, width), f32),
            pltpu.VMEM((line, own_rows, width), bf16),
            pltpu.VMEM((nx, 2, 2) + rows_half, bf16),
            pltpu.VMEM((nx, 2, 2) + rows_half, bf16),
            pltpu.VMEM((nx, 2, 2) + rows_half, f32),
            pltpu.VMEM((nx, 2, 2) + rows_half, bf16),
            pltpu.VMEM((nx, 2) + rows_half, bf16),
            pltpu.VMEM((nx,) + rows_half, bf16),
            pltpu.VMEM(rows_half, bf16),
            pltpu.VMEM((nx,) + rows_half, bf16),
        ]
        + sems(
            3 * nx, 1 + nx, 4 * nx, 4 * nx, 4 * nx, line * cuts, line * cuts, line * cuts,
            blocks, blocks, line, line, line, line, line, line,
            2 * nx, 2 * nx, 2 * nx, 2 * nx, nx, nx, 1, 1, nx, nx,
        ),
        [vmem] * 6,
        40,
    )(
        query_unit,
        negative_unit.reshape(2, block // 2, width),
        positive_ids.reshape((1, -1) if own_rows % 128 == 0 else (nneg, own_rows)),
        negative_ids.reshape((1, -1) if block % 128 == 0 else (ndp, block)),
        negative_counts.reshape((1, -1) if block % 128 == 0 else (ndp, block)),
        positive_exp.reshape(1, own_rows),
    )
    own_denom = denom.reshape(-1)
    loss_part = jnp.sum(jnp.log(own_denom) - positive_logit)
    positive_slope = positive_exp / own_denom - 1.0
    query_sum = query_total / own_denom[:, None]
    negative_sum = negative_sum.reshape(width, block).T
    query_grad = (
        query_sum + positive_slope[:, None] * positive_unit.astype(jnp.float32)
    ) * inv_temp
    positive_grad = positive_slope[:, None] * query_unit.astype(jnp.float32) * inv_temp
    item_grad = jnp.concatenate([positive_grad, negative_sum * inv_temp], axis=0)
    query_grads = tower_backward(query_features, query_second, query_third, query_saved, query_grad)
    item_grads = tower_backward(item_features, item_second, item_third, item_saved, item_grad)
    gradients = query_grads + item_grads
    parts = [part for gradient in gradients for part in to_packed(gradient, ndp)]
    packed = jnp.concatenate(parts, axis=1)
    rows = packed.shape[1] // nneg
    packed = packed.reshape(ndp, nneg, 2, rows // 2, pack_columns).transpose(1, 0, 2, 3, 4)
    piece = (rows // 2, pack_columns)
    gathered, stats = call(
        weight_kernel,
        3,
        ndp,
        nneg,
        (jax.ShapeDtypeStruct((nneg, 2) + piece, bf16), jax.ShapeDtypeStruct((8, 128), f32)),
        [
            pltpu.VMEM((nx, ndp, 2) + piece, bf16),
            pltpu.VMEM((nx, 2, line) + piece, bf16),
            pltpu.VMEM((2, nx, line) + piece, bf16),
            pltpu.VMEM((nx, 2, line) + piece, bf16),
            pltpu.VMEM((nx, line) + piece, bf16),
            pltpu.VMEM((2, line) + piece, bf16),
            pltpu.VMEM((nx, line) + piece, bf16),
            pltpu.VMEM((line,) + piece, bf16),
            pltpu.VMEM((nx, line) + piece, bf16),
            pltpu.VMEM((2, line) + piece, bf16),
            pltpu.VMEM((2, line) + piece, bf16),
            pltpu.VMEM((8, 128), f32),
            pltpu.VMEM((ndp, 8, 128), f32),
            pltpu.VMEM((8, 128), f32),
            pltpu.VMEM((nneg, 8, 128), f32),
        ]
        + sems(nx, nx, 2 * nx, 2 * nx, 2, 2, ndp, ndp, ndp, ndp, nneg, nneg, nx, nx, nx, nx),
        [vmem, pl.BlockSpec(memory_space=pltpu.SMEM)],
    )(packed, loss_part.reshape(1))
    grad_norm = jnp.sqrt(stats[0, 0])
    mean_loss = stats[0, 1] / (own_rows * ndp * nneg)
    clip_factor = clip_norm / jnp.maximum(grad_norm, clip_norm)
    flat = gathered.reshape(nneg * rows, pack_columns)
    clipped = []
    start = 0
    for gradient in gradients:
        height, columns = gradient.shape[0] // ndp, gradient.shape[1]
        groups = columns // pack_columns
        blocks = [flat[start + g * height : start + (g + 1) * height] for g in range(groups)]
        start += groups * height
        clipped.append(jnp.concatenate(blocks, axis=1).astype(jnp.float32) * clip_factor)
    return (mean_loss, *clipped)


def solution(mesh):
    placed = (
        P(("dp", "neg"), None),
        P(("dp", "neg"), None),
        P(("neg", "dp"), None),
        P("dp"),
        P(("dp", "neg")),
        P("neg"),
        P("neg"),
        P(),
        P(),
        P(),
        P(),
        P(),
        P(),
    )
    return jax.shard_map(
        per_device,
        mesh=mesh,
        in_specs=placed,
        out_specs=(
            P(),
            P("dp", None),
            P("dp", None),
            P("dp", None),
            P("dp", None),
            P("dp", None),
            P("dp", None),
        ),
        check_vma=False,
    )
```

```python
import functools

import jax
import jax.numpy as jnp
from jax import lax
from jax.experimental import pallas as pl
from jax.experimental.pallas import tpu as pltpu
from jax.sharding import PartitionSpec as P

inv_temp = 20.0
log2_e = 1.4426950408889634
clip_norm = 256.0


def silu_slope(pre):
    sigma = jax.nn.sigmoid(pre)
    return sigma * (1.0 + pre * (1.0 - sigma))


def contract_rows(left, right):
    return lax.dot_general(
        left, right, (((0,), (0,)), ((), ())), preferred_element_type=jnp.float32
    )


def contract_cols(left, right):
    return lax.dot_general(
        left, right, (((1,), (1,)), ((), ())), preferred_element_type=jnp.float32
    )


def tower_forward(features, first, second, third):
    first_pre = jnp.dot(features, first, preferred_element_type=jnp.float32)
    first_act = jax.nn.silu(first_pre).astype(jnp.bfloat16)
    second_pre = jnp.dot(first_act, second, preferred_element_type=jnp.float32)
    second_act = jax.nn.silu(second_pre).astype(jnp.bfloat16)
    embedding = jnp.dot(second_act, third, preferred_element_type=jnp.float32)
    inv_norm = lax.rsqrt(jnp.sum(embedding * embedding, axis=1, keepdims=True) + 1.0)
    unit = (embedding * inv_norm).astype(jnp.bfloat16)
    saved = (silu_slope(first_pre), first_act, silu_slope(second_pre), second_act, embedding, inv_norm)
    return saved, unit


def tower_backward(features, second, third, saved, unit_grad):
    first_slope, first_act, second_slope, second_act, embedding, inv_norm = saved
    along = jnp.sum(embedding * unit_grad, axis=1, keepdims=True)
    embed_grad = (inv_norm * unit_grad - inv_norm * inv_norm * inv_norm * embedding * along).astype(
        jnp.bfloat16
    )
    third_grad = contract_rows(second_act, embed_grad)
    second_step = (contract_cols(embed_grad, third) * second_slope).astype(jnp.bfloat16)
    second_grad = contract_rows(first_act, second_step)
    first_step = (contract_cols(second_step, second) * first_slope).astype(jnp.bfloat16)
    first_grad = contract_rows(features, first_step)
    return (first_grad, second_grad, third_grad)


pack_columns = 256
vmem = pl.BlockSpec(memory_space=pltpu.VMEM)


def greet(ndp, nneg, me_dp, me_neg):
    barrier = pltpu.get_barrier_semaphore()
    for k in range(1, nneg):
        pl.semaphore_signal(
            barrier, inc=1, device_id={"neg": lax.rem(me_neg + k, nneg)}, device_id_type=pl.DeviceIdType.MESH
        )
    for k in range(1, ndp):
        pl.semaphore_signal(
            barrier, inc=1, device_id={"dp": lax.rem(me_dp + k, ndp)}, device_id_type=pl.DeviceIdType.MESH
        )
    pl.semaphore_wait(barrier, (nneg - 1) + (ndp - 1))


def send(src, dst, send_sem, recv_sem, axis, target):
    copy = pltpu.make_async_remote_copy(
        src_ref=src,
        dst_ref=dst,
        send_sem=send_sem,
        recv_sem=recv_sem,
        device_id={axis: target},
        device_id_type=pl.DeviceIdType.MESH,
    )
    copy.start()
    return copy


def share(axis, n, me, src_of, dst, send_sem, recv_sem):
    return [
        send(src_of(lax.rem(me + k, n)), dst.at[me], send_sem.at[k], recv_sem.at[k], axis, lax.rem(me + k, n))
        for k in range(1, n)
    ]


def finish(copies):
    for copy in copies:
        copy.wait()


def link(src, dst, sems, index, axis, target, send_index=None):
    send_sems, recv_sems = sems
    return pltpu.make_async_remote_copy(
        src_ref=src,
        dst_ref=dst,
        send_sem=send_sems.at[index if send_index is None else send_index],
        recv_sem=recv_sems.at[index],
        device_id={axis: target},
        device_id_type=pl.DeviceIdType.MESH,
    )


def score_kernel(
    ndp, nneg, query_ref, negative_ref, pid_ref, nid_ref, count_ref, pexp_ref, sum_ref, denom_ref, nsum_ref,
    q_land, n_land, meta_out, meta, rows, pid_out, pid_land, pid_col, w, den, dpart, dland, scaled,
    q_out, q_part, q_in, c_out, c_in, own, out, lx, ly, l2y, l2x,
    sx, sy, rn, sm, rm, sr, sl, rq, s_meta, r_meta, s_pid, r_pid, sd, rd, sq, rqs,
    sc, rc, s1x, r1x, s1y, r1y, s2y, r2y, s2x, r2x,
):
    me_dp, me_neg = lax.axis_index("dp"), lax.axis_index("neg")
    line, nx = ndp // 2, nneg // 2
    place, side = me_dp // 2, lax.rem(me_dp, 2)
    me_x, me_core = me_neg // 2, lax.rem(me_neg, 2)
    far, other = 1 - side, 1 - me_core
    partner, mate = 2 * place + far, 2 * me_x + other
    rows_q, width = query_ref.shape
    block = 2 * negative_ref.shape[1]
    lanes = den.shape[2]
    cuts = q_land.shape[1]
    half_w = width // 2
    blocks = nneg * 2
    here = (me_x * 2 + side) * 2 + me_core

    def along(k):
        return lax.rem(me_x + k, nx)

    def at_place(z):
        return 2 * z + side

    barrier = pltpu.get_barrier_semaphore()
    for k in range(1, line):
        pl.semaphore_signal(
            barrier, inc=1, device_id={"dp": at_place(lax.rem(place + k, line))}, device_id_type=pl.DeviceIdType.MESH
        )

    def quad(k):
        b = lax.rem(here + k, blocks)
        return {"dp": 2 * place + lax.rem(b // 2, 2), "neg": 2 * (b // 4) + lax.rem(b, 2)}

    for k in range(1, blocks):
        pl.semaphore_signal(barrier, inc=1, device_id=quad(k), device_id_type=pl.DeviceIdType.MESH)
    def own_ids(ref, index, count):
        if count % 128 == 0:
            return ref[:, pl.ds(pl.multiple_of(index * count, count), count)]
        return ref[pl.ds(index, 1), :]

    meta_out[0:1, :] = own_ids(nid_ref, me_dp, block)
    meta_out[1:2, :] = own_ids(count_ref, me_dp, block)
    pid_out[...] = own_ids(pid_ref, me_neg, rows_q)
    pl.semaphore_wait(barrier, (line - 1) + (blocks - 1))

    def slot(x, y, half):
        return (x * 2 + y) * 2 + half

    def piece(x, y, half):
        return n_land.at[(x * 2 + y) * 2 + me_core, half]

    def push(src, x, y, half, send_sems, index, axis, target):
        return link(src, piece(x, y, half), (send_sems, rn), slot(x, y, half), axis, target, index)

    def relay(src, x, y, half):
        i = slot(x, y, half)
        return link(src, piece(x, y, half), (sm, rm), i, "neg", mate)

    def landed(x, y, half):
        ref = piece(x, y, half)
        link(ref, ref, (sy, rn), slot(x, y, half), "neg", mate, 0).wait_recv()

    sends = []

    def go(copy):
        copy.start()
        sends.append(copy)

    def to_x(src, x, y, half, kind):
        for k in range(1, nx):
            go(push(src, x, y, half, sx, kind * nx + k, "neg", 2 * along(k) + me_core))

    def to_y(src, x, y, half, index):
        go(push(src, x, y, half, sy, index, "dp", partner))

    first, second = negative_ref.at[0], negative_ref.at[1]
    to_x(first, me_x, side, 0, 0)
    to_y(second, me_x, side, 1, 0)
    to_x(second, me_x, side, 1, 1)
    to_y(first, me_x, side, 0, 1)
    go(relay(first, me_x, side, 0))
    go(relay(second, me_x, side, 1))

    def chain(slot_z, j, distance, sems, target):
        src = query_ref.at[pl.ds(j * (rows_q // cuts), rows_q // cuts)] if distance == 0 else q_land.at[slot_z, j]
        return link(src, q_land.at[slot_z, j], (sems, rq), slot_z * cuts + j, "dp", target, distance * cuts + j)

    def right(distance, j):
        return chain(place - distance, j, distance, sr, at_place(lax.rem(place + 1, line)))

    def left(distance, j):
        return chain(place + distance, j, distance, sl, at_place(lax.rem(place + line - 1, line)))

    goes_right, goes_left = place < line - 1, place > 0
    for j in range(cuts):
        pl.when(goes_right)(lambda j=j: right(0, j).start())
        pl.when(goes_left)(lambda j=j: left(0, j).start())
    for k in range(1, blocks):
        b = lax.rem(here + k, blocks)
        copy = pltpu.make_async_remote_copy(
            src_ref=meta_out, dst_ref=meta.at[here], send_sem=s_meta.at[k], recv_sem=r_meta.at[here],
            device_id=quad(k), device_id_type=pl.DeviceIdType.MESH,
        )
        go(copy)
    for k in range(1, line):
        z = lax.rem(place + k, line)
        go(link(pid_out, pid_land.at[place], (s_pid, r_pid), place, "dp", at_place(z), k))
    n_land[here] = negative_ref[...]
    for j in range(cuts):
        q_land[place, j] = query_ref[pl.ds(j * (rows_q // cuts), rows_q // cuts), :]
    meta[here] = meta_out[...]
    pid_land[place] = pid_out[...]

    for k in range(1, nx):
        x = along(k)
        landed(x, side, 0)
        to_y(piece(x, side, 0), x, side, 0, 1 + k)
        go(relay(piece(x, side, 0), x, side, 0))
    landed(me_x, far, 1)
    to_x(piece(me_x, far, 1), me_x, far, 1, 2)
    go(relay(piece(me_x, far, 1), me_x, far, 1))

    def q_step(distance):
        for j in range(cuts):

            @pl.when(place >= distance)
            def _():
                ref = q_land.at[place - distance, j]
                link(ref, ref, (sr, rq), (place - distance) * cuts + j, "dp", partner, 0).wait_recv()
                pl.when(goes_right)(lambda: right(distance, j).start())

            @pl.when(place + distance < line)
            def _():
                ref = q_land.at[place + distance, j]
                link(ref, ref, (sl, rq), (place + distance) * cuts + j, "dp", partner, 0).wait_recv()
                pl.when(goes_left)(lambda: left(distance, j).start())

    q_step(1)
    for k in range(1, nx):
        x = along(k)
        landed(x, side, 1)
        go(relay(piece(x, side, 1), x, side, 1))
    landed(me_x, far, 0)
    go(relay(piece(me_x, far, 0), me_x, far, 0))
    for distance in range(2, line):
        q_step(distance)
    for half in range(2):
        for k in range(1, nx):
            x = along(k)
            landed(x, far, half)
            go(relay(piece(x, far, half), x, far, half))
    for x in range(nx):
        for y in range(2):
            for half in range(2):
                i = slot(x, y, half)
                ref = n_land.at[(x * 2 + y) * 2 + other, half]
                link(ref, ref, (sm, rm), i, "neg", mate).wait_recv()
    for k in range(1, blocks):
        b = lax.rem(here + k, blocks)
        link(meta.at[b], meta.at[b], (s_meta, r_meta), b, "neg", mate).wait_recv()
    for k in range(1, line):
        z = lax.rem(place + k, line)
        link(pid_land.at[z], pid_land.at[z], (s_pid, r_pid), z, "dp", partner).wait_recv()

    for b in range(blocks):
        rows[b, 0:1, :] = meta[b, 0:1, :].astype(jnp.float32)
        rows[b, 1:2, :] = jnp.log2(meta[b, 1:2, :].astype(jnp.float32))
    for z in range(line):
        pid_col[z] = jnp.broadcast_to(pid_land[z].astype(jnp.float32), (lanes, rows_q)).T
        den[z] = jnp.zeros((rows_q, lanes), jnp.float32)

    def unit(b, z):
        dots = contract_cols(q_land[z].reshape(rows_q, width), n_land[b].reshape(block, width))
        value = jnp.exp2(dots * (inv_temp * log2_e) - rows[b, 1:2, :])
        ids = jnp.concatenate([pid_col[z]] * (block // lanes), axis=1)
        value = jnp.where(ids != rows[b, 0:1, :], value, 0.0)
        w[b, z] = value.astype(jnp.bfloat16)
        total = den[z]
        for c in range(0, block, lanes):
            total = total + value[:, c : c + lanes]
        den[z] = total

    def units(b, carry):
        for z in range(line):
            unit(b, z)
        return carry

    lax.fori_loop(0, blocks, units, 0)
    for z in range(line):
        dpart[z] = jnp.sum(den[z].T, axis=0, keepdims=True)
    dpart[place] = dpart[place] + pexp_ref[...]
    for k in range(1, line):
        z = lax.rem(place + k, line)
        go(link(dpart, dland.at[place], (sd, rd), place, "dp", at_place(z), k))

    def q_block(z):
        if block % 128 == 0:
            left_side = jnp.concatenate([w[b, z] for b in range(blocks)], axis=1)
            return jnp.dot(
                left_side, n_land[...].reshape(blocks * block, width), preferred_element_type=jnp.float32
            )
        total = jnp.zeros((rows_q, width), jnp.float32)
        for b in range(blocks):
            total = total + jnp.dot(w[b, z], n_land[b].reshape(block, width), preferred_element_type=jnp.float32)
        return total

    def q_send(k, z):
        return link(q_out.at[z], q_in.at[place], (sq, rqs), place, "dp", at_place(z), k)

    def q_push(k, carry):
        z = lax.rem(place + k, line)
        q_out[z] = q_block(z).astype(jnp.bfloat16)
        q_send(k, z).start()
        return carry

    lax.fori_loop(1, line, q_push, 0)
    q_part[...] = q_block(place)
    total = dpart[...]
    for k in range(1, line):
        z = lax.rem(place + k, line)
        link(dland.at[z], dland.at[z], (sd, rd), z, "dp", partner).wait_recv()
        total = total + dland[z]
    dpart2 = 1.0 / total
    for z in range(line):
        q_t = q_land[z].reshape(rows_q, width).astype(jnp.float32).T
        scaled[:, z * rows_q : (z + 1) * rows_q] = (q_t * dpart2[z]).astype(jnp.bfloat16)
    denom_ref[...] = dpart[place]
    for k in range(1, line):
        denom_ref[...] = denom_ref[...] + dland[lax.rem(place + k, line), place]

    def dest(i):
        x = lax.rem(me_x + 1 + i // 2, nx)
        y = lax.rem(side + 1 + lax.rem(i, 2), 2)
        return x, y

    def part(x, y, core):
        return jnp.dot(
            scaled[...], w[(x * 2 + y) * 2 + core].reshape(line * rows_q, block), preferred_element_type=jnp.float32
        )

    def c_send(i):
        x, y = dest(i)
        return link(c_out.at[x, y], c_in.at[x, y], (sc, rc), x * 2 + y, "neg", mate)

    def far_step(i, carry):
        x, y = dest(i)
        c_out[x, y] = part(x, y, other).astype(jnp.bfloat16).reshape(2, half_w, block)
        c_send(i).start()
        return carry

    def send_1x(i):
        x, y = dest(i)
        return link(out.at[x, y, 0], lx.at[me_x, y], (s1x, r1x), me_x * 2 + y, "neg", 2 * x + me_core, x * 2 + y)

    def send_1y(i):
        x, y = dest(i)
        return link(out.at[x, y, 1], ly.at[x], (s1y, r1y), x, "dp", partner)

    def own_step(i, carry):
        x, y = dest(i)
        value = part(x, y, me_core).reshape(2, half_w, block)
        link(c_in.at[x, y], c_in.at[x, y], (sc, rc), x * 2 + y, "neg", mate).wait_recv()
        value = value + c_in[x, y].astype(jnp.float32)
        own[x, y] = value

        @pl.when(i < 2 * (nx - 1))
        def _():
            out[x, y, 0] = value[0].astype(jnp.bfloat16)
            send_1x(i).start()

        @pl.when(lax.rem(i, 2) == 0)
        def _():
            out[x, y, 1] = value[1].astype(jnp.bfloat16)
            send_1y(i).start()

        return carry

    lax.fori_loop(0, 2 * nx, far_step, 0)
    lax.fori_loop(0, 2 * nx, own_step, 0)
    value = own[me_x, far, 0]
    for k in range(1, nx):
        x = along(k)
        ref = lx.at[x, far]
        link(ref, ref, (s1x, r1x), x * 2 + far, "neg", mate).wait_recv()
        value = value + lx[x, far].astype(jnp.float32)
    out[me_x, far, 0] = value.astype(jnp.bfloat16)
    go(link(out.at[me_x, far, 0], l2y, (s2y, r2y), 0, "dp", partner))
    for k in range(1, nx):
        x = along(k)
        link(ly.at[x], ly.at[x], (s1y, r1y), x, "dp", partner).wait_recv()
        out[x, side, 1] = (own[x, side, 1] + ly[x].astype(jnp.float32)).astype(jnp.bfloat16)
        go(link(out.at[x, side, 1], l2x.at[me_x], (s2x, r2x), me_x, "neg", 2 * x + me_core, x))
    result = q_part[...]
    for k in range(1, line):
        z = lax.rem(place + k, line)
        link(q_in.at[z], q_in.at[z], (sq, rqs), z, "dp", partner).wait_recv()
        result = result + q_in[z].astype(jnp.float32)
    sum_ref[...] = result
    low = own[me_x, side, 0]
    for k in range(1, nx):
        x = along(k)
        ref = lx.at[x, side]
        link(ref, ref, (s1x, r1x), x * 2 + side, "neg", mate).wait_recv()
        low = low + lx[x, side].astype(jnp.float32)
    link(ly.at[me_x], ly.at[me_x], (s1y, r1y), me_x, "dp", partner).wait_recv()
    high = own[me_x, side, 1] + ly[me_x].astype(jnp.float32)
    link(l2y, l2y, (s2y, r2y), 0, "dp", partner).wait_recv()
    nsum_ref[0] = low + l2y[...].astype(jnp.float32)
    for k in range(1, nx):
        x = along(k)
        link(l2x.at[x], l2x.at[x], (s2x, r2x), x, "neg", mate).wait_recv()
        high = high + l2x[x].astype(jnp.float32)
    nsum_ref[1] = high

    for copy in sends:
        copy.wait_send()
    for distance in range(line):
        for j in range(cuts):
            if distance < line - 1:
                pl.when((place >= distance) & goes_right)(lambda: right(distance, j).wait_send())
                pl.when((place + distance < line) & goes_left)(lambda: left(distance, j).wait_send())
    for k in range(1, line):
        q_send(k, lax.rem(place + k, line)).wait_send()
    for i in range(2 * nx):
        c_send(i).wait_send()
        if i < 2 * (nx - 1):
            send_1x(i).wait_send()
        if i % 2 == 0:
            send_1y(i).wait_send()


def weight_kernel(
    ndp, nneg, packed_ref, loss_ref, gathered_ref, stats_ref,
    core_land, sum_a, sum_b, land_a, land_b, half_a, half_b, last_a, last_b, line_sum, line_land,
    stat_dp, stat_dp_land, stat_neg, stat_neg_land,
    cs, cr, xs, xr, ys, yr, ps, pr, ss, sr, ts, tr, gs, gr, hs, hr,
):
    me_dp, me_neg = lax.axis_index("dp"), lax.axis_index("neg")
    nx, line = nneg // 2, ndp // 2
    me_x, me_core = me_neg // 2, lax.rem(me_neg, 2)
    place, side = me_dp // 2, lax.rem(me_dp, 2)
    other, far = 1 - me_core, 1 - side
    mate, partner = 2 * me_x + other, 2 * place + far
    greet(ndp, nneg, me_dp, me_neg)
    turn = list(range(1, nx)) + [0]

    def x_of(k):
        return lax.rem(me_x + k, nx)

    core = {}
    for k in turn:
        x = x_of(k)
        core[k] = send(packed_ref.at[2 * x + other], core_land.at[x], cs.at[k], cr.at[k], "neg", mate)

    def add_core(x, y, half, target):
        def body(z, carry):
            target[z] = (
                packed_ref[2 * x + me_core, 2 * z + y, half].astype(jnp.float32)
                + core_land[x, 2 * z + y, half].astype(jnp.float32)
            ).astype(jnp.bfloat16)
            return carry

        lax.fori_loop(0, line, body, 0)

    def add(target, *terms):
        def body(z, carry):
            value = terms[0][z].astype(jnp.float32)
            for term in terms[1:]:
                value = value + term[z].astype(jnp.float32)
            target[z] = value.astype(jnp.bfloat16)
            return carry

        lax.fori_loop(0, line, body, 0)

    first_a = []
    for k in turn:
        x = x_of(k)
        core[k].wait_recv()
        if k:
            for y in range(2):
                add_core(x, y, 0, sum_a.at[x, y])
            first_a.append(send(sum_a.at[x], land_a.at[k], xs.at[k], xr.at[k], "neg", 2 * x + me_core))
        add_core(x, far, 1, sum_b.at[far, x])
    first_b = send(sum_b.at[far], land_b, ys.at[0], yr.at[0], "dp", partner)
    for y in range(2):
        add_core(me_x, y, 0, sum_a.at[me_x, y])
    for k in range(nx):
        add_core(x_of(k), side, 1, sum_b.at[side, x_of(k)])
    for copy in first_a:
        copy.wait_recv()
    add(half_a.at[far], sum_a.at[me_x, far], *[land_a.at[k, far] for k in range(1, nx)])
    second_a = send(half_a.at[far], last_a, ys.at[1], yr.at[1], "dp", partner)
    first_b.wait_recv()
    second_b = []
    for k in turn:
        x = x_of(k)
        add(half_b.at[x], sum_b.at[side, x], land_b.at[x])
        if k:
            second_b.append(
                send(half_b.at[x], last_b.at[k], xs.at[nx + k], xr.at[nx + k], "neg", 2 * x + me_core)
            )
    add(half_a.at[side], sum_a.at[me_x, side], *[land_a.at[k, side] for k in range(1, nx)])
    second_a.wait_recv()
    add(line_sum.at[0], half_a.at[side], last_a)
    third = []
    for half in range(2):
        if half:
            for copy in second_b:
                copy.wait_recv()
            add(line_sum.at[1], half_b.at[me_x], *[last_b.at[k] for k in range(1, nx)])
        for k in range(1, line):
            z = lax.rem(place + k, line)
            third.append(
                send(line_sum.at[half, z], line_land.at[half, k], ps.at[half * line + k], pr.at[half * line + k], "dp", 2 * z + side)
            )
    for copy in third:
        copy.wait_recv()
    squares = jnp.zeros((), jnp.float32)
    for half in range(2):
        piece = line_sum[half, place].astype(jnp.float32)
        for k in range(1, line):
            piece = piece + line_land[half, k].astype(jnp.float32)
        gathered_ref[me_neg, half] = piece.astype(jnp.bfloat16)
        squares = squares + jnp.sum(piece * piece)
    lane = lax.broadcasted_iota(jnp.int32, (8, 128), 1)
    stat_dp[...] = jnp.where(lane == 0, squares, loss_ref[0])
    stat_copies = share("dp", ndp, me_dp, lambda t: stat_dp, stat_dp_land, ss, sr)
    mine = gathered_ref.at[me_neg]
    spread = [send(mine, mine, gs.at[k], gr.at[k], "neg", 2 * x_of(k) + me_core) for k in range(1, nx)]
    spread.append(send(mine, mine, gs.at[0], gr.at[0], "neg", mate))
    finish(stat_copies)
    total = stat_dp[...]
    for k in range(1, ndp):
        total = total + stat_dp_land[lax.rem(me_dp + k, ndp)]
    stat_neg[...] = total
    stat_copies = share("neg", nneg, me_neg, lambda t: stat_neg, stat_neg_land, ts, tr)
    relay = []
    for k in range(1, nx):
        spread[k - 1].wait_recv()
        x = lax.rem(me_x + nx - k, nx)
        came = gathered_ref.at[2 * x + me_core]
        relay.append(send(came, came, hs.at[k], hr.at[k], "neg", mate))
    finish(stat_copies)
    total = stat_neg[...]
    for k in range(1, nneg):
        total = total + stat_neg_land[lax.rem(me_neg + k, nneg)]
    stats_ref[...] = total
    spread[-1].wait_recv()
    finish(relay)
    for copy in [*core.values(), *first_a, first_b, second_a, *second_b, *third, *spread]:
        copy.wait_send()


def call(kernel, collective, ndp, nneg, out_shape, scratch, in_specs, megabytes=48):
    return pl.pallas_call(
        functools.partial(kernel, ndp, nneg),
        out_shape=out_shape,
        in_specs=in_specs,
        out_specs=tuple(vmem for _ in out_shape),
        scratch_shapes=scratch,
        compiler_params=pltpu.CompilerParams(
            collective_id=collective, has_side_effects=True, vmem_limit_bytes=megabytes * 1024 * 1024
        ),
    )


def sems(*counts):
    return [pltpu.SemaphoreType.DMA((count,)) for count in counts]


def to_packed(gradient, ndp):
    rows, columns = gradient.shape
    blocks = gradient.astype(jnp.bfloat16).reshape(ndp, rows // ndp, columns)
    return [blocks[:, :, c : c + pack_columns] for c in range(0, columns, pack_columns)]


step_inputs = (
    "query_features", "positive_features", "negative_features", "positive_ids", "positive_counts", "negative_ids",
    "negative_counts", "query_first", "query_second", "query_third", "item_first", "item_second", "item_third",
)


def step_kernel(ndp, nneg, names, groups, *refs):
    refs = list(refs)
    inputs = dict(zip(step_inputs, refs))
    stats_ref, gathered = refs[13], refs[14:18]
    (
        sources, q_unit, n_unit, p_unit, towers, grads, pexp, logit,
        q_land, n_land, meta_out, meta, rows, pid_out, pid_land, pid_col, w, den, dpart, dland, scaled,
        q_out, q_part, q_in, c_out, c_in, own, out, lx, ly, l2y, l2x,
        sx, sy, rn, sm, rm, sr, sl, rq, s_meta, r_meta, s_pid, r_pid, sd, rd, sq, rqs,
        sc, rc, s1x, r1x, s1y, r1y, s2y, r2y, s2x, r2x, loaded,
        scratch, bufs, stat, stat_land, ss, sr2, left_sems,
    ) = jax.tree.unflatten(names, refs[18:])
    me_dp, me_neg = lax.axis_index("dp"), lax.axis_index("neg")
    line, nx = ndp // 2, nneg // 2
    place, side = me_dp // 2, lax.rem(me_dp, 2)
    me_x, me_core = me_neg // 2, lax.rem(me_neg, 2)
    far, other = 1 - side, 1 - me_core
    partner, mate = 2 * place + far, 2 * me_x + other
    f32, bf16 = jnp.float32, jnp.bfloat16
    rows_q, width = q_unit.shape
    block = 2 * n_unit.shape[1]
    half_n = block // 2
    lanes = den.shape[2]
    cuts = q_land.shape[1]
    half_w = width // 2
    blocks = nneg * 2
    here = (me_x * 2 + side) * 2 + me_core

    order = (
        "query_features", "query_first", "query_second", "query_third", "negative_features", "item_first", "item_second",
        "item_third", "negative_ids", "negative_counts", "positive_ids", "positive_features", "positive_counts",
    )
    item_features = sources["item_features"]
    places = dict(sources)
    places["negative_features"] = item_features.at[0:block]
    places["positive_features"] = item_features.at[block : block + rows_q]
    loads = {}
    for i, name in enumerate(order):
        loads[name] = pltpu.make_async_copy(inputs[name], places[name], loaded.at[i])
    for name in order[:4]:
        loads[name].start()

    def along(k):
        return lax.rem(me_x + k, nx)

    def at_place(z):
        return 2 * z + side

    barrier = pltpu.get_barrier_semaphore()

    def quad(k):
        b = lax.rem(here + k, blocks)
        return {"dp": 2 * place + lax.rem(b // 2, 2), "neg": 2 * (b // 4) + lax.rem(b, 2)}

    devices = ndp * nneg
    me = me_dp * nneg + me_neg

    def everyone(n):
        target = lax.rem(me + n, devices)
        return target // nneg, lax.rem(target, nneg)

    for n in range(1, devices):
        dp, neg = everyone(n)
        pl.semaphore_signal(barrier, inc=1, device_id={"dp": dp, "neg": neg}, device_id_type=pl.DeviceIdType.MESH)

    def slot(x, y, half):
        return (x * 2 + y) * 2 + half

    def piece(x, y, half):
        return n_land.at[(x * 2 + y) * 2 + me_core, half]

    def push(src, x, y, half, send_sems, index, axis, target):
        return link(src, piece(x, y, half), (send_sems, rn), slot(x, y, half), axis, target, index)

    def relay(src, x, y, half):
        i = slot(x, y, half)
        return link(src, piece(x, y, half), (sm, rm), i, "neg", mate)

    def landed(x, y, half):
        ref = piece(x, y, half)
        link(ref, ref, (sy, rn), slot(x, y, half), "neg", mate, 0).wait_recv()

    sends = []

    def go(copy):
        copy.start()
        sends.append(copy)

    def to_x(src, x, y, half, kind):
        for k in range(1, nx):
            go(push(src, x, y, half, sx, kind * nx + k, "neg", 2 * along(k) + me_core))

    def to_y(src, x, y, half, index):
        go(push(src, x, y, half, sy, index, "dp", partner))

    def chain(slot_z, j, distance, sems, target):
        src = q_unit.at[pl.ds(j * (rows_q // cuts), rows_q // cuts)] if distance == 0 else q_land.at[slot_z, j]
        return link(src, q_land.at[slot_z, j], (sems, rq), slot_z * cuts + j, "dp", target, distance * cuts + j)

    def right(distance, j):
        return chain(place - distance, j, distance, sr, at_place(lax.rem(place + 1, line)))

    def left(distance, j):
        return chain(place + distance, j, distance, sl, at_place(lax.rem(place + line - 1, line)))

    goes_right, goes_left = place < line - 1, place > 0

    def q_step(distance, lo=0, hi=cuts):
        for j in range(lo, hi):

            @pl.when(place >= distance)
            def _():
                ref = q_land.at[place - distance, j]
                link(ref, ref, (sr, rq), (place - distance) * cuts + j, "dp", partner, 0).wait_recv()
                pl.when(goes_right)(lambda: right(distance, j).start())

            @pl.when(place + distance < line)
            def _():
                ref = q_land.at[place + distance, j]
                link(ref, ref, (sl, rq), (place + distance) * cuts + j, "dp", partner, 0).wait_recv()
                pl.when(goes_left)(lambda: left(distance, j).start())

    def forward(lo, count, features, first, second, third, saved, unit_ref, waits=((), (), ()), starts=()):
        act1, slope1, act2, slope2, emb = saved
        span = slice(lo, lo + count)

        def layer(source, weight, act, slope):
            columns = weight.shape[1]
            step = 512 if columns % 512 == 0 else columns
            for c in range(0, columns, step):
                pre = jnp.dot(source[span, :], weight[:, c : c + step], preferred_element_type=f32)
                sigma = jax.nn.sigmoid(pre)
                act[span, c : c + step] = (pre * sigma).astype(bf16)
                slope[span, c : c + step] = sigma * (1.0 + pre * (1.0 - sigma))

        ready(waits[0])
        for name in starts:
            loads[name].start()
        layer(features, first, act1, slope1)
        ready(waits[1])
        layer(act1, second, act2, slope2)
        ready(waits[2])
        value = jnp.dot(act2[span, :], third[...], preferred_element_type=f32)
        emb[span, :] = value
        inv_norm = lax.rsqrt(jnp.sum(value * value, axis=1, keepdims=True) + 1.0)
        unit_ref[...] = (value * inv_norm).astype(bf16)

    def ready(chosen):
        for name in chosen:
            loads[name].wait()

    item_weights = tuple(sources[name] for name in ("item_first", "item_second", "item_third"))
    query_weights = tuple(sources[name] for name in ("query_first", "query_second", "query_third"))
    def own_ids(ref, index, count):
        return ref[:, pl.ds(pl.multiple_of(index * count, count), count)]

    forward(
        0, rows_q, sources["query_features"], *query_weights, towers[0], q_unit,
        (("query_features", "query_first"), ("query_second",), ("query_third",)),
        order[4:],
    )
    pl.semaphore_wait(barrier, devices - 1)
    for j in range(cuts):
        pl.when(goes_right)(lambda j=j: right(0, j).start())
        pl.when(goes_left)(lambda j=j: left(0, j).start())
    for j in range(cuts):
        q_land[place, j] = q_unit[pl.ds(j * (rows_q // cuts), rows_q // cuts), :]
    ready(("negative_ids", "negative_counts", "positive_ids"))
    meta_out[0:1, :] = own_ids(sources["negative_ids"], me_dp, block)
    meta_out[1:2, :] = own_ids(sources["negative_counts"], me_dp, block)
    pid_out[...] = own_ids(sources["positive_ids"], me_neg, rows_q)
    meta[here] = meta_out[...]
    pid_land[place] = pid_out[...]
    for k in range(1, blocks):
        copy = pltpu.make_async_remote_copy(
            src_ref=meta_out, dst_ref=meta.at[here], send_sem=s_meta.at[k], recv_sem=r_meta.at[here],
            device_id=quad(k), device_id_type=pl.DeviceIdType.MESH,
        )
        go(copy)
    for k in range(1, line):
        z = lax.rem(place + k, line)
        go(link(pid_out, pid_land.at[place], (s_pid, r_pid), place, "dp", at_place(z), k))
    n_first, n_second = n_unit.at[0], n_unit.at[1]
    forward(
        0, half_n, item_features, *item_weights, towers[1], n_first,
        (("negative_features", "item_first"), ("item_second",), ("item_third",)),
    )
    to_x(n_first, me_x, side, 0, 0)
    go(relay(n_first, me_x, side, 0))
    n_land[here, 0] = n_unit[0]
    forward(half_n, half_n, item_features, *item_weights, towers[1], n_second)
    to_y(n_second, me_x, side, 1, 0)
    to_x(n_second, me_x, side, 1, 1)
    to_y(n_first, me_x, side, 0, 1)
    go(relay(n_second, me_x, side, 1))
    n_land[here, 1] = n_unit[1]
    ready(("positive_features", "positive_counts"))
    forward(block, rows_q, item_features, *item_weights, towers[1], p_unit)
    q_step(1)
    product = q_unit[...].astype(f32) * p_unit[...].astype(f32)
    logit[...] = jnp.sum(product.T, axis=0, keepdims=True) * inv_temp - jnp.log(sources["positive_counts"][...].astype(f32))
    pexp[...] = jnp.exp(logit[...])

    for k in range(1, nx):
        x = along(k)
        landed(x, side, 0)
        to_y(piece(x, side, 0), x, side, 0, 1 + k)
        go(relay(piece(x, side, 0), x, side, 0))
    for k in range(1, blocks):
        b = lax.rem(here + k, blocks)
        link(meta.at[b], meta.at[b], (s_meta, r_meta), b, "neg", mate).wait_recv()
    for k in range(1, line):
        z = lax.rem(place + k, line)
        link(pid_land.at[z], pid_land.at[z], (s_pid, r_pid), z, "dp", partner).wait_recv()
    for b in range(blocks):
        rows[b, 0:1, :] = meta[b, 0:1, :].astype(f32)
        rows[b, 1:2, :] = jnp.log2(meta[b, 1:2, :].astype(f32))
    for z in range(line):
        pid_col[z] = jnp.broadcast_to(pid_land[z].astype(f32), (lanes, rows_q)).T
        den[z] = jnp.zeros((rows_q, lanes), f32)

    def unit(b, z):
        dots = contract_cols(q_land[z].reshape(rows_q, width), n_land[b].reshape(block, width))
        value = jnp.exp2(dots * (inv_temp * log2_e) - rows[b, 1:2, :])
        ids = jnp.concatenate([pid_col[z]] * (block // lanes), axis=1)
        value = jnp.where(ids != rows[b, 0:1, :], value, 0.0)
        w[b, z] = value.astype(jnp.bfloat16)
        total = den[z]
        for c in range(0, block, lanes):
            total = total + value[:, c : c + lanes]
        den[z] = total

    def relayed(x, y):
        for half in range(2):
            ref = n_land.at[(x * 2 + y) * 2 + other, half]
            link(ref, ref, (sm, rm), slot(x, y, half), "neg", mate).wait_recv()

    def both_cores(x, y):
        return [(x * 2 + y) * 2 + core for core in range(2)]

    near_blocks = both_cores(me_x, side)
    mid_blocks = both_cores(me_x, far)
    far_blocks = []
    for k in range(1, nx):
        mid_blocks = mid_blocks + both_cores(along(k), side)
        far_blocks = far_blocks + both_cores(along(k), far)

    def units(lo, hi, chosen):
        def body(z, carry):
            for b in chosen:
                unit(b, z)
            return carry

        lax.fori_loop(jnp.maximum(lo, 0), jnp.minimum(hi, line), body, 0)

    relayed(me_x, side)
    q_step(2, 0, cuts // 2)
    units(place - 1, place + 2, near_blocks)
    landed(me_x, far, 1)
    to_x(piece(me_x, far, 1), me_x, far, 1, 2)
    go(relay(piece(me_x, far, 1), me_x, far, 1))
    q_step(2, cuts // 2)
    units(place - 2, place - 1, near_blocks)
    units(place + 2, place + 3, near_blocks)
    for k in range(1, nx):
        x = along(k)
        landed(x, side, 1)
        go(relay(piece(x, side, 1), x, side, 1))
    for k in range(1, nx):
        relayed(along(k), side)
    landed(me_x, far, 0)
    go(relay(piece(me_x, far, 0), me_x, far, 0))
    relayed(me_x, far)
    units(place - 2, place + 3, mid_blocks)
    for distance in range(3, line):
        q_step(distance)
    for half in range(2):
        for k in range(1, nx):
            x = along(k)
            landed(x, far, half)
            go(relay(piece(x, far, half), x, far, half))
    units(0, place - 2, near_blocks + mid_blocks)
    units(place + 3, line, near_blocks + mid_blocks)
    for k in range(1, nx):
        relayed(along(k), far)
    units(0, line, far_blocks)
    for z in range(line):
        dpart[z] = jnp.sum(den[z].T, axis=0, keepdims=True)
    dpart[place] = dpart[place] + pexp[...]
    for k in range(1, line):
        z = lax.rem(place + k, line)
        go(link(dpart, dland.at[place], (sd, rd), place, "dp", at_place(z), k))

    def q_block(z):
        if block % 128 == 0:
            left_side = jnp.concatenate([w[b, z] for b in range(blocks)], axis=1)
            return jnp.dot(
                left_side, n_land[...].reshape(blocks * block, width), preferred_element_type=jnp.float32
            )
        total = jnp.zeros((rows_q, width), jnp.float32)
        for b in range(blocks):
            total = total + jnp.dot(w[b, z], n_land[b].reshape(block, width), preferred_element_type=jnp.float32)
        return total

    def q_send(k, z):
        return link(q_out.at[z], q_in.at[place], (sq, rqs), place, "dp", at_place(z), k)

    def q_push(k, carry):
        z = lax.rem(place + k, line)
        q_out[z] = q_block(z).astype(jnp.bfloat16)
        q_send(k, z).start()
        return carry

    lax.fori_loop(1, line, q_push, 0)
    q_part[...] = q_block(place)
    total = dpart[...]
    for k in range(1, line):
        z = lax.rem(place + k, line)
        link(dland.at[z], dland.at[z], (sd, rd), z, "dp", partner).wait_recv()
        total = total + dland[z]
    dpart2 = 1.0 / total
    for z in range(line):
        q_t = q_land[z].reshape(rows_q, width).astype(jnp.float32).T
        scaled[:, z * rows_q : (z + 1) * rows_q] = (q_t * dpart2[z]).astype(jnp.bfloat16)
    def dest(i):
        x = lax.rem(me_x + 1 + i // 2, nx)
        y = lax.rem(side + 1 + lax.rem(i, 2), 2)
        return x, y

    def part(x, y, core):
        return jnp.dot(
            scaled[...], w[(x * 2 + y) * 2 + core].reshape(line * rows_q, block), preferred_element_type=jnp.float32
        )

    def c_send(i):
        x, y = dest(i)
        return link(c_out.at[x, y], c_in.at[x, y], (sc, rc), x * 2 + y, "neg", mate)

    def far_step(i, carry):
        x, y = dest(i)
        c_out[x, y] = part(x, y, other).astype(jnp.bfloat16).reshape(2, half_w, block)
        c_send(i).start()
        return carry

    def send_1x(i):
        x, y = dest(i)
        return link(out.at[x, y, 0], lx.at[me_x, y], (s1x, r1x), me_x * 2 + y, "neg", 2 * x + me_core, x * 2 + y)

    def send_1y(i):
        x, y = dest(i)
        return link(out.at[x, y, 1], ly.at[x], (s1y, r1y), x, "dp", partner)

    def own_step(i, carry):
        x, y = dest(i)
        value = part(x, y, me_core).reshape(2, half_w, block)
        link(c_in.at[x, y], c_in.at[x, y], (sc, rc), x * 2 + y, "neg", mate).wait_recv()
        value = value + c_in[x, y].astype(jnp.float32)
        own[x, y] = value

        @pl.when(i < 2 * (nx - 1))
        def _():
            out[x, y, 0] = value[0].astype(jnp.bfloat16)
            send_1x(i).start()

        @pl.when(lax.rem(i, 2) == 0)
        def _():
            out[x, y, 1] = value[1].astype(jnp.bfloat16)
            send_1y(i).start()

        return carry

    ahead = 2

    def both_steps(i, carry):
        far_step(i + ahead, 0)
        own_step(i, 0)
        return carry

    lax.fori_loop(0, ahead, far_step, 0)
    lax.fori_loop(0, 2 * nx - ahead, both_steps, 0)
    lax.fori_loop(2 * nx - ahead, 2 * nx, own_step, 0)
    value = own[me_x, far, 0]
    for k in range(1, nx):
        x = along(k)
        ref = lx.at[x, far]
        link(ref, ref, (s1x, r1x), x * 2 + far, "neg", mate).wait_recv()
        value = value + lx[x, far].astype(jnp.float32)
    out[me_x, far, 0] = value.astype(jnp.bfloat16)
    go(link(out.at[me_x, far, 0], l2y, (s2y, r2y), 0, "dp", partner))
    for k in range(1, nx):
        x = along(k)
        link(ly.at[x], ly.at[x], (s1y, r1y), x, "dp", partner).wait_recv()
        out[x, side, 1] = (own[x, side, 1] + ly[x].astype(jnp.float32)).astype(jnp.bfloat16)
        go(link(out.at[x, side, 1], l2x.at[me_x], (s2x, r2x), me_x, "neg", 2 * x + me_core, x))
    denom = dpart[place]
    for k in range(1, line):
        denom = denom + dland[lax.rem(place + k, line), place]
    loss_part = jnp.sum(jnp.log(denom) - logit[...])

    def to_columns(row):
        column = jnp.broadcast_to(row, (lanes, rows_q)).T
        return jnp.concatenate([column] * (width // lanes), axis=1)

    slope_columns = to_columns(pexp[...] / denom - 1.0) * inv_temp
    grads[1][block : block + rows_q, :] = slope_columns * q_unit[...].astype(f32)
    result = q_part[...]
    for k in range(1, line):
        z = lax.rem(place + k, line)
        link(q_in.at[z], q_in.at[z], (sq, rqs), z, "dp", partner).wait_recv()
        result = result + q_in[z].astype(jnp.float32)
    grads[0][...] = result * (to_columns(1.0 / denom) * inv_temp) + slope_columns * p_unit[...].astype(f32)

    pending = []

    def queue(copy):
        copy.start()
        pending.append(copy)

    def x_of(k):
        return lax.rem(me_x + k, nx)

    def same_core(x):
        return 2 * x + me_core

    def z_of(k):
        return lax.rem(place + k, line)

    def arrived(ref, sem_array, index):
        link(ref, ref, (sem_array, sem_array), index, "neg", mate).wait_recv()

    steps = [
        (sources["query_features"], *towers[0], grads[0], sources["query_second"], sources["query_third"]),
        (item_features, *towers[1], grads[1], sources["item_second"], sources["item_third"]),
    ]

    def store(group, offset, value, dp, hg):
        packed = bufs[group]["packed"]
        pieces = hg // nneg
        for p in range(value.shape[1] // pack_columns):
            part = value[:, p * pack_columns : (p + 1) * pack_columns].astype(bf16)
            part = part.reshape(value.shape[0] // hg, nx, 2, pieces, pack_columns)
            lo = offset + p * pieces
            for core in range(2):
                packed[core, pl.ds(dp, value.shape[0] // hg), :, lo : lo + pieces, :] = part[:, :, core]

    def weight_grad(group, offset, left_ref, right_ref):
        rows, columns = left_ref.shape[1], right_ref.shape[1]
        hg = rows // ndp
        step = 2 * hg

        def body(m, carry):
            left = left_ref[:, pl.ds(pl.multiple_of(m * step, step), step)]
            store(group, offset, contract_rows(left, right_ref[...]), 2 * m, hg)
            return carry

        lax.fori_loop(0, rows // step, body, 0, unroll=True)
        return offset + hg // nneg * (columns // pack_columns)

    def row_loop(count, body):
        step = 256 if count % 256 == 0 else count

        def wrapped(i, carry):
            body(pl.ds(pl.multiple_of(i * step, step), step))
            return carry

        lax.fori_loop(0, count // step, wrapped, 0)

    def embed_stage(t):
        feat, act1, slope1, act2, slope2, emb_ref, grad_ref, second, third = steps[t]
        eg, s2, s1 = scratch[t]

        def body(rows):
            emb, grad = emb_ref[rows, :], grad_ref[rows, :]
            inv_norm = lax.rsqrt(jnp.sum(emb * emb, axis=1, keepdims=True) + 1.0)
            along = jnp.sum(emb * grad, axis=1, keepdims=True)
            value = (inv_norm * grad - inv_norm * inv_norm * inv_norm * emb * along).astype(bf16)
            eg[rows, :] = value
            s2[rows, :] = (contract_cols(value, third[...]) * slope2[rows, :]).astype(bf16)

        row_loop(feat.shape[0], body)

    def second_stage(t, group):
        feat, act1, slope1, act2, slope2, emb_ref, grad_ref, second, third = steps[t]
        eg, s2, s1 = scratch[t]
        offset = weight_grad(group, 0, act2, eg)
        weight_grad(group, offset, act1, s2)

    def slope_stage(t):
        feat, act1, slope1, act2, slope2, emb_ref, grad_ref, second, third = steps[t]
        eg, s2, s1 = scratch[t]
        columns = second.shape[0]

        def body(rows):
            for c in range(0, columns, 512):
                value = contract_cols(s2[rows, :], second[c : c + 512, :]) * slope1[rows, c : c + 512]
                s1[rows, c : c + 512] = value.astype(bf16)

        row_loop(feat.shape[0], body)

    def first_stage(t, group):
        weight_grad(group, 0, steps[t][0], scratch[t][2])

    def stage0(g):
        b = bufs[g]
        queue(link(b["packed"].at[other], b["c_in"], (b["cs"], b["cr"]), 0, "neg", mate))

    def base(b, dp, x, lo, hi):
        return b["packed"][me_core, dp, x, lo:hi, :].astype(f32) + b["c_in"][dp, x, lo:hi, :].astype(f32)

    def loop(count, body):
        def wrapped(i, carry):
            body(i)
            return carry

        lax.fori_loop(0, count, wrapped, 0)

    def stage1(g):
        b, (r1, r, full) = bufs[g], groups[g]
        arrived(b["c_in"], b["cr"], 0)
        for k in range(1, line):
            z = z_of(k)
            for y in range(2):
                for x in range(nx):
                    b["o1z"][z, y, x] = base(b, 2 * z + y, x, r, full).astype(bf16)
            queue(link(b["o1z"].at[z], b["l1z"].at[place], (b["s1z"], b["r1z"]), place, "dp", 2 * z + side, z))
        for k in range(1, nx):
            x = x_of(k)

            def body(dp):
                b["o1x"][x, dp] = base(b, dp, x, 0, r1).astype(bf16)

            loop(ndp, body)
            queue(link(b["o1x"].at[x], b["l1x"].at[me_x], (b["s1x"], b["r1x"]), me_x, "neg", same_core(x), x))

        def body_y(z):
            for x in range(nx):
                b["o1y"][z, x] = base(b, 2 * z + far, x, r1, r).astype(bf16)

        loop(line, body_y)
        queue(link(b["o1y"], b["l1y"], (b["s1y"], b["r1y"]), 0, "dp", partner))

    def low(b, dp, r1):
        value = base(b, dp, me_x, 0, r1)
        for k in range(1, nx):
            value = value + b["l1x"][x_of(k), dp].astype(f32)
        return value

    def stage2(g):
        b, (r1, r, full) = bufs[g], groups[g]
        for k in range(1, nx):
            x = x_of(k)
            arrived(b["l1x"].at[x], b["r1x"], x)

        def body(z):
            b["o2y"][z] = low(b, 2 * z + far, r1).astype(bf16)

        loop(line, body)
        queue(link(b["o2y"], b["l2y"], (b["s2y"], b["r2y"]), 0, "dp", partner))
        arrived(b["l1y"], b["r1y"], 0)
        for k in range(1, nx):
            x = x_of(k)

            def body_x(z):
                value = base(b, 2 * z + side, x, r1, r) + b["l1y"][z, x].astype(f32)
                b["o2x"][x, z] = value.astype(bf16)

            loop(line, body_x)
            queue(link(b["o2x"].at[x], b["l2x"].at[me_x], (b["s2x"], b["r2x"]), me_x, "neg", same_core(x), x))

    def stage3(g):
        b, (r1, r, full) = bufs[g], groups[g]
        arrived(b["l2y"], b["r2y"], 0)
        for k in range(1, nx):
            x = x_of(k)
            arrived(b["l2x"].at[x], b["r2x"], x)

        def body(z):
            dp = 2 * z + side
            b["zs"][z, 0:r1, :] = (low(b, dp, r1) + b["l2y"][z].astype(f32)).astype(bf16)
            value = base(b, dp, me_x, r1, r) + b["l1y"][z, me_x].astype(f32)
            for k in range(1, nx):
                value = value + b["l2x"][x_of(k), z].astype(f32)
            b["zs"][z, r1:r, :] = value.astype(bf16)

        loop(line, body)
        for k in range(1, line):
            z = z_of(k)
            queue(link(b["zs"].at[z], b["l3"].at[place], (b["s3"], b["r3"]), place, "dp", 2 * z + side, z))

    def z_sum(g, y, x):
        b, (_, r, full) = bufs[g], groups[g]
        value = base(b, 2 * place + y, x, r, full)
        for k in range(1, line):
            value = value + b["l1z"][z_of(k), y, x].astype(f32)
        return value

    def x_sum(g, y):
        value = z_sum(g, y, me_x)
        for k in range(1, nx):
            value = value + bufs[g]["l2z"][x_of(k), y].astype(f32)
        return value

    def stage2z(g):
        b = bufs[g]
        for k in range(1, line):
            z = z_of(k)
            arrived(b["l1z"].at[z], b["r1z"], z)
        for k in range(1, nx):
            x = x_of(k)
            for y in range(2):
                b["o2z"][x, y] = z_sum(g, y, x).astype(bf16)
            queue(link(b["o2z"].at[x], b["l2z"].at[me_x], (b["s2z"], b["r2z"]), me_x, "neg", same_core(x), x))

    def stage3z(g):
        b = bufs[g]
        for k in range(1, nx):
            x = x_of(k)
            arrived(b["l2z"].at[x], b["r2z"], x)
        b["o3z"][...] = x_sum(g, far).astype(bf16)
        queue(link(b["o3z"], b["l3z"], (b["s3z"], b["r3z"]), 0, "dp", partner))

    squares = []

    def stage4(g):
        b, (_, r, full) = bufs[g], groups[g]
        for k in range(1, line):
            z = z_of(k)
            arrived(b["l3"].at[z], b["r3"], z)
        value = b["zs"][place].astype(f32)
        for k in range(1, line):
            value = value + b["l3"][z_of(k)].astype(f32)
        arrived(b["l3z"], b["r3z"], 0)
        last = x_sum(g, side) + b["l3z"][...].astype(f32)
        squares.append(jnp.sum(value * value) + jnp.sum(last * last))
        b["ag"][me_neg, 0:r] = value.astype(bf16)
        b["ag"][me_neg, r:full] = last.astype(bf16)

    def spread(g):
        b = bufs[g]
        mine = b["ag"].at[me_neg]
        for k in range(1, nx):
            x = x_of(k)
            queue(link(mine, mine, (b["sg"], b["rg"]), me_x, "neg", same_core(x), x))
        queue(link(mine, mine, (b["sh"], b["rh"]), me_x, "neg", mate))

    def stage5(g):
        b = bufs[g]
        for k in range(1, nx):
            x = x_of(k)
            ref = b["ag"].at[same_core(x)]
            arrived(ref, b["rg"], x)
            queue(link(ref, ref, (b["sh"], b["rh"]), x, "neg", mate))

    leaving = []

    def leave(source, target, index):
        copy = pltpu.make_async_copy(source, target, left_sems.at[index])
        copy.start()
        leaving.append(copy)

    def stage6(g):
        b = bufs[g]
        for x in range(nx):
            arrived(b["ag"].at[2 * x + other], b["rh"], x)
        leave(b["ag"], gathered[g], g)

    embed_stage(0)
    second_stage(0, 0)
    stage0(0)
    slope_stage(0)
    first_stage(0, 1)
    stage0(1)
    stage1(0)
    n_low = own[me_x, side, 0]
    for k in range(1, nx):
        x = along(k)
        ref = lx.at[x, side]
        link(ref, ref, (s1x, r1x), x * 2 + side, "neg", mate).wait_recv()
        n_low = n_low + lx[x, side].astype(jnp.float32)
    link(ly.at[me_x], ly.at[me_x], (s1y, r1y), me_x, "dp", partner).wait_recv()
    n_high = own[me_x, side, 1] + ly[me_x].astype(jnp.float32)
    link(l2y, l2y, (s2y, r2y), 0, "dp", partner).wait_recv()
    n_low = n_low + l2y[...].astype(jnp.float32)
    for k in range(1, nx):
        x = along(k)
        link(l2x.at[x], l2x.at[x], (s2x, r2x), x, "neg", mate).wait_recv()
        n_high = n_high + l2x[x].astype(jnp.float32)

    grads[1][0:block, 0:half_w] = n_low.T * inv_temp
    grads[1][0:block, half_w:width] = n_high.T * inv_temp
    stage1(1)
    embed_stage(1)
    second_stage(1, 2)
    stage0(2)
    slope_stage(1)
    stage2(0)
    stage1(2)
    first_stage(1, 3)
    stage0(3)
    stage2(1)
    stage1(3)
    stage3(0)
    stage2z(0)
    stage2(2)
    stage2z(1)
    stage3(1)
    stage2z(2)
    stage2(3)
    stage2z(3)
    stage3z(0)
    stage3z(1)
    stage3(2)
    stage3z(2)
    stage3(3)
    stage3z(3)
    for g in range(2):
        stage4(g)
        spread(g)
    for g in range(2, 4):
        stage4(g)
    total_squares = squares[0] + squares[1] + squares[2] + squares[3]
    lane = lax.broadcasted_iota(jnp.int32, (1, 128), 1)
    stat[...] = jnp.where(lane == 0, total_squares, loss_part)
    for n in range(1, devices):
        dp, neg = everyone(n)
        copy = pltpu.make_async_remote_copy(
            src_ref=stat, dst_ref=stat_land.at[me], send_sem=ss.at[n], recv_sem=sr2.at[me],
            device_id={"dp": dp, "neg": neg}, device_id_type=pl.DeviceIdType.MESH,
        )
        queue(copy)
    for g in range(2, 4):
        spread(g)
    for g in range(4):
        stage5(g)
    for g in range(4):
        stage6(g)
    stat_land[me] = stat[...]
    for n in range(1, devices):
        source = lax.rem(me + n, devices)
        arrived(stat_land.at[source], sr2, source)
    stat_land[me] = jnp.sum(stat_land[...], axis=0)
    leave(stat_land.at[me], stats_ref, 4)
    for copy in pending:
        copy.wait_send()
    for copy in leaving:
        copy.wait()


    for copy in sends:
        copy.wait_send()
    for distance in range(line):
        for j in range(cuts):
            if distance < line - 1:
                pl.when((place >= distance) & goes_right)(lambda: right(distance, j).wait_send())
                pl.when((place + distance < line) & goes_left)(lambda: left(distance, j).wait_send())
    for k in range(1, line):
        q_send(k, lax.rem(place + k, line)).wait_send()
    for i in range(2 * nx):
        c_send(i).wait_send()
        if i < 2 * (nx - 1):
            send_1x(i).wait_send()
        if i % 2 == 0:
            send_1y(i).wait_send()


def fused_step(ndp, nneg, arguments):
    line, nx = ndp // 2, nneg // 2
    bf16, f32, i32 = jnp.bfloat16, jnp.float32, jnp.int32
    named = dict(zip(step_inputs, arguments))
    fin, h1 = named["item_first"].shape
    h2, width = named["item_third"].shape
    own_rows, block = named["query_features"].shape[0], named["negative_features"].shape[0]
    blocks, cuts, lanes = 2 * nneg, 4, 128
    rows_half = (width // 2, block)
    sources = {"item_features": pltpu.VMEM((block + own_rows, fin), bf16)}
    for name, value in named.items():
        if name not in ("positive_features", "negative_features"):
            sources[name] = pltpu.VMEM(value.shape, value.dtype)
    counts = (own_rows, block + own_rows)
    towers = [
        [
            pltpu.VMEM((count, h1), bf16), pltpu.VMEM((count, h1), f32), pltpu.VMEM((count, h2), bf16),
            pltpu.VMEM((count, h2), f32), pltpu.VMEM((count, width), f32),
        ]
        for count in counts
    ]
    scratch = [
        [pltpu.VMEM((count, width), bf16), pltpu.VMEM((count, h2), bf16), pltpu.VMEM((count, h1), bf16)]
        for count in counts
    ]
    row = pltpu.VMEM((1, own_rows), f32)
    score = [
        pltpu.VMEM((line, cuts, own_rows // cuts, width), bf16),
        pltpu.VMEM((blocks, 2, block // 2, width), bf16),
        pltpu.VMEM((2, block), i32),
        pltpu.VMEM((blocks, 2, block), i32),
        pltpu.VMEM((blocks, 2, block), f32),
        pltpu.VMEM((1, own_rows), i32),
        pltpu.VMEM((line, 1, own_rows), i32),
        pltpu.VMEM((line, own_rows, lanes), f32),
        pltpu.VMEM((blocks, line, own_rows, block), bf16),
        pltpu.VMEM((line, own_rows, lanes), f32),
        pltpu.VMEM((line, 1, own_rows), f32),
        pltpu.VMEM((line, line, 1, own_rows), f32),
        pltpu.VMEM((width, line * own_rows), bf16),
        pltpu.VMEM((line, own_rows, width), bf16),
        pltpu.VMEM((own_rows, width), f32),
        pltpu.VMEM((line, own_rows, width), bf16),
        pltpu.VMEM((nx, 2, 2) + rows_half, bf16),
        pltpu.VMEM((nx, 2, 2) + rows_half, bf16),
        pltpu.VMEM((nx, 2, 2) + rows_half, f32),
        pltpu.VMEM((nx, 2, 2) + rows_half, bf16),
        pltpu.VMEM((nx, 2) + rows_half, bf16),
        pltpu.VMEM((nx,) + rows_half, bf16),
        pltpu.VMEM(rows_half, bf16),
        pltpu.VMEM((nx,) + rows_half, bf16),
    ] + sems(
        3 * nx, 1 + nx, 4 * nx, 4 * nx, 4 * nx, line * cuts, line * cuts, line * cuts,
        blocks, blocks, line, line, line, line, line, line,
        2 * nx, 2 * nx, 2 * nx, 2 * nx, nx, nx, 1, 1, nx, nx, len(step_inputs),
    )
    groups, outs, bufs = [], [], []
    for _ in counts:
        for height, columns in ((fin, h1), (h1, h2), (h2, width)):
            outs.append(jax.ShapeDtypeStruct((height // ndp, columns), f32))
        both = h2 // (ndp * nneg) * (width // pack_columns) + h1 // (ndp * nneg) * (h2 // pack_columns)
        alone = fin // (ndp * nneg) * (h1 // pack_columns)
        for r in (both, alone):
            spare = r // 16 - 1
            low = spare // 2 + (spare % 2 if len(groups) == 3 else 0)
            groups.append((low * 16, spare * 16, r))
    c = pack_columns
    sem_names = ["cs", "cr", "s1x", "r1x", "s1y", "r1y", "s2y", "r2y", "s2x", "r2x", "s3", "r3", "sg", "rg", "sh", "rh"]
    sem_names += ["s1z", "r1z", "s2z", "r2z", "s3z", "r3z"]
    for r1, r, full in groups:
        r2, r4 = r - r1, full - r
        shapes = dict(
            packed=(2, ndp, nx, full, c), c_in=(ndp, nx, full, c), o1x=(nx, ndp, r1, c), l1x=(nx, ndp, r1, c),
            o1y=(line, nx, r2, c), l1y=(line, nx, r2, c), o2y=(line, r1, c), l2y=(line, r1, c),
            o2x=(nx, line, r2, c), l2x=(nx, line, r2, c), zs=(line, r, c), l3=(line, r, c), ag=(nneg, full, c),
            o1z=(line, 2, nx, r4, c), l1z=(line, 2, nx, r4, c), o2z=(nx, 2, r4, c), l2z=(nx, 2, r4, c), o3z=(r4, c), l3z=(r4, c),
        )
        buf = {name: pltpu.VMEM(shape, bf16) for name, shape in shapes.items()}
        buf.update(zip(sem_names, sems(1, 1, nx, nx, 1, 1, 1, 1, nx, nx, line, line, nx, nx, nx, nx, line, line, nx, nx, 1, 1)))
        bufs.append(buf)
    tree = (
        sources, pltpu.VMEM((own_rows, width), bf16), pltpu.VMEM((2, block // 2, width), bf16),
        pltpu.VMEM((own_rows, width), bf16), towers, [pltpu.VMEM((count, width), f32) for count in counts], row, row,
        *score, scratch, bufs,
        pltpu.VMEM((1, 128), f32), pltpu.VMEM((ndp * nneg, 1, 128), f32), *sems(ndp * nneg, ndp * nneg, 5),
    )
    leaves, names = jax.tree.flatten(tree)
    space = sems(1)[0].memory_space
    is_flag = [leaf.memory_space == space for leaf in leaves]
    flags = [leaf for leaf, flag in zip(leaves, is_flag) if flag]
    kept = [leaf for leaf, flag in zip(leaves, is_flag) if not flag]

    def kernel(*refs):
        fixed = refs[: len(refs) - len(kept)]
        held = refs[len(refs) - len(kept) :]

        def scoped(*flag_refs):
            held_refs, flags_left = iter(held), iter(flag_refs)
            merged = [next(flags_left) if flag else next(held_refs) for flag in is_flag]
            step_kernel(ndp, nneg, names, tuple(groups), *fixed, *merged)

        pl.run_scoped(scoped, *flags)

    any_space = pl.BlockSpec(memory_space=pl.ANY)
    stats, *gathered = pl.pallas_call(
        kernel,
        out_shape=(
            jax.ShapeDtypeStruct((1, 128), f32),
            *[jax.ShapeDtypeStruct((nneg, group[-1], pack_columns), bf16) for group in groups],
        ),
        in_specs=[any_space] * len(arguments),
        out_specs=(any_space,) * 5,
        scratch_shapes=kept,
        compiler_params=pltpu.CompilerParams(
            collective_id=1, has_side_effects=True, vmem_limit_bytes=67043328
        ),
    )(*arguments)
    mean_loss, *clipped = pl.pallas_call(
        functools.partial(finish_kernel, nneg, own_rows * ndp * nneg),
        out_shape=(jax.ShapeDtypeStruct((1,), f32), *outs),
        in_specs=[any_space] * 5,
        out_specs=(pl.BlockSpec(memory_space=pltpu.SMEM), *([any_space] * 6)),
        scratch_shapes=[pltpu.VMEM((1, 128), f32)]
        + [pltpu.VMEM((nneg, group[-1], pack_columns), bf16) for group in groups]
        + [pltpu.VMEM(out.shape, f32) for out in outs]
        + sems(5, 6),
    )(stats, *gathered)
    return (mean_loss.reshape(()), *clipped)


def finish_kernel(nneg, count, *refs):
    given, loss_ref, outs, stats_ref, gathered, staged = refs[:5], refs[5], refs[6:12], refs[12], refs[13:17], refs[17:23]
    loaded, done = refs[23:]
    loads = [
        pltpu.make_async_copy(source, target, loaded.at[i])
        for i, (source, target) in enumerate(zip(given, (stats_ref, *gathered)))
    ]
    for copy in loads:
        copy.start()
    for copy in loads:
        copy.wait()
    clip = clip_norm / jnp.maximum(jnp.sqrt(stats_ref[0:1, 0:1]), clip_norm)
    copies = []
    for t in range(2):
        third_ref, second_ref, first_ref = staged[3 * t + 2], staged[3 * t + 1], staged[3 * t]
        for index, group, ref, offset in (
            (3 * t + 1, 2 * t, second_ref, third_ref.shape[0] // nneg),
            (3 * t, 2 * t + 1, first_ref, 0),
            (3 * t + 2, 2 * t, third_ref, 0),
        ):
            pieces = ref.shape[0] // nneg
            for p in range(ref.shape[1] // pack_columns):
                lo = offset + p * pieces
                for n in range(nneg):
                    value = gathered[group][n, lo : lo + pieces, :].astype(jnp.float32) * clip
                    ref[n * pieces : (n + 1) * pieces, p * pack_columns : (p + 1) * pack_columns] = value
            copy = pltpu.make_async_copy(ref, outs[index], done.at[index])
            copy.start()
            copies.append(copy)
    loss_ref[0] = jnp.sum(stats_ref[0:1, 1:2]) / count
    for copy in copies:
        copy.wait()


def per_device(
    query_features,
    positive_features,
    negative_features,
    positive_ids,
    positive_counts,
    negative_ids,
    negative_counts,
    query_first,
    query_second,
    query_third,
    item_first,
    item_second,
    item_third,
):
    own_rows = query_features.shape[0]
    ndp, nneg = lax.axis_size("dp"), lax.axis_size("neg")
    heights = (query_first.shape[0], query_second.shape[0], query_third.shape[0])
    tiled = all(height % (16 * ndp * nneg) == 0 for height in heights)
    if tiled and own_rows % 256 == 0 and negative_features.shape[0] % 256 == 0:
        return fused_step(
            ndp,
            nneg,
            (
                query_features, positive_features, negative_features, positive_ids.reshape(1, -1),
                positive_counts.reshape(1, -1), negative_ids.reshape(1, -1), negative_counts.reshape(1, -1),
                query_first, query_second, query_third, item_first, item_second, item_third,
            ),
        )
    query_saved, query_unit = tower_forward(query_features, query_first, query_second, query_third)
    item_features = jnp.concatenate([positive_features, negative_features], axis=0)
    item_saved, item_unit = tower_forward(item_features, item_first, item_second, item_third)
    positive_unit = item_unit[:own_rows]
    negative_unit = item_unit[own_rows:]
    ndp, nneg = lax.axis_size("dp"), lax.axis_size("neg")
    width = query_unit.shape[1]
    line, nx = ndp // 2, nneg // 2
    block = negative_unit.shape[0]
    blocks, cuts, lanes = 2 * nneg, 2, min(block, 128)
    bf16, f32, i32 = jnp.bfloat16, jnp.float32, jnp.int32
    positive_logit = jnp.sum(
        query_unit.astype(f32) * positive_unit.astype(f32), axis=1
    ) * inv_temp - jnp.log(positive_counts.astype(f32))
    positive_exp = jnp.exp(positive_logit)
    rows_half = (width // 2, block)
    query_total, denom, negative_sum = call(
        score_kernel,
        0,
        ndp,
        nneg,
        (
            jax.ShapeDtypeStruct((own_rows, width), f32),
            jax.ShapeDtypeStruct((1, own_rows), f32),
            jax.ShapeDtypeStruct((2,) + rows_half, f32),
        ),
        [
            pltpu.VMEM((line, cuts, own_rows // cuts, width), bf16),
            pltpu.VMEM((blocks, 2, block // 2, width), bf16),
            pltpu.VMEM((2, block), i32),
            pltpu.VMEM((blocks, 2, block), i32),
            pltpu.VMEM((blocks, 2, block), f32),
            pltpu.VMEM((1, own_rows), i32),
            pltpu.VMEM((line, 1, own_rows), i32),
            pltpu.VMEM((line, own_rows, lanes), f32),
            pltpu.VMEM((blocks, line, own_rows, block), bf16),
            pltpu.VMEM((line, own_rows, lanes), f32),
            pltpu.VMEM((line, 1, own_rows), f32),
            pltpu.VMEM((line, line, 1, own_rows), f32),
            pltpu.VMEM((width, line * own_rows), bf16),
            pltpu.VMEM((line, own_rows, width), bf16),
            pltpu.VMEM((own_rows, width), f32),
            pltpu.VMEM((line, own_rows, width), bf16),
            pltpu.VMEM((nx, 2, 2) + rows_half, bf16),
            pltpu.VMEM((nx, 2, 2) + rows_half, bf16),
            pltpu.VMEM((nx, 2, 2) + rows_half, f32),
            pltpu.VMEM((nx, 2, 2) + rows_half, bf16),
            pltpu.VMEM((nx, 2) + rows_half, bf16),
            pltpu.VMEM((nx,) + rows_half, bf16),
            pltpu.VMEM(rows_half, bf16),
            pltpu.VMEM((nx,) + rows_half, bf16),
        ]
        + sems(
            3 * nx, 1 + nx, 4 * nx, 4 * nx, 4 * nx, line * cuts, line * cuts, line * cuts,
            blocks, blocks, line, line, line, line, line, line,
            2 * nx, 2 * nx, 2 * nx, 2 * nx, nx, nx, 1, 1, nx, nx,
        ),
        [vmem] * 6,
        40,
    )(
        query_unit,
        negative_unit.reshape(2, block // 2, width),
        positive_ids.reshape((1, -1) if own_rows % 128 == 0 else (nneg, own_rows)),
        negative_ids.reshape((1, -1) if block % 128 == 0 else (ndp, block)),
        negative_counts.reshape((1, -1) if block % 128 == 0 else (ndp, block)),
        positive_exp.reshape(1, own_rows),
    )
    own_denom = denom.reshape(-1)
    loss_part = jnp.sum(jnp.log(own_denom) - positive_logit)
    positive_slope = positive_exp / own_denom - 1.0
    query_sum = query_total / own_denom[:, None]
    negative_sum = negative_sum.reshape(width, block).T
    query_grad = (
        query_sum + positive_slope[:, None] * positive_unit.astype(jnp.float32)
    ) * inv_temp
    positive_grad = positive_slope[:, None] * query_unit.astype(jnp.float32) * inv_temp
    item_grad = jnp.concatenate([positive_grad, negative_sum * inv_temp], axis=0)
    query_grads = tower_backward(query_features, query_second, query_third, query_saved, query_grad)
    item_grads = tower_backward(item_features, item_second, item_third, item_saved, item_grad)
    gradients = query_grads + item_grads
    parts = [part for gradient in gradients for part in to_packed(gradient, ndp)]
    packed = jnp.concatenate(parts, axis=1)
    rows = packed.shape[1] // nneg
    packed = packed.reshape(ndp, nneg, 2, rows // 2, pack_columns).transpose(1, 0, 2, 3, 4)
    piece = (rows // 2, pack_columns)
    gathered, stats = call(
        weight_kernel,
        3,
        ndp,
        nneg,
        (jax.ShapeDtypeStruct((nneg, 2) + piece, bf16), jax.ShapeDtypeStruct((8, 128), f32)),
        [
            pltpu.VMEM((nx, ndp, 2) + piece, bf16),
            pltpu.VMEM((nx, 2, line) + piece, bf16),
            pltpu.VMEM((2, nx, line) + piece, bf16),
            pltpu.VMEM((nx, 2, line) + piece, bf16),
            pltpu.VMEM((nx, line) + piece, bf16),
            pltpu.VMEM((2, line) + piece, bf16),
            pltpu.VMEM((nx, line) + piece, bf16),
            pltpu.VMEM((line,) + piece, bf16),
            pltpu.VMEM((nx, line) + piece, bf16),
            pltpu.VMEM((2, line) + piece, bf16),
            pltpu.VMEM((2, line) + piece, bf16),
            pltpu.VMEM((8, 128), f32),
            pltpu.VMEM((ndp, 8, 128), f32),
            pltpu.VMEM((8, 128), f32),
            pltpu.VMEM((nneg, 8, 128), f32),
        ]
        + sems(nx, nx, 2 * nx, 2 * nx, 2, 2, ndp, ndp, ndp, ndp, nneg, nneg, nx, nx, nx, nx),
        [vmem, pl.BlockSpec(memory_space=pltpu.SMEM)],
    )(packed, loss_part.reshape(1))
    grad_norm = jnp.sqrt(stats[0, 0])
    mean_loss = stats[0, 1] / (own_rows * ndp * nneg)
    clip_factor = clip_norm / jnp.maximum(grad_norm, clip_norm)
    flat = gathered.reshape(nneg * rows, pack_columns)
    clipped = []
    start = 0
    for gradient in gradients:
        height, columns = gradient.shape[0] // ndp, gradient.shape[1]
        groups = columns // pack_columns
        blocks = [flat[start + g * height : start + (g + 1) * height] for g in range(groups)]
        start += groups * height
        clipped.append(jnp.concatenate(blocks, axis=1).astype(jnp.float32) * clip_factor)
    return (mean_loss, *clipped)


def solution(mesh):
    placed = (
        P(("dp", "neg"), None),
        P(("dp", "neg"), None),
        P(("neg", "dp"), None),
        P("dp"),
        P(("dp", "neg")),
        P("neg"),
        P("neg"),
        P(),
        P(),
        P(),
        P(),
        P(),
        P(),
    )
    return jax.shard_map(
        per_device,
        mesh=mesh,
        in_specs=placed,
        out_specs=(
            P(),
            P("dp", None),
            P("dp", None),
            P("dp", None),
            P("dp", None),
            P("dp", None),
            P("dp", None),
        ),
        check_vma=False,
    )
```

```python
import functools

import jax
import jax.numpy as jnp
from jax import lax
from jax.experimental import pallas as pl
from jax.experimental.pallas import tpu as pltpu
from jax.sharding import PartitionSpec as P

inv_temp = 20.0
log2_e = 1.4426950408889634
clip_norm = 256.0


def silu_slope(pre):
    sigma = jax.nn.sigmoid(pre)
    return sigma * (1.0 + pre * (1.0 - sigma))


def contract_rows(left, right):
    return lax.dot_general(
        left, right, (((0,), (0,)), ((), ())), preferred_element_type=jnp.float32
    )


def contract_cols(left, right):
    return lax.dot_general(
        left, right, (((1,), (1,)), ((), ())), preferred_element_type=jnp.float32
    )


def tower_forward(features, first, second, third):
    first_pre = jnp.dot(features, first, preferred_element_type=jnp.float32)
    first_act = jax.nn.silu(first_pre).astype(jnp.bfloat16)
    second_pre = jnp.dot(first_act, second, preferred_element_type=jnp.float32)
    second_act = jax.nn.silu(second_pre).astype(jnp.bfloat16)
    embedding = jnp.dot(second_act, third, preferred_element_type=jnp.float32)
    inv_norm = lax.rsqrt(jnp.sum(embedding * embedding, axis=1, keepdims=True) + 1.0)
    unit = (embedding * inv_norm).astype(jnp.bfloat16)
    saved = (silu_slope(first_pre), first_act, silu_slope(second_pre), second_act, embedding, inv_norm)
    return saved, unit


def tower_backward(features, second, third, saved, unit_grad):
    first_slope, first_act, second_slope, second_act, embedding, inv_norm = saved
    along = jnp.sum(embedding * unit_grad, axis=1, keepdims=True)
    embed_grad = (inv_norm * unit_grad - inv_norm * inv_norm * inv_norm * embedding * along).astype(
        jnp.bfloat16
    )
    third_grad = contract_rows(second_act, embed_grad)
    second_step = (contract_cols(embed_grad, third) * second_slope).astype(jnp.bfloat16)
    second_grad = contract_rows(first_act, second_step)
    first_step = (contract_cols(second_step, second) * first_slope).astype(jnp.bfloat16)
    first_grad = contract_rows(features, first_step)
    return (first_grad, second_grad, third_grad)


pack_columns = 256
vmem = pl.BlockSpec(memory_space=pltpu.VMEM)


def greet(ndp, nneg, me_dp, me_neg):
    barrier = pltpu.get_barrier_semaphore()
    for k in range(1, nneg):
        pl.semaphore_signal(
            barrier, inc=1, device_id={"neg": lax.rem(me_neg + k, nneg)}, device_id_type=pl.DeviceIdType.MESH
        )
    for k in range(1, ndp):
        pl.semaphore_signal(
            barrier, inc=1, device_id={"dp": lax.rem(me_dp + k, ndp)}, device_id_type=pl.DeviceIdType.MESH
        )
    pl.semaphore_wait(barrier, (nneg - 1) + (ndp - 1))


def send(src, dst, send_sem, recv_sem, axis, target):
    copy = pltpu.make_async_remote_copy(
        src_ref=src,
        dst_ref=dst,
        send_sem=send_sem,
        recv_sem=recv_sem,
        device_id={axis: target},
        device_id_type=pl.DeviceIdType.MESH,
    )
    copy.start()
    return copy


def share(axis, n, me, src_of, dst, send_sem, recv_sem):
    return [
        send(src_of(lax.rem(me + k, n)), dst.at[me], send_sem.at[k], recv_sem.at[k], axis, lax.rem(me + k, n))
        for k in range(1, n)
    ]


def finish(copies):
    for copy in copies:
        copy.wait()


def link(src, dst, sems, index, axis, target, send_index=None):
    send_sems, recv_sems = sems
    return pltpu.make_async_remote_copy(
        src_ref=src,
        dst_ref=dst,
        send_sem=send_sems.at[index if send_index is None else send_index],
        recv_sem=recv_sems.at[index],
        device_id={axis: target},
        device_id_type=pl.DeviceIdType.MESH,
    )


def score_kernel(
    ndp, nneg, query_ref, negative_ref, pid_ref, nid_ref, count_ref, pexp_ref, sum_ref, denom_ref, nsum_ref,
    q_land, n_land, meta_out, meta, rows, pid_out, pid_land, pid_col, w, den, dpart, dland, scaled,
    q_out, q_part, q_in, c_out, c_in, own, out, lx, ly, l2y, l2x,
    sx, sy, rn, sm, rm, sr, sl, rq, s_meta, r_meta, s_pid, r_pid, sd, rd, sq, rqs,
    sc, rc, s1x, r1x, s1y, r1y, s2y, r2y, s2x, r2x,
):
    me_dp, me_neg = lax.axis_index("dp"), lax.axis_index("neg")
    line, nx = ndp // 2, nneg // 2
    place, side = me_dp // 2, lax.rem(me_dp, 2)
    me_x, me_core = me_neg // 2, lax.rem(me_neg, 2)
    far, other = 1 - side, 1 - me_core
    partner, mate = 2 * place + far, 2 * me_x + other
    rows_q, width = query_ref.shape
    block = 2 * negative_ref.shape[1]
    lanes = den.shape[2]
    cuts = q_land.shape[1]
    half_w = width // 2
    blocks = nneg * 2
    here = (me_x * 2 + side) * 2 + me_core

    def along(k):
        return lax.rem(me_x + k, nx)

    def at_place(z):
        return 2 * z + side

    barrier = pltpu.get_barrier_semaphore()
    for k in range(1, line):
        pl.semaphore_signal(
            barrier, inc=1, device_id={"dp": at_place(lax.rem(place + k, line))}, device_id_type=pl.DeviceIdType.MESH
        )

    def quad(k):
        b = lax.rem(here + k, blocks)
        return {"dp": 2 * place + lax.rem(b // 2, 2), "neg": 2 * (b // 4) + lax.rem(b, 2)}

    for k in range(1, blocks):
        pl.semaphore_signal(barrier, inc=1, device_id=quad(k), device_id_type=pl.DeviceIdType.MESH)
    def own_ids(ref, index, count):
        if count % 128 == 0:
            return ref[:, pl.ds(pl.multiple_of(index * count, count), count)]
        return ref[pl.ds(index, 1), :]

    meta_out[0:1, :] = own_ids(nid_ref, me_dp, block)
    meta_out[1:2, :] = own_ids(count_ref, me_dp, block)
    pid_out[...] = own_ids(pid_ref, me_neg, rows_q)
    pl.semaphore_wait(barrier, (line - 1) + (blocks - 1))

    def slot(x, y, half):
        return (x * 2 + y) * 2 + half

    def piece(x, y, half):
        return n_land.at[(x * 2 + y) * 2 + me_core, half]

    def push(src, x, y, half, send_sems, index, axis, target):
        return link(src, piece(x, y, half), (send_sems, rn), slot(x, y, half), axis, target, index)

    def relay(src, x, y, half):
        i = slot(x, y, half)
        return link(src, piece(x, y, half), (sm, rm), i, "neg", mate)

    def landed(x, y, half):
        ref = piece(x, y, half)
        link(ref, ref, (sy, rn), slot(x, y, half), "neg", mate, 0).wait_recv()

    sends = []

    def go(copy):
        copy.start()
        sends.append(copy)

    def to_x(src, x, y, half, kind):
        for k in range(1, nx):
            go(push(src, x, y, half, sx, kind * nx + k, "neg", 2 * along(k) + me_core))

    def to_y(src, x, y, half, index):
        go(push(src, x, y, half, sy, index, "dp", partner))

    first, second = negative_ref.at[0], negative_ref.at[1]
    to_x(first, me_x, side, 0, 0)
    to_y(second, me_x, side, 1, 0)
    to_x(second, me_x, side, 1, 1)
    to_y(first, me_x, side, 0, 1)
    go(relay(first, me_x, side, 0))
    go(relay(second, me_x, side, 1))

    def chain(slot_z, j, distance, sems, target):
        src = query_ref.at[pl.ds(j * (rows_q // cuts), rows_q // cuts)] if distance == 0 else q_land.at[slot_z, j]
        return link(src, q_land.at[slot_z, j], (sems, rq), slot_z * cuts + j, "dp", target, distance * cuts + j)

    def right(distance, j):
        return chain(place - distance, j, distance, sr, at_place(lax.rem(place + 1, line)))

    def left(distance, j):
        return chain(place + distance, j, distance, sl, at_place(lax.rem(place + line - 1, line)))

    goes_right, goes_left = place < line - 1, place > 0
    for j in range(cuts):
        pl.when(goes_right)(lambda j=j: right(0, j).start())
        pl.when(goes_left)(lambda j=j: left(0, j).start())
    for k in range(1, blocks):
        b = lax.rem(here + k, blocks)
        copy = pltpu.make_async_remote_copy(
            src_ref=meta_out, dst_ref=meta.at[here], send_sem=s_meta.at[k], recv_sem=r_meta.at[here],
            device_id=quad(k), device_id_type=pl.DeviceIdType.MESH,
        )
        go(copy)
    for k in range(1, line):
        z = lax.rem(place + k, line)
        go(link(pid_out, pid_land.at[place], (s_pid, r_pid), place, "dp", at_place(z), k))
    n_land[here] = negative_ref[...]
    for j in range(cuts):
        q_land[place, j] = query_ref[pl.ds(j * (rows_q // cuts), rows_q // cuts), :]
    meta[here] = meta_out[...]
    pid_land[place] = pid_out[...]

    for k in range(1, nx):
        x = along(k)
        landed(x, side, 0)
        to_y(piece(x, side, 0), x, side, 0, 1 + k)
        go(relay(piece(x, side, 0), x, side, 0))
    landed(me_x, far, 1)
    to_x(piece(me_x, far, 1), me_x, far, 1, 2)
    go(relay(piece(me_x, far, 1), me_x, far, 1))

    def q_step(distance):
        for j in range(cuts):

            @pl.when(place >= distance)
            def _():
                ref = q_land.at[place - distance, j]
                link(ref, ref, (sr, rq), (place - distance) * cuts + j, "dp", partner, 0).wait_recv()
                pl.when(goes_right)(lambda: right(distance, j).start())

            @pl.when(place + distance < line)
            def _():
                ref = q_land.at[place + distance, j]
                link(ref, ref, (sl, rq), (place + distance) * cuts + j, "dp", partner, 0).wait_recv()
                pl.when(goes_left)(lambda: left(distance, j).start())

    q_step(1)
    for k in range(1, nx):
        x = along(k)
        landed(x, side, 1)
        go(relay(piece(x, side, 1), x, side, 1))
    landed(me_x, far, 0)
    go(relay(piece(me_x, far, 0), me_x, far, 0))
    for distance in range(2, line):
        q_step(distance)
    for half in range(2):
        for k in range(1, nx):
            x = along(k)
            landed(x, far, half)
            go(relay(piece(x, far, half), x, far, half))
    for x in range(nx):
        for y in range(2):
            for half in range(2):
                i = slot(x, y, half)
                ref = n_land.at[(x * 2 + y) * 2 + other, half]
                link(ref, ref, (sm, rm), i, "neg", mate).wait_recv()
    for k in range(1, blocks):
        b = lax.rem(here + k, blocks)
        link(meta.at[b], meta.at[b], (s_meta, r_meta), b, "neg", mate).wait_recv()
    for k in range(1, line):
        z = lax.rem(place + k, line)
        link(pid_land.at[z], pid_land.at[z], (s_pid, r_pid), z, "dp", partner).wait_recv()

    for b in range(blocks):
        rows[b, 0:1, :] = meta[b, 0:1, :].astype(jnp.float32)
        rows[b, 1:2, :] = jnp.log2(meta[b, 1:2, :].astype(jnp.float32))
    for z in range(line):
        pid_col[z] = jnp.broadcast_to(pid_land[z].astype(jnp.float32), (lanes, rows_q)).T
        den[z] = jnp.zeros((rows_q, lanes), jnp.float32)

    def unit(b, z):
        dots = contract_cols(q_land[z].reshape(rows_q, width), n_land[b].reshape(block, width))
        value = jnp.exp2(dots * (inv_temp * log2_e) - rows[b, 1:2, :])
        ids = jnp.concatenate([pid_col[z]] * (block // lanes), axis=1)
        value = jnp.where(ids != rows[b, 0:1, :], value, 0.0)
        w[b, z] = value.astype(jnp.bfloat16)
        total = den[z]
        for c in range(0, block, lanes):
            total = total + value[:, c : c + lanes]
        den[z] = total

    def units(b, carry):
        for z in range(line):
            unit(b, z)
        return carry

    lax.fori_loop(0, blocks, units, 0)
    for z in range(line):
        dpart[z] = jnp.sum(den[z].T, axis=0, keepdims=True)
    dpart[place] = dpart[place] + pexp_ref[...]
    for k in range(1, line):
        z = lax.rem(place + k, line)
        go(link(dpart, dland.at[place], (sd, rd), place, "dp", at_place(z), k))

    def q_block(z):
        if block % 128 == 0:
            left_side = jnp.concatenate([w[b, z] for b in range(blocks)], axis=1)
            return jnp.dot(
                left_side, n_land[...].reshape(blocks * block, width), preferred_element_type=jnp.float32
            )
        total = jnp.zeros((rows_q, width), jnp.float32)
        for b in range(blocks):
            total = total + jnp.dot(w[b, z], n_land[b].reshape(block, width), preferred_element_type=jnp.float32)
        return total

    def q_send(k, z):
        return link(q_out.at[z], q_in.at[place], (sq, rqs), place, "dp", at_place(z), k)

    def q_push(k, carry):
        z = lax.rem(place + k, line)
        q_out[z] = q_block(z).astype(jnp.bfloat16)
        q_send(k, z).start()
        return carry

    lax.fori_loop(1, line, q_push, 0)
    q_part[...] = q_block(place)
    total = dpart[...]
    for k in range(1, line):
        z = lax.rem(place + k, line)
        link(dland.at[z], dland.at[z], (sd, rd), z, "dp", partner).wait_recv()
        total = total + dland[z]
    dpart2 = 1.0 / total
    for z in range(line):
        q_t = q_land[z].reshape(rows_q, width).astype(jnp.float32).T
        scaled[:, z * rows_q : (z + 1) * rows_q] = (q_t * dpart2[z]).astype(jnp.bfloat16)
    denom_ref[...] = dpart[place]
    for k in range(1, line):
        denom_ref[...] = denom_ref[...] + dland[lax.rem(place + k, line), place]

    def dest(i):
        x = lax.rem(me_x + 1 + i // 2, nx)
        y = lax.rem(side + 1 + lax.rem(i, 2), 2)
        return x, y

    def part(x, y, core):
        return jnp.dot(
            scaled[...], w[(x * 2 + y) * 2 + core].reshape(line * rows_q, block), preferred_element_type=jnp.float32
        )

    def c_send(i):
        x, y = dest(i)
        return link(c_out.at[x, y], c_in.at[x, y], (sc, rc), x * 2 + y, "neg", mate)

    def far_step(i, carry):
        x, y = dest(i)
        c_out[x, y] = part(x, y, other).astype(jnp.bfloat16).reshape(2, half_w, block)
        c_send(i).start()
        return carry

    def send_1x(i):
        x, y = dest(i)
        return link(out.at[x, y, 0], lx.at[me_x, y], (s1x, r1x), me_x * 2 + y, "neg", 2 * x + me_core, x * 2 + y)

    def send_1y(i):
        x, y = dest(i)
        return link(out.at[x, y, 1], ly.at[x], (s1y, r1y), x, "dp", partner)

    def own_step(i, carry):
        x, y = dest(i)
        value = part(x, y, me_core).reshape(2, half_w, block)
        link(c_in.at[x, y], c_in.at[x, y], (sc, rc), x * 2 + y, "neg", mate).wait_recv()
        value = value + c_in[x, y].astype(jnp.float32)
        own[x, y] = value

        @pl.when(i < 2 * (nx - 1))
        def _():
            out[x, y, 0] = value[0].astype(jnp.bfloat16)
            send_1x(i).start()

        @pl.when(lax.rem(i, 2) == 0)
        def _():
            out[x, y, 1] = value[1].astype(jnp.bfloat16)
            send_1y(i).start()

        return carry

    lax.fori_loop(0, 2 * nx, far_step, 0)
    lax.fori_loop(0, 2 * nx, own_step, 0)
    value = own[me_x, far, 0]
    for k in range(1, nx):
        x = along(k)
        ref = lx.at[x, far]
        link(ref, ref, (s1x, r1x), x * 2 + far, "neg", mate).wait_recv()
        value = value + lx[x, far].astype(jnp.float32)
    out[me_x, far, 0] = value.astype(jnp.bfloat16)
    go(link(out.at[me_x, far, 0], l2y, (s2y, r2y), 0, "dp", partner))
    for k in range(1, nx):
        x = along(k)
        link(ly.at[x], ly.at[x], (s1y, r1y), x, "dp", partner).wait_recv()
        out[x, side, 1] = (own[x, side, 1] + ly[x].astype(jnp.float32)).astype(jnp.bfloat16)
        go(link(out.at[x, side, 1], l2x.at[me_x], (s2x, r2x), me_x, "neg", 2 * x + me_core, x))
    result = q_part[...]
    for k in range(1, line):
        z = lax.rem(place + k, line)
        link(q_in.at[z], q_in.at[z], (sq, rqs), z, "dp", partner).wait_recv()
        result = result + q_in[z].astype(jnp.float32)
    sum_ref[...] = result
    low = own[me_x, side, 0]
    for k in range(1, nx):
        x = along(k)
        ref = lx.at[x, side]
        link(ref, ref, (s1x, r1x), x * 2 + side, "neg", mate).wait_recv()
        low = low + lx[x, side].astype(jnp.float32)
    link(ly.at[me_x], ly.at[me_x], (s1y, r1y), me_x, "dp", partner).wait_recv()
    high = own[me_x, side, 1] + ly[me_x].astype(jnp.float32)
    link(l2y, l2y, (s2y, r2y), 0, "dp", partner).wait_recv()
    nsum_ref[0] = low + l2y[...].astype(jnp.float32)
    for k in range(1, nx):
        x = along(k)
        link(l2x.at[x], l2x.at[x], (s2x, r2x), x, "neg", mate).wait_recv()
        high = high + l2x[x].astype(jnp.float32)
    nsum_ref[1] = high

    for copy in sends:
        copy.wait_send()
    for distance in range(line):
        for j in range(cuts):
            if distance < line - 1:
                pl.when((place >= distance) & goes_right)(lambda: right(distance, j).wait_send())
                pl.when((place + distance < line) & goes_left)(lambda: left(distance, j).wait_send())
    for k in range(1, line):
        q_send(k, lax.rem(place + k, line)).wait_send()
    for i in range(2 * nx):
        c_send(i).wait_send()
        if i < 2 * (nx - 1):
            send_1x(i).wait_send()
        if i % 2 == 0:
            send_1y(i).wait_send()


def weight_kernel(
    ndp, nneg, packed_ref, loss_ref, gathered_ref, stats_ref,
    core_land, sum_a, sum_b, land_a, land_b, half_a, half_b, last_a, last_b, line_sum, line_land,
    stat_dp, stat_dp_land, stat_neg, stat_neg_land,
    cs, cr, xs, xr, ys, yr, ps, pr, ss, sr, ts, tr, gs, gr, hs, hr,
):
    me_dp, me_neg = lax.axis_index("dp"), lax.axis_index("neg")
    nx, line = nneg // 2, ndp // 2
    me_x, me_core = me_neg // 2, lax.rem(me_neg, 2)
    place, side = me_dp // 2, lax.rem(me_dp, 2)
    other, far = 1 - me_core, 1 - side
    mate, partner = 2 * me_x + other, 2 * place + far
    greet(ndp, nneg, me_dp, me_neg)
    turn = list(range(1, nx)) + [0]

    def x_of(k):
        return lax.rem(me_x + k, nx)

    core = {}
    for k in turn:
        x = x_of(k)
        core[k] = send(packed_ref.at[2 * x + other], core_land.at[x], cs.at[k], cr.at[k], "neg", mate)

    def add_core(x, y, half, target):
        def body(z, carry):
            target[z] = (
                packed_ref[2 * x + me_core, 2 * z + y, half].astype(jnp.float32)
                + core_land[x, 2 * z + y, half].astype(jnp.float32)
            ).astype(jnp.bfloat16)
            return carry

        lax.fori_loop(0, line, body, 0)

    def add(target, *terms):
        def body(z, carry):
            value = terms[0][z].astype(jnp.float32)
            for term in terms[1:]:
                value = value + term[z].astype(jnp.float32)
            target[z] = value.astype(jnp.bfloat16)
            return carry

        lax.fori_loop(0, line, body, 0)

    first_a = []
    for k in turn:
        x = x_of(k)
        core[k].wait_recv()
        if k:
            for y in range(2):
                add_core(x, y, 0, sum_a.at[x, y])
            first_a.append(send(sum_a.at[x], land_a.at[k], xs.at[k], xr.at[k], "neg", 2 * x + me_core))
        add_core(x, far, 1, sum_b.at[far, x])
    first_b = send(sum_b.at[far], land_b, ys.at[0], yr.at[0], "dp", partner)
    for y in range(2):
        add_core(me_x, y, 0, sum_a.at[me_x, y])
    for k in range(nx):
        add_core(x_of(k), side, 1, sum_b.at[side, x_of(k)])
    for copy in first_a:
        copy.wait_recv()
    add(half_a.at[far], sum_a.at[me_x, far], *[land_a.at[k, far] for k in range(1, nx)])
    second_a = send(half_a.at[far], last_a, ys.at[1], yr.at[1], "dp", partner)
    first_b.wait_recv()
    second_b = []
    for k in turn:
        x = x_of(k)
        add(half_b.at[x], sum_b.at[side, x], land_b.at[x])
        if k:
            second_b.append(
                send(half_b.at[x], last_b.at[k], xs.at[nx + k], xr.at[nx + k], "neg", 2 * x + me_core)
            )
    add(half_a.at[side], sum_a.at[me_x, side], *[land_a.at[k, side] for k in range(1, nx)])
    second_a.wait_recv()
    add(line_sum.at[0], half_a.at[side], last_a)
    third = []
    for half in range(2):
        if half:
            for copy in second_b:
                copy.wait_recv()
            add(line_sum.at[1], half_b.at[me_x], *[last_b.at[k] for k in range(1, nx)])
        for k in range(1, line):
            z = lax.rem(place + k, line)
            third.append(
                send(line_sum.at[half, z], line_land.at[half, k], ps.at[half * line + k], pr.at[half * line + k], "dp", 2 * z + side)
            )
    for copy in third:
        copy.wait_recv()
    squares = jnp.zeros((), jnp.float32)
    for half in range(2):
        piece = line_sum[half, place].astype(jnp.float32)
        for k in range(1, line):
            piece = piece + line_land[half, k].astype(jnp.float32)
        gathered_ref[me_neg, half] = piece.astype(jnp.bfloat16)
        squares = squares + jnp.sum(piece * piece)
    lane = lax.broadcasted_iota(jnp.int32, (8, 128), 1)
    stat_dp[...] = jnp.where(lane == 0, squares, loss_ref[0])
    stat_copies = share("dp", ndp, me_dp, lambda t: stat_dp, stat_dp_land, ss, sr)
    mine = gathered_ref.at[me_neg]
    spread = [send(mine, mine, gs.at[k], gr.at[k], "neg", 2 * x_of(k) + me_core) for k in range(1, nx)]
    spread.append(send(mine, mine, gs.at[0], gr.at[0], "neg", mate))
    finish(stat_copies)
    total = stat_dp[...]
    for k in range(1, ndp):
        total = total + stat_dp_land[lax.rem(me_dp + k, ndp)]
    stat_neg[...] = total
    stat_copies = share("neg", nneg, me_neg, lambda t: stat_neg, stat_neg_land, ts, tr)
    relay = []
    for k in range(1, nx):
        spread[k - 1].wait_recv()
        x = lax.rem(me_x + nx - k, nx)
        came = gathered_ref.at[2 * x + me_core]
        relay.append(send(came, came, hs.at[k], hr.at[k], "neg", mate))
    finish(stat_copies)
    total = stat_neg[...]
    for k in range(1, nneg):
        total = total + stat_neg_land[lax.rem(me_neg + k, nneg)]
    stats_ref[...] = total
    spread[-1].wait_recv()
    finish(relay)
    for copy in [*core.values(), *first_a, first_b, second_a, *second_b, *third, *spread]:
        copy.wait_send()


def call(kernel, collective, ndp, nneg, out_shape, scratch, in_specs, megabytes=48):
    return pl.pallas_call(
        functools.partial(kernel, ndp, nneg),
        out_shape=out_shape,
        in_specs=in_specs,
        out_specs=tuple(vmem for _ in out_shape),
        scratch_shapes=scratch,
        compiler_params=pltpu.CompilerParams(
            collective_id=collective, has_side_effects=True, vmem_limit_bytes=megabytes * 1024 * 1024
        ),
    )


def sems(*counts):
    return [pltpu.SemaphoreType.DMA((count,)) for count in counts]


def to_packed(gradient, ndp):
    rows, columns = gradient.shape
    blocks = gradient.astype(jnp.bfloat16).reshape(ndp, rows // ndp, columns)
    return [blocks[:, :, c : c + pack_columns] for c in range(0, columns, pack_columns)]


step_inputs = (
    "query_features", "positive_features", "negative_features", "positive_ids", "positive_counts", "negative_ids",
    "negative_counts", "query_first", "query_second", "query_third", "item_first", "item_second", "item_third",
)


def step_kernel(ndp, nneg, names, groups, *refs):
    refs = list(refs)
    inputs = dict(zip(step_inputs, refs))
    stats_ref, gathered = refs[13], refs[14:18]
    (
        sources, q_unit, n_unit, p_unit, towers, grads, pexp, logit,
        q_land, n_land, meta_out, meta, rows, pid_out, pid_land, pid_col, w, den, dpart, dland, scaled,
        q_out, q_part, q_in, c_out, c_in, own, out, lx, ly, l2y, l2x,
        sx, sy, rn, sm, rm, sr, sl, rq, s_meta, r_meta, s_pid, r_pid, sd, rd, sq, rqs,
        sc, rc, s1x, r1x, s1y, r1y, s2y, r2y, s2x, r2x, loaded,
        scratch, bufs, stat, stat_land, ss, sr2, left_sems,
    ) = jax.tree.unflatten(names, refs[18:])
    me_dp, me_neg = lax.axis_index("dp"), lax.axis_index("neg")
    line, nx = ndp // 2, nneg // 2
    place, side = me_dp // 2, lax.rem(me_dp, 2)
    me_x, me_core = me_neg // 2, lax.rem(me_neg, 2)
    far, other = 1 - side, 1 - me_core
    partner, mate = 2 * place + far, 2 * me_x + other
    f32, bf16 = jnp.float32, jnp.bfloat16
    rows_q, width = q_unit.shape
    block = 2 * n_unit.shape[1]
    half_n = block // 2
    lanes = den.shape[2]
    cuts = q_land.shape[1]
    half_w = width // 2
    blocks = nneg * 2
    here = (me_x * 2 + side) * 2 + me_core

    order = (
        "query_features", "query_first", "query_second", "query_third", "negative_features", "item_first", "item_second",
        "item_third", "negative_ids", "negative_counts", "positive_ids", "positive_features", "positive_counts",
    )
    item_features = sources["item_features"]
    places = dict(sources)
    places["negative_features"] = item_features.at[0:block]
    places["positive_features"] = item_features.at[block : block + rows_q]
    loads = {}
    for i, name in enumerate(order):
        loads[name] = pltpu.make_async_copy(inputs[name], places[name], loaded.at[i])
    for name in order[:4]:
        loads[name].start()

    def along(k):
        return lax.rem(me_x + k, nx)

    def at_place(z):
        return 2 * z + side

    barrier = pltpu.get_barrier_semaphore()

    def quad(k):
        b = lax.rem(here + k, blocks)
        return {"dp": 2 * place + lax.rem(b // 2, 2), "neg": 2 * (b // 4) + lax.rem(b, 2)}

    devices = ndp * nneg
    me = me_dp * nneg + me_neg

    def everyone(n):
        target = lax.rem(me + n, devices)
        return target // nneg, lax.rem(target, nneg)

    for n in range(1, devices):
        dp, neg = everyone(n)
        pl.semaphore_signal(barrier, inc=1, device_id={"dp": dp, "neg": neg}, device_id_type=pl.DeviceIdType.MESH)

    def slot(x, y, half):
        return (x * 2 + y) * 2 + half

    def piece(x, y, half):
        return n_land.at[(x * 2 + y) * 2 + me_core, half]

    def push(src, x, y, half, send_sems, index, axis, target):
        return link(src, piece(x, y, half), (send_sems, rn), slot(x, y, half), axis, target, index)

    def relay(src, x, y, half):
        i = slot(x, y, half)
        return link(src, piece(x, y, half), (sm, rm), i, "neg", mate)

    def landed(x, y, half):
        ref = piece(x, y, half)
        link(ref, ref, (sy, rn), slot(x, y, half), "neg", mate, 0).wait_recv()

    sends = []

    def go(copy):
        copy.start()
        sends.append(copy)

    def to_x(src, x, y, half, kind):
        for k in range(1, nx):
            go(push(src, x, y, half, sx, kind * nx + k, "neg", 2 * along(k) + me_core))

    def to_y(src, x, y, half, index):
        go(push(src, x, y, half, sy, index, "dp", partner))

    def chain(slot_z, j, distance, sems, target):
        src = q_unit.at[pl.ds(j * (rows_q // cuts), rows_q // cuts)] if distance == 0 else q_land.at[slot_z, j]
        return link(src, q_land.at[slot_z, j], (sems, rq), slot_z * cuts + j, "dp", target, distance * cuts + j)

    def right(distance, j):
        return chain(place - distance, j, distance, sr, at_place(lax.rem(place + 1, line)))

    def left(distance, j):
        return chain(place + distance, j, distance, sl, at_place(lax.rem(place + line - 1, line)))

    goes_right, goes_left = place < line - 1, place > 0

    def q_step(distance, lo=0, hi=cuts):
        for j in range(lo, hi):

            @pl.when(place >= distance)
            def _():
                ref = q_land.at[place - distance, j]
                link(ref, ref, (sr, rq), (place - distance) * cuts + j, "dp", partner, 0).wait_recv()
                pl.when(goes_right)(lambda: right(distance, j).start())

            @pl.when(place + distance < line)
            def _():
                ref = q_land.at[place + distance, j]
                link(ref, ref, (sl, rq), (place + distance) * cuts + j, "dp", partner, 0).wait_recv()
                pl.when(goes_left)(lambda: left(distance, j).start())

    def forward(lo, count, features, first, second, third, saved, unit_ref, waits=((), (), ()), starts=()):
        act1, slope1, act2, slope2, emb = saved
        span = slice(lo, lo + count)

        def layer(source, weight, act, slope):
            columns = weight.shape[1]
            step = 512 if columns % 512 == 0 else columns
            for c in range(0, columns, step):
                pre = jnp.dot(source[span, :], weight[:, c : c + step], preferred_element_type=f32)
                sigma = 0.5 * jnp.tanh(0.5 * pre) + 0.5
                value = pre * sigma
                act[span, c : c + step] = value.astype(bf16)
                slope[span, c : c + step] = sigma + value * (1.0 - sigma)

        ready(waits[0])
        for name in starts:
            loads[name].start()
        layer(features, first, act1, slope1)
        ready(waits[1])
        layer(act1, second, act2, slope2)
        ready(waits[2])
        value = jnp.dot(act2[span, :], third[...], preferred_element_type=f32)
        emb[span, :] = value
        inv_norm = lax.rsqrt(jnp.sum(value * value, axis=1, keepdims=True) + 1.0)
        unit_ref[...] = (value * inv_norm).astype(bf16)

    def ready(chosen):
        for name in chosen:
            loads[name].wait()

    item_weights = tuple(sources[name] for name in ("item_first", "item_second", "item_third"))
    query_weights = tuple(sources[name] for name in ("query_first", "query_second", "query_third"))
    def own_ids(ref, index, count):
        return ref[:, pl.ds(pl.multiple_of(index * count, count), count)]

    forward(
        0, rows_q, sources["query_features"], *query_weights, towers[0], q_unit,
        (("query_features", "query_first"), ("query_second",), ("query_third",)),
        order[4:],
    )
    pl.semaphore_wait(barrier, devices - 1)
    for j in range(cuts):
        pl.when(goes_right)(lambda j=j: right(0, j).start())
        pl.when(goes_left)(lambda j=j: left(0, j).start())
    for j in range(cuts):
        q_land[place, j] = q_unit[pl.ds(j * (rows_q // cuts), rows_q // cuts), :]
    ready(("negative_ids", "negative_counts", "positive_ids"))
    meta_out[0:1, :] = own_ids(sources["negative_ids"], me_dp, block)
    meta_out[1:2, :] = own_ids(sources["negative_counts"], me_dp, block)
    pid_out[...] = own_ids(sources["positive_ids"], me_neg, rows_q)
    meta[here] = meta_out[...]
    pid_land[place] = pid_out[...]
    for k in range(1, blocks):
        copy = pltpu.make_async_remote_copy(
            src_ref=meta_out, dst_ref=meta.at[here], send_sem=s_meta.at[k], recv_sem=r_meta.at[here],
            device_id=quad(k), device_id_type=pl.DeviceIdType.MESH,
        )
        go(copy)
    for k in range(1, line):
        z = lax.rem(place + k, line)
        go(link(pid_out, pid_land.at[place], (s_pid, r_pid), place, "dp", at_place(z), k))
    n_first, n_second = n_unit.at[0], n_unit.at[1]
    forward(
        0, half_n, item_features, *item_weights, towers[1], n_first,
        (("negative_features", "item_first"), ("item_second",), ("item_third",)),
    )
    to_x(n_first, me_x, side, 0, 0)
    go(relay(n_first, me_x, side, 0))
    n_land[here, 0] = n_unit[0]
    forward(half_n, half_n, item_features, *item_weights, towers[1], n_second)
    to_y(n_second, me_x, side, 1, 0)
    to_x(n_second, me_x, side, 1, 1)
    to_y(n_first, me_x, side, 0, 1)
    go(relay(n_second, me_x, side, 1))
    n_land[here, 1] = n_unit[1]
    ready(("positive_features", "positive_counts"))
    forward(block, rows_q, item_features, *item_weights, towers[1], p_unit)
    q_step(1)
    product = q_unit[...].astype(f32) * p_unit[...].astype(f32)
    logit[...] = jnp.sum(product.T, axis=0, keepdims=True) * inv_temp - jnp.log(sources["positive_counts"][...].astype(f32))
    pexp[...] = jnp.exp(logit[...])

    for k in range(1, nx):
        x = along(k)
        landed(x, side, 0)
        to_y(piece(x, side, 0), x, side, 0, 1 + k)
        go(relay(piece(x, side, 0), x, side, 0))
    for k in range(1, blocks):
        b = lax.rem(here + k, blocks)
        link(meta.at[b], meta.at[b], (s_meta, r_meta), b, "neg", mate).wait_recv()
    for k in range(1, line):
        z = lax.rem(place + k, line)
        link(pid_land.at[z], pid_land.at[z], (s_pid, r_pid), z, "dp", partner).wait_recv()
    for b in range(blocks):
        rows[b, 0:1, :] = meta[b, 0:1, :].astype(f32)
        rows[b, 1:2, :] = jnp.log2(meta[b, 1:2, :].astype(f32))
    for z in range(line):
        pid_col[z] = jnp.broadcast_to(pid_land[z].astype(f32), (lanes, rows_q)).T
        den[z] = jnp.zeros((rows_q, lanes), f32)

    def unit(b, z):
        dots = contract_cols(q_land[z].reshape(rows_q, width), n_land[b].reshape(block, width))
        value = jnp.exp2(dots * (inv_temp * log2_e) - rows[b, 1:2, :])
        ids = jnp.concatenate([pid_col[z]] * (block // lanes), axis=1)
        value = jnp.where(ids != rows[b, 0:1, :], value, 0.0)
        w[b, z] = value.astype(jnp.bfloat16)
        total = den[z]
        for c in range(0, block, lanes):
            total = total + value[:, c : c + lanes]
        den[z] = total

    def relayed(x, y):
        for half in range(2):
            ref = n_land.at[(x * 2 + y) * 2 + other, half]
            link(ref, ref, (sm, rm), slot(x, y, half), "neg", mate).wait_recv()

    def both_cores(x, y):
        return [(x * 2 + y) * 2 + core for core in range(2)]

    near_blocks = both_cores(me_x, side)
    side_blocks = both_cores(me_x, far)
    along_blocks = []
    for k in range(1, nx):
        along_blocks = along_blocks + both_cores(along(k), side)
    mid_blocks = along_blocks + side_blocks

    def units(lo, hi, chosen):
        def body(z, carry):
            for b in chosen:
                unit(b, z)
            return carry

        lax.fori_loop(jnp.maximum(lo, 0), jnp.minimum(hi, line), body, 0)

    relayed(me_x, side)
    q_step(2, 0, cuts // 2)
    units(place - 1, place + 2, near_blocks)
    landed(me_x, far, 1)
    to_x(piece(me_x, far, 1), me_x, far, 1, 2)
    go(relay(piece(me_x, far, 1), me_x, far, 1))
    q_step(2, cuts // 2)
    units(place - 2, place - 1, near_blocks)
    units(place + 2, place + 3, near_blocks)
    for k in range(1, nx):
        x = along(k)
        landed(x, side, 1)
        go(relay(piece(x, side, 1), x, side, 1))
    landed(me_x, far, 0)
    go(relay(piece(me_x, far, 0), me_x, far, 0))
    for k in range(1, nx):
        relayed(along(k), side)
    units(place - 2, place + 3, along_blocks)
    relayed(me_x, far)
    units(place - 2, place, side_blocks)
    for half in range(2):
        for k in range(1, nx):
            x = along(k)
            landed(x, far, half)
            go(relay(piece(x, far, half), x, far, half))
    units(place, place + 3, side_blocks)
    for distance in range(3, line):
        q_step(distance)
    units(0, place - 2, near_blocks + mid_blocks)
    units(place + 3, line, near_blocks + mid_blocks)
    for core in (me_core, other):
        for k in range(1, nx):
            if core is other:
                relayed(along(k), far)
            for z in range(line):
                unit((along(k) * 2 + far) * 2 + core, z)
    for z in range(line):
        dpart[z] = jnp.sum(den[z].T, axis=0, keepdims=True)
    dpart[place] = dpart[place] + pexp[...]
    for k in range(1, line):
        z = lax.rem(place + k, line)
        go(link(dpart, dland.at[place], (sd, rd), place, "dp", at_place(z), k))

    def q_block(z):
        if block % 128 == 0:
            left_side = jnp.concatenate([w[b, z] for b in range(blocks)], axis=1)
            return jnp.dot(
                left_side, n_land[...].reshape(blocks * block, width), preferred_element_type=jnp.float32
            )
        total = jnp.zeros((rows_q, width), jnp.float32)
        for b in range(blocks):
            total = total + jnp.dot(w[b, z], n_land[b].reshape(block, width), preferred_element_type=jnp.float32)
        return total

    def q_send(k, z):
        return link(q_out.at[z], q_in.at[place], (sq, rqs), place, "dp", at_place(z), k)

    def q_push(k, carry):
        z = lax.rem(place + k, line)
        q_out[z] = q_block(z).astype(jnp.bfloat16)
        q_send(k, z).start()
        return carry

    lax.fori_loop(1, line, q_push, 0)
    q_part[...] = q_block(place)
    total = dpart[...]
    for k in range(1, line):
        z = lax.rem(place + k, line)
        link(dland.at[z], dland.at[z], (sd, rd), z, "dp", partner).wait_recv()
        total = total + dland[z]
    dpart2 = 1.0 / total
    for z in range(line):
        q_t = q_land[z].reshape(rows_q, width).astype(jnp.float32).T
        scaled[:, z * rows_q : (z + 1) * rows_q] = (q_t * dpart2[z]).astype(jnp.bfloat16)
    def dest(i):
        x = lax.rem(me_x + 1 + i // 2, nx)
        y = lax.rem(side + 1 + lax.rem(i, 2), 2)
        return x, y

    def part(x, y, core):
        return jnp.dot(
            scaled[...], w[(x * 2 + y) * 2 + core].reshape(line * rows_q, block), preferred_element_type=jnp.float32
        )

    def c_send(i):
        x, y = dest(i)
        return link(c_out.at[x, y], c_in.at[x, y], (sc, rc), x * 2 + y, "neg", mate)

    def far_step(i, carry):
        x, y = dest(i)
        c_out[x, y] = part(x, y, other).astype(jnp.bfloat16).reshape(2, half_w, block)
        c_send(i).start()
        return carry

    def send_1x(i):
        x, y = dest(i)
        return link(out.at[x, y, 0], lx.at[me_x, y], (s1x, r1x), me_x * 2 + y, "neg", 2 * x + me_core, x * 2 + y)

    def send_1y(i):
        x, y = dest(i)
        return link(out.at[x, y, 1], ly.at[x], (s1y, r1y), x, "dp", partner)

    def own_step(i, carry):
        x, y = dest(i)
        value = part(x, y, me_core).reshape(2, half_w, block)
        link(c_in.at[x, y], c_in.at[x, y], (sc, rc), x * 2 + y, "neg", mate).wait_recv()
        value = value + c_in[x, y].astype(jnp.float32)
        own[x, y] = value

        @pl.when(i < 2 * (nx - 1))
        def _():
            out[x, y, 0] = value[0].astype(jnp.bfloat16)
            send_1x(i).start()

        @pl.when(lax.rem(i, 2) == 0)
        def _():
            out[x, y, 1] = value[1].astype(jnp.bfloat16)
            send_1y(i).start()

        return carry

    ahead = 2

    def both_steps(i, carry):
        far_step(i + ahead, 0)
        own_step(i, 0)
        return carry

    lax.fori_loop(0, ahead, far_step, 0)
    lax.fori_loop(0, 2 * nx - ahead, both_steps, 0)
    lax.fori_loop(2 * nx - ahead, 2 * nx, own_step, 0)
    value = own[me_x, far, 0]
    for k in range(1, nx):
        x = along(k)
        ref = lx.at[x, far]
        link(ref, ref, (s1x, r1x), x * 2 + far, "neg", mate).wait_recv()
        value = value + lx[x, far].astype(jnp.float32)
    out[me_x, far, 0] = value.astype(jnp.bfloat16)
    go(link(out.at[me_x, far, 0], l2y, (s2y, r2y), 0, "dp", partner))
    for k in range(1, nx):
        x = along(k)
        link(ly.at[x], ly.at[x], (s1y, r1y), x, "dp", partner).wait_recv()
        out[x, side, 1] = (own[x, side, 1] + ly[x].astype(jnp.float32)).astype(jnp.bfloat16)
        go(link(out.at[x, side, 1], l2x.at[me_x], (s2x, r2x), me_x, "neg", 2 * x + me_core, x))
    denom = dpart[place]
    for k in range(1, line):
        denom = denom + dland[lax.rem(place + k, line), place]
    loss_part = jnp.sum(jnp.log(denom) - logit[...])

    def to_columns(row):
        column = jnp.broadcast_to(row, (lanes, rows_q)).T
        return jnp.concatenate([column] * (width // lanes), axis=1)

    slope_columns = to_columns(pexp[...] / denom - 1.0) * inv_temp
    grads[1][block : block + rows_q, :] = slope_columns * q_unit[...].astype(f32)
    result = q_part[...]
    for k in range(1, line):
        z = lax.rem(place + k, line)
        link(q_in.at[z], q_in.at[z], (sq, rqs), z, "dp", partner).wait_recv()
        result = result + q_in[z].astype(jnp.float32)
    grads[0][...] = result * (to_columns(1.0 / denom) * inv_temp) + slope_columns * p_unit[...].astype(f32)

    pending = []

    def queue(copy):
        copy.start()
        pending.append(copy)

    def x_of(k):
        return lax.rem(me_x + k, nx)

    def same_core(x):
        return 2 * x + me_core

    def z_of(k):
        return lax.rem(place + k, line)

    def arrived(ref, sem_array, index):
        link(ref, ref, (sem_array, sem_array), index, "neg", mate).wait_recv()

    steps = [
        (sources["query_features"], *towers[0], grads[0], sources["query_second"], sources["query_third"]),
        (item_features, *towers[1], grads[1], sources["item_second"], sources["item_third"]),
    ]

    def store(group, offset, value, dp, hg):
        packed = bufs[group]["packed"]
        pieces = hg // nneg
        for p in range(value.shape[1] // pack_columns):
            part = value[:, p * pack_columns : (p + 1) * pack_columns].astype(bf16)
            part = part.reshape(value.shape[0] // hg, nx, 2, pieces, pack_columns)
            lo = offset + p * pieces
            for core in range(2):
                packed[core, pl.ds(dp, value.shape[0] // hg), :, lo : lo + pieces, :] = part[:, :, core]

    def weight_grad(group, offset, left_ref, right_ref):
        rows, columns = left_ref.shape[1], right_ref.shape[1]
        hg = rows // ndp
        step = 2 * hg

        def body(m, carry):
            left = left_ref[:, pl.ds(pl.multiple_of(m * step, step), step)]
            store(group, offset, contract_rows(left, right_ref[...]), 2 * m, hg)
            return carry

        lax.fori_loop(0, rows // step, body, 0, unroll=True)
        return offset + hg // nneg * (columns // pack_columns)

    def row_loop(start, stop, body):
        def wrapped(i, carry):
            body(pl.ds(pl.multiple_of(i * 256, 256), 256))
            return carry

        lax.fori_loop(start // 256, stop // 256, wrapped, 0)

    def embed_stage(t, start, stop):
        feat, act1, slope1, act2, slope2, emb_ref, grad_ref, second, third = steps[t]
        eg, s2, s1 = scratch[t]

        def body(rows):
            emb, grad = emb_ref[rows, :], grad_ref[rows, :]
            inv_norm = lax.rsqrt(jnp.sum(emb * emb, axis=1, keepdims=True) + 1.0)
            along = jnp.sum(emb * grad, axis=1, keepdims=True)
            value = (inv_norm * grad - inv_norm * inv_norm * inv_norm * emb * along).astype(bf16)
            eg[rows, :] = value
            s2[rows, :] = (contract_cols(value, third[...]) * slope2[rows, :]).astype(bf16)

        row_loop(start, stop, body)

    def second_stage(t, group):
        feat, act1, slope1, act2, slope2, emb_ref, grad_ref, second, third = steps[t]
        eg, s2, s1 = scratch[t]
        offset = weight_grad(group, 0, act2, eg)
        weight_grad(group, offset, act1, s2)

    def slope_stage(t, start, stop):
        feat, act1, slope1, act2, slope2, emb_ref, grad_ref, second, third = steps[t]
        eg, s2, s1 = scratch[t]
        columns = second.shape[0]

        def body(rows):
            for c in range(0, columns, 512):
                value = contract_cols(s2[rows, :], second[c : c + 512, :]) * slope1[rows, c : c + 512]
                s1[rows, c : c + 512] = value.astype(bf16)

        row_loop(start, stop, body)

    def first_stage(t, group):
        weight_grad(group, 0, steps[t][0], scratch[t][2])

    def stage0(g):
        b = bufs[g]
        queue(link(b["packed"].at[other], b["c_in"], (b["cs"], b["cr"]), 0, "neg", mate))

    def base(b, dp, x, lo, hi):
        return b["packed"][me_core, dp, x, lo:hi, :].astype(f32) + b["c_in"][dp, x, lo:hi, :].astype(f32)

    def loop(count, body):
        def wrapped(i, carry):
            body(i)
            return carry

        lax.fori_loop(0, count, wrapped, 0)

    def stage1(g):
        b, (r1, r, full) = bufs[g], groups[g]
        arrived(b["c_in"], b["cr"], 0)
        for k in range(1, line):
            z = z_of(k)
            for y in range(2):
                for x in range(nx):
                    b["o1z"][z, y, x] = base(b, 2 * z + y, x, r, full).astype(bf16)
            queue(link(b["o1z"].at[z], b["l1z"].at[place], (b["s1z"], b["r1z"]), place, "dp", 2 * z + side, z))
        for k in range(1, nx):
            x = x_of(k)

            def body(dp):
                b["o1x"][x, dp] = base(b, dp, x, 0, r1).astype(bf16)

            loop(ndp, body)
            queue(link(b["o1x"].at[x], b["l1x"].at[me_x], (b["s1x"], b["r1x"]), me_x, "neg", same_core(x), x))

        def body_y(z):
            for x in range(nx):
                b["o1y"][z, x] = base(b, 2 * z + far, x, r1, r).astype(bf16)

        loop(line, body_y)
        queue(link(b["o1y"], b["l1y"], (b["s1y"], b["r1y"]), 0, "dp", partner))

    def low(b, dp, r1):
        value = base(b, dp, me_x, 0, r1)
        for k in range(1, nx):
            value = value + b["l1x"][x_of(k), dp].astype(f32)
        return value

    def stage2(g):
        b, (r1, r, full) = bufs[g], groups[g]
        for k in range(1, nx):
            x = x_of(k)
            arrived(b["l1x"].at[x], b["r1x"], x)

        def body(z):
            b["o2y"][z] = low(b, 2 * z + far, r1).astype(bf16)

        loop(line, body)
        queue(link(b["o2y"], b["l2y"], (b["s2y"], b["r2y"]), 0, "dp", partner))
        arrived(b["l1y"], b["r1y"], 0)
        for k in range(1, nx):
            x = x_of(k)

            def body_x(z):
                value = base(b, 2 * z + side, x, r1, r) + b["l1y"][z, x].astype(f32)
                b["o2x"][x, z] = value.astype(bf16)

            loop(line, body_x)
            queue(link(b["o2x"].at[x], b["l2x"].at[me_x], (b["s2x"], b["r2x"]), me_x, "neg", same_core(x), x))

    def stage3(g):
        b, (r1, r, full) = bufs[g], groups[g]
        arrived(b["l2y"], b["r2y"], 0)
        for k in range(1, nx):
            x = x_of(k)
            arrived(b["l2x"].at[x], b["r2x"], x)

        def body(z):
            dp = 2 * z + side
            b["zs"][z, 0:r1, :] = (low(b, dp, r1) + b["l2y"][z].astype(f32)).astype(bf16)
            value = base(b, dp, me_x, r1, r) + b["l1y"][z, me_x].astype(f32)
            for k in range(1, nx):
                value = value + b["l2x"][x_of(k), z].astype(f32)
            b["zs"][z, r1:r, :] = value.astype(bf16)

        loop(line, body)
        for k in range(1, line):
            z = z_of(k)
            queue(link(b["zs"].at[z], b["l3"].at[place], (b["s3"], b["r3"]), place, "dp", 2 * z + side, z))

    def z_sum(g, y, x):
        b, (_, r, full) = bufs[g], groups[g]
        value = base(b, 2 * place + y, x, r, full)
        for k in range(1, line):
            value = value + b["l1z"][z_of(k), y, x].astype(f32)
        return value

    def x_sum(g, y):
        value = z_sum(g, y, me_x)
        for k in range(1, nx):
            value = value + bufs[g]["l2z"][x_of(k), y].astype(f32)
        return value

    def stage2z(g):
        b = bufs[g]
        for k in range(1, line):
            z = z_of(k)
            arrived(b["l1z"].at[z], b["r1z"], z)
        for k in range(1, nx):
            x = x_of(k)
            for y in range(2):
                b["o2z"][x, y] = z_sum(g, y, x).astype(bf16)
            queue(link(b["o2z"].at[x], b["l2z"].at[me_x], (b["s2z"], b["r2z"]), me_x, "neg", same_core(x), x))

    def stage3z(g):
        b = bufs[g]
        for k in range(1, nx):
            x = x_of(k)
            arrived(b["l2z"].at[x], b["r2z"], x)
        b["o3z"][...] = x_sum(g, far).astype(bf16)
        queue(link(b["o3z"], b["l3z"], (b["s3z"], b["r3z"]), 0, "dp", partner))

    squares = []

    def stage4(g):
        b, (_, r, full) = bufs[g], groups[g]
        for k in range(1, line):
            z = z_of(k)
            arrived(b["l3"].at[z], b["r3"], z)
        value = b["zs"][place].astype(f32)
        for k in range(1, line):
            value = value + b["l3"][z_of(k)].astype(f32)
        arrived(b["l3z"], b["r3z"], 0)
        last = x_sum(g, side) + b["l3z"][...].astype(f32)
        squares.append(jnp.sum(value * value) + jnp.sum(last * last))
        b["ag"][me_neg, 0:r] = value.astype(bf16)
        b["ag"][me_neg, r:full] = last.astype(bf16)

    def spread(g):
        b = bufs[g]
        mine = b["ag"].at[me_neg]
        for k in range(1, nx):
            x = x_of(k)
            queue(link(mine, mine, (b["sg"], b["rg"]), me_x, "neg", same_core(x), x))
        queue(link(mine, mine, (b["sh"], b["rh"]), me_x, "neg", mate))

    def stage5(g):
        b = bufs[g]
        for k in range(1, nx):
            x = x_of(k)
            ref = b["ag"].at[same_core(x)]
            arrived(ref, b["rg"], x)
            queue(link(ref, ref, (b["sh"], b["rh"]), x, "neg", mate))

    leaving = []

    def leave(source, target, index):
        copy = pltpu.make_async_copy(source, target, left_sems.at[index])
        copy.start()
        leaving.append(copy)

    def stage6(g):
        b = bufs[g]
        for x in range(nx):
            arrived(b["ag"].at[2 * x + other], b["rh"], x)
        leave(b["ag"], gathered[g], g)

    embed_stage(0, 0, rows_q)
    second_stage(0, 0)
    stage0(0)
    slope_stage(0, 0, rows_q)
    first_stage(0, 1)
    stage0(1)
    stage1(0)
    embed_stage(1, block, block + rows_q)
    slope_stage(1, block, block + rows_q)
    stage1(1)
    n_low = own[me_x, side, 0]
    for k in range(1, nx):
        x = along(k)
        ref = lx.at[x, side]
        link(ref, ref, (s1x, r1x), x * 2 + side, "neg", mate).wait_recv()
        n_low = n_low + lx[x, side].astype(jnp.float32)
    link(ly.at[me_x], ly.at[me_x], (s1y, r1y), me_x, "dp", partner).wait_recv()
    n_high = own[me_x, side, 1] + ly[me_x].astype(jnp.float32)
    link(l2y, l2y, (s2y, r2y), 0, "dp", partner).wait_recv()
    n_low = n_low + l2y[...].astype(jnp.float32)
    for k in range(1, nx):
        x = along(k)
        link(l2x.at[x], l2x.at[x], (s2x, r2x), x, "neg", mate).wait_recv()
        n_high = n_high + l2x[x].astype(jnp.float32)

    grads[1][0:block, 0:half_w] = n_low.T * inv_temp
    grads[1][0:block, half_w:width] = n_high.T * inv_temp
    embed_stage(1, 0, block)
    second_stage(1, 2)
    stage0(2)
    slope_stage(1, 0, block)
    stage2(0)
    stage1(2)
    first_stage(1, 3)
    stage0(3)
    stage2(1)
    stage1(3)
    stage3(0)
    stage2z(0)
    stage2(2)
    stage2z(1)
    stage3(1)
    stage2z(2)
    stage2(3)
    stage3(2)
    stage3z(0)
    stage2z(3)
    stage3z(1)
    stage3(3)
    stage3z(2)
    stage3z(3)
    for g in range(3):
        stage4(g)
        spread(g)
    stage4(3)
    total_squares = squares[0] + squares[1] + squares[2] + squares[3]
    lane = lax.broadcasted_iota(jnp.int32, (1, 128), 1)
    stat[...] = jnp.where(lane == 0, total_squares, loss_part)
    for n in range(1, devices):
        dp, neg = everyone(n)
        copy = pltpu.make_async_remote_copy(
            src_ref=stat, dst_ref=stat_land.at[me], send_sem=ss.at[n], recv_sem=sr2.at[me],
            device_id={"dp": dp, "neg": neg}, device_id_type=pl.DeviceIdType.MESH,
        )
        queue(copy)
    spread(3)
    for g in range(4):
        stage5(g)
    for g in range(4):
        stage6(g)
    stat_land[me] = stat[...]
    for n in range(1, devices):
        source = lax.rem(me + n, devices)
        arrived(stat_land.at[source], sr2, source)
    stat_land[me] = jnp.sum(stat_land[...], axis=0)
    leave(stat_land.at[me], stats_ref, 4)
    for copy in pending:
        copy.wait_send()
    for copy in leaving:
        copy.wait()


    for copy in sends:
        copy.wait_send()
    for distance in range(line):
        for j in range(cuts):
            if distance < line - 1:
                pl.when((place >= distance) & goes_right)(lambda: right(distance, j).wait_send())
                pl.when((place + distance < line) & goes_left)(lambda: left(distance, j).wait_send())
    for k in range(1, line):
        q_send(k, lax.rem(place + k, line)).wait_send()
    for i in range(2 * nx):
        c_send(i).wait_send()
        if i < 2 * (nx - 1):
            send_1x(i).wait_send()
        if i % 2 == 0:
            send_1y(i).wait_send()


def fused_step(ndp, nneg, arguments):
    line, nx = ndp // 2, nneg // 2
    bf16, f32, i32 = jnp.bfloat16, jnp.float32, jnp.int32
    named = dict(zip(step_inputs, arguments))
    fin, h1 = named["item_first"].shape
    h2, width = named["item_third"].shape
    own_rows, block = named["query_features"].shape[0], named["negative_features"].shape[0]
    blocks, cuts, lanes = 2 * nneg, 4, 128
    rows_half = (width // 2, block)
    sources = {"item_features": pltpu.VMEM((block + own_rows, fin), bf16)}
    for name, value in named.items():
        if name not in ("positive_features", "negative_features"):
            sources[name] = pltpu.VMEM(value.shape, value.dtype)
    counts = (own_rows, block + own_rows)
    towers = [
        [
            pltpu.VMEM((count, h1), bf16), pltpu.VMEM((count, h1), f32), pltpu.VMEM((count, h2), bf16),
            pltpu.VMEM((count, h2), f32), pltpu.VMEM((count, width), f32),
        ]
        for count in counts
    ]
    scratch = [
        [pltpu.VMEM((count, width), bf16), pltpu.VMEM((count, h2), bf16), pltpu.VMEM((count, h1), bf16)]
        for count in counts
    ]
    row = pltpu.VMEM((1, own_rows), f32)
    score = [
        pltpu.VMEM((line, cuts, own_rows // cuts, width), bf16),
        pltpu.VMEM((blocks, 2, block // 2, width), bf16),
        pltpu.VMEM((2, block), i32),
        pltpu.VMEM((blocks, 2, block), i32),
        pltpu.VMEM((blocks, 2, block), f32),
        pltpu.VMEM((1, own_rows), i32),
        pltpu.VMEM((line, 1, own_rows), i32),
        pltpu.VMEM((line, own_rows, lanes), f32),
        pltpu.VMEM((blocks, line, own_rows, block), bf16),
        pltpu.VMEM((line, own_rows, lanes), f32),
        pltpu.VMEM((line, 1, own_rows), f32),
        pltpu.VMEM((line, line, 1, own_rows), f32),
        pltpu.VMEM((width, line * own_rows), bf16),
        pltpu.VMEM((line, own_rows, width), bf16),
        pltpu.VMEM((own_rows, width), f32),
        pltpu.VMEM((line, own_rows, width), bf16),
        pltpu.VMEM((nx, 2, 2) + rows_half, bf16),
        pltpu.VMEM((nx, 2, 2) + rows_half, bf16),
        pltpu.VMEM((nx, 2, 2) + rows_half, f32),
        pltpu.VMEM((nx, 2, 2) + rows_half, bf16),
        pltpu.VMEM((nx, 2) + rows_half, bf16),
        pltpu.VMEM((nx,) + rows_half, bf16),
        pltpu.VMEM(rows_half, bf16),
        pltpu.VMEM((nx,) + rows_half, bf16),
    ] + sems(
        3 * nx, 1 + nx, 4 * nx, 4 * nx, 4 * nx, line * cuts, line * cuts, line * cuts,
        blocks, blocks, line, line, line, line, line, line,
        2 * nx, 2 * nx, 2 * nx, 2 * nx, nx, nx, 1, 1, nx, nx, len(step_inputs),
    )
    groups, outs, bufs = [], [], []
    for _ in counts:
        for height, columns in ((fin, h1), (h1, h2), (h2, width)):
            outs.append(jax.ShapeDtypeStruct((height // ndp, columns), f32))
        both = h2 // (ndp * nneg) * (width // pack_columns) + h1 // (ndp * nneg) * (h2 // pack_columns)
        alone = fin // (ndp * nneg) * (h1 // pack_columns)
        for r in (both, alone):
            spare = r // 16 - 1
            low = spare // 2 + (spare % 2 if len(groups) == 3 else 0)
            groups.append((low * 16, spare * 16, r))
    c = pack_columns
    sem_names = ["cs", "cr", "s1x", "r1x", "s1y", "r1y", "s2y", "r2y", "s2x", "r2x", "s3", "r3", "sg", "rg", "sh", "rh"]
    sem_names += ["s1z", "r1z", "s2z", "r2z", "s3z", "r3z"]
    for r1, r, full in groups:
        r2, r4 = r - r1, full - r
        shapes = dict(
            packed=(2, ndp, nx, full, c), c_in=(ndp, nx, full, c), o1x=(nx, ndp, r1, c), l1x=(nx, ndp, r1, c),
            o1y=(line, nx, r2, c), l1y=(line, nx, r2, c), o2y=(line, r1, c), l2y=(line, r1, c),
            o2x=(nx, line, r2, c), l2x=(nx, line, r2, c), zs=(line, r, c), l3=(line, r, c), ag=(nneg, full, c),
            o1z=(line, 2, nx, r4, c), l1z=(line, 2, nx, r4, c), o2z=(nx, 2, r4, c), l2z=(nx, 2, r4, c), o3z=(r4, c), l3z=(r4, c),
        )
        buf = {name: pltpu.VMEM(shape, bf16) for name, shape in shapes.items()}
        buf.update(zip(sem_names, sems(1, 1, nx, nx, 1, 1, 1, 1, nx, nx, line, line, nx, nx, nx, nx, line, line, nx, nx, 1, 1)))
        bufs.append(buf)
    tree = (
        sources, pltpu.VMEM((own_rows, width), bf16), pltpu.VMEM((2, block // 2, width), bf16),
        pltpu.VMEM((own_rows, width), bf16), towers, [pltpu.VMEM((count, width), f32) for count in counts], row, row,
        *score, scratch, bufs,
        pltpu.VMEM((1, 128), f32), pltpu.VMEM((ndp * nneg, 1, 128), f32), *sems(ndp * nneg, ndp * nneg, 5),
    )
    leaves, names = jax.tree.flatten(tree)
    space = sems(1)[0].memory_space
    is_flag = [leaf.memory_space == space for leaf in leaves]
    flags = [leaf for leaf, flag in zip(leaves, is_flag) if flag]
    kept = [leaf for leaf, flag in zip(leaves, is_flag) if not flag]

    def kernel(*refs):
        fixed = refs[: len(refs) - len(kept)]
        held = refs[len(refs) - len(kept) :]

        def scoped(*flag_refs):
            held_refs, flags_left = iter(held), iter(flag_refs)
            merged = [next(flags_left) if flag else next(held_refs) for flag in is_flag]
            step_kernel(ndp, nneg, names, tuple(groups), *fixed, *merged)

        pl.run_scoped(scoped, *flags)

    any_space = pl.BlockSpec(memory_space=pl.ANY)
    stats, *gathered = pl.pallas_call(
        kernel,
        out_shape=(
            jax.ShapeDtypeStruct((1, 128), f32),
            *[jax.ShapeDtypeStruct((nneg, group[-1], pack_columns), bf16) for group in groups],
        ),
        in_specs=[any_space] * len(arguments),
        out_specs=(any_space,) * 5,
        scratch_shapes=kept,
        compiler_params=pltpu.CompilerParams(
            collective_id=1, has_side_effects=True, vmem_limit_bytes=67043328
        ),
    )(*arguments)
    mean_loss, *clipped = pl.pallas_call(
        functools.partial(finish_kernel, nneg, own_rows * ndp * nneg),
        out_shape=(jax.ShapeDtypeStruct((1,), f32), *outs),
        in_specs=[any_space] * 5,
        out_specs=(pl.BlockSpec(memory_space=pltpu.SMEM), *([any_space] * 6)),
        scratch_shapes=[pltpu.VMEM((1, 128), f32)]
        + [pltpu.VMEM((nneg, group[-1], pack_columns), bf16) for group in groups]
        + [pltpu.VMEM(out.shape, f32) for out in outs]
        + sems(5, 6),
    )(stats, *gathered)
    return (mean_loss.reshape(()), *clipped)


def finish_kernel(nneg, count, *refs):
    given, loss_ref, outs, stats_ref, gathered, staged = refs[:5], refs[5], refs[6:12], refs[12], refs[13:17], refs[17:23]
    loaded, done = refs[23:]
    loads = [
        pltpu.make_async_copy(source, target, loaded.at[i])
        for i, (source, target) in enumerate(zip(given, (stats_ref, *gathered)))
    ]
    for copy in loads:
        copy.start()
    loads[0].wait()
    clip = clip_norm / jnp.maximum(jnp.sqrt(stats_ref[0:1, 0:1]), clip_norm)
    copies = []
    for t in range(2):
        third_ref, second_ref, first_ref = staged[3 * t + 2], staged[3 * t + 1], staged[3 * t]
        loads[2 * t + 1].wait()
        loads[2 * t + 2].wait()
        for index, group, ref, offset in (
            (3 * t + 1, 2 * t, second_ref, third_ref.shape[0] // nneg),
            (3 * t, 2 * t + 1, first_ref, 0),
            (3 * t + 2, 2 * t, third_ref, 0),
        ):
            pieces = ref.shape[0] // nneg
            for p in range(ref.shape[1] // pack_columns):
                lo = offset + p * pieces
                for n in range(nneg):
                    value = gathered[group][n, lo : lo + pieces, :].astype(jnp.float32) * clip
                    ref[n * pieces : (n + 1) * pieces, p * pack_columns : (p + 1) * pack_columns] = value
            copy = pltpu.make_async_copy(ref, outs[index], done.at[index])
            copy.start()
            copies.append(copy)
    loss_ref[0] = jnp.sum(stats_ref[0:1, 1:2]) / count
    for copy in copies:
        copy.wait()


def per_device(
    query_features,
    positive_features,
    negative_features,
    positive_ids,
    positive_counts,
    negative_ids,
    negative_counts,
    query_first,
    query_second,
    query_third,
    item_first,
    item_second,
    item_third,
):
    own_rows = query_features.shape[0]
    ndp, nneg = lax.axis_size("dp"), lax.axis_size("neg")
    heights = (query_first.shape[0], query_second.shape[0], query_third.shape[0])
    tiled = all(height % (16 * ndp * nneg) == 0 for height in heights)
    if tiled and own_rows % 256 == 0 and negative_features.shape[0] % 256 == 0:
        return fused_step(
            ndp,
            nneg,
            (
                query_features, positive_features, negative_features, positive_ids.reshape(1, -1),
                positive_counts.reshape(1, -1), negative_ids.reshape(1, -1), negative_counts.reshape(1, -1),
                query_first, query_second, query_third, item_first, item_second, item_third,
            ),
        )
    query_saved, query_unit = tower_forward(query_features, query_first, query_second, query_third)
    item_features = jnp.concatenate([positive_features, negative_features], axis=0)
    item_saved, item_unit = tower_forward(item_features, item_first, item_second, item_third)
    positive_unit = item_unit[:own_rows]
    negative_unit = item_unit[own_rows:]
    ndp, nneg = lax.axis_size("dp"), lax.axis_size("neg")
    width = query_unit.shape[1]
    line, nx = ndp // 2, nneg // 2
    block = negative_unit.shape[0]
    blocks, cuts, lanes = 2 * nneg, 2, min(block, 128)
    bf16, f32, i32 = jnp.bfloat16, jnp.float32, jnp.int32
    positive_logit = jnp.sum(
        query_unit.astype(f32) * positive_unit.astype(f32), axis=1
    ) * inv_temp - jnp.log(positive_counts.astype(f32))
    positive_exp = jnp.exp(positive_logit)
    rows_half = (width // 2, block)
    query_total, denom, negative_sum = call(
        score_kernel,
        0,
        ndp,
        nneg,
        (
            jax.ShapeDtypeStruct((own_rows, width), f32),
            jax.ShapeDtypeStruct((1, own_rows), f32),
            jax.ShapeDtypeStruct((2,) + rows_half, f32),
        ),
        [
            pltpu.VMEM((line, cuts, own_rows // cuts, width), bf16),
            pltpu.VMEM((blocks, 2, block // 2, width), bf16),
            pltpu.VMEM((2, block), i32),
            pltpu.VMEM((blocks, 2, block), i32),
            pltpu.VMEM((blocks, 2, block), f32),
            pltpu.VMEM((1, own_rows), i32),
            pltpu.VMEM((line, 1, own_rows), i32),
            pltpu.VMEM((line, own_rows, lanes), f32),
            pltpu.VMEM((blocks, line, own_rows, block), bf16),
            pltpu.VMEM((line, own_rows, lanes), f32),
            pltpu.VMEM((line, 1, own_rows), f32),
            pltpu.VMEM((line, line, 1, own_rows), f32),
            pltpu.VMEM((width, line * own_rows), bf16),
            pltpu.VMEM((line, own_rows, width), bf16),
            pltpu.VMEM((own_rows, width), f32),
            pltpu.VMEM((line, own_rows, width), bf16),
            pltpu.VMEM((nx, 2, 2) + rows_half, bf16),
            pltpu.VMEM((nx, 2, 2) + rows_half, bf16),
            pltpu.VMEM((nx, 2, 2) + rows_half, f32),
            pltpu.VMEM((nx, 2, 2) + rows_half, bf16),
            pltpu.VMEM((nx, 2) + rows_half, bf16),
            pltpu.VMEM((nx,) + rows_half, bf16),
            pltpu.VMEM(rows_half, bf16),
            pltpu.VMEM((nx,) + rows_half, bf16),
        ]
        + sems(
            3 * nx, 1 + nx, 4 * nx, 4 * nx, 4 * nx, line * cuts, line * cuts, line * cuts,
            blocks, blocks, line, line, line, line, line, line,
            2 * nx, 2 * nx, 2 * nx, 2 * nx, nx, nx, 1, 1, nx, nx,
        ),
        [vmem] * 6,
        40,
    )(
        query_unit,
        negative_unit.reshape(2, block // 2, width),
        positive_ids.reshape((1, -1) if own_rows % 128 == 0 else (nneg, own_rows)),
        negative_ids.reshape((1, -1) if block % 128 == 0 else (ndp, block)),
        negative_counts.reshape((1, -1) if block % 128 == 0 else (ndp, block)),
        positive_exp.reshape(1, own_rows),
    )
    own_denom = denom.reshape(-1)
    loss_part = jnp.sum(jnp.log(own_denom) - positive_logit)
    positive_slope = positive_exp / own_denom - 1.0
    query_sum = query_total / own_denom[:, None]
    negative_sum = negative_sum.reshape(width, block).T
    query_grad = (
        query_sum + positive_slope[:, None] * positive_unit.astype(jnp.float32)
    ) * inv_temp
    positive_grad = positive_slope[:, None] * query_unit.astype(jnp.float32) * inv_temp
    item_grad = jnp.concatenate([positive_grad, negative_sum * inv_temp], axis=0)
    query_grads = tower_backward(query_features, query_second, query_third, query_saved, query_grad)
    item_grads = tower_backward(item_features, item_second, item_third, item_saved, item_grad)
    gradients = query_grads + item_grads
    parts = [part for gradient in gradients for part in to_packed(gradient, ndp)]
    packed = jnp.concatenate(parts, axis=1)
    rows = packed.shape[1] // nneg
    packed = packed.reshape(ndp, nneg, 2, rows // 2, pack_columns).transpose(1, 0, 2, 3, 4)
    piece = (rows // 2, pack_columns)
    gathered, stats = call(
        weight_kernel,
        3,
        ndp,
        nneg,
        (jax.ShapeDtypeStruct((nneg, 2) + piece, bf16), jax.ShapeDtypeStruct((8, 128), f32)),
        [
            pltpu.VMEM((nx, ndp, 2) + piece, bf16),
            pltpu.VMEM((nx, 2, line) + piece, bf16),
            pltpu.VMEM((2, nx, line) + piece, bf16),
            pltpu.VMEM((nx, 2, line) + piece, bf16),
            pltpu.VMEM((nx, line) + piece, bf16),
            pltpu.VMEM((2, line) + piece, bf16),
            pltpu.VMEM((nx, line) + piece, bf16),
            pltpu.VMEM((line,) + piece, bf16),
            pltpu.VMEM((nx, line) + piece, bf16),
            pltpu.VMEM((2, line) + piece, bf16),
            pltpu.VMEM((2, line) + piece, bf16),
            pltpu.VMEM((8, 128), f32),
            pltpu.VMEM((ndp, 8, 128), f32),
            pltpu.VMEM((8, 128), f32),
            pltpu.VMEM((nneg, 8, 128), f32),
        ]
        + sems(nx, nx, 2 * nx, 2 * nx, 2, 2, ndp, ndp, ndp, ndp, nneg, nneg, nx, nx, nx, nx),
        [vmem, pl.BlockSpec(memory_space=pltpu.SMEM)],
    )(packed, loss_part.reshape(1))
    grad_norm = jnp.sqrt(stats[0, 0])
    mean_loss = stats[0, 1] / (own_rows * ndp * nneg)
    clip_factor = clip_norm / jnp.maximum(grad_norm, clip_norm)
    flat = gathered.reshape(nneg * rows, pack_columns)
    clipped = []
    start = 0
    for gradient in gradients:
        height, columns = gradient.shape[0] // ndp, gradient.shape[1]
        groups = columns // pack_columns
        blocks = [flat[start + g * height : start + (g + 1) * height] for g in range(groups)]
        start += groups * height
        clipped.append(jnp.concatenate(blocks, axis=1).astype(jnp.float32) * clip_factor)
    return (mean_loss, *clipped)


def solution(mesh):
    placed = (
        P(("dp", "neg"), None),
        P(("dp", "neg"), None),
        P(("neg", "dp"), None),
        P("dp"),
        P(("dp", "neg")),
        P("neg"),
        P("neg"),
        P(),
        P(),
        P(),
        P(),
        P(),
        P(),
    )
    return jax.shard_map(
        per_device,
        mesh=mesh,
        in_specs=placed,
        out_specs=(
            P(),
            P("dp", None),
            P("dp", None),
            P("dp", None),
            P("dp", None),
            P("dp", None),
            P("dp", None),
        ),
        check_vma=False,
    )
```

```python
import functools

import jax
import jax.numpy as jnp
from jax import lax
from jax.experimental import pallas as pl
from jax.experimental.pallas import tpu as pltpu
from jax.sharding import PartitionSpec as P

inv_temp = 20.0
log2_e = 1.4426950408889634
clip_norm = 256.0


def silu_slope(pre):
    sigma = jax.nn.sigmoid(pre)
    return sigma * (1.0 + pre * (1.0 - sigma))


def contract_rows(left, right):
    return lax.dot_general(
        left, right, (((0,), (0,)), ((), ())), preferred_element_type=jnp.float32
    )


def contract_cols(left, right):
    return lax.dot_general(
        left, right, (((1,), (1,)), ((), ())), preferred_element_type=jnp.float32
    )


def tower_forward(features, first, second, third):
    first_pre = jnp.dot(features, first, preferred_element_type=jnp.float32)
    first_act = jax.nn.silu(first_pre).astype(jnp.bfloat16)
    second_pre = jnp.dot(first_act, second, preferred_element_type=jnp.float32)
    second_act = jax.nn.silu(second_pre).astype(jnp.bfloat16)
    embedding = jnp.dot(second_act, third, preferred_element_type=jnp.float32)
    inv_norm = lax.rsqrt(jnp.sum(embedding * embedding, axis=1, keepdims=True) + 1.0)
    unit = (embedding * inv_norm).astype(jnp.bfloat16)
    saved = (silu_slope(first_pre), first_act, silu_slope(second_pre), second_act, embedding, inv_norm)
    return saved, unit


def tower_backward(features, second, third, saved, unit_grad):
    first_slope, first_act, second_slope, second_act, embedding, inv_norm = saved
    along = jnp.sum(embedding * unit_grad, axis=1, keepdims=True)
    embed_grad = (inv_norm * unit_grad - inv_norm * inv_norm * inv_norm * embedding * along).astype(
        jnp.bfloat16
    )
    third_grad = contract_rows(second_act, embed_grad)
    second_step = (contract_cols(embed_grad, third) * second_slope).astype(jnp.bfloat16)
    second_grad = contract_rows(first_act, second_step)
    first_step = (contract_cols(second_step, second) * first_slope).astype(jnp.bfloat16)
    first_grad = contract_rows(features, first_step)
    return (first_grad, second_grad, third_grad)


pack_columns = 256
vmem = pl.BlockSpec(memory_space=pltpu.VMEM)


def greet(ndp, nneg, me_dp, me_neg):
    barrier = pltpu.get_barrier_semaphore()
    for k in range(1, nneg):
        pl.semaphore_signal(
            barrier, inc=1, device_id={"neg": lax.rem(me_neg + k, nneg)}, device_id_type=pl.DeviceIdType.MESH
        )
    for k in range(1, ndp):
        pl.semaphore_signal(
            barrier, inc=1, device_id={"dp": lax.rem(me_dp + k, ndp)}, device_id_type=pl.DeviceIdType.MESH
        )
    pl.semaphore_wait(barrier, (nneg - 1) + (ndp - 1))


def send(src, dst, send_sem, recv_sem, axis, target):
    copy = pltpu.make_async_remote_copy(
        src_ref=src,
        dst_ref=dst,
        send_sem=send_sem,
        recv_sem=recv_sem,
        device_id={axis: target},
        device_id_type=pl.DeviceIdType.MESH,
    )
    copy.start()
    return copy


def share(axis, n, me, src_of, dst, send_sem, recv_sem):
    return [
        send(src_of(lax.rem(me + k, n)), dst.at[me], send_sem.at[k], recv_sem.at[k], axis, lax.rem(me + k, n))
        for k in range(1, n)
    ]


def finish(copies):
    for copy in copies:
        copy.wait()


def link(src, dst, sems, index, axis, target, send_index=None):
    send_sems, recv_sems = sems
    return pltpu.make_async_remote_copy(
        src_ref=src,
        dst_ref=dst,
        send_sem=send_sems.at[index if send_index is None else send_index],
        recv_sem=recv_sems.at[index],
        device_id={axis: target},
        device_id_type=pl.DeviceIdType.MESH,
    )


def score_kernel(
    ndp, nneg, query_ref, negative_ref, pid_ref, nid_ref, count_ref, pexp_ref, sum_ref, denom_ref, nsum_ref,
    q_land, n_land, meta_out, meta, rows, pid_out, pid_land, pid_col, w, den, dpart, dland, scaled,
    q_out, q_part, q_in, c_out, c_in, own, out, lx, ly, l2y, l2x,
    sx, sy, rn, sm, rm, sr, sl, rq, s_meta, r_meta, s_pid, r_pid, sd, rd, sq, rqs,
    sc, rc, s1x, r1x, s1y, r1y, s2y, r2y, s2x, r2x,
):
    me_dp, me_neg = lax.axis_index("dp"), lax.axis_index("neg")
    line, nx = ndp // 2, nneg // 2
    place, side = me_dp // 2, lax.rem(me_dp, 2)
    me_x, me_core = me_neg // 2, lax.rem(me_neg, 2)
    far, other = 1 - side, 1 - me_core
    partner, mate = 2 * place + far, 2 * me_x + other
    rows_q, width = query_ref.shape
    block = 2 * negative_ref.shape[1]
    lanes = den.shape[2]
    cuts = q_land.shape[1]
    half_w = width // 2
    blocks = nneg * 2
    here = (me_x * 2 + side) * 2 + me_core

    def along(k):
        return lax.rem(me_x + k, nx)

    def at_place(z):
        return 2 * z + side

    barrier = pltpu.get_barrier_semaphore()
    for k in range(1, line):
        pl.semaphore_signal(
            barrier, inc=1, device_id={"dp": at_place(lax.rem(place + k, line))}, device_id_type=pl.DeviceIdType.MESH
        )

    def quad(k):
        b = lax.rem(here + k, blocks)
        return {"dp": 2 * place + lax.rem(b // 2, 2), "neg": 2 * (b // 4) + lax.rem(b, 2)}

    for k in range(1, blocks):
        pl.semaphore_signal(barrier, inc=1, device_id=quad(k), device_id_type=pl.DeviceIdType.MESH)
    def own_ids(ref, index, count):
        if count % 128 == 0:
            return ref[:, pl.ds(pl.multiple_of(index * count, count), count)]
        return ref[pl.ds(index, 1), :]

    meta_out[0:1, :] = own_ids(nid_ref, me_dp, block)
    meta_out[1:2, :] = own_ids(count_ref, me_dp, block)
    pid_out[...] = own_ids(pid_ref, me_neg, rows_q)
    pl.semaphore_wait(barrier, (line - 1) + (blocks - 1))

    def slot(x, y, half):
        return (x * 2 + y) * 2 + half

    def piece(x, y, half):
        return n_land.at[(x * 2 + y) * 2 + me_core, half]

    def push(src, x, y, half, send_sems, index, axis, target):
        return link(src, piece(x, y, half), (send_sems, rn), slot(x, y, half), axis, target, index)

    def relay(src, x, y, half):
        i = slot(x, y, half)
        return link(src, piece(x, y, half), (sm, rm), i, "neg", mate)

    def landed(x, y, half):
        ref = piece(x, y, half)
        link(ref, ref, (sy, rn), slot(x, y, half), "neg", mate, 0).wait_recv()

    sends = []

    def go(copy):
        copy.start()
        sends.append(copy)

    def to_x(src, x, y, half, kind):
        for k in range(1, nx):
            go(push(src, x, y, half, sx, kind * nx + k, "neg", 2 * along(k) + me_core))

    def to_y(src, x, y, half, index):
        go(push(src, x, y, half, sy, index, "dp", partner))

    first, second = negative_ref.at[0], negative_ref.at[1]
    to_x(first, me_x, side, 0, 0)
    to_y(second, me_x, side, 1, 0)
    to_x(second, me_x, side, 1, 1)
    to_y(first, me_x, side, 0, 1)
    go(relay(first, me_x, side, 0))
    go(relay(second, me_x, side, 1))

    def chain(slot_z, j, distance, sems, target):
        src = query_ref.at[pl.ds(j * (rows_q // cuts), rows_q // cuts)] if distance == 0 else q_land.at[slot_z, j]
        return link(src, q_land.at[slot_z, j], (sems, rq), slot_z * cuts + j, "dp", target, distance * cuts + j)

    def right(distance, j):
        return chain(place - distance, j, distance, sr, at_place(lax.rem(place + 1, line)))

    def left(distance, j):
        return chain(place + distance, j, distance, sl, at_place(lax.rem(place + line - 1, line)))

    goes_right, goes_left = place < line - 1, place > 0
    for j in range(cuts):
        pl.when(goes_right)(lambda j=j: right(0, j).start())
        pl.when(goes_left)(lambda j=j: left(0, j).start())
    for k in range(1, blocks):
        b = lax.rem(here + k, blocks)
        copy = pltpu.make_async_remote_copy(
            src_ref=meta_out, dst_ref=meta.at[here], send_sem=s_meta.at[k], recv_sem=r_meta.at[here],
            device_id=quad(k), device_id_type=pl.DeviceIdType.MESH,
        )
        go(copy)
    for k in range(1, line):
        z = lax.rem(place + k, line)
        go(link(pid_out, pid_land.at[place], (s_pid, r_pid), place, "dp", at_place(z), k))
    n_land[here] = negative_ref[...]
    for j in range(cuts):
        q_land[place, j] = query_ref[pl.ds(j * (rows_q // cuts), rows_q // cuts), :]
    meta[here] = meta_out[...]
    pid_land[place] = pid_out[...]

    for k in range(1, nx):
        x = along(k)
        landed(x, side, 0)
        to_y(piece(x, side, 0), x, side, 0, 1 + k)
        go(relay(piece(x, side, 0), x, side, 0))
    landed(me_x, far, 1)
    to_x(piece(me_x, far, 1), me_x, far, 1, 2)
    go(relay(piece(me_x, far, 1), me_x, far, 1))

    def q_step(distance):
        for j in range(cuts):

            @pl.when(place >= distance)
            def _():
                ref = q_land.at[place - distance, j]
                link(ref, ref, (sr, rq), (place - distance) * cuts + j, "dp", partner, 0).wait_recv()
                pl.when(goes_right)(lambda: right(distance, j).start())

            @pl.when(place + distance < line)
            def _():
                ref = q_land.at[place + distance, j]
                link(ref, ref, (sl, rq), (place + distance) * cuts + j, "dp", partner, 0).wait_recv()
                pl.when(goes_left)(lambda: left(distance, j).start())

    q_step(1)
    for k in range(1, nx):
        x = along(k)
        landed(x, side, 1)
        go(relay(piece(x, side, 1), x, side, 1))
    landed(me_x, far, 0)
    go(relay(piece(me_x, far, 0), me_x, far, 0))
    for distance in range(2, line):
        q_step(distance)
    for half in range(2):
        for k in range(1, nx):
            x = along(k)
            landed(x, far, half)
            go(relay(piece(x, far, half), x, far, half))
    for x in range(nx):
        for y in range(2):
            for half in range(2):
                i = slot(x, y, half)
                ref = n_land.at[(x * 2 + y) * 2 + other, half]
                link(ref, ref, (sm, rm), i, "neg", mate).wait_recv()
    for k in range(1, blocks):
        b = lax.rem(here + k, blocks)
        link(meta.at[b], meta.at[b], (s_meta, r_meta), b, "neg", mate).wait_recv()
    for k in range(1, line):
        z = lax.rem(place + k, line)
        link(pid_land.at[z], pid_land.at[z], (s_pid, r_pid), z, "dp", partner).wait_recv()

    for b in range(blocks):
        rows[b, 0:1, :] = meta[b, 0:1, :].astype(jnp.float32)
        rows[b, 1:2, :] = jnp.log2(meta[b, 1:2, :].astype(jnp.float32))
    for z in range(line):
        pid_col[z] = jnp.broadcast_to(pid_land[z].astype(jnp.float32), (lanes, rows_q)).T
        den[z] = jnp.zeros((rows_q, lanes), jnp.float32)

    def unit(b, z):
        dots = contract_cols(q_land[z].reshape(rows_q, width), n_land[b].reshape(block, width))
        value = jnp.exp2(dots * (inv_temp * log2_e) - rows[b, 1:2, :])
        ids = jnp.concatenate([pid_col[z]] * (block // lanes), axis=1)
        value = jnp.where(ids != rows[b, 0:1, :], value, 0.0)
        w[b, z] = value.astype(jnp.bfloat16)
        total = den[z]
        for c in range(0, block, lanes):
            total = total + value[:, c : c + lanes]
        den[z] = total

    def units(b, carry):
        for z in range(line):
            unit(b, z)
        return carry

    lax.fori_loop(0, blocks, units, 0)
    for z in range(line):
        dpart[z] = jnp.sum(den[z].T, axis=0, keepdims=True)
    dpart[place] = dpart[place] + pexp_ref[...]
    for k in range(1, line):
        z = lax.rem(place + k, line)
        go(link(dpart, dland.at[place], (sd, rd), place, "dp", at_place(z), k))

    def q_block(z):
        if block % 128 == 0:
            left_side = jnp.concatenate([w[b, z] for b in range(blocks)], axis=1)
            return jnp.dot(
                left_side, n_land[...].reshape(blocks * block, width), preferred_element_type=jnp.float32
            )
        total = jnp.zeros((rows_q, width), jnp.float32)
        for b in range(blocks):
            total = total + jnp.dot(w[b, z], n_land[b].reshape(block, width), preferred_element_type=jnp.float32)
        return total

    def q_send(k, z):
        return link(q_out.at[z], q_in.at[place], (sq, rqs), place, "dp", at_place(z), k)

    def q_push(k, carry):
        z = lax.rem(place + k, line)
        q_out[z] = q_block(z).astype(jnp.bfloat16)
        q_send(k, z).start()
        return carry

    lax.fori_loop(1, line, q_push, 0)
    q_part[...] = q_block(place)
    total = dpart[...]
    for k in range(1, line):
        z = lax.rem(place + k, line)
        link(dland.at[z], dland.at[z], (sd, rd), z, "dp", partner).wait_recv()
        total = total + dland[z]
    dpart2 = 1.0 / total
    for z in range(line):
        q_t = q_land[z].reshape(rows_q, width).astype(jnp.float32).T
        scaled[:, z * rows_q : (z + 1) * rows_q] = (q_t * dpart2[z]).astype(jnp.bfloat16)
    denom_ref[...] = dpart[place]
    for k in range(1, line):
        denom_ref[...] = denom_ref[...] + dland[lax.rem(place + k, line), place]

    def dest(i):
        x = lax.rem(me_x + 1 + i // 2, nx)
        y = lax.rem(side + 1 + lax.rem(i, 2), 2)
        return x, y

    def part(x, y, core):
        return jnp.dot(
            scaled[...], w[(x * 2 + y) * 2 + core].reshape(line * rows_q, block), preferred_element_type=jnp.float32
        )

    def c_send(i):
        x, y = dest(i)
        return link(c_out.at[x, y], c_in.at[x, y], (sc, rc), x * 2 + y, "neg", mate)

    def far_step(i, carry):
        x, y = dest(i)
        c_out[x, y] = part(x, y, other).astype(jnp.bfloat16).reshape(2, half_w, block)
        c_send(i).start()
        return carry

    def send_1x(i):
        x, y = dest(i)
        return link(out.at[x, y, 0], lx.at[me_x, y], (s1x, r1x), me_x * 2 + y, "neg", 2 * x + me_core, x * 2 + y)

    def send_1y(i):
        x, y = dest(i)
        return link(out.at[x, y, 1], ly.at[x], (s1y, r1y), x, "dp", partner)

    def own_step(i, carry):
        x, y = dest(i)
        value = part(x, y, me_core).reshape(2, half_w, block)
        link(c_in.at[x, y], c_in.at[x, y], (sc, rc), x * 2 + y, "neg", mate).wait_recv()
        value = value + c_in[x, y].astype(jnp.float32)
        own[x, y] = value

        @pl.when(i < 2 * (nx - 1))
        def _():
            out[x, y, 0] = value[0].astype(jnp.bfloat16)
            send_1x(i).start()

        @pl.when(lax.rem(i, 2) == 0)
        def _():
            out[x, y, 1] = value[1].astype(jnp.bfloat16)
            send_1y(i).start()

        return carry

    lax.fori_loop(0, 2 * nx, far_step, 0)
    lax.fori_loop(0, 2 * nx, own_step, 0)
    value = own[me_x, far, 0]
    for k in range(1, nx):
        x = along(k)
        ref = lx.at[x, far]
        link(ref, ref, (s1x, r1x), x * 2 + far, "neg", mate).wait_recv()
        value = value + lx[x, far].astype(jnp.float32)
    out[me_x, far, 0] = value.astype(jnp.bfloat16)
    go(link(out.at[me_x, far, 0], l2y, (s2y, r2y), 0, "dp", partner))
    for k in range(1, nx):
        x = along(k)
        link(ly.at[x], ly.at[x], (s1y, r1y), x, "dp", partner).wait_recv()
        out[x, side, 1] = (own[x, side, 1] + ly[x].astype(jnp.float32)).astype(jnp.bfloat16)
        go(link(out.at[x, side, 1], l2x.at[me_x], (s2x, r2x), me_x, "neg", 2 * x + me_core, x))
    result = q_part[...]
    for k in range(1, line):
        z = lax.rem(place + k, line)
        link(q_in.at[z], q_in.at[z], (sq, rqs), z, "dp", partner).wait_recv()
        result = result + q_in[z].astype(jnp.float32)
    sum_ref[...] = result
    low = own[me_x, side, 0]
    for k in range(1, nx):
        x = along(k)
        ref = lx.at[x, side]
        link(ref, ref, (s1x, r1x), x * 2 + side, "neg", mate).wait_recv()
        low = low + lx[x, side].astype(jnp.float32)
    link(ly.at[me_x], ly.at[me_x], (s1y, r1y), me_x, "dp", partner).wait_recv()
    high = own[me_x, side, 1] + ly[me_x].astype(jnp.float32)
    link(l2y, l2y, (s2y, r2y), 0, "dp", partner).wait_recv()
    nsum_ref[0] = low + l2y[...].astype(jnp.float32)
    for k in range(1, nx):
        x = along(k)
        link(l2x.at[x], l2x.at[x], (s2x, r2x), x, "neg", mate).wait_recv()
        high = high + l2x[x].astype(jnp.float32)
    nsum_ref[1] = high

    for copy in sends:
        copy.wait_send()
    for distance in range(line):
        for j in range(cuts):
            if distance < line - 1:
                pl.when((place >= distance) & goes_right)(lambda: right(distance, j).wait_send())
                pl.when((place + distance < line) & goes_left)(lambda: left(distance, j).wait_send())
    for k in range(1, line):
        q_send(k, lax.rem(place + k, line)).wait_send()
    for i in range(2 * nx):
        c_send(i).wait_send()
        if i < 2 * (nx - 1):
            send_1x(i).wait_send()
        if i % 2 == 0:
            send_1y(i).wait_send()


def weight_kernel(
    ndp, nneg, packed_ref, loss_ref, gathered_ref, stats_ref,
    core_land, sum_a, sum_b, land_a, land_b, half_a, half_b, last_a, last_b, line_sum, line_land,
    stat_dp, stat_dp_land, stat_neg, stat_neg_land,
    cs, cr, xs, xr, ys, yr, ps, pr, ss, sr, ts, tr, gs, gr, hs, hr,
):
    me_dp, me_neg = lax.axis_index("dp"), lax.axis_index("neg")
    nx, line = nneg // 2, ndp // 2
    me_x, me_core = me_neg // 2, lax.rem(me_neg, 2)
    place, side = me_dp // 2, lax.rem(me_dp, 2)
    other, far = 1 - me_core, 1 - side
    mate, partner = 2 * me_x + other, 2 * place + far
    greet(ndp, nneg, me_dp, me_neg)
    turn = list(range(1, nx)) + [0]

    def x_of(k):
        return lax.rem(me_x + k, nx)

    core = {}
    for k in turn:
        x = x_of(k)
        core[k] = send(packed_ref.at[2 * x + other], core_land.at[x], cs.at[k], cr.at[k], "neg", mate)

    def add_core(x, y, half, target):
        def body(z, carry):
            target[z] = (
                packed_ref[2 * x + me_core, 2 * z + y, half].astype(jnp.float32)
                + core_land[x, 2 * z + y, half].astype(jnp.float32)
            ).astype(jnp.bfloat16)
            return carry

        lax.fori_loop(0, line, body, 0)

    def add(target, *terms):
        def body(z, carry):
            value = terms[0][z].astype(jnp.float32)
            for term in terms[1:]:
                value = value + term[z].astype(jnp.float32)
            target[z] = value.astype(jnp.bfloat16)
            return carry

        lax.fori_loop(0, line, body, 0)

    first_a = []
    for k in turn:
        x = x_of(k)
        core[k].wait_recv()
        if k:
            for y in range(2):
                add_core(x, y, 0, sum_a.at[x, y])
            first_a.append(send(sum_a.at[x], land_a.at[k], xs.at[k], xr.at[k], "neg", 2 * x + me_core))
        add_core(x, far, 1, sum_b.at[far, x])
    first_b = send(sum_b.at[far], land_b, ys.at[0], yr.at[0], "dp", partner)
    for y in range(2):
        add_core(me_x, y, 0, sum_a.at[me_x, y])
    for k in range(nx):
        add_core(x_of(k), side, 1, sum_b.at[side, x_of(k)])
    for copy in first_a:
        copy.wait_recv()
    add(half_a.at[far], sum_a.at[me_x, far], *[land_a.at[k, far] for k in range(1, nx)])
    second_a = send(half_a.at[far], last_a, ys.at[1], yr.at[1], "dp", partner)
    first_b.wait_recv()
    second_b = []
    for k in turn:
        x = x_of(k)
        add(half_b.at[x], sum_b.at[side, x], land_b.at[x])
        if k:
            second_b.append(
                send(half_b.at[x], last_b.at[k], xs.at[nx + k], xr.at[nx + k], "neg", 2 * x + me_core)
            )
    add(half_a.at[side], sum_a.at[me_x, side], *[land_a.at[k, side] for k in range(1, nx)])
    second_a.wait_recv()
    add(line_sum.at[0], half_a.at[side], last_a)
    third = []
    for half in range(2):
        if half:
            for copy in second_b:
                copy.wait_recv()
            add(line_sum.at[1], half_b.at[me_x], *[last_b.at[k] for k in range(1, nx)])
        for k in range(1, line):
            z = lax.rem(place + k, line)
            third.append(
                send(line_sum.at[half, z], line_land.at[half, k], ps.at[half * line + k], pr.at[half * line + k], "dp", 2 * z + side)
            )
    for copy in third:
        copy.wait_recv()
    squares = jnp.zeros((), jnp.float32)
    for half in range(2):
        piece = line_sum[half, place].astype(jnp.float32)
        for k in range(1, line):
            piece = piece + line_land[half, k].astype(jnp.float32)
        gathered_ref[me_neg, half] = piece.astype(jnp.bfloat16)
        squares = squares + jnp.sum(piece * piece)
    lane = lax.broadcasted_iota(jnp.int32, (8, 128), 1)
    stat_dp[...] = jnp.where(lane == 0, squares, loss_ref[0])
    stat_copies = share("dp", ndp, me_dp, lambda t: stat_dp, stat_dp_land, ss, sr)
    mine = gathered_ref.at[me_neg]
    spread = [send(mine, mine, gs.at[k], gr.at[k], "neg", 2 * x_of(k) + me_core) for k in range(1, nx)]
    spread.append(send(mine, mine, gs.at[0], gr.at[0], "neg", mate))
    finish(stat_copies)
    total = stat_dp[...]
    for k in range(1, ndp):
        total = total + stat_dp_land[lax.rem(me_dp + k, ndp)]
    stat_neg[...] = total
    stat_copies = share("neg", nneg, me_neg, lambda t: stat_neg, stat_neg_land, ts, tr)
    relay = []
    for k in range(1, nx):
        spread[k - 1].wait_recv()
        x = lax.rem(me_x + nx - k, nx)
        came = gathered_ref.at[2 * x + me_core]
        relay.append(send(came, came, hs.at[k], hr.at[k], "neg", mate))
    finish(stat_copies)
    total = stat_neg[...]
    for k in range(1, nneg):
        total = total + stat_neg_land[lax.rem(me_neg + k, nneg)]
    stats_ref[...] = total
    spread[-1].wait_recv()
    finish(relay)
    for copy in [*core.values(), *first_a, first_b, second_a, *second_b, *third, *spread]:
        copy.wait_send()


def call(kernel, collective, ndp, nneg, out_shape, scratch, in_specs, megabytes=48):
    return pl.pallas_call(
        functools.partial(kernel, ndp, nneg),
        out_shape=out_shape,
        in_specs=in_specs,
        out_specs=tuple(vmem for _ in out_shape),
        scratch_shapes=scratch,
        compiler_params=pltpu.CompilerParams(
            collective_id=collective, has_side_effects=True, vmem_limit_bytes=megabytes * 1024 * 1024
        ),
    )


def sems(*counts):
    return [pltpu.SemaphoreType.DMA((count,)) for count in counts]


def to_packed(gradient, ndp):
    rows, columns = gradient.shape
    blocks = gradient.astype(jnp.bfloat16).reshape(ndp, rows // ndp, columns)
    return [blocks[:, :, c : c + pack_columns] for c in range(0, columns, pack_columns)]


step_inputs = (
    "query_features", "positive_features", "negative_features", "positive_ids", "positive_counts", "negative_ids",
    "negative_counts", "query_first", "query_second", "query_third", "item_first", "item_second", "item_third",
)


def step_kernel(ndp, nneg, names, groups, *refs):
    refs = list(refs)
    inputs = dict(zip(step_inputs, refs))
    stats_ref, gathered = refs[13], refs[14:18]
    (
        sources, q_unit, n_unit, p_unit, towers, grads, pexp, logit,
        q_land, n_land, meta_out, meta, rows, pid_out, pid_land, pid_col, w, den, dpart, dland, scaled,
        q_out, q_part, q_in, c_out, c_in, own, out, lx, ly, l2y, l2x,
        sx, sy, rn, sm, rm, sr, sl, rq, s_meta, r_meta, s_pid, r_pid, sd, rd, sq, rqs,
        sc, rc, s1x, r1x, s1y, r1y, s2y, r2y, s2x, r2x, loaded,
        scratch, bufs, stat, stat_land, ss, sr2, left_sems,
    ) = jax.tree.unflatten(names, refs[18:])
    me_dp, me_neg = lax.axis_index("dp"), lax.axis_index("neg")
    line, nx = ndp // 2, nneg // 2
    place, side = me_dp // 2, lax.rem(me_dp, 2)
    me_x, me_core = me_neg // 2, lax.rem(me_neg, 2)
    far, other = 1 - side, 1 - me_core
    partner, mate = 2 * place + far, 2 * me_x + other
    f32, bf16 = jnp.float32, jnp.bfloat16
    rows_q, width = q_unit.shape
    block = 2 * n_unit.shape[1]
    half_n = block // 2
    lanes = den.shape[2]
    cuts = q_land.shape[1]
    half_w = width // 2
    blocks = nneg * 2
    here = (me_x * 2 + side) * 2 + me_core

    order = (
        "query_features", "query_first", "query_second", "query_third", "negative_features", "item_first", "item_second",
        "item_third", "negative_ids", "negative_counts", "positive_ids", "positive_features", "positive_counts",
    )
    item_features = sources["item_features"]
    places = dict(sources)
    places["negative_features"] = item_features.at[0:block]
    places["positive_features"] = item_features.at[block : block + rows_q]
    loads = {}
    for i, name in enumerate(order):
        loads[name] = pltpu.make_async_copy(inputs[name], places[name], loaded.at[i])
    for name in order[:4]:
        loads[name].start()

    def along(k):
        return lax.rem(me_x + k, nx)

    def at_place(z):
        return 2 * z + side

    barrier = pltpu.get_barrier_semaphore()

    def quad(k):
        b = lax.rem(here + k, blocks)
        return {"dp": 2 * place + lax.rem(b // 2, 2), "neg": 2 * (b // 4) + lax.rem(b, 2)}

    devices = ndp * nneg
    me = me_dp * nneg + me_neg

    def everyone(n):
        target = lax.rem(me + n, devices)
        return target // nneg, lax.rem(target, nneg)

    for n in range(1, devices):
        dp, neg = everyone(n)
        pl.semaphore_signal(barrier, inc=1, device_id={"dp": dp, "neg": neg}, device_id_type=pl.DeviceIdType.MESH)

    def slot(x, y, half):
        return (x * 2 + y) * 2 + half

    def piece(x, y, half):
        return n_land.at[(x * 2 + y) * 2 + me_core, half]

    def push(src, x, y, half, send_sems, index, axis, target):
        return link(src, piece(x, y, half), (send_sems, rn), slot(x, y, half), axis, target, index)

    def relay(src, x, y, half):
        i = slot(x, y, half)
        return link(src, piece(x, y, half), (sm, rm), i, "neg", mate)

    def landed(x, y, half):
        ref = piece(x, y, half)
        link(ref, ref, (sy, rn), slot(x, y, half), "neg", mate, 0).wait_recv()

    sends = []

    def go(copy):
        copy.start()
        sends.append(copy)

    def to_x(src, x, y, half, kind):
        for k in range(1, nx):
            go(push(src, x, y, half, sx, kind * nx + k, "neg", 2 * along(k) + me_core))

    def to_y(src, x, y, half, index):
        go(push(src, x, y, half, sy, index, "dp", partner))

    def chain(slot_z, j, distance, sems, target):
        src = q_unit.at[pl.ds(j * (rows_q // cuts), rows_q // cuts)] if distance == 0 else q_land.at[slot_z, j]
        return link(src, q_land.at[slot_z, j], (sems, rq), slot_z * cuts + j, "dp", target, distance * cuts + j)

    def right(distance, j):
        return chain(place - distance, j, distance, sr, at_place(lax.rem(place + 1, line)))

    def left(distance, j):
        return chain(place + distance, j, distance, sl, at_place(lax.rem(place + line - 1, line)))

    goes_right, goes_left = place < line - 1, place > 0

    def q_step(distance, lo=0, hi=cuts):
        for j in range(lo, hi):

            @pl.when(place >= distance)
            def _():
                ref = q_land.at[place - distance, j]
                link(ref, ref, (sr, rq), (place - distance) * cuts + j, "dp", partner, 0).wait_recv()
                pl.when(goes_right)(lambda: right(distance, j).start())

            @pl.when(place + distance < line)
            def _():
                ref = q_land.at[place + distance, j]
                link(ref, ref, (sl, rq), (place + distance) * cuts + j, "dp", partner, 0).wait_recv()
                pl.when(goes_left)(lambda: left(distance, j).start())

    def forward(lo, count, features, first, second, third, saved, unit_ref, waits=((), (), ()), starts=()):
        act1, slope1, act2, slope2, emb = saved
        span = slice(lo, lo + count)

        def layer(source, weight, act, slope):
            columns = weight.shape[1]
            step = 256 if columns % 256 == 0 else columns
            for c in range(0, columns, step):
                pre = jnp.dot(source[span, :], weight[:, c : c + step], preferred_element_type=f32)
                sigma = 0.5 * jnp.tanh(0.5 * pre) + 0.5
                value = pre * sigma
                act[span, c : c + step] = value.astype(bf16)
                slope[span, c : c + step] = sigma + value * (1.0 - sigma)

        ready(waits[0])
        for name in starts:
            loads[name].start()
        layer(features, first, act1, slope1)
        ready(waits[1])
        layer(act1, second, act2, slope2)
        ready(waits[2])
        value = jnp.dot(act2[span, :], third[...], preferred_element_type=f32)
        emb[span, :] = value
        inv_norm = lax.rsqrt(jnp.sum(value * value, axis=1, keepdims=True) + 1.0)
        unit_ref[...] = (value * inv_norm).astype(bf16)

    def ready(chosen):
        for name in chosen:
            loads[name].wait()

    item_weights = tuple(sources[name] for name in ("item_first", "item_second", "item_third"))
    query_weights = tuple(sources[name] for name in ("query_first", "query_second", "query_third"))
    def own_ids(ref, index, count):
        return ref[:, pl.ds(pl.multiple_of(index * count, count), count)]

    forward(
        0, rows_q, sources["query_features"], *query_weights, towers[0], q_unit,
        (("query_features", "query_first"), ("query_second",), ("query_third",)),
        order[4:],
    )
    pl.semaphore_wait(barrier, devices - 1)
    for j in range(cuts):
        pl.when(goes_right)(lambda j=j: right(0, j).start())
        pl.when(goes_left)(lambda j=j: left(0, j).start())
    for j in range(cuts):
        q_land[place, j] = q_unit[pl.ds(j * (rows_q // cuts), rows_q // cuts), :]
    ready(("negative_ids", "negative_counts", "positive_ids"))
    meta_out[0:1, :] = own_ids(sources["negative_ids"], me_dp, block)
    meta_out[1:2, :] = own_ids(sources["negative_counts"], me_dp, block)
    pid_out[...] = own_ids(sources["positive_ids"], me_neg, rows_q)
    meta[here] = meta_out[...]
    pid_land[place] = pid_out[...]
    for k in range(1, blocks):
        copy = pltpu.make_async_remote_copy(
            src_ref=meta_out, dst_ref=meta.at[here], send_sem=s_meta.at[k], recv_sem=r_meta.at[here],
            device_id=quad(k), device_id_type=pl.DeviceIdType.MESH,
        )
        go(copy)
    for k in range(1, line):
        z = lax.rem(place + k, line)
        go(link(pid_out, pid_land.at[place], (s_pid, r_pid), place, "dp", at_place(z), k))
    n_first, n_second = n_unit.at[0], n_unit.at[1]
    forward(
        0, half_n, item_features, *item_weights, towers[1], n_first,
        (("negative_features", "item_first"), ("item_second",), ("item_third",)),
    )
    to_x(n_first, me_x, side, 0, 0)
    go(relay(n_first, me_x, side, 0))
    n_land[here, 0] = n_unit[0]
    forward(half_n, half_n, item_features, *item_weights, towers[1], n_second)
    to_y(n_second, me_x, side, 1, 0)
    to_x(n_second, me_x, side, 1, 1)
    to_y(n_first, me_x, side, 0, 1)
    go(relay(n_second, me_x, side, 1))
    n_land[here, 1] = n_unit[1]
    ready(("positive_features", "positive_counts"))
    forward(block, rows_q, item_features, *item_weights, towers[1], p_unit)
    q_step(1)
    product = q_unit[...].astype(f32) * p_unit[...].astype(f32)
    logit[...] = jnp.sum(product.T, axis=0, keepdims=True) * inv_temp - jnp.log(sources["positive_counts"][...].astype(f32))
    pexp[...] = jnp.exp(logit[...])

    for k in range(1, nx):
        x = along(k)
        landed(x, side, 0)
        to_y(piece(x, side, 0), x, side, 0, 1 + k)
        go(relay(piece(x, side, 0), x, side, 0))
    for k in range(1, blocks):
        b = lax.rem(here + k, blocks)
        link(meta.at[b], meta.at[b], (s_meta, r_meta), b, "neg", mate).wait_recv()
    for k in range(1, line):
        z = lax.rem(place + k, line)
        link(pid_land.at[z], pid_land.at[z], (s_pid, r_pid), z, "dp", partner).wait_recv()
    for b in range(blocks):
        rows[b, 0:1, :] = meta[b, 0:1, :].astype(f32)
        rows[b, 1:2, :] = jnp.log2(meta[b, 1:2, :].astype(f32))
    for z in range(line):
        pid_col[z] = jnp.broadcast_to(pid_land[z].astype(f32), (lanes, rows_q)).T
        den[z] = jnp.zeros((rows_q, lanes), f32)

    def unit(b, z):
        dots = contract_cols(q_land[z].reshape(rows_q, width), n_land[b].reshape(block, width))
        value = jnp.exp2(dots * (inv_temp * log2_e) - rows[b, 1:2, :])
        ids = jnp.concatenate([pid_col[z]] * (block // lanes), axis=1)
        value = jnp.where(ids != rows[b, 0:1, :], value, 0.0)
        w[b, z] = value.astype(jnp.bfloat16)
        total = den[z]
        for c in range(0, block, lanes):
            total = total + value[:, c : c + lanes]
        den[z] = total

    def relayed(x, y):
        for half in range(2):
            ref = n_land.at[(x * 2 + y) * 2 + other, half]
            link(ref, ref, (sm, rm), slot(x, y, half), "neg", mate).wait_recv()

    def both_cores(x, y):
        return [(x * 2 + y) * 2 + core for core in range(2)]

    near_blocks = both_cores(me_x, side)
    side_blocks = both_cores(me_x, far)
    along_blocks = []
    for k in range(1, nx):
        along_blocks = along_blocks + both_cores(along(k), side)
    mid_blocks = along_blocks + side_blocks

    def units(lo, hi, chosen):
        def body(z, carry):
            for b in chosen:
                unit(b, z)
            return carry

        lax.fori_loop(jnp.maximum(lo, 0), jnp.minimum(hi, line), body, 0)

    relayed(me_x, side)
    q_step(2, 0, cuts // 2)
    units(place - 1, place + 2, near_blocks)
    landed(me_x, far, 1)
    to_x(piece(me_x, far, 1), me_x, far, 1, 2)
    go(relay(piece(me_x, far, 1), me_x, far, 1))
    q_step(2, cuts // 2)
    units(place - 2, place - 1, near_blocks)
    units(place + 2, place + 3, near_blocks)
    for k in range(1, nx):
        x = along(k)
        landed(x, side, 1)
        go(relay(piece(x, side, 1), x, side, 1))
    landed(me_x, far, 0)
    go(relay(piece(me_x, far, 0), me_x, far, 0))
    for k in range(1, nx):
        relayed(along(k), side)
    units(place - 2, place + 3, along_blocks)
    relayed(me_x, far)
    units(place - 2, place, side_blocks)
    for half in range(2):
        for k in range(1, nx):
            x = along(k)
            landed(x, far, half)
            go(relay(piece(x, far, half), x, far, half))
    units(place, place + 3, side_blocks)
    for distance in range(3, line):
        q_step(distance)
    units(0, place - 2, near_blocks + mid_blocks)
    units(place + 3, line, near_blocks + mid_blocks)
    for core in (me_core, other):
        for k in range(1, nx):
            if core is other:
                relayed(along(k), far)
            for z in range(line):
                unit((along(k) * 2 + far) * 2 + core, z)
    for z in range(line):
        dpart[z] = jnp.sum(den[z].T, axis=0, keepdims=True)
    dpart[place] = dpart[place] + pexp[...]
    for k in range(1, line):
        z = lax.rem(place + k, line)
        go(link(dpart, dland.at[place], (sd, rd), place, "dp", at_place(z), k))

    def q_block(z):
        if block % 128 == 0:
            left_side = jnp.concatenate([w[b, z] for b in range(blocks)], axis=1)
            return jnp.dot(
                left_side, n_land[...].reshape(blocks * block, width), preferred_element_type=jnp.float32
            )
        total = jnp.zeros((rows_q, width), jnp.float32)
        for b in range(blocks):
            total = total + jnp.dot(w[b, z], n_land[b].reshape(block, width), preferred_element_type=jnp.float32)
        return total

    def q_send(k, z):
        return link(q_out.at[z], q_in.at[place], (sq, rqs), place, "dp", at_place(z), k)

    def q_push(k, carry):
        z = lax.rem(place + k, line)
        q_out[z] = q_block(z).astype(jnp.bfloat16)
        q_send(k, z).start()
        return carry

    lax.fori_loop(1, line, q_push, 0)
    q_part[...] = q_block(place)
    total = dpart[...]
    for k in range(1, line):
        z = lax.rem(place + k, line)
        link(dland.at[z], dland.at[z], (sd, rd), z, "dp", partner).wait_recv()
        total = total + dland[z]
    dpart2 = 1.0 / total
    for z in range(line):
        q_t = q_land[z].reshape(rows_q, width).astype(jnp.float32).T
        scaled[:, z * rows_q : (z + 1) * rows_q] = (q_t * dpart2[z]).astype(jnp.bfloat16)
    def dest(i):
        x = lax.rem(me_x + 1 + i // 2, nx)
        y = lax.rem(side + 1 + lax.rem(i, 2), 2)
        return x, y

    def part(x, y, core):
        return jnp.dot(
            scaled[...], w[(x * 2 + y) * 2 + core].reshape(line * rows_q, block), preferred_element_type=jnp.float32
        )

    def c_send(i):
        x, y = dest(i)
        return link(c_out.at[x, y], c_in.at[x, y], (sc, rc), x * 2 + y, "neg", mate)

    def far_step(i, carry):
        x, y = dest(i)
        c_out[x, y] = part(x, y, other).astype(jnp.bfloat16).reshape(2, half_w, block)
        c_send(i).start()
        return carry

    def send_1x(i):
        x, y = dest(i)
        return link(out.at[x, y, 0], lx.at[me_x, y], (s1x, r1x), me_x * 2 + y, "neg", 2 * x + me_core, x * 2 + y)

    def send_1y(i):
        x, y = dest(i)
        return link(out.at[x, y, 1], ly.at[x], (s1y, r1y), x, "dp", partner)

    def own_step(i, carry):
        x, y = dest(i)
        value = part(x, y, me_core).reshape(2, half_w, block)
        link(c_in.at[x, y], c_in.at[x, y], (sc, rc), x * 2 + y, "neg", mate).wait_recv()
        value = value + c_in[x, y].astype(jnp.float32)
        own[x, y] = value

        @pl.when(i < 2 * (nx - 1))
        def _():
            out[x, y, 0] = value[0].astype(jnp.bfloat16)
            send_1x(i).start()

        @pl.when(lax.rem(i, 2) == 0)
        def _():
            out[x, y, 1] = value[1].astype(jnp.bfloat16)
            send_1y(i).start()

        return carry

    ahead = 2

    def both_steps(i, carry):
        far_step(i + ahead, 0)
        own_step(i, 0)
        return carry

    lax.fori_loop(0, ahead, far_step, 0)
    lax.fori_loop(0, 2 * nx - ahead, both_steps, 0)
    lax.fori_loop(2 * nx - ahead, 2 * nx, own_step, 0)
    value = own[me_x, far, 0]
    for k in range(1, nx):
        x = along(k)
        ref = lx.at[x, far]
        link(ref, ref, (s1x, r1x), x * 2 + far, "neg", mate).wait_recv()
        value = value + lx[x, far].astype(jnp.float32)
    out[me_x, far, 0] = value.astype(jnp.bfloat16)
    go(link(out.at[me_x, far, 0], l2y, (s2y, r2y), 0, "dp", partner))
    for k in range(1, nx):
        x = along(k)
        link(ly.at[x], ly.at[x], (s1y, r1y), x, "dp", partner).wait_recv()
        out[x, side, 1] = (own[x, side, 1] + ly[x].astype(jnp.float32)).astype(jnp.bfloat16)
        go(link(out.at[x, side, 1], l2x.at[me_x], (s2x, r2x), me_x, "neg", 2 * x + me_core, x))
    denom = dpart[place]
    for k in range(1, line):
        denom = denom + dland[lax.rem(place + k, line), place]
    loss_part = jnp.sum(jnp.log(denom) - logit[...])

    def to_columns(row):
        column = jnp.broadcast_to(row, (lanes, rows_q)).T
        return jnp.concatenate([column] * (width // lanes), axis=1)

    slope_columns = to_columns(pexp[...] / denom - 1.0) * inv_temp
    grads[1][block : block + rows_q, :] = slope_columns * q_unit[...].astype(f32)
    result = q_part[...]
    for k in range(1, line):
        z = lax.rem(place + k, line)
        link(q_in.at[z], q_in.at[z], (sq, rqs), z, "dp", partner).wait_recv()
        result = result + q_in[z].astype(jnp.float32)
    grads[0][...] = result * (to_columns(1.0 / denom) * inv_temp) + slope_columns * p_unit[...].astype(f32)

    pending = []

    def queue(copy):
        copy.start()
        pending.append(copy)

    def x_of(k):
        return lax.rem(me_x + k, nx)

    def same_core(x):
        return 2 * x + me_core

    def z_of(k):
        return lax.rem(place + k, line)

    def arrived(ref, sem_array, index):
        link(ref, ref, (sem_array, sem_array), index, "neg", mate).wait_recv()

    steps = [
        (sources["query_features"], *towers[0], grads[0], sources["query_second"], sources["query_third"]),
        (item_features, *towers[1], grads[1], sources["item_second"], sources["item_third"]),
    ]

    def store(group, offset, value, dp, hg):
        packed = bufs[group]["packed"]
        pieces = hg // nneg
        for p in range(value.shape[1] // pack_columns):
            part = value[:, p * pack_columns : (p + 1) * pack_columns].astype(bf16)
            part = part.reshape(value.shape[0] // hg, nx, 2, pieces, pack_columns)
            lo = offset + p * pieces
            for core in range(2):
                packed[core, pl.ds(dp, value.shape[0] // hg), :, lo : lo + pieces, :] = part[:, :, core]

    def weight_grad(group, offset, left_ref, right_ref):
        rows, columns = left_ref.shape[1], right_ref.shape[1]
        hg = rows // ndp
        step = 2 * hg

        def body(m, carry):
            left = left_ref[:, pl.ds(pl.multiple_of(m * step, step), step)]
            store(group, offset, contract_rows(left, right_ref[...]), 2 * m, hg)
            return carry

        lax.fori_loop(0, rows // step, body, 0, unroll=True)
        return offset + hg // nneg * (columns // pack_columns)

    def row_loop(start, stop, body):
        def wrapped(i, carry):
            body(pl.ds(pl.multiple_of(i * 256, 256), 256))
            return carry

        lax.fori_loop(start // 256, stop // 256, wrapped, 0)

    def embed_stage(t, start, stop):
        feat, act1, slope1, act2, slope2, emb_ref, grad_ref, second, third = steps[t]
        eg, s2, s1 = scratch[t]

        def body(rows):
            emb, grad = emb_ref[rows, :], grad_ref[rows, :]
            inv_norm = lax.rsqrt(jnp.sum(emb * emb, axis=1, keepdims=True) + 1.0)
            along = jnp.sum(emb * grad, axis=1, keepdims=True)
            value = (inv_norm * grad - inv_norm * inv_norm * inv_norm * emb * along).astype(bf16)
            eg[rows, :] = value
            s2[rows, :] = (contract_cols(value, third[...]) * slope2[rows, :]).astype(bf16)

        row_loop(start, stop, body)

    def second_stage(t, group):
        feat, act1, slope1, act2, slope2, emb_ref, grad_ref, second, third = steps[t]
        eg, s2, s1 = scratch[t]
        offset = weight_grad(group, 0, act2, eg)
        weight_grad(group, offset, act1, s2)

    def slope_stage(t, start, stop):
        feat, act1, slope1, act2, slope2, emb_ref, grad_ref, second, third = steps[t]
        eg, s2, s1 = scratch[t]
        columns = second.shape[0]

        def body(rows):
            for c in range(0, columns, 512):
                value = contract_cols(s2[rows, :], second[c : c + 512, :]) * slope1[rows, c : c + 512]
                s1[rows, c : c + 512] = value.astype(bf16)

        row_loop(start, stop, body)

    def first_stage(t, group):
        weight_grad(group, 0, steps[t][0], scratch[t][2])

    def stage0(g):
        b = bufs[g]
        queue(link(b["packed"].at[other], b["c_in"], (b["cs"], b["cr"]), 0, "neg", mate))

    def base(b, dp, x, lo, hi):
        return b["packed"][me_core, dp, x, lo:hi, :].astype(f32) + b["c_in"][dp, x, lo:hi, :].astype(f32)

    def loop(count, body):
        def wrapped(i, carry):
            body(i)
            return carry

        lax.fori_loop(0, count, wrapped, 0, unroll=True)

    def stage1(g):
        b, (r1, r, full) = bufs[g], groups[g]
        arrived(b["c_in"], b["cr"], 0)
        for k in range(1, line):
            z = z_of(k)
            for y in range(2):
                for x in range(nx):
                    b["o1z"][z, y, x] = base(b, 2 * z + y, x, r, full).astype(bf16)
            queue(link(b["o1z"].at[z], b["l1z"].at[place], (b["s1z"], b["r1z"]), place, "dp", 2 * z + side, z))
        for k in range(1, nx):
            x = x_of(k)

            def body(dp):
                b["o1x"][x, dp] = base(b, dp, x, 0, r1).astype(bf16)

            loop(ndp, body)
            queue(link(b["o1x"].at[x], b["l1x"].at[me_x], (b["s1x"], b["r1x"]), me_x, "neg", same_core(x), x))

        def body_y(z):
            for x in range(nx):
                b["o1y"][z, x] = base(b, 2 * z + far, x, r1, r).astype(bf16)

        loop(line, body_y)
        queue(link(b["o1y"], b["l1y"], (b["s1y"], b["r1y"]), 0, "dp", partner))

    def low(b, dp, r1):
        value = base(b, dp, me_x, 0, r1)
        for k in range(1, nx):
            value = value + b["l1x"][x_of(k), dp].astype(f32)
        return value

    def stage2(g):
        b, (r1, r, full) = bufs[g], groups[g]
        for k in range(1, nx):
            x = x_of(k)
            arrived(b["l1x"].at[x], b["r1x"], x)

        def body(z):
            b["o2y"][z] = low(b, 2 * z + far, r1).astype(bf16)

        loop(line, body)
        queue(link(b["o2y"], b["l2y"], (b["s2y"], b["r2y"]), 0, "dp", partner))
        arrived(b["l1y"], b["r1y"], 0)
        for k in range(1, nx):
            x = x_of(k)

            def body_x(z):
                value = base(b, 2 * z + side, x, r1, r) + b["l1y"][z, x].astype(f32)
                b["o2x"][x, z] = value.astype(bf16)

            loop(line, body_x)
            queue(link(b["o2x"].at[x], b["l2x"].at[me_x], (b["s2x"], b["r2x"]), me_x, "neg", same_core(x), x))

    def stage3(g):
        b, (r1, r, full) = bufs[g], groups[g]
        arrived(b["l2y"], b["r2y"], 0)
        for k in range(1, nx):
            x = x_of(k)
            arrived(b["l2x"].at[x], b["r2x"], x)

        def body(z):
            dp = 2 * z + side
            b["zs"][z, 0:r1, :] = (low(b, dp, r1) + b["l2y"][z].astype(f32)).astype(bf16)
            value = base(b, dp, me_x, r1, r) + b["l1y"][z, me_x].astype(f32)
            for k in range(1, nx):
                value = value + b["l2x"][x_of(k), z].astype(f32)
            b["zs"][z, r1:r, :] = value.astype(bf16)

        loop(line, body)
        for k in range(1, line):
            z = z_of(k)
            queue(link(b["zs"].at[z], b["l3"].at[place], (b["s3"], b["r3"]), place, "dp", 2 * z + side, z))

    def z_sum(g, y, x):
        b, (_, r, full) = bufs[g], groups[g]
        value = base(b, 2 * place + y, x, r, full)
        for k in range(1, line):
            value = value + b["l1z"][z_of(k), y, x].astype(f32)
        return value

    def x_sum(g, y):
        value = z_sum(g, y, me_x)
        for k in range(1, nx):
            value = value + bufs[g]["l2z"][x_of(k), y].astype(f32)
        return value

    def stage2z(g):
        b = bufs[g]
        for k in range(1, line):
            z = z_of(k)
            arrived(b["l1z"].at[z], b["r1z"], z)
        for k in range(1, nx):
            x = x_of(k)
            for y in range(2):
                b["o2z"][x, y] = z_sum(g, y, x).astype(bf16)
            queue(link(b["o2z"].at[x], b["l2z"].at[me_x], (b["s2z"], b["r2z"]), me_x, "neg", same_core(x), x))

    def stage3z(g):
        b = bufs[g]
        for k in range(1, nx):
            x = x_of(k)
            arrived(b["l2z"].at[x], b["r2z"], x)
        b["o3z"][...] = x_sum(g, far).astype(bf16)
        queue(link(b["o3z"], b["l3z"], (b["s3z"], b["r3z"]), 0, "dp", partner))

    squares = []

    def stage4(g):
        b, (_, r, full) = bufs[g], groups[g]
        for k in range(1, line):
            z = z_of(k)
            arrived(b["l3"].at[z], b["r3"], z)
        value = b["zs"][place].astype(f32)
        for k in range(1, line):
            value = value + b["l3"][z_of(k)].astype(f32)
        arrived(b["l3z"], b["r3z"], 0)
        last = x_sum(g, side) + b["l3z"][...].astype(f32)
        squares.append(jnp.sum(value * value) + jnp.sum(last * last))
        b["ag"][me_neg, 0:r] = value.astype(bf16)
        b["ag"][me_neg, r:full] = last.astype(bf16)

    def spread(g):
        b = bufs[g]
        mine = b["ag"].at[me_neg]
        for k in range(1, nx):
            x = x_of(k)
            queue(link(mine, mine, (b["sg"], b["rg"]), me_x, "neg", same_core(x), x))
        queue(link(mine, mine, (b["sh"], b["rh"]), me_x, "neg", mate))

    def stage5(g):
        b = bufs[g]
        for k in range(1, nx):
            x = x_of(k)
            ref = b["ag"].at[same_core(x)]
            arrived(ref, b["rg"], x)
            queue(link(ref, ref, (b["sh"], b["rh"]), x, "neg", mate))

    leaving = []

    def leave(source, target, index):
        copy = pltpu.make_async_copy(source, target, left_sems.at[index])
        copy.start()
        leaving.append(copy)

    def stage6(g):
        b = bufs[g]
        for x in range(nx):
            arrived(b["ag"].at[2 * x + other], b["rh"], x)
        leave(b["ag"], gathered[g], g)

    embed_stage(0, 0, rows_q)
    second_stage(0, 0)
    stage0(0)
    slope_stage(0, 0, rows_q)
    first_stage(0, 1)
    stage0(1)
    stage1(0)
    embed_stage(1, block, block + rows_q)
    slope_stage(1, block, block + rows_q)
    stage1(1)
    n_low = own[me_x, side, 0]
    for k in range(1, nx):
        x = along(k)
        ref = lx.at[x, side]
        link(ref, ref, (s1x, r1x), x * 2 + side, "neg", mate).wait_recv()
        n_low = n_low + lx[x, side].astype(jnp.float32)
    link(ly.at[me_x], ly.at[me_x], (s1y, r1y), me_x, "dp", partner).wait_recv()
    n_high = own[me_x, side, 1] + ly[me_x].astype(jnp.float32)
    link(l2y, l2y, (s2y, r2y), 0, "dp", partner).wait_recv()
    n_low = n_low + l2y[...].astype(jnp.float32)
    for k in range(1, nx):
        x = along(k)
        link(l2x.at[x], l2x.at[x], (s2x, r2x), x, "neg", mate).wait_recv()
        n_high = n_high + l2x[x].astype(jnp.float32)

    grads[1][0:block, 0:half_w] = n_low.T * inv_temp
    grads[1][0:block, half_w:width] = n_high.T * inv_temp
    embed_stage(1, 0, block)
    second_stage(1, 2)
    stage0(2)
    slope_stage(1, 0, block)
    stage2(0)
    stage1(2)
    first_stage(1, 3)
    stage0(3)
    stage2(1)
    stage1(3)
    stage3(0)
    stage2z(0)
    stage2(2)
    stage2z(1)
    stage3(1)
    stage2z(2)
    stage2(3)
    stage3(2)
    stage3z(0)
    stage2z(3)
    stage3z(1)
    stage3(3)
    stage3z(2)
    stage3z(3)
    for g in range(3):
        stage4(g)
        spread(g)
    stage4(3)
    total_squares = squares[0] + squares[1] + squares[2] + squares[3]
    lane = lax.broadcasted_iota(jnp.int32, (1, 128), 1)
    stat[...] = jnp.where(lane == 0, total_squares, loss_part)
    for n in range(1, devices):
        dp, neg = everyone(n)
        copy = pltpu.make_async_remote_copy(
            src_ref=stat, dst_ref=stat_land.at[me], send_sem=ss.at[n], recv_sem=sr2.at[me],
            device_id={"dp": dp, "neg": neg}, device_id_type=pl.DeviceIdType.MESH,
        )
        queue(copy)
    spread(3)
    for g in range(4):
        stage5(g)
    for g in range(4):
        stage6(g)
    stat_land[me] = stat[...]
    for n in range(1, devices):
        source = lax.rem(me + n, devices)
        arrived(stat_land.at[source], sr2, source)
    stat_land[me] = jnp.sum(stat_land[...], axis=0)
    leave(stat_land.at[me], stats_ref, 4)
    for copy in pending:
        copy.wait_send()
    for copy in leaving:
        copy.wait()


    for copy in sends:
        copy.wait_send()
    for distance in range(line):
        for j in range(cuts):
            if distance < line - 1:
                pl.when((place >= distance) & goes_right)(lambda: right(distance, j).wait_send())
                pl.when((place + distance < line) & goes_left)(lambda: left(distance, j).wait_send())
    for k in range(1, line):
        q_send(k, lax.rem(place + k, line)).wait_send()
    for i in range(2 * nx):
        c_send(i).wait_send()
        if i < 2 * (nx - 1):
            send_1x(i).wait_send()
        if i % 2 == 0:
            send_1y(i).wait_send()


def fused_step(ndp, nneg, arguments):
    line, nx = ndp // 2, nneg // 2
    bf16, f32, i32 = jnp.bfloat16, jnp.float32, jnp.int32
    named = dict(zip(step_inputs, arguments))
    fin, h1 = named["item_first"].shape
    h2, width = named["item_third"].shape
    own_rows, block = named["query_features"].shape[0], named["negative_features"].shape[0]
    blocks, cuts, lanes = 2 * nneg, 4, 128
    rows_half = (width // 2, block)
    sources = {"item_features": pltpu.VMEM((block + own_rows, fin), bf16)}
    for name, value in named.items():
        if name not in ("positive_features", "negative_features"):
            sources[name] = pltpu.VMEM(value.shape, value.dtype)
    counts = (own_rows, block + own_rows)
    towers = [
        [
            pltpu.VMEM((count, h1), bf16), pltpu.VMEM((count, h1), f32), pltpu.VMEM((count, h2), bf16),
            pltpu.VMEM((count, h2), f32), pltpu.VMEM((count, width), f32),
        ]
        for count in counts
    ]
    scratch = [
        [pltpu.VMEM((count, width), bf16), pltpu.VMEM((count, h2), bf16), pltpu.VMEM((count, h1), bf16)]
        for count in counts
    ]
    row = pltpu.VMEM((1, own_rows), f32)
    score = [
        pltpu.VMEM((line, cuts, own_rows // cuts, width), bf16),
        pltpu.VMEM((blocks, 2, block // 2, width), bf16),
        pltpu.VMEM((2, block), i32),
        pltpu.VMEM((blocks, 2, block), i32),
        pltpu.VMEM((blocks, 2, block), f32),
        pltpu.VMEM((1, own_rows), i32),
        pltpu.VMEM((line, 1, own_rows), i32),
        pltpu.VMEM((line, own_rows, lanes), f32),
        pltpu.VMEM((blocks, line, own_rows, block), bf16),
        pltpu.VMEM((line, own_rows, lanes), f32),
        pltpu.VMEM((line, 1, own_rows), f32),
        pltpu.VMEM((line, line, 1, own_rows), f32),
        pltpu.VMEM((width, line * own_rows), bf16),
        pltpu.VMEM((line, own_rows, width), bf16),
        pltpu.VMEM((own_rows, width), f32),
        pltpu.VMEM((line, own_rows, width), bf16),
        pltpu.VMEM((nx, 2, 2) + rows_half, bf16),
        pltpu.VMEM((nx, 2, 2) + rows_half, bf16),
        pltpu.VMEM((nx, 2, 2) + rows_half, f32),
        pltpu.VMEM((nx, 2, 2) + rows_half, bf16),
        pltpu.VMEM((nx, 2) + rows_half, bf16),
        pltpu.VMEM((nx,) + rows_half, bf16),
        pltpu.VMEM(rows_half, bf16),
        pltpu.VMEM((nx,) + rows_half, bf16),
    ] + sems(
        3 * nx, 1 + nx, 4 * nx, 4 * nx, 4 * nx, line * cuts, line * cuts, line * cuts,
        blocks, blocks, line, line, line, line, line, line,
        2 * nx, 2 * nx, 2 * nx, 2 * nx, nx, nx, 1, 1, nx, nx, len(step_inputs),
    )
    groups, outs, bufs = [], [], []
    for _ in counts:
        for height, columns in ((fin, h1), (h1, h2), (h2, width)):
            outs.append(jax.ShapeDtypeStruct((height // ndp, columns), f32))
        both = h2 // (ndp * nneg) * (width // pack_columns) + h1 // (ndp * nneg) * (h2 // pack_columns)
        alone = fin // (ndp * nneg) * (h1 // pack_columns)
        for r in (both, alone):
            spare = r // 16 - 1
            low = spare // 2 + (spare % 2 if len(groups) == 3 else 0)
            groups.append((low * 16, spare * 16, r))
    c = pack_columns
    sem_names = ["cs", "cr", "s1x", "r1x", "s1y", "r1y", "s2y", "r2y", "s2x", "r2x", "s3", "r3", "sg", "rg", "sh", "rh"]
    sem_names += ["s1z", "r1z", "s2z", "r2z", "s3z", "r3z"]
    for r1, r, full in groups:
        r2, r4 = r - r1, full - r
        shapes = dict(
            packed=(2, ndp, nx, full, c), c_in=(ndp, nx, full, c), o1x=(nx, ndp, r1, c), l1x=(nx, ndp, r1, c),
            o1y=(line, nx, r2, c), l1y=(line, nx, r2, c), o2y=(line, r1, c), l2y=(line, r1, c),
            o2x=(nx, line, r2, c), l2x=(nx, line, r2, c), zs=(line, r, c), l3=(line, r, c), ag=(nneg, full, c),
            o1z=(line, 2, nx, r4, c), l1z=(line, 2, nx, r4, c), o2z=(nx, 2, r4, c), l2z=(nx, 2, r4, c), o3z=(r4, c), l3z=(r4, c),
        )
        buf = {name: pltpu.VMEM(shape, bf16) for name, shape in shapes.items()}
        buf.update(zip(sem_names, sems(1, 1, nx, nx, 1, 1, 1, 1, nx, nx, line, line, nx, nx, nx, nx, line, line, nx, nx, 1, 1)))
        bufs.append(buf)
    tree = (
        sources, pltpu.VMEM((own_rows, width), bf16), pltpu.VMEM((2, block // 2, width), bf16),
        pltpu.VMEM((own_rows, width), bf16), towers, [pltpu.VMEM((count, width), f32) for count in counts], row, row,
        *score, scratch, bufs,
        pltpu.VMEM((1, 128), f32), pltpu.VMEM((ndp * nneg, 1, 128), f32), *sems(ndp * nneg, ndp * nneg, 5),
    )
    leaves, names = jax.tree.flatten(tree)
    space = sems(1)[0].memory_space
    is_flag = [leaf.memory_space == space for leaf in leaves]
    flags = [leaf for leaf, flag in zip(leaves, is_flag) if flag]
    kept = [leaf for leaf, flag in zip(leaves, is_flag) if not flag]

    def kernel(*refs):
        fixed = refs[: len(refs) - len(kept)]
        held = refs[len(refs) - len(kept) :]

        def scoped(*flag_refs):
            held_refs, flags_left = iter(held), iter(flag_refs)
            merged = [next(flags_left) if flag else next(held_refs) for flag in is_flag]
            step_kernel(ndp, nneg, names, tuple(groups), *fixed, *merged)

        pl.run_scoped(scoped, *flags)

    any_space = pl.BlockSpec(memory_space=pl.ANY)
    stats, *gathered = pl.pallas_call(
        kernel,
        out_shape=(
            jax.ShapeDtypeStruct((1, 128), f32),
            *[jax.ShapeDtypeStruct((nneg, group[-1], pack_columns), bf16) for group in groups],
        ),
        in_specs=[any_space] * len(arguments),
        out_specs=(any_space,) * 5,
        scratch_shapes=kept,
        compiler_params=pltpu.CompilerParams(
            collective_id=1, has_side_effects=True, vmem_limit_bytes=67043328
        ),
    )(*arguments)
    mean_loss, *clipped = pl.pallas_call(
        functools.partial(finish_kernel, nneg, own_rows * ndp * nneg),
        out_shape=(jax.ShapeDtypeStruct((1,), f32), *outs),
        in_specs=[any_space] * 5,
        out_specs=(pl.BlockSpec(memory_space=pltpu.SMEM), *([any_space] * 6)),
        scratch_shapes=[pltpu.VMEM((1, 128), f32)]
        + [pltpu.VMEM((nneg, group[-1], pack_columns), bf16) for group in groups]
        + [pltpu.VMEM(out.shape, f32) for out in outs]
        + sems(5, 6),
    )(stats, *gathered)
    return (mean_loss.reshape(()), *clipped)


def finish_kernel(nneg, count, *refs):
    given, loss_ref, outs, stats_ref, gathered, staged = refs[:5], refs[5], refs[6:12], refs[12], refs[13:17], refs[17:23]
    loaded, done = refs[23:]
    loads = [
        pltpu.make_async_copy(source, target, loaded.at[i])
        for i, (source, target) in enumerate(zip(given, (stats_ref, *gathered)))
    ]
    for copy in loads:
        copy.start()
    loads[0].wait()
    clip = clip_norm / jnp.maximum(jnp.sqrt(stats_ref[0:1, 0:1]), clip_norm)
    copies = []
    for t in range(2):
        third_ref, second_ref, first_ref = staged[3 * t + 2], staged[3 * t + 1], staged[3 * t]
        loads[2 * t + 1].wait()
        loads[2 * t + 2].wait()
        for index, group, ref, offset in (
            (3 * t + 1, 2 * t, second_ref, third_ref.shape[0] // nneg),
            (3 * t, 2 * t + 1, first_ref, 0),
            (3 * t + 2, 2 * t, third_ref, 0),
        ):
            pieces = ref.shape[0] // nneg
            for p in range(ref.shape[1] // pack_columns):
                lo = offset + p * pieces
                for n in range(nneg):
                    value = gathered[group][n, lo : lo + pieces, :].astype(jnp.float32) * clip
                    ref[n * pieces : (n + 1) * pieces, p * pack_columns : (p + 1) * pack_columns] = value
            copy = pltpu.make_async_copy(ref, outs[index], done.at[index])
            copy.start()
            copies.append(copy)
    loss_ref[0] = jnp.sum(stats_ref[0:1, 1:2]) / count
    for copy in copies:
        copy.wait()


def per_device(
    query_features,
    positive_features,
    negative_features,
    positive_ids,
    positive_counts,
    negative_ids,
    negative_counts,
    query_first,
    query_second,
    query_third,
    item_first,
    item_second,
    item_third,
):
    own_rows = query_features.shape[0]
    ndp, nneg = lax.axis_size("dp"), lax.axis_size("neg")
    heights = (query_first.shape[0], query_second.shape[0], query_third.shape[0])
    tiled = all(height % (16 * ndp * nneg) == 0 for height in heights)
    if tiled and own_rows % 256 == 0 and negative_features.shape[0] % 256 == 0:
        return fused_step(
            ndp,
            nneg,
            (
                query_features, positive_features, negative_features, positive_ids.reshape(1, -1),
                positive_counts.reshape(1, -1), negative_ids.reshape(1, -1), negative_counts.reshape(1, -1),
                query_first, query_second, query_third, item_first, item_second, item_third,
            ),
        )
    query_saved, query_unit = tower_forward(query_features, query_first, query_second, query_third)
    item_features = jnp.concatenate([positive_features, negative_features], axis=0)
    item_saved, item_unit = tower_forward(item_features, item_first, item_second, item_third)
    positive_unit = item_unit[:own_rows]
    negative_unit = item_unit[own_rows:]
    ndp, nneg = lax.axis_size("dp"), lax.axis_size("neg")
    width = query_unit.shape[1]
    line, nx = ndp // 2, nneg // 2
    block = negative_unit.shape[0]
    blocks, cuts, lanes = 2 * nneg, 2, min(block, 128)
    bf16, f32, i32 = jnp.bfloat16, jnp.float32, jnp.int32
    positive_logit = jnp.sum(
        query_unit.astype(f32) * positive_unit.astype(f32), axis=1
    ) * inv_temp - jnp.log(positive_counts.astype(f32))
    positive_exp = jnp.exp(positive_logit)
    rows_half = (width // 2, block)
    query_total, denom, negative_sum = call(
        score_kernel,
        0,
        ndp,
        nneg,
        (
            jax.ShapeDtypeStruct((own_rows, width), f32),
            jax.ShapeDtypeStruct((1, own_rows), f32),
            jax.ShapeDtypeStruct((2,) + rows_half, f32),
        ),
        [
            pltpu.VMEM((line, cuts, own_rows // cuts, width), bf16),
            pltpu.VMEM((blocks, 2, block // 2, width), bf16),
            pltpu.VMEM((2, block), i32),
            pltpu.VMEM((blocks, 2, block), i32),
            pltpu.VMEM((blocks, 2, block), f32),
            pltpu.VMEM((1, own_rows), i32),
            pltpu.VMEM((line, 1, own_rows), i32),
            pltpu.VMEM((line, own_rows, lanes), f32),
            pltpu.VMEM((blocks, line, own_rows, block), bf16),
            pltpu.VMEM((line, own_rows, lanes), f32),
            pltpu.VMEM((line, 1, own_rows), f32),
            pltpu.VMEM((line, line, 1, own_rows), f32),
            pltpu.VMEM((width, line * own_rows), bf16),
            pltpu.VMEM((line, own_rows, width), bf16),
            pltpu.VMEM((own_rows, width), f32),
            pltpu.VMEM((line, own_rows, width), bf16),
            pltpu.VMEM((nx, 2, 2) + rows_half, bf16),
            pltpu.VMEM((nx, 2, 2) + rows_half, bf16),
            pltpu.VMEM((nx, 2, 2) + rows_half, f32),
            pltpu.VMEM((nx, 2, 2) + rows_half, bf16),
            pltpu.VMEM((nx, 2) + rows_half, bf16),
            pltpu.VMEM((nx,) + rows_half, bf16),
            pltpu.VMEM(rows_half, bf16),
            pltpu.VMEM((nx,) + rows_half, bf16),
        ]
        + sems(
            3 * nx, 1 + nx, 4 * nx, 4 * nx, 4 * nx, line * cuts, line * cuts, line * cuts,
            blocks, blocks, line, line, line, line, line, line,
            2 * nx, 2 * nx, 2 * nx, 2 * nx, nx, nx, 1, 1, nx, nx,
        ),
        [vmem] * 6,
        40,
    )(
        query_unit,
        negative_unit.reshape(2, block // 2, width),
        positive_ids.reshape((1, -1) if own_rows % 128 == 0 else (nneg, own_rows)),
        negative_ids.reshape((1, -1) if block % 128 == 0 else (ndp, block)),
        negative_counts.reshape((1, -1) if block % 128 == 0 else (ndp, block)),
        positive_exp.reshape(1, own_rows),
    )
    own_denom = denom.reshape(-1)
    loss_part = jnp.sum(jnp.log(own_denom) - positive_logit)
    positive_slope = positive_exp / own_denom - 1.0
    query_sum = query_total / own_denom[:, None]
    negative_sum = negative_sum.reshape(width, block).T
    query_grad = (
        query_sum + positive_slope[:, None] * positive_unit.astype(jnp.float32)
    ) * inv_temp
    positive_grad = positive_slope[:, None] * query_unit.astype(jnp.float32) * inv_temp
    item_grad = jnp.concatenate([positive_grad, negative_sum * inv_temp], axis=0)
    query_grads = tower_backward(query_features, query_second, query_third, query_saved, query_grad)
    item_grads = tower_backward(item_features, item_second, item_third, item_saved, item_grad)
    gradients = query_grads + item_grads
    parts = [part for gradient in gradients for part in to_packed(gradient, ndp)]
    packed = jnp.concatenate(parts, axis=1)
    rows = packed.shape[1] // nneg
    packed = packed.reshape(ndp, nneg, 2, rows // 2, pack_columns).transpose(1, 0, 2, 3, 4)
    piece = (rows // 2, pack_columns)
    gathered, stats = call(
        weight_kernel,
        3,
        ndp,
        nneg,
        (jax.ShapeDtypeStruct((nneg, 2) + piece, bf16), jax.ShapeDtypeStruct((8, 128), f32)),
        [
            pltpu.VMEM((nx, ndp, 2) + piece, bf16),
            pltpu.VMEM((nx, 2, line) + piece, bf16),
            pltpu.VMEM((2, nx, line) + piece, bf16),
            pltpu.VMEM((nx, 2, line) + piece, bf16),
            pltpu.VMEM((nx, line) + piece, bf16),
            pltpu.VMEM((2, line) + piece, bf16),
            pltpu.VMEM((nx, line) + piece, bf16),
            pltpu.VMEM((line,) + piece, bf16),
            pltpu.VMEM((nx, line) + piece, bf16),
            pltpu.VMEM((2, line) + piece, bf16),
            pltpu.VMEM((2, line) + piece, bf16),
            pltpu.VMEM((8, 128), f32),
            pltpu.VMEM((ndp, 8, 128), f32),
            pltpu.VMEM((8, 128), f32),
            pltpu.VMEM((nneg, 8, 128), f32),
        ]
        + sems(nx, nx, 2 * nx, 2 * nx, 2, 2, ndp, ndp, ndp, ndp, nneg, nneg, nx, nx, nx, nx),
        [vmem, pl.BlockSpec(memory_space=pltpu.SMEM)],
    )(packed, loss_part.reshape(1))
    grad_norm = jnp.sqrt(stats[0, 0])
    mean_loss = stats[0, 1] / (own_rows * ndp * nneg)
    clip_factor = clip_norm / jnp.maximum(grad_norm, clip_norm)
    flat = gathered.reshape(nneg * rows, pack_columns)
    clipped = []
    start = 0
    for gradient in gradients:
        height, columns = gradient.shape[0] // ndp, gradient.shape[1]
        groups = columns // pack_columns
        blocks = [flat[start + g * height : start + (g + 1) * height] for g in range(groups)]
        start += groups * height
        clipped.append(jnp.concatenate(blocks, axis=1).astype(jnp.float32) * clip_factor)
    return (mean_loss, *clipped)


def solution(mesh):
    placed = (
        P(("dp", "neg"), None),
        P(("dp", "neg"), None),
        P(("neg", "dp"), None),
        P("dp"),
        P(("dp", "neg")),
        P("neg"),
        P("neg"),
        P(),
        P(),
        P(),
        P(),
        P(),
        P(),
    )
    return jax.shard_map(
        per_device,
        mesh=mesh,
        in_specs=placed,
        out_specs=(
            P(),
            P("dp", None),
            P("dp", None),
            P("dp", None),
            P("dp", None),
            P("dp", None),
            P("dp", None),
        ),
        check_vma=False,
    )
```
